32 devices in a mesh: section: 2 (over x), dp: 8 (over z, y), tensor: 2 (over core).
Axes of the slice: x: 2, y: 2, z: 4, core: 2. Of those that a mesh axis runs over, the one named last changes fastest.
Arguments:
- inputs: float32 [2, 1024, 2048], P(None, ('dp', 'tensor')), may hold values from -6 to 6
- table: int32 [2, 8], replicated, may hold values from 0 to 7, each once within a row
- cotangent: float32 [2, 1024, 2048], P(None, ('dp', 'tensor')), may hold values from -6 to 6
- wq: bfloat16 [2, 2048, 2048], P('section', 'dp', 'tensor'), may hold values from -0.125 to 0.125
- wk: bfloat16 [2, 2048, 512], P('section', 'dp', 'tensor'), may hold values from -0.125 to 0.125
- wv: bfloat16 [2, 2048, 512], P('section', 'dp', 'tensor'), may hold values from -0.125 to 0.125
- wo: bfloat16 [2, 2048, 2048], P('section', 'tensor', 'dp'), may hold values from -1 to 1
- w_gate: bfloat16 [2, 2048, 8192], P('section', 'dp', 'tensor'), may hold values from -0.125 to 0.125
- w_up: bfloat16 [2, 2048, 8192], P('section', 'dp', 'tensor'), may hold values from -0.125 to 0.125
- w_down: bfloat16 [2, 8192, 2048], P('section', 'tensor', 'dp'), may hold values from -0.0625 to 0.0625
- gain_attn: bfloat16 [2, 2048], P('section', 'dp'), may hold values from 0.5 to 1.5
- gain_mlp: bfloat16 [2, 2048], P('section', 'dp'), may hold values from 0.5 to 1.5
Outputs:
- outputs: float32 [2, 2, 1024, 2048], P('section', None, ('dp', 'tensor'))
- input_grad: float32 [2, 2, 1024, 2048], P('section', None, ('dp', 'tensor'))
- grad_wq: float32 [2, 2048, 2048], P('section', 'dp', 'tensor')
- grad_wk: float32 [2, 2048, 512], P('section', 'dp', 'tensor')
- grad_wv: float32 [2, 2048, 512], P('section', 'dp', 'tensor')
- grad_wo: float32 [2, 2048, 2048], P('section', 'tensor', 'dp')
- grad_gate: float32 [2, 2048, 8192], P('section', 'dp', 'tensor')
- grad_up: float32 [2, 2048, 8192], P('section', 'dp', 'tensor')
- grad_down: float32 [2, 8192, 2048], P('section', 'tensor', 'dp')
- grad_gain_attn: float32 [2, 2048], P('section', ('dp', 'tensor'))
- grad_gain_mlp: float32 [2, 2048], P('section', ('dp', 'tensor'))
The draws below stay inside these ranges and needn't reach their ends.
Inputs may be any that keep to these rules, and one draw needn't show every extreme that they name: `table`: each row holds every number from 0 to 7 once.
All inputs are finite; a program needn't handle non-finite values.
Results may differ from the reference program's by a relative error of at most 0.025.
Values may be sent and summed in bfloat16 or wider, within the bound.
A program may use at most 384 MiB of HBM per device.

```python
import math
import jax
import jax.numpy as jnp
from jax import lax

MODEL_WIDTH = 2048
QUERY_HEADS = 32
KEY_VALUE_HEADS = 8
HEAD_SIZE = 64
FF = 8192
BLOCK = 128
M = 2
LAYER_SECTIONS = 2
TOK_MB = 1024
N_SECTION = 2
N_DP = 8


def shard_levels(rng, extent, split, smallest, high):
    def one(axis_at, blocks):
        steps = jax.random.uniform(jax.random.fold_in(jax.random.fold_in(rng, 6), axis_at), (blocks,), jnp.float32, smallest / len(split), high / len(split))
        return jnp.repeat(jnp.exp(steps), extent[axis_at] // blocks).reshape((-1,) + (1,) * (len(extent) - axis_at - 1))

    level = one(*split[0])
    for cut in split[1:]:
        level = level * one(*cut)
    return level


def scatter_about(rng, dims, width, bound, shards=(), kind=jnp.bfloat16):
    values = jax.random.normal(rng, dims, jnp.float32) * width
    if len(shards) > 0:
        values = shard_levels(rng, dims, shards, -0.22, 0.18) * values
    return jnp.clip(values, min=-bound, max=bound).astype(kind)


def setup_inputs(seed: int = 0) -> dict:
    splits = jax.random.split(jax.random.key(seed), 13)
    inputs = scatter_about(splits[0], (M, TOK_MB, MODEL_WIDTH), 1.0, 6.0, ((1, 16),), jnp.float32)
    table = jax.vmap(lambda own: jax.random.permutation(own, N_DP))(jax.random.split(splits[1], M)).reshape((M, N_DP)).astype(jnp.int32)
    cotangent = scatter_about(splits[2], (M, TOK_MB, MODEL_WIDTH), 1.0, 6.0, ((1, 16),), jnp.float32)
    wq = scatter_about(splits[3], (LAYER_SECTIONS, MODEL_WIDTH, QUERY_HEADS * HEAD_SIZE), MODEL_WIDTH ** -0.5, 0.125, ((0, 2), (1, 8), (2, 2)))
    wk = scatter_about(splits[4], (LAYER_SECTIONS, MODEL_WIDTH, KEY_VALUE_HEADS * HEAD_SIZE), MODEL_WIDTH ** -0.5, 0.125, ((0, 2), (1, 8), (2, 2)))
    wv = scatter_about(splits[5], (LAYER_SECTIONS, MODEL_WIDTH, KEY_VALUE_HEADS * HEAD_SIZE), MODEL_WIDTH ** -0.5, 0.125, ((0, 2), (1, 8), (2, 2)))
    wo = scatter_about(splits[6], (LAYER_SECTIONS, QUERY_HEADS * HEAD_SIZE, MODEL_WIDTH), (max(1, QUERY_HEADS * HEAD_SIZE // 64)) ** -0.5, 1.0, ((0, 2), (1, 2), (2, 8)))
    w_gate = scatter_about(splits[7], (LAYER_SECTIONS, MODEL_WIDTH, FF), MODEL_WIDTH ** -0.5, 0.125, ((0, 2), (1, 8), (2, 2)))
    w_up = scatter_about(splits[8], (LAYER_SECTIONS, MODEL_WIDTH, FF), MODEL_WIDTH ** -0.5, 0.125, ((0, 2), (1, 8), (2, 2)))
    w_down = scatter_about(splits[9], (LAYER_SECTIONS, FF, MODEL_WIDTH), FF ** -0.5, 0.0625, ((0, 2), (1, 2), (2, 8)))
    gain_attn = jnp.clip(1.0 + 0.1 * jax.random.normal(splits[10], (LAYER_SECTIONS, MODEL_WIDTH), jnp.float32), 0.5, 1.5).astype(jnp.bfloat16)
    gain_mlp = jnp.clip(1.0 + 0.1 * jax.random.normal(splits[11], (LAYER_SECTIONS, MODEL_WIDTH), jnp.float32), 0.5, 1.5).astype(jnp.bfloat16)
    return dict(inputs=inputs, table=table, cotangent=cotangent, wq=wq, wk=wk, wv=wv, wo=wo, w_gate=w_gate, w_up=w_up, w_down=w_down, gain_attn=gain_attn, gain_mlp=gain_mlp)


epsilon = 1e-05

def rope_frequencies(head):
    index = jnp.arange(head // 2, dtype=jnp.float32)
    base = 1.0 / 500000.0 ** (index * 2.0 / head)
    wavelength = 2.0 * math.pi / base
    blend = (8192.0 / wavelength - 1.0) / 3.0
    middle = (1.0 - blend) * base / 32.0 + blend * base
    return jnp.where(wavelength < 2048.0, base, jnp.where(wavelength > 8192.0, base / 32.0, middle))

def rotate(values, positions, head):
    step_count = values.shape[0]
    shaped = values.reshape(step_count, -1, head)
    angle = positions.astype(jnp.float32)[:, None] * rope_frequencies(head)[None, :]
    cosine = jnp.cos(angle)[:, None, :]
    sine = jnp.sin(angle)[:, None, :]
    first = shaped[:, :, :head // 2]
    second = shaped[:, :, head // 2:]
    return jnp.concatenate([first * cosine - second * sine, second * cosine + first * sine], axis=-1).reshape(step_count, -1)

def unrotate(values, positions, head):
    step_count = values.shape[0]
    shaped = values.reshape(step_count, -1, head)
    angle = positions.astype(jnp.float32)[:, None] * rope_frequencies(head)[None, :]
    cosine = jnp.cos(angle)[:, None, :]
    sine = jnp.sin(angle)[:, None, :]
    first = shaped[:, :, :head // 2]
    second = shaped[:, :, head // 2:]
    return jnp.concatenate([first * cosine + second * sine, second * cosine - first * sine], axis=-1).reshape(step_count, -1)

def norm_stats(rows):
    inverse = lax.rsqrt(lax.optimization_barrier(jnp.mean(rows * rows, axis=-1, keepdims=True)) + epsilon)
    return (rows * inverse, inverse)

def norm_back(grad, unit, inverse, gain):
    scaled = grad * gain
    inner = lax.optimization_barrier(jnp.mean(scaled * unit, axis=-1, keepdims=True))
    return (inverse * (scaled - unit * inner), lax.optimization_barrier(jnp.sum(grad * unit, axis=0)))

def matmul(left, right):
    return jnp.dot(left, right, preferred_element_type=jnp.float32)

def attend_forward(query_rows, key, value_rows, allowed):
    step_count = query_rows.shape[0]
    head_group = QUERY_HEADS // KEY_VALUE_HEADS
    scale = 1.0 / math.sqrt(HEAD_SIZE)
    query_rows, key, value_rows = lax.optimization_barrier((query_rows, key, value_rows))
    query_layers = query_rows.reshape(step_count, KEY_VALUE_HEADS, head_group * HEAD_SIZE).transpose(1, 0, 2)
    key_layers = key.reshape(step_count, KEY_VALUE_HEADS, HEAD_SIZE).transpose(1, 0, 2)
    value_layers = value_rows.reshape(step_count, KEY_VALUE_HEADS, HEAD_SIZE).transpose(1, 0, 2)

    def one_head(parts):
        q_head, k_head, v_head = parts
        q_three = q_head.reshape(step_count, head_group, HEAD_SIZE).astype(jnp.float32)
        scores = jnp.einsum('qgd,kd->gqk', q_three, k_head.astype(jnp.float32)) * scale
        total = lax.optimization_barrier(jnp.sum(jnp.where(allowed, jnp.exp(scores), 0.0), axis=-1))
        log_total = jnp.log(total)
        probs = jnp.where(allowed, jnp.exp(scores - log_total[..., None]), 0.0)
        rounded = lax.optimization_barrier(probs.astype(jnp.bfloat16)).astype(jnp.float32)
        mixed = jnp.einsum('gqk,kd->qgd', rounded, v_head.astype(jnp.float32)).astype(jnp.bfloat16)
        return (mixed.reshape(step_count, head_group * HEAD_SIZE), log_total)
    mixed, log_total = lax.map(one_head, (query_layers, key_layers, value_layers))
    return (mixed.transpose(1, 0, 2).reshape(step_count, QUERY_HEADS * HEAD_SIZE), log_total)

def attend_backward(blended_gradient, query_rows, key, value_rows, log_total, allowed):
    step_count = query_rows.shape[0]
    head_group = QUERY_HEADS // KEY_VALUE_HEADS
    scale = 1.0 / math.sqrt(HEAD_SIZE)
    blended_gradient, query_rows, key, value_rows = lax.optimization_barrier((blended_gradient, query_rows, key, value_rows))
    query_layers = query_rows.reshape(step_count, KEY_VALUE_HEADS, head_group * HEAD_SIZE).transpose(1, 0, 2)
    key_layers = key.reshape(step_count, KEY_VALUE_HEADS, HEAD_SIZE).transpose(1, 0, 2)
    value_layers = value_rows.reshape(step_count, KEY_VALUE_HEADS, HEAD_SIZE).transpose(1, 0, 2)
    gain_layers = blended_gradient.reshape(step_count, KEY_VALUE_HEADS, head_group * HEAD_SIZE).transpose(1, 0, 2)

    def one_head(parts):
        q_head, k_head, v_head, g_head, l_head = parts
        q_three = q_head.reshape(step_count, head_group, HEAD_SIZE).astype(jnp.float32)
        g_three = g_head.reshape(step_count, head_group, HEAD_SIZE).astype(jnp.float32)
        k_wide = k_head.astype(jnp.float32)
        v_wide = v_head.astype(jnp.float32)
        scores = jnp.einsum('qgd,kd->gqk', q_three, k_wide) * scale
        probs = jnp.where(allowed, jnp.exp(scores - l_head[..., None]), 0.0)
        rounded = lax.optimization_barrier(probs.astype(jnp.bfloat16)).astype(jnp.float32)
        prob_grad = jnp.einsum('qgd,kd->gqk', g_three, v_wide)
        value_total_sum = jnp.einsum('gqk,qgd->kd', rounded, g_three)
        rowdot = lax.optimization_barrier(jnp.sum(probs * prob_grad, axis=-1, keepdims=True))
        score_grad = probs * (prob_grad - rowdot) * scale
        score_round = lax.optimization_barrier(score_grad.astype(jnp.bfloat16)).astype(jnp.float32)
        query_grad = jnp.einsum('gqk,kd->qgd', score_round, k_wide).reshape(step_count, head_group * HEAD_SIZE)
        key_gradient = jnp.einsum('gqk,qgd->kd', score_round, q_three)
        return (query_grad, key_gradient, value_total_sum)
    query_grad, key_gradient, value_total_sum = lax.map(one_head, (query_layers, key_layers, value_layers, gain_layers, log_total))
    query_grad = query_grad.transpose(1, 0, 2).reshape(step_count, QUERY_HEADS * HEAD_SIZE)
    key_gradient = key_gradient.transpose(1, 0, 2).reshape(step_count, KEY_VALUE_HEADS * HEAD_SIZE)
    value_total_sum = value_total_sum.transpose(1, 0, 2).reshape(step_count, KEY_VALUE_HEADS * HEAD_SIZE)
    return (query_grad, key_gradient, value_total_sum)

def layer_forward(source, weights, positions, allowed):
    wq, wk, wv, wo, w_gate, w_up, w_down, gain_attn, gain_mlp = weights
    unit1, inverse1 = norm_stats(source)
    normed1 = (unit1 * gain_attn.astype(jnp.float32)).astype(jnp.bfloat16)
    query_rows = rotate(matmul(normed1, wq), positions, HEAD_SIZE).astype(jnp.bfloat16)
    key = rotate(matmul(normed1, wk), positions, HEAD_SIZE).astype(jnp.bfloat16)
    value_rows = matmul(normed1, wv).astype(jnp.bfloat16)
    mixed, log_total = attend_forward(query_rows, key, value_rows, allowed)
    second = source + matmul(mixed, wo)
    unit2, inverse2 = norm_stats(second)
    normed2 = (unit2 * gain_mlp.astype(jnp.float32)).astype(jnp.bfloat16)
    gate = matmul(normed2, w_gate)
    upper = matmul(normed2, w_up)
    hidden = (jax.nn.silu(gate) * upper).astype(jnp.bfloat16)
    result = second + matmul(hidden, w_down)
    return (result, (source, query_rows, key, value_rows, mixed, log_total, second, gate, upper, hidden))

def layer_backward(incoming, context, weights, positions, allowed):
    wq, wk, wv, wo, w_gate, w_up, w_down, gain_attn, gain_mlp = weights
    source, query_rows, key, value_rows, mixed, log_total, second, gate, upper, hidden = context
    out_grad = incoming.astype(jnp.bfloat16)
    grad_down = matmul(hidden.T, out_grad)
    hidden_grad = matmul(out_grad, w_down.T)
    sigma = jax.nn.sigmoid(gate)
    gate_grad = (hidden_grad * upper * sigma * (1.0 + gate * (1.0 - sigma))).astype(jnp.bfloat16)
    up_grad = (hidden_grad * gate * sigma).astype(jnp.bfloat16)
    unit2, inverse2 = norm_stats(second)
    normed2 = (unit2 * gain_mlp.astype(jnp.float32)).astype(jnp.bfloat16)
    grad_gate = matmul(normed2.T, gate_grad)
    grad_up = matmul(normed2.T, up_grad)
    normed2_grad = matmul(gate_grad, w_gate.T) + matmul(up_grad, w_up.T)
    second_part, grad_gain_mlp = norm_back(normed2_grad, unit2, inverse2, gain_mlp.astype(jnp.float32))
    second_grad = incoming + second_part
    attn_grad = second_grad.astype(jnp.bfloat16)
    grad_wo = matmul(mixed.T, attn_grad)
    blended_gradient = matmul(attn_grad, wo.T).astype(jnp.bfloat16)
    query_grad, key_gradient, value_total_sum = attend_backward(blended_gradient, query_rows, key, value_rows, log_total, allowed)
    query_round = unrotate(query_grad, positions, HEAD_SIZE).astype(jnp.bfloat16)
    key_round = unrotate(key_gradient, positions, HEAD_SIZE).astype(jnp.bfloat16)
    value_round = value_total_sum.astype(jnp.bfloat16)
    unit1, inverse1 = norm_stats(source)
    normed1 = (unit1 * gain_attn.astype(jnp.float32)).astype(jnp.bfloat16)
    grad_wq = matmul(normed1.T, query_round)
    grad_wk = matmul(normed1.T, key_round)
    grad_wv = matmul(normed1.T, value_round)
    normed1_grad = matmul(query_round, wq.T) + matmul(key_round, wk.T) + matmul(value_round, wv.T)
    first_part, grad_gain_attn = norm_back(normed1_grad, unit1, inverse1, gain_attn.astype(jnp.float32))
    input_grad = second_grad + first_part
    return (input_grad, (grad_wq, grad_wk, grad_wv, grad_wo, grad_gate, grad_up, grad_down, grad_gain_attn, grad_gain_mlp))

def reference(inputs, table, cotangent, wq, wk, wv, wo, w_gate, w_up, w_down, gain_attn, gain_mlp):
    span = N_DP // 2
    tokens = inputs.shape[1]
    rows = jnp.arange(tokens, dtype=jnp.int32)
    layouts = []
    for micro in range(M):
        block_ids = table[micro][rows // BLOCK].astype(jnp.int32)
        sequence = block_ids // span
        position = (block_ids % span * BLOCK + rows % BLOCK).astype(jnp.int32)
        allowed = (sequence[:, None] == sequence[None, :]) & (position[None, :] <= position[:, None])
        layouts.append((position, allowed))

    def section_weights(section):
        return (wq[section], wk[section], wv[section], wo[section], w_gate[section], w_up[section], w_down[section], gain_attn[section], gain_mlp[section])
    section_outputs = []
    contexts = []
    for section in range(N_SECTION):
        results = []
        saved = []
        for micro in range(M):
            source = inputs[micro] if section == 0 else section_outputs[section - 1][micro]
            result, context = layer_forward(source, section_weights(section), layouts[micro][0], layouts[micro][1])
            results.append(result)
            saved.append(context)
        section_outputs.append(results)
        contexts.append(saved)
    input_grads = [None] * N_SECTION
    grad_totals = [None] * N_SECTION
    for section in reversed(range(N_SECTION)):
        grads_in = []
        totals = None
        for micro in range(M):
            incoming = cotangent[micro] if section == N_SECTION - 1 else input_grads[section + 1][micro]
            din, pieces = layer_backward(incoming, contexts[section][micro], section_weights(section), layouts[micro][0], layouts[micro][1])
            grads_in.append(din)
            totals = pieces if totals is None else tuple((left + right for left, right in zip(totals, pieces)))
        input_grads[section] = grads_in
        grad_totals[section] = totals
    outputs = jnp.stack([jnp.stack(section_outputs[section]) for section in range(N_SECTION)])
    input_grad = jnp.stack([jnp.stack(input_grads[section]) for section in range(N_SECTION)])
    stacked = [jnp.stack([grad_totals[section][index] for section in range(N_SECTION)]) for index in range(9)]
    return (outputs, input_grad, stacked[0], stacked[1], stacked[2], stacked[3], stacked[4], stacked[5], stacked[6], stacked[7], stacked[8])
```

```python
import functools
import math

import jax
import jax.numpy as jnp
from jax import lax
from jax.experimental import pallas as pl
from jax.experimental.pallas import tpu as pltpu
from jax.sharding import PartitionSpec as P

HEAD_SIZE = 64


epsilon = 1e-05


def passed_along(value, axis, steps):
    count = lax.axis_size(axis)
    initial, last = (max(0, -steps), min(count, count - steps))
    return lax.ppermute(value, axis, [(source, source + steps) for source in range(initial, last)])


def rope_frequencies(head):
    index = jnp.arange(head // 2, dtype=jnp.float32)
    base = 1.0 / 500000.0 ** (index * 2.0 / head)
    wavelength = 2.0 * math.pi / base
    blend = (8192.0 / wavelength - 1.0) / 3.0
    middle = (1.0 - blend) * base / 32.0 + blend * base
    return jnp.where(wavelength < 2048.0, base, jnp.where(wavelength > 8192.0, base / 32.0, middle))


def rotate(values, positions, head):
    step_count = values.shape[0]
    shaped = values.reshape(step_count, -1, head)
    angle = positions.astype(jnp.float32)[:, None] * rope_frequencies(head)[None, :]
    cosine = jnp.cos(angle)[:, None, :]
    sine = jnp.sin(angle)[:, None, :]
    first = shaped[:, :, : head // 2]
    second = shaped[:, :, head // 2 :]
    return jnp.concatenate(
        [first * cosine - second * sine, second * cosine + first * sine], axis=-1
    ).reshape(step_count, -1)


def unrotate(values, positions, head):
    step_count = values.shape[0]
    shaped = values.reshape(step_count, -1, head)
    angle = positions.astype(jnp.float32)[:, None] * rope_frequencies(head)[None, :]
    cosine = jnp.cos(angle)[:, None, :]
    sine = jnp.sin(angle)[:, None, :]
    first = shaped[:, :, : head // 2]
    second = shaped[:, :, head // 2 :]
    return jnp.concatenate(
        [first * cosine + second * sine, second * cosine - first * sine], axis=-1
    ).reshape(step_count, -1)


def norm_stats(rows):
    inverse = lax.rsqrt(jnp.mean(rows * rows, axis=-1, keepdims=True) + epsilon)
    return (rows * inverse, inverse)


def norm_back(grad, unit, inverse, gain):
    scaled = grad * gain
    inner = jnp.mean(scaled * unit, axis=-1, keepdims=True)
    return (inverse * (scaled - unit * inner), jnp.sum(grad * unit, axis=0))


def matmul(left, right):
    return jnp.dot(left, right, preferred_element_type=jnp.float32)


def block_layout(table, micro, groups, block):
    layout_row = lax.dynamic_index_in_dim(table, micro, 0, keepdims=False)
    span = groups // 2
    mine = lax.dynamic_index_in_dim(layout_row, lax.axis_index("dp"), 0, keepdims=False)
    sequence = mine // span
    place = mine % span
    slot_ids = jnp.arange(groups, dtype=jnp.int32)
    holder = jnp.sum(
        jnp.where(layout_row[None, :] == slot_ids[:, None], slot_ids[None, :], 0), axis=1
    )
    slots = lax.dynamic_slice_in_dim(holder, sequence * span, span)
    positions = place * block + jnp.arange(block, dtype=jnp.int32)
    return (slots, positions)


def attend(query_rows, key_seq, value_seq, positions, heads_kv, head):
    step_count = query_rows.shape[0]
    keys_total = key_seq.shape[0]
    head_group = query_rows.shape[1] // (heads_kv * head)
    scale = 1.0 / math.sqrt(head)
    allowed = jnp.arange(keys_total, dtype=jnp.int32)[None, :] <= positions[:, None]
    query_layers = query_rows.reshape(step_count, heads_kv, head_group * head).transpose(1, 0, 2)
    key_layers = key_seq.reshape(keys_total, heads_kv, head).transpose(1, 0, 2)
    value_layers = value_seq.reshape(keys_total, heads_kv, head).transpose(1, 0, 2)

    def one_head(parts):
        q_head, k_head, v_head = parts
        q_three = q_head.reshape(step_count, head_group, head)
        scores = (
            jnp.einsum("qgd,kd->gqk", q_three, k_head, preferred_element_type=jnp.float32) * scale
        )
        total = jnp.sum(jnp.where(allowed, jnp.exp(scores), 0.0), axis=-1)
        log_total = jnp.log(total)
        probs = jnp.where(allowed, jnp.exp(scores - log_total[..., None]), 0.0).astype(jnp.bfloat16)
        mixed = jnp.einsum("gqk,kd->qgd", probs, v_head, preferred_element_type=jnp.float32).astype(
            jnp.bfloat16
        )
        return (mixed.reshape(step_count, head_group * head), log_total)

    mixed, log_total = lax.map(one_head, (query_layers, key_layers, value_layers))
    return (mixed.transpose(1, 0, 2).reshape(step_count, -1), log_total)


def attend_back(
    blended_gradient, query_rows, key_seq, value_seq, log_total, positions, heads_kv, head
):
    step_count = query_rows.shape[0]
    keys_total = key_seq.shape[0]
    head_group = query_rows.shape[1] // (heads_kv * head)
    scale = 1.0 / math.sqrt(head)
    allowed = jnp.arange(keys_total, dtype=jnp.int32)[None, :] <= positions[:, None]
    query_layers = query_rows.reshape(step_count, heads_kv, head_group * head).transpose(1, 0, 2)
    key_layers = key_seq.reshape(keys_total, heads_kv, head).transpose(1, 0, 2)
    value_layers = value_seq.reshape(keys_total, heads_kv, head).transpose(1, 0, 2)
    gain_layers = blended_gradient.reshape(step_count, heads_kv, head_group * head).transpose(
        1, 0, 2
    )

    def one_head(parts):
        q_head, k_head, v_head, g_head, l_head = parts
        q_three = q_head.reshape(step_count, head_group, head)
        g_three = g_head.reshape(step_count, head_group, head)
        scores = (
            jnp.einsum("qgd,kd->gqk", q_three, k_head, preferred_element_type=jnp.float32) * scale
        )
        probs = jnp.where(allowed, jnp.exp(scores - l_head[..., None]), 0.0)
        rounded = probs.astype(jnp.bfloat16)
        prob_grad = jnp.einsum("qgd,kd->gqk", g_three, v_head, preferred_element_type=jnp.float32)
        value_total_sum = jnp.einsum(
            "gqk,qgd->kd", rounded, g_three, preferred_element_type=jnp.float32
        )
        rowdot = jnp.sum(probs * prob_grad, axis=-1, keepdims=True)
        score_grad = (probs * (prob_grad - rowdot) * scale).astype(jnp.bfloat16)
        query_grad = jnp.einsum(
            "gqk,kd->qgd", score_grad, k_head, preferred_element_type=jnp.float32
        )
        key_gradient = jnp.einsum(
            "gqk,qgd->kd", score_grad, q_three, preferred_element_type=jnp.float32
        )
        return (query_grad.reshape(step_count, head_group * head), key_gradient, value_total_sum)

    query_grad, key_gradient, value_total_sum = lax.map(
        one_head, (query_layers, key_layers, value_layers, gain_layers, log_total)
    )
    query_grad = query_grad.transpose(1, 0, 2).reshape(step_count, -1)
    key_gradient = key_gradient.transpose(1, 0, 2).reshape(keys_total, -1)
    value_total_sum = value_total_sum.transpose(1, 0, 2).reshape(keys_total, -1)
    return (query_grad, key_gradient, value_total_sum)


def layer_forward(rows, table, micro, weights, groups, heads_kv, head):
    wq, wk, wv, wo, w_gate, w_up, w_down, gain_attn, gain_mlp = weights
    full = lax.all_gather(rows, "tensor", axis=0, tiled=True)
    block = full.shape[0]
    slots, positions = block_layout(table, micro, groups, block)
    unit1, inverse1 = norm_stats(full)
    normed1 = (unit1 * gain_attn.astype(jnp.float32)).astype(jnp.bfloat16)
    query_rows = rotate(matmul(normed1, wq), positions, head).astype(jnp.bfloat16)
    key = rotate(matmul(normed1, wk), positions, head).astype(jnp.bfloat16)
    value_rows = matmul(normed1, wv).astype(jnp.bfloat16)
    key_all, value_all = (
        lax.all_gather(key, "dp", axis=0, tiled=True),
        lax.all_gather(value_rows, "dp", axis=0, tiled=True),
    )
    kv_width = key.shape[1]
    key_seq = key_all.reshape(groups, block, kv_width)[slots].reshape(-1, kv_width)
    value_seq = value_all.reshape(groups, block, kv_width)[slots].reshape(-1, kv_width)
    mixed, log_total = attend(query_rows, key_seq, value_seq, positions, heads_kv, head)
    second = rows + lax.psum_scatter(matmul(mixed, wo), "tensor", scatter_dimension=0, tiled=True)
    full_second = lax.all_gather(second, "tensor", axis=0, tiled=True)
    unit2, inverse2 = norm_stats(full_second)
    normed2 = (unit2 * gain_mlp.astype(jnp.float32)).astype(jnp.bfloat16)
    gate = matmul(normed2, w_gate)
    upper = matmul(normed2, w_up)
    hidden = (jax.nn.silu(gate) * upper).astype(jnp.bfloat16)
    result = second + lax.psum_scatter(
        matmul(hidden, w_down), "tensor", scatter_dimension=0, tiled=True
    )
    return (
        result,
        (
            full,
            query_rows,
            key_seq,
            value_seq,
            mixed,
            log_total,
            full_second,
            gate,
            upper,
            hidden,
            slots,
            positions,
        ),
    )


def layer_backward(grad_rows, context, weights, groups, parts, heads_kv, head):
    wq, wk, wv, wo, w_gate, w_up, w_down, gain_attn, gain_mlp = weights
    (
        full,
        query_rows,
        key_seq,
        value_seq,
        mixed,
        log_total,
        full_second,
        gate,
        upper,
        hidden,
        slots,
        positions,
    ) = context
    block = full.shape[0]
    out_grad = lax.all_gather(grad_rows.astype(jnp.bfloat16), "tensor", axis=0, tiled=True)
    grad_down = matmul(hidden.T, out_grad)
    hidden_grad = matmul(out_grad, w_down.T)
    sigma = jax.nn.sigmoid(gate)
    gate_grad = (hidden_grad * upper * sigma * (1.0 + gate * (1.0 - sigma))).astype(jnp.bfloat16)
    up_grad = (hidden_grad * gate * sigma).astype(jnp.bfloat16)
    unit2, inverse2 = norm_stats(full_second)
    normed2 = (unit2 * gain_mlp.astype(jnp.float32)).astype(jnp.bfloat16)
    grad_gate = matmul(normed2.T, gate_grad)
    grad_up = matmul(normed2.T, up_grad)
    normed2_grad = matmul(gate_grad, w_gate.T) + matmul(up_grad, w_up.T)
    second_terms, gain_mlp_terms = norm_back(
        normed2_grad, unit2, inverse2, gain_mlp.astype(jnp.float32)
    )
    piece_width = gain_mlp_terms.shape[0] // (groups * parts)
    second_part, gain_mlp_part = (
        lax.psum_scatter(
            second_terms.astype(jnp.bfloat16), "tensor", scatter_dimension=0, tiled=True
        ).astype(jnp.float32),
        lax.psum_scatter(
            gain_mlp_terms.reshape(groups, parts, piece_width).astype(jnp.bfloat16),
            "tensor",
            scatter_dimension=1,
            tiled=True,
        ).astype(jnp.float32),
    )
    second_grad = grad_rows + second_part
    attn_grad = lax.all_gather(second_grad.astype(jnp.bfloat16), "tensor", axis=0, tiled=True)
    grad_wo = matmul(mixed.T, attn_grad)
    blended_gradient = matmul(attn_grad, wo.T).astype(jnp.bfloat16)
    query_grad, key_seq_grad, value_seq_grad = attend_back(
        blended_gradient, query_rows, key_seq, value_seq, log_total, positions, heads_kv, head
    )
    kv_width = key_seq.shape[1]
    key_spread = (
        jnp.zeros((groups, block, kv_width), jnp.float32)
        .at[slots]
        .set(key_seq_grad.reshape(-1, block, kv_width))
    )
    value_spread = (
        jnp.zeros((groups, block, kv_width), jnp.float32)
        .at[slots]
        .set(value_seq_grad.reshape(-1, block, kv_width))
    )
    key_own, value_own = (
        lax.psum_scatter(
            key_spread.astype(jnp.bfloat16), "dp", scatter_dimension=0, tiled=True
        ).astype(jnp.float32),
        lax.psum_scatter(
            value_spread.astype(jnp.bfloat16), "dp", scatter_dimension=0, tiled=True
        ).astype(jnp.float32),
    )
    query_round = unrotate(query_grad, positions, head).astype(jnp.bfloat16)
    key_round = unrotate(key_own.reshape(block, kv_width), positions, head).astype(jnp.bfloat16)
    value_round = value_own.reshape(block, kv_width).astype(jnp.bfloat16)
    unit1, inverse1 = norm_stats(full)
    normed1 = (unit1 * gain_attn.astype(jnp.float32)).astype(jnp.bfloat16)
    grad_wq = matmul(normed1.T, query_round)
    grad_wk = matmul(normed1.T, key_round)
    grad_wv = matmul(normed1.T, value_round)
    normed1_grad = matmul(query_round, wq.T) + matmul(key_round, wk.T) + matmul(value_round, wv.T)
    first_terms, gain_attn_terms = norm_back(
        normed1_grad, unit1, inverse1, gain_attn.astype(jnp.float32)
    )
    first_part, gain_attn_part = (
        lax.psum_scatter(first_terms, "tensor", scatter_dimension=0, tiled=True),
        lax.psum_scatter(
            gain_attn_terms.reshape(groups, parts, piece_width),
            "tensor",
            scatter_dimension=1,
            tiled=True,
        ),
    )
    input_grad = second_grad + first_part
    return (
        input_grad,
        (
            grad_wq,
            grad_wk,
            grad_wv,
            grad_wo,
            grad_gate,
            grad_up,
            grad_down,
            gain_attn_part,
            gain_mlp_part,
        ),
    )


def reduce_grads(pieces):
    return (
        lax.psum_scatter(
            pieces[0].astype(jnp.bfloat16), "dp", scatter_dimension=0, tiled=True
        ).astype(jnp.float32),
        lax.psum_scatter(
            pieces[1].astype(jnp.bfloat16), "dp", scatter_dimension=0, tiled=True
        ).astype(jnp.float32),
        lax.psum_scatter(
            pieces[2].astype(jnp.bfloat16), "dp", scatter_dimension=0, tiled=True
        ).astype(jnp.float32),
        lax.psum_scatter(
            pieces[3].astype(jnp.bfloat16), "dp", scatter_dimension=1, tiled=True
        ).astype(jnp.float32),
        lax.psum_scatter(
            pieces[4].astype(jnp.bfloat16), "dp", scatter_dimension=0, tiled=True
        ).astype(jnp.float32),
        lax.psum_scatter(
            pieces[5].astype(jnp.bfloat16), "dp", scatter_dimension=0, tiled=True
        ).astype(jnp.float32),
        lax.psum_scatter(
            pieces[6].astype(jnp.bfloat16), "dp", scatter_dimension=1, tiled=True
        ).astype(jnp.float32),
        lax.psum_scatter(
            pieces[7].astype(jnp.bfloat16), "dp", scatter_dimension=0, tiled=True
        ).astype(jnp.float32),
        lax.psum_scatter(
            pieces[8].astype(jnp.bfloat16), "dp", scatter_dimension=0, tiled=True
        ).astype(jnp.float32),
    )


def general_shards(inputs, table, cotangent, wq, wk, wv, wo, w_gate, w_up, w_down, gain_attn, gain_mlp):
    groups = lax.axis_size("dp")
    parts = lax.axis_size("tensor")
    micro_count = inputs.shape[0]
    section = lax.axis_index("section")
    first_section = section == 0
    weights = (
        lax.all_gather(wq[0], "dp", axis=0, tiled=True),
        lax.all_gather(wk[0], "dp", axis=0, tiled=True),
        lax.all_gather(wv[0], "dp", axis=0, tiled=True),
        lax.all_gather(wo[0], "dp", axis=1, tiled=True),
        lax.all_gather(w_gate[0], "dp", axis=0, tiled=True),
        lax.all_gather(w_up[0], "dp", axis=0, tiled=True),
        lax.all_gather(w_down[0], "dp", axis=1, tiled=True),
        lax.all_gather(gain_attn[0], "dp", axis=0, tiled=True),
        lax.all_gather(gain_mlp[0], "dp", axis=0, tiled=True),
    )
    head = HEAD_SIZE
    heads_kv = wk.shape[2] // head
    received = jnp.zeros_like(inputs[0])
    produced = []
    saved = []
    for step in range(micro_count + 1):
        own_rows = inputs[step] if step < micro_count else jnp.zeros_like(inputs[0])
        start_rows = jnp.where(first_section, own_rows, received)
        micro = jnp.clip(step - section, 0, micro_count - 1)
        result, context = layer_forward(start_rows, table, micro, weights, groups, heads_kv, head)
        produced.append(result)
        saved.append(context)
        if step < micro_count:
            received = passed_along(result, "section", 1)
    stacked = jnp.stack(produced)
    outputs = jnp.where(first_section, stacked[:micro_count], stacked[1:])[None]
    returned = jnp.zeros_like(inputs[0])
    returned_list = []
    totals = None
    for step in range(micro_count + 1):
        index = micro_count - 1 - step
        given = cotangent[index] if index >= 0 else jnp.zeros_like(cotangent[0])
        start_grad = jnp.where(first_section, returned, given)
        din, pieces = layer_backward(
            start_grad, saved[micro_count - step], weights, groups, parts, heads_kv, head
        )
        returned_list.append(din)
        if step < micro_count:
            returned = passed_along(din.astype(jnp.bfloat16), "section", -1).astype(din.dtype)
        totals = (
            pieces
            if totals is None
            else tuple((left + right for left, right in zip(totals, pieces)))
        )
    totals = reduce_grads(totals)
    reverse_stack = jnp.stack(returned_list[::-1])
    input_grad = jnp.where(first_section, reverse_stack[:micro_count], reverse_stack[1:])[None]
    (
        grad_wq,
        grad_wk,
        grad_wv,
        grad_wo,
        grad_gate,
        grad_up,
        grad_down,
        gain_attn_sum,
        gain_mlp_sum,
    ) = totals
    width_piece = gain_attn_sum.shape[-1]
    return (
        outputs,
        input_grad,
        grad_wq[None],
        grad_wk[None],
        grad_wv[None],
        grad_wo[None],
        grad_gate[None],
        grad_up[None],
        grad_down[None],
        gain_attn_sum.reshape(1, width_piece),
        gain_mlp_sum.reshape(1, width_piece),
    )


MESH = pl.DeviceIdType.MESH

def ring_place(index, count):
    return jnp.where(lax.rem(index, 2) == 0, index // 2, count - (index + 1) // 2)

def ring_index(place, count):
    place = lax.rem(place + 2 * count, count)
    return jnp.where(place < count // 2, 2 * place, 2 * count - 1 - 2 * place)

def greet(others):
    barrier = pltpu.get_barrier_semaphore()
    for other in others:
        pl.semaphore_signal(barrier, inc=1, device_id=other, device_id_type=MESH)
    pl.semaphore_wait(barrier, len(others))

def gather_kernel(count, subs, x_ref, o_ref, ring_send, ring_recv, side_send, side_recv, own_sem):
    rows = x_ref.shape[0]
    piece = rows // subs
    me = lax.axis_index("dp")
    core = lax.axis_index("tensor")
    place = ring_place(me, count)
    near = ({"dp": ring_index(place + 1, count)}, {"dp": ring_index(place - 1, count)})
    side = {"tensor": 1 - core}
    greet((*near, side))
    far = count // 2

    def spot(step_from, sub):
        index = ring_index(place + step_from, count)
        start = pl.multiple_of((index * 2 + core) * rows, rows) + sub * piece
        return o_ref.at[pl.ds(pl.multiple_of(start, piece), piece), :]

    own = pltpu.make_async_copy(x_ref, o_ref.at[pl.ds(pl.multiple_of((me * 2 + core) * rows, rows), rows), :], own_sem)
    own.start()
    sends = []

    def travels(way, hop, sub):
        return hop < far or (sub < subs // 2) == (way == 0)

    def ring_copy(way, hop, sub):
        source = x_ref.at[pl.ds(sub * piece, piece), :] if hop == 1 else spot((1 - hop) if way == 0 else (hop - 1), sub)
        return pltpu.make_async_remote_copy(source, spot((1 - hop) if way == 0 else (hop - 1), sub),
            ring_send.at[way, hop - 1, sub], ring_recv.at[way, hop - 1, sub], device_id=near[way], device_id_type=MESH)

    def side_copy(step_from, sub, slot):
        source = x_ref.at[pl.ds(sub * piece, piece), :] if step_from == 0 else spot(step_from, sub)
        return pltpu.make_async_remote_copy(source, spot(step_from, sub), side_send.at[slot, sub], side_recv.at[slot, sub],
            device_id=side, device_id_type=MESH)

    def side_start(copy):
        copy.start()
        sends.append(copy)

    order = lambda way: range(subs) if way == 0 else range(subs - 1, -1, -1)
    for k in range(subs):
        for way in range(2):
            sub = list(order(way))[k]
            copy = ring_copy(way, 1, sub)
            copy.start(); sends.append(copy)
    for sub in range(subs):
        copy = side_copy(0, sub, 0)
        copy.start(); sends.append(copy)
    sides = [(0, sub) for sub in range(subs)]
    for hop in range(1, far + 1):
        for k in range(subs):
            for way in range(2):
                sub = list(order(way))[k]
                if not travels(way, hop, sub):
                    continue
                arrive = pltpu.make_async_remote_copy(spot(-hop if way == 0 else hop, sub), spot(-hop if way == 0 else hop, sub),
                    ring_send.at[way, hop - 1, sub], ring_recv.at[way, hop - 1, sub], device_id=near[way], device_id_type=MESH)
                arrive.wait_recv()
                if hop < far and travels(way, hop + 1, sub):
                    copy = ring_copy(way, hop + 1, sub)
                    copy.start(); sends.append(copy)
                slot = hop if way == 0 or hop == far else count - hop
                copy = side_copy(-hop if way == 0 else hop, sub, slot)
                copy.start(); sends.append(copy)
    for copy in sends:
        copy.wait_send()
    for slot in range(count):
        for sub in range(subs):
            step_from = -slot if slot <= far else count - slot
            index = ring_index(place + step_from, count)
            start = pl.multiple_of((index * 2 + 1 - core) * rows, rows) + sub * piece
            there = o_ref.at[pl.ds(pl.multiple_of(start, piece), piece), :]
            pltpu.make_async_remote_copy(there, there, side_send.at[slot, sub], side_recv.at[slot, sub], device_id=side, device_id_type=MESH).wait_recv()
    own.wait()

def gather_rows(x, count, cid, subs=2):
    rows, width = x.shape
    far = count // 2
    return pl.pallas_call(
        functools.partial(gather_kernel, count, subs),
        out_shape=jax.ShapeDtypeStruct((count * 2 * rows, width), x.dtype),
        in_specs=[pl.BlockSpec(memory_space=pltpu.VMEM)],
        out_specs=pl.BlockSpec(memory_space=pltpu.VMEM),
        scratch_shapes=[
            pltpu.SemaphoreType.DMA((2, far, subs)), pltpu.SemaphoreType.DMA((2, far, subs)),
            pltpu.SemaphoreType.DMA((count, subs)), pltpu.SemaphoreType.DMA((count, subs)),
            pltpu.SemaphoreType.DMA],
        compiler_params=pltpu.CompilerParams(collective_id=cid, has_side_effects=True),
        name="gather_rows")(x)

def reduce_kernel(count, subs, p_ref, o_ref, side_buf, send_buf, recv_buf, ring_send, ring_recv, side_send, side_recv):
    rows, width = o_ref.shape
    piece = rows // subs
    me = lax.axis_index("dp")
    core = lax.axis_index("tensor")
    place = ring_place(me, count)
    near = ({"dp": ring_index(place + 1, count)}, {"dp": ring_index(place - 1, count)})
    side = {"tensor": 1 - core}
    greet((*near, side))
    far = count // 2
    steps = [far]
    for k in range(far - 1, 0, -1):
        steps += [k, -k]
    steps += [0]
    sends = []

    def part(step_to, of_core):
        index = ring_index(place + step_to, count)
        return pl.multiple_of((index * 2 + of_core) * rows, rows)

    side_copies = {}
    for slot, step_to in enumerate(steps):
        copy = pltpu.make_async_remote_copy(p_ref.at[pl.ds(part(step_to, 1 - core), rows), :], side_buf.at[slot],
            side_send.at[slot], side_recv.at[slot], device_id=side, device_id_type=MESH)
        copy.start()
        side_copies[step_to] = (slot, copy)

    def mine(step_to, sub):
        slot, _ = side_copies[step_to]
        start = pl.multiple_of(part(step_to, core) + sub * piece, piece)
        return p_ref[pl.ds(start, piece), :].astype(jnp.float32) + side_buf[slot, sub * piece:(sub + 1) * piece, :].astype(jnp.float32)

    def travels(way, step, sub):
        return step > 1 or (sub < subs // 2) == (way == 0)

    def ring_copy(way, step, sub):
        span = slice(sub * piece, (sub + 1) * piece)
        return pltpu.make_async_remote_copy(send_buf.at[way, step - 1, span, :], recv_buf.at[way, step - 1, span, :],
            ring_send.at[way, step - 1, sub], ring_recv.at[way, step - 1, sub], device_id=near[way], device_id_type=MESH)

    order = lambda way: list(range(subs)) if way == 0 else list(range(subs - 1, -1, -1))
    seen = set()
    for step in range(1, far + 1):
        for k in range(subs):
            for way in range(2):
                sub = order(way)[k]
                if not travels(way, step, sub):
                    continue
                step_to = far + 1 - step
                step_to = step_to if way == 0 or step_to == far else -step_to
                if step_to not in seen:
                    side_copies[step_to][1].wait_recv()
                    seen.add(step_to)
                value = mine(step_to, sub)
                span = slice(sub * piece, (sub + 1) * piece)
                if step > 1 and travels(way, step - 1, sub):
                    ring_copy(way, step - 1, sub).wait_recv()
                    value = value + recv_buf[way, step - 2, span, :].astype(jnp.float32)
                send_buf[way, step - 1, span, :] = value.astype(send_buf.dtype)
                copy = ring_copy(way, step, sub)
                copy.start()
                sends.append(copy)
    side_copies[0][1].wait_recv()
    for sub in range(subs):
        span = slice(sub * piece, (sub + 1) * piece)
        value = mine(0, sub)
        for way in range(2):
            ring_copy(way, far, sub).wait_recv()
            value = value + recv_buf[way, far - 1, span, :].astype(jnp.float32)
        o_ref[span, :] = value.astype(o_ref.dtype)
    for copy in sends:
        copy.wait_send()
    for _, copy in side_copies.values():
        copy.wait_send()

def reduce_rows(p, count, cid, subs=2, dtype=jnp.float32):
    total, width = p.shape
    rows = total // (2 * count)
    far = count // 2
    return pl.pallas_call(
        functools.partial(reduce_kernel, count, subs),
        out_shape=jax.ShapeDtypeStruct((rows, width), dtype),
        in_specs=[pl.BlockSpec(memory_space=pltpu.VMEM)],
        out_specs=pl.BlockSpec(memory_space=pltpu.VMEM),
        scratch_shapes=[
            pltpu.VMEM((count, rows, width), p.dtype),
            pltpu.VMEM((2, far, rows, width), p.dtype),
            pltpu.VMEM((2, far, rows, width), p.dtype),
            pltpu.SemaphoreType.DMA((2, far, subs)), pltpu.SemaphoreType.DMA((2, far, subs)),
            pltpu.SemaphoreType.DMA((count,)), pltpu.SemaphoreType.DMA((count,))],
        compiler_params=pltpu.CompilerParams(collective_id=cid, has_side_effects=True),
        name="reduce_rows")(p)


def weight_pieces(source, target, count, heads, srcs, dsts, layer):
    qkv, wo, gate, up, down, gains = srcs
    out_qkv, out_wo, out_gu, out_down, out_gains = dsts
    depth = gate.shape[0]
    hidden = gate.shape[1] // count
    q_rows = wo.shape[0] // count
    kv_rows = (qkv.shape[0] - wo.shape[0]) // 2
    shared = count * heads // kv_rows
    cols = pl.ds(pl.multiple_of(source * depth, depth), depth)

    def at(index, size):
        return pl.ds(pl.multiple_of(index * size, size), size)

    k_from = pl.multiple_of(wo.shape[0] + target // shared * heads, heads)
    v_from = pl.multiple_of(wo.shape[0] + kv_rows + target // shared * heads, heads)
    return (
        (gains, out_gains.at[layer, :, cols]),
        (qkv.at[at(target, q_rows), :], out_qkv.at[layer, pl.ds(0, q_rows), cols]),
        (qkv.at[pl.ds(k_from, heads), :], out_qkv.at[layer, pl.ds(q_rows, heads), cols]),
        (qkv.at[pl.ds(v_from, heads), :], out_qkv.at[layer, pl.ds(q_rows + heads, heads), cols]),
        (wo.at[at(target, q_rows), :], out_wo.at[layer, :, cols]),
        (gate.at[:, at(target, hidden)], out_gu.at[layer, cols, pl.ds(0, hidden)]),
        (up.at[:, at(target, hidden)], out_gu.at[layer, cols, pl.ds(hidden, hidden)]),
        (down.at[at(target, hidden), :], out_down.at[layer, :, cols]),
    )


KINDS = 8


def spread_kernel(count, heads, *refs):
    srcs = refs[:6]
    dsts = refs[6:11]
    send, recv, cross_send, cross_recv, own_sem = refs[11:]
    me = lax.axis_index("dp")
    layer = lax.axis_index("section")
    peers = [lax.rem(me + k, count) for k in range(1, count)]
    across = {"section": 1 - layer}
    greet([{"dp": peer} for peer in peers] + [across])
    waits = []
    local = []
    own = weight_pieces(me, me, count, heads, srcs, dsts, layer)
    for kind in range(KINDS):
        for k, peer in enumerate(peers):
            there = weight_pieces(me, peer, count, heads, srcs, dsts, layer)[kind]
            copy = pltpu.make_async_remote_copy(
                there[0], there[1], send.at[kind, k], recv.at[kind, k],
                device_id={"dp": peer}, device_id_type=MESH,
            )
            copy.start()
            waits.append(copy)
        copy = pltpu.make_async_remote_copy(
            own[kind][0], own[kind][1], cross_send.at[kind, count - 1], cross_recv.at[kind, count - 1],
            device_id=across, device_id_type=MESH,
        )
        copy.start()
        waits.append(copy)
        copy = pltpu.make_async_copy(own[kind][0], own[kind][1], own_sem.at[kind])
        copy.start()
        local.append(copy)
    for kind in range(KINDS):
        for k in range(count - 1):
            origin = lax.rem(me + count - 1 - k, count)
            here = weight_pieces(origin, me, count, heads, srcs, dsts, layer)[kind][1]
            pltpu.make_async_remote_copy(
                here, here, send.at[kind, k], recv.at[kind, k],
                device_id={"dp": origin}, device_id_type=MESH,
            ).wait_recv()
            copy = pltpu.make_async_remote_copy(
                here, here, cross_send.at[kind, k], cross_recv.at[kind, k],
                device_id=across, device_id_type=MESH,
            )
            copy.start()
            waits.append(copy)
    for copy in local:
        copy.wait()
    for copy in waits:
        copy.wait_send()
    for kind in range(KINDS):
        for k in range(count):
            origin = lax.rem(me + count - 1 - k, count)
            there = weight_pieces(origin, me, count, heads, srcs, dsts, 1 - layer)[kind][1]
            pltpu.make_async_remote_copy(
                there, there, cross_send.at[kind, k], cross_recv.at[kind, k],
                device_id=across, device_id_type=MESH,
            ).wait_recv()


def spread_weights(qkv, wo, gate, up, down, gains, count, heads, cid):
    depth = gate.shape[0]
    width = depth * count
    hidden = gate.shape[1] // count
    q_rows = wo.shape[0] // count
    shape = lambda *dims: jax.ShapeDtypeStruct((2, *dims), jnp.bfloat16)
    hbm = pl.BlockSpec(memory_space=pl.ANY)
    return pl.pallas_call(
        functools.partial(spread_kernel, count, heads),
        out_shape=(
            shape(q_rows + 2 * heads, width),
            shape(q_rows, width),
            shape(width, 2 * hidden),
            shape(hidden, width),
            jax.ShapeDtypeStruct((2, gains.shape[0], width), gains.dtype),
        ),
        in_specs=[hbm] * 6,
        out_specs=(hbm,) * 5,
        scratch_shapes=[
            pltpu.SemaphoreType.DMA((KINDS, count - 1)),
            pltpu.SemaphoreType.DMA((KINDS, count - 1)),
            pltpu.SemaphoreType.DMA((KINDS, count)),
            pltpu.SemaphoreType.DMA((KINDS, count)),
            pltpu.SemaphoreType.DMA((KINDS,)),
        ],
        compiler_params=pltpu.CompilerParams(collective_id=cid, has_side_effects=True),
        name="spread_weights",
    )(qkv, wo, gate, up, down, gains)


def swap_halves(rows, head):
    width = rows.shape[1]
    lane = lax.broadcasted_iota(jnp.int32, rows.shape, 1)
    half = head // 2
    return jnp.where(
        lax.rem(lane, head) < half, pltpu.roll(rows, width - half, 1), pltpu.roll(rows, half, 1)
    )


def low_lanes(shape, head):
    return lax.broadcasted_iota(jnp.int32, shape, 1) < head


def dot(left, right, contract):
    return lax.dot_general(
        left, right, (contract, ((), ())), preferred_element_type=jnp.float32
    )


def two_heads(rows, head):
    low = low_lanes(rows.shape, head)
    zero = jnp.zeros_like(rows)
    return jnp.concatenate([jnp.where(low, rows, zero), jnp.where(low, zero, rows)], axis=0)


def one_row(rows, head):
    half = rows.shape[0] // 2
    return jnp.where(low_lanes((half, rows.shape[1]), head), rows[:half], rows[half:])


def triangle(block, keys):
    row = lax.rem(lax.broadcasted_iota(jnp.int32, (2 * block, keys), 0), block)
    column = lax.broadcasted_iota(jnp.int32, (2 * block, keys), 1)
    return column <= row + (keys - block)


def attend_kernel(groups, head, slots, qkv_ref, cos_ref, sin_ref, mixed_ref, kept_ref, lse_ref, key2, value2):
    tokens = qkv_ref.shape[0]
    block = tokens // groups
    span = groups // 2
    wide = 2 * head
    scale = 1.0 / math.sqrt(head)
    for spot in range(groups):
        rows = pl.ds(pl.multiple_of(slots[spot] * block, block), block)
        cosine = cos_ref[rows, :]
        sine = sin_ref[rows, :]
        query = qkv_ref[rows, :wide]
        query = (query * cosine + swap_halves(query, head) * sine).astype(jnp.bfloat16)
        pair = qkv_ref[rows, wide:]
        low = low_lanes(pair.shape, head)
        pair = jnp.where(low, pair * cosine + swap_halves(pair, head) * sine, pair)
        turned = pltpu.roll(pair, head, 1)
        kept_ref[rows, :wide] = query
        kept_ref[rows, wide:] = pair.astype(jnp.bfloat16)
        here = slice(spot * block, (spot + 1) * block)
        key2[here, :] = jnp.where(low, pair, turned).astype(jnp.bfloat16)
        value2[here, :] = jnp.where(low, turned, pair).astype(jnp.bfloat16)
    for spot in range(groups):
        first = spot // span * span * block
        keys = (spot % span + 1) * block
        rows = pl.ds(pl.multiple_of(slots[spot] * block, block), block)
        query = two_heads(kept_ref[rows, :wide], head)
        score = dot(query, key2[first : first + keys, :], ((1,), (1,))) * scale
        power = jnp.where(triangle(block, keys), jnp.exp(score), 0.0)
        total = jnp.sum(power, axis=1, keepdims=True)
        lse = jnp.log(total)
        probs = jnp.where(triangle(block, keys), jnp.exp(score - lse), 0.0).astype(jnp.bfloat16)
        mixed = dot(probs, value2[first : first + keys, :], ((1,), (0,)))
        mixed_ref[rows, :] = one_row(mixed, head).astype(jnp.bfloat16)
        lse_ref[spot] = lse


def attend_blocks(slots, qkv, cosine, sine, groups, head):
    tokens = qkv.shape[0]
    block = tokens // groups
    vmem = pl.BlockSpec(memory_space=pltpu.VMEM)
    return pl.pallas_call(
        functools.partial(attend_kernel, groups, head),
        out_shape=(
            jax.ShapeDtypeStruct((tokens, 2 * head), jnp.bfloat16),
            jax.ShapeDtypeStruct((tokens, 4 * head), jnp.bfloat16),
            jax.ShapeDtypeStruct((groups, 2 * block, 1), jnp.float32),
        ),
        in_specs=[pl.BlockSpec(memory_space=pltpu.SMEM), vmem, vmem, vmem],
        out_specs=(vmem, vmem, vmem),
        scratch_shapes=[
            pltpu.VMEM((tokens, 2 * head), jnp.bfloat16),
            pltpu.VMEM((tokens, 2 * head), jnp.bfloat16),
        ],
        name="attend_blocks",
    )(slots, qkv, cosine, sine)


def attend_back_kernel(
    groups, head, slots, grad_ref, kept_ref, lse_ref, cos_ref, sin_ref, out_ref, key2, value2, key_sum, value_sum
):
    tokens = kept_ref.shape[0]
    block = tokens // groups
    span = groups // 2
    wide = 2 * head
    scale = 1.0 / math.sqrt(head)
    for spot in range(groups):
        rows = pl.ds(pl.multiple_of(slots[spot] * block, block), block)
        pair = kept_ref[rows, wide:].astype(jnp.float32)
        low = low_lanes(pair.shape, head)
        turned = pltpu.roll(pair, head, 1)
        here = slice(spot * block, (spot + 1) * block)
        key2[here, :] = jnp.where(low, pair, turned).astype(jnp.bfloat16)
        value2[here, :] = jnp.where(low, turned, pair).astype(jnp.bfloat16)
    for spot in range(groups - 1, -1, -1):
        place = spot % span
        first = spot // span * span * block
        keys = (place + 1) * block
        rows = pl.ds(pl.multiple_of(slots[spot] * block, block), block)
        query = two_heads(kept_ref[rows, :wide], head)
        grad = two_heads(grad_ref[rows, :], head)
        key = key2[first : first + keys, :]
        value = value2[first : first + keys, :]
        score = dot(query, key, ((1,), (1,))) * scale
        probs = jnp.where(triangle(block, keys), jnp.exp(score - lse_ref[spot]), 0.0)
        prob_grad = dot(grad, value, ((1,), (1,)))
        rowdot = jnp.sum(probs * prob_grad, axis=1, keepdims=True)
        score_grad = (probs * (prob_grad - rowdot) * scale).astype(jnp.bfloat16)
        value_part = dot(probs.astype(jnp.bfloat16), grad, ((0,), (0,)))
        key_part = dot(score_grad, query, ((0,), (0,)))
        if place == span - 1:
            value_sum[first : first + keys, :] = value_part
            key_sum[first : first + keys, :] = key_part
        else:
            value_sum[first : first + keys, :] += value_part
            key_sum[first : first + keys, :] += key_part
        query_grad = one_row(dot(score_grad, key, ((1,), (0,))), head)
        query_grad = query_grad * cos_ref[rows, :] - swap_halves(query_grad, head) * sin_ref[rows, :]
        out_ref[rows, :wide] = query_grad.astype(jnp.bfloat16)
    for spot in range(groups):
        rows = pl.ds(pl.multiple_of(slots[spot] * block, block), block)
        here = slice(spot * block, (spot + 1) * block)
        key = key_sum[here, :]
        key = key + pltpu.roll(key, head, 1)
        key = key * cos_ref[rows, :] - swap_halves(key, head) * sin_ref[rows, :]
        value = value_sum[here, :]
        value = value + pltpu.roll(value, head, 1)
        low = low_lanes(key.shape, head)
        out_ref[rows, wide:] = jnp.where(low, key, value).astype(jnp.bfloat16)


def attend_blocks_back(slots, grad, kept, lse, cosine, sine, groups, head):
    tokens = kept.shape[0]
    vmem = pl.BlockSpec(memory_space=pltpu.VMEM)
    return pl.pallas_call(
        functools.partial(attend_back_kernel, groups, head),
        out_shape=jax.ShapeDtypeStruct((tokens, 4 * head), jnp.bfloat16),
        in_specs=[pl.BlockSpec(memory_space=pltpu.SMEM)] + [vmem] * 5,
        out_specs=vmem,
        scratch_shapes=[
            pltpu.VMEM((tokens, 2 * head), jnp.bfloat16),
            pltpu.VMEM((tokens, 2 * head), jnp.bfloat16),
            pltpu.VMEM((tokens, 2 * head), jnp.float32),
            pltpu.VMEM((tokens, 2 * head), jnp.float32),
        ],
        name="attend_blocks_back",
    )(slots, grad, kept, lse, cosine, sine)


def rope_tables(table_row, block, head):
    groups = table_row.shape[0]
    place = table_row % (groups // 2)
    positions = (place[:, None] * block + jnp.arange(block, dtype=jnp.int32)).reshape(-1)
    angle = positions.astype(jnp.float32)[:, None] * rope_frequencies(head)[None, :]
    cosine = jnp.cos(angle)
    sine = jnp.sin(angle)
    return (
        jnp.concatenate([cosine] * 4, axis=1),
        jnp.concatenate([-sine, sine] * 2, axis=1),
    )


def matmul_nt(left, right):
    return dot(left, right, ((1,), (1,)))


def matmul_tn(left, right):
    return dot(left, right, ((0,), (0,)))


def section_swap(value):
    return lax.ppermute(value, "section", [(0, 1), (1, 0)])


def section_move(value, source):
    return lax.ppermute(value, "section", [(source, 1 - source)])


def fast_forward(rows, weights, layer, tools):
    qkv_w, wo_w, gu_w, down_w, gain_attn, gain_mlp = [w[layer] for w in weights]
    count, slots, cosine, sine, head = tools
    unit1, inverse1 = norm_stats(rows)
    normed1 = gather_rows((unit1 * gain_attn).astype(jnp.bfloat16), count, 1)
    qkv = matmul_nt(normed1, qkv_w)
    mixed, kept, lse = attend_blocks(slots, qkv, cosine, sine, count, head)
    second = rows + reduce_rows(matmul(mixed, wo_w).astype(jnp.bfloat16), count, 2)
    unit2, inverse2 = norm_stats(second)
    normed2 = gather_rows((unit2 * gain_mlp).astype(jnp.bfloat16), count, 1)
    gate_up = matmul(normed2, gu_w)
    gate, upper = jnp.split(gate_up, 2, axis=1)
    hidden = (jax.nn.silu(gate) * upper).astype(jnp.bfloat16)
    result = second + reduce_rows(matmul(hidden, down_w).astype(jnp.bfloat16), count, 2)
    return result, (unit1, inverse1, normed1, kept, lse, mixed, unit2, inverse2, normed2, gate_up, hidden)


def fast_backward(grad_rows, context, weights, layer, tools):
    qkv_w, wo_w, gu_w, down_w, gain_attn, gain_mlp = [w[layer] for w in weights]
    count, slots, cosine, sine, head = tools
    unit1, inverse1, normed1, kept, lse, mixed, unit2, inverse2, normed2, gate_up, hidden = context
    gate, upper = jnp.split(gate_up, 2, axis=1)
    out_grad = gather_rows(grad_rows.astype(jnp.bfloat16), count, 1)
    hidden_grad = matmul_nt(out_grad, down_w)
    grad_down = matmul_tn(hidden, out_grad).astype(jnp.bfloat16)
    sigma = jax.nn.sigmoid(gate)
    gate_grad = (hidden_grad * upper * sigma * (1.0 + gate * (1.0 - sigma))).astype(jnp.bfloat16)
    up_grad = (hidden_grad * gate * sigma).astype(jnp.bfloat16)
    gu_grad = jnp.concatenate([gate_grad, up_grad], axis=1)
    grad_gu = matmul_tn(normed2, gu_grad).astype(jnp.bfloat16)
    normed2_grad = reduce_rows(matmul_nt(gu_grad, gu_w).astype(jnp.bfloat16), count, 2)
    second_part, gain_mlp_part = norm_back(normed2_grad, unit2, inverse2, gain_mlp)
    second_grad = grad_rows + second_part
    attn_grad = gather_rows(second_grad.astype(jnp.bfloat16), count, 1)
    grad_wo = matmul_tn(mixed, attn_grad).astype(jnp.bfloat16)
    mixed_grad = matmul_nt(attn_grad, wo_w).astype(jnp.bfloat16)
    qkv_grad = attend_blocks_back(slots, mixed_grad, kept, lse, cosine, sine, count, head)
    grad_qkv = matmul_tn(qkv_grad, normed1).astype(jnp.bfloat16)
    normed1_grad = reduce_rows(matmul(qkv_grad, qkv_w).astype(jnp.bfloat16), count, 2)
    first_part, gain_attn_part = norm_back(normed1_grad, unit1, inverse1, gain_attn)
    return second_grad + first_part, (grad_gu, grad_down, grad_wo, grad_qkv), (gain_attn_part, gain_mlp_part)


def fast_shards(inputs, table, cotangent, wq, wk, wv, wo, w_gate, w_up, w_down, gain_attn, gain_mlp):
    count = lax.axis_size("dp")
    parts = lax.axis_size("tensor")
    head = HEAD_SIZE
    section = lax.axis_index("section")
    first_section = section == 0
    block = inputs.shape[1] * parts
    depth = wq.shape[1]
    width = depth * count
    q_rows = wo.shape[1] // count
    hidden = w_gate.shape[2] // count

    qkv_t = jnp.concatenate([wq[0], wk[0], wv[0]], axis=1).T
    gains = jnp.concatenate([gain_attn, gain_mlp], axis=0).astype(jnp.float32)
    gains = jnp.concatenate([gains] * 4, axis=0)
    qkv_w, wo_w, gu_w, down_w, all_gains = spread_weights(
        qkv_t, wo[0], w_gate[0], w_up[0], w_down[0], gains, count, head, 0
    )
    weights = (qkv_w, wo_w, gu_w, down_w, all_gains[:, 0], all_gains[:, 1])

    rows = lax.dynamic_index_in_dim(inputs, section, 0, keepdims=False)
    given = lax.dynamic_index_in_dim(cotangent, section, 0, keepdims=False)
    table_row = lax.dynamic_index_in_dim(table, section, 0, keepdims=False)
    slot_ids = jnp.arange(count, dtype=jnp.int32)
    slots = jnp.sum(jnp.where(table_row[None, :] == slot_ids[:, None], slot_ids[None, :], 0), axis=1)
    cosine, sine = rope_tables(table_row, block, head)
    tools = (count, slots, cosine, sine, head)

    result0, context0 = fast_forward(rows, weights, 0, tools)
    result1, context1 = fast_forward(result0, weights, 1, tools)
    din1, grads1, gains1 = fast_backward(given, context1, weights, 1, tools)
    moved1 = [section_move(g, 0) for g in grads1]
    din0, grads0, gains0 = fast_backward(din1, context0, weights, 0, tools)
    moved0 = [section_move(g, 1) for g in grads0]

    def both(at0, at1):
        other = section_swap(jnp.where(first_section, at1, at0))
        return jnp.where(
            first_section, jnp.stack([at0, other]), jnp.stack([other, at1])
        )[None]

    outputs = both(result0, result1)
    input_grad = both(din0, din1)

    def total(at):
        mine = jnp.where(first_section, grads0[at], grads1[at]).astype(jnp.float32)
        theirs = jnp.where(first_section, moved0[at], moved1[at]).astype(jnp.float32)
        return (mine + theirs).astype(jnp.bfloat16)

    gu_total, down_total, wo_total, qkv_total = [total(at) for at in range(4)]
    cut = lambda value: value.reshape(value.shape[0], count, depth).transpose(1, 0, 2)
    exchange = lambda value: lax.all_to_all(value, "dp", split_axis=0, concat_axis=0, tiled=True)
    gu_own = exchange(gu_total.reshape(count, depth, 2 * hidden))
    down_own = exchange(cut(down_total))
    wo_own = exchange(cut(wo_total))
    qkv_own = exchange(cut(qkv_total))
    grad_gate = gu_own[:, :, :hidden].transpose(1, 0, 2).reshape(depth, -1).astype(jnp.float32)
    grad_up = gu_own[:, :, hidden:].transpose(1, 0, 2).reshape(depth, -1).astype(jnp.float32)
    grad_down = down_own.reshape(-1, depth).astype(jnp.float32)
    grad_wo = wo_own.reshape(-1, depth).astype(jnp.float32)
    grad_wq = qkv_own[:, :q_rows].reshape(-1, depth).astype(jnp.float32).T
    shared = count * head // wk.shape[2]
    joined = qkv_own[:, q_rows:].astype(jnp.float32).reshape(count // shared, shared, 2, head, depth)
    joined = jnp.sum(joined, axis=1)
    grad_wk = joined[:, 0].reshape(-1, depth).T
    grad_wv = joined[:, 1].reshape(-1, depth).T

    gain_rows = jnp.stack(
        [jnp.stack(gains0), jnp.stack(gains1)]
    ).reshape(2, 2, count * parts, -1).transpose(0, 2, 1, 3)
    gain_piece = gain_rows.shape[-1]
    gain_rows = gain_rows.reshape(2 * count * parts, 2 * gain_piece)
    gain_sums = lax.psum_scatter(
        gain_rows, ("section", "dp", "tensor"), scatter_dimension=0, tiled=True
    ).reshape(2, gain_piece)
    return (
        outputs,
        input_grad,
        grad_wq[None],
        grad_wk[None],
        grad_wv[None],
        grad_wo[None],
        grad_gate[None],
        grad_up[None],
        grad_down[None],
        gain_sums[:1],
        gain_sums[1:],
    )


def fits(mesh, inputs, table, cotangent, wq, wk, wv, wo, w_gate, w_up, w_down, gain_attn, gain_mlp):
    sections, count, parts = (mesh.shape[axis] for axis in ("section", "dp", "tensor"))
    head = HEAD_SIZE
    if sections != 2 or parts != 2 or inputs.shape[0] != sections or count % 4:
        return False
    devices = count * parts
    queries, keys = wq.shape[2] // head, wk.shape[2] // head
    if queries != 2 * devices or devices % keys or keys % parts or 4 * head != 256:
        return False
    return (
        wq.shape[1] % (128 * count) == 0
        and w_gate.shape[2] % (128 * devices) == 0
        and inputs.shape[1] % (64 * devices) == 0
    )


def shards(mesh, whole, *args):
    if fits(mesh, *whole):
        return fast_shards(*args)
    return general_shards(*args)


def solution(mesh):
    in_specs = (
        P(None, ("dp", "tensor"), None),
        P(),
        P(None, ("dp", "tensor"), None),
        P("section", "dp", "tensor"),
        P("section", "dp", "tensor"),
        P("section", "dp", "tensor"),
        P("section", "tensor", "dp"),
        P("section", "dp", "tensor"),
        P("section", "dp", "tensor"),
        P("section", "tensor", "dp"),
        P("section", "dp"),
        P("section", "dp"),
    )
    out_specs = (
        P("section", None, ("dp", "tensor"), None),
        P("section", None, ("dp", "tensor"), None),
        P("section", "dp", "tensor"),
        P("section", "dp", "tensor"),
        P("section", "dp", "tensor"),
        P("section", "tensor", "dp"),
        P("section", "dp", "tensor"),
        P("section", "dp", "tensor"),
        P("section", "tensor", "dp"),
        P("section", ("dp", "tensor")),
        P("section", ("dp", "tensor")),
    )

    def step(*args):
        return jax.shard_map(
            functools.partial(shards, mesh, args),
            mesh=mesh,
            in_specs=in_specs,
            out_specs=out_specs,
            check_vma=False,
        )(*args)

    return step
```

```python
import functools
import math

import jax
import jax.numpy as jnp
from jax import lax
from jax.experimental import pallas as pl
from jax.experimental.pallas import tpu as pltpu
from jax.sharding import PartitionSpec as P

HEAD_SIZE = 64


epsilon = 1e-05


def passed_along(value, axis, steps):
    count = lax.axis_size(axis)
    initial, last = (max(0, -steps), min(count, count - steps))
    return lax.ppermute(value, axis, [(source, source + steps) for source in range(initial, last)])


def rope_frequencies(head):
    index = jnp.arange(head // 2, dtype=jnp.float32)
    base = 1.0 / 500000.0 ** (index * 2.0 / head)
    wavelength = 2.0 * math.pi / base
    blend = (8192.0 / wavelength - 1.0) / 3.0
    middle = (1.0 - blend) * base / 32.0 + blend * base
    return jnp.where(wavelength < 2048.0, base, jnp.where(wavelength > 8192.0, base / 32.0, middle))


def rotate(values, positions, head):
    step_count = values.shape[0]
    shaped = values.reshape(step_count, -1, head)
    angle = positions.astype(jnp.float32)[:, None] * rope_frequencies(head)[None, :]
    cosine = jnp.cos(angle)[:, None, :]
    sine = jnp.sin(angle)[:, None, :]
    first = shaped[:, :, : head // 2]
    second = shaped[:, :, head // 2 :]
    return jnp.concatenate(
        [first * cosine - second * sine, second * cosine + first * sine], axis=-1
    ).reshape(step_count, -1)


def unrotate(values, positions, head):
    step_count = values.shape[0]
    shaped = values.reshape(step_count, -1, head)
    angle = positions.astype(jnp.float32)[:, None] * rope_frequencies(head)[None, :]
    cosine = jnp.cos(angle)[:, None, :]
    sine = jnp.sin(angle)[:, None, :]
    first = shaped[:, :, : head // 2]
    second = shaped[:, :, head // 2 :]
    return jnp.concatenate(
        [first * cosine + second * sine, second * cosine - first * sine], axis=-1
    ).reshape(step_count, -1)


def norm_stats(rows):
    inverse = lax.rsqrt(jnp.mean(rows * rows, axis=-1, keepdims=True) + epsilon)
    return (rows * inverse, inverse)


def norm_back(grad, unit, inverse, gain):
    scaled = grad * gain
    inner = jnp.mean(scaled * unit, axis=-1, keepdims=True)
    return (inverse * (scaled - unit * inner), jnp.sum(grad * unit, axis=0))


def matmul(left, right):
    return jnp.dot(left, right, preferred_element_type=jnp.float32)


def block_layout(table, micro, groups, block):
    layout_row = lax.dynamic_index_in_dim(table, micro, 0, keepdims=False)
    span = groups // 2
    mine = lax.dynamic_index_in_dim(layout_row, lax.axis_index("dp"), 0, keepdims=False)
    sequence = mine // span
    place = mine % span
    slot_ids = jnp.arange(groups, dtype=jnp.int32)
    holder = jnp.sum(
        jnp.where(layout_row[None, :] == slot_ids[:, None], slot_ids[None, :], 0), axis=1
    )
    slots = lax.dynamic_slice_in_dim(holder, sequence * span, span)
    positions = place * block + jnp.arange(block, dtype=jnp.int32)
    return (slots, positions)


def attend(query_rows, key_seq, value_seq, positions, heads_kv, head):
    step_count = query_rows.shape[0]
    keys_total = key_seq.shape[0]
    head_group = query_rows.shape[1] // (heads_kv * head)
    scale = 1.0 / math.sqrt(head)
    allowed = jnp.arange(keys_total, dtype=jnp.int32)[None, :] <= positions[:, None]
    query_layers = query_rows.reshape(step_count, heads_kv, head_group * head).transpose(1, 0, 2)
    key_layers = key_seq.reshape(keys_total, heads_kv, head).transpose(1, 0, 2)
    value_layers = value_seq.reshape(keys_total, heads_kv, head).transpose(1, 0, 2)

    def one_head(parts):
        q_head, k_head, v_head = parts
        q_three = q_head.reshape(step_count, head_group, head)
        scores = (
            jnp.einsum("qgd,kd->gqk", q_three, k_head, preferred_element_type=jnp.float32) * scale
        )
        total = jnp.sum(jnp.where(allowed, jnp.exp(scores), 0.0), axis=-1)
        log_total = jnp.log(total)
        probs = jnp.where(allowed, jnp.exp(scores - log_total[..., None]), 0.0).astype(jnp.bfloat16)
        mixed = jnp.einsum("gqk,kd->qgd", probs, v_head, preferred_element_type=jnp.float32).astype(
            jnp.bfloat16
        )
        return (mixed.reshape(step_count, head_group * head), log_total)

    mixed, log_total = lax.map(one_head, (query_layers, key_layers, value_layers))
    return (mixed.transpose(1, 0, 2).reshape(step_count, -1), log_total)


def attend_back(
    blended_gradient, query_rows, key_seq, value_seq, log_total, positions, heads_kv, head
):
    step_count = query_rows.shape[0]
    keys_total = key_seq.shape[0]
    head_group = query_rows.shape[1] // (heads_kv * head)
    scale = 1.0 / math.sqrt(head)
    allowed = jnp.arange(keys_total, dtype=jnp.int32)[None, :] <= positions[:, None]
    query_layers = query_rows.reshape(step_count, heads_kv, head_group * head).transpose(1, 0, 2)
    key_layers = key_seq.reshape(keys_total, heads_kv, head).transpose(1, 0, 2)
    value_layers = value_seq.reshape(keys_total, heads_kv, head).transpose(1, 0, 2)
    gain_layers = blended_gradient.reshape(step_count, heads_kv, head_group * head).transpose(
        1, 0, 2
    )

    def one_head(parts):
        q_head, k_head, v_head, g_head, l_head = parts
        q_three = q_head.reshape(step_count, head_group, head)
        g_three = g_head.reshape(step_count, head_group, head)
        scores = (
            jnp.einsum("qgd,kd->gqk", q_three, k_head, preferred_element_type=jnp.float32) * scale
        )
        probs = jnp.where(allowed, jnp.exp(scores - l_head[..., None]), 0.0)
        rounded = probs.astype(jnp.bfloat16)
        prob_grad = jnp.einsum("qgd,kd->gqk", g_three, v_head, preferred_element_type=jnp.float32)
        value_total_sum = jnp.einsum(
            "gqk,qgd->kd", rounded, g_three, preferred_element_type=jnp.float32
        )
        rowdot = jnp.sum(probs * prob_grad, axis=-1, keepdims=True)
        score_grad = (probs * (prob_grad - rowdot) * scale).astype(jnp.bfloat16)
        query_grad = jnp.einsum(
            "gqk,kd->qgd", score_grad, k_head, preferred_element_type=jnp.float32
        )
        key_gradient = jnp.einsum(
            "gqk,qgd->kd", score_grad, q_three, preferred_element_type=jnp.float32
        )
        return (query_grad.reshape(step_count, head_group * head), key_gradient, value_total_sum)

    query_grad, key_gradient, value_total_sum = lax.map(
        one_head, (query_layers, key_layers, value_layers, gain_layers, log_total)
    )
    query_grad = query_grad.transpose(1, 0, 2).reshape(step_count, -1)
    key_gradient = key_gradient.transpose(1, 0, 2).reshape(keys_total, -1)
    value_total_sum = value_total_sum.transpose(1, 0, 2).reshape(keys_total, -1)
    return (query_grad, key_gradient, value_total_sum)


def layer_forward(rows, table, micro, weights, groups, heads_kv, head):
    wq, wk, wv, wo, w_gate, w_up, w_down, gain_attn, gain_mlp = weights
    full = lax.all_gather(rows, "tensor", axis=0, tiled=True)
    block = full.shape[0]
    slots, positions = block_layout(table, micro, groups, block)
    unit1, inverse1 = norm_stats(full)
    normed1 = (unit1 * gain_attn.astype(jnp.float32)).astype(jnp.bfloat16)
    query_rows = rotate(matmul(normed1, wq), positions, head).astype(jnp.bfloat16)
    key = rotate(matmul(normed1, wk), positions, head).astype(jnp.bfloat16)
    value_rows = matmul(normed1, wv).astype(jnp.bfloat16)
    key_all, value_all = (
        lax.all_gather(key, "dp", axis=0, tiled=True),
        lax.all_gather(value_rows, "dp", axis=0, tiled=True),
    )
    kv_width = key.shape[1]
    key_seq = key_all.reshape(groups, block, kv_width)[slots].reshape(-1, kv_width)
    value_seq = value_all.reshape(groups, block, kv_width)[slots].reshape(-1, kv_width)
    mixed, log_total = attend(query_rows, key_seq, value_seq, positions, heads_kv, head)
    second = rows + lax.psum_scatter(matmul(mixed, wo), "tensor", scatter_dimension=0, tiled=True)
    full_second = lax.all_gather(second, "tensor", axis=0, tiled=True)
    unit2, inverse2 = norm_stats(full_second)
    normed2 = (unit2 * gain_mlp.astype(jnp.float32)).astype(jnp.bfloat16)
    gate = matmul(normed2, w_gate)
    upper = matmul(normed2, w_up)
    hidden = (jax.nn.silu(gate) * upper).astype(jnp.bfloat16)
    result = second + lax.psum_scatter(
        matmul(hidden, w_down), "tensor", scatter_dimension=0, tiled=True
    )
    return (
        result,
        (
            full,
            query_rows,
            key_seq,
            value_seq,
            mixed,
            log_total,
            full_second,
            gate,
            upper,
            hidden,
            slots,
            positions,
        ),
    )


def layer_backward(grad_rows, context, weights, groups, parts, heads_kv, head):
    wq, wk, wv, wo, w_gate, w_up, w_down, gain_attn, gain_mlp = weights
    (
        full,
        query_rows,
        key_seq,
        value_seq,
        mixed,
        log_total,
        full_second,
        gate,
        upper,
        hidden,
        slots,
        positions,
    ) = context
    block = full.shape[0]
    out_grad = lax.all_gather(grad_rows.astype(jnp.bfloat16), "tensor", axis=0, tiled=True)
    grad_down = matmul(hidden.T, out_grad)
    hidden_grad = matmul(out_grad, w_down.T)
    sigma = jax.nn.sigmoid(gate)
    gate_grad = (hidden_grad * upper * sigma * (1.0 + gate * (1.0 - sigma))).astype(jnp.bfloat16)
    up_grad = (hidden_grad * gate * sigma).astype(jnp.bfloat16)
    unit2, inverse2 = norm_stats(full_second)
    normed2 = (unit2 * gain_mlp.astype(jnp.float32)).astype(jnp.bfloat16)
    grad_gate = matmul(normed2.T, gate_grad)
    grad_up = matmul(normed2.T, up_grad)
    normed2_grad = matmul(gate_grad, w_gate.T) + matmul(up_grad, w_up.T)
    second_terms, gain_mlp_terms = norm_back(
        normed2_grad, unit2, inverse2, gain_mlp.astype(jnp.float32)
    )
    piece_width = gain_mlp_terms.shape[0] // (groups * parts)
    second_part, gain_mlp_part = (
        lax.psum_scatter(
            second_terms.astype(jnp.bfloat16), "tensor", scatter_dimension=0, tiled=True
        ).astype(jnp.float32),
        lax.psum_scatter(
            gain_mlp_terms.reshape(groups, parts, piece_width).astype(jnp.bfloat16),
            "tensor",
            scatter_dimension=1,
            tiled=True,
        ).astype(jnp.float32),
    )
    second_grad = grad_rows + second_part
    attn_grad = lax.all_gather(second_grad.astype(jnp.bfloat16), "tensor", axis=0, tiled=True)
    grad_wo = matmul(mixed.T, attn_grad)
    blended_gradient = matmul(attn_grad, wo.T).astype(jnp.bfloat16)
    query_grad, key_seq_grad, value_seq_grad = attend_back(
        blended_gradient, query_rows, key_seq, value_seq, log_total, positions, heads_kv, head
    )
    kv_width = key_seq.shape[1]
    key_spread = (
        jnp.zeros((groups, block, kv_width), jnp.float32)
        .at[slots]
        .set(key_seq_grad.reshape(-1, block, kv_width))
    )
    value_spread = (
        jnp.zeros((groups, block, kv_width), jnp.float32)
        .at[slots]
        .set(value_seq_grad.reshape(-1, block, kv_width))
    )
    key_own, value_own = (
        lax.psum_scatter(
            key_spread.astype(jnp.bfloat16), "dp", scatter_dimension=0, tiled=True
        ).astype(jnp.float32),
        lax.psum_scatter(
            value_spread.astype(jnp.bfloat16), "dp", scatter_dimension=0, tiled=True
        ).astype(jnp.float32),
    )
    query_round = unrotate(query_grad, positions, head).astype(jnp.bfloat16)
    key_round = unrotate(key_own.reshape(block, kv_width), positions, head).astype(jnp.bfloat16)
    value_round = value_own.reshape(block, kv_width).astype(jnp.bfloat16)
    unit1, inverse1 = norm_stats(full)
    normed1 = (unit1 * gain_attn.astype(jnp.float32)).astype(jnp.bfloat16)
    grad_wq = matmul(normed1.T, query_round)
    grad_wk = matmul(normed1.T, key_round)
    grad_wv = matmul(normed1.T, value_round)
    normed1_grad = matmul(query_round, wq.T) + matmul(key_round, wk.T) + matmul(value_round, wv.T)
    first_terms, gain_attn_terms = norm_back(
        normed1_grad, unit1, inverse1, gain_attn.astype(jnp.float32)
    )
    first_part, gain_attn_part = (
        lax.psum_scatter(first_terms, "tensor", scatter_dimension=0, tiled=True),
        lax.psum_scatter(
            gain_attn_terms.reshape(groups, parts, piece_width),
            "tensor",
            scatter_dimension=1,
            tiled=True,
        ),
    )
    input_grad = second_grad + first_part
    return (
        input_grad,
        (
            grad_wq,
            grad_wk,
            grad_wv,
            grad_wo,
            grad_gate,
            grad_up,
            grad_down,
            gain_attn_part,
            gain_mlp_part,
        ),
    )


def reduce_grads(pieces):
    return (
        lax.psum_scatter(
            pieces[0].astype(jnp.bfloat16), "dp", scatter_dimension=0, tiled=True
        ).astype(jnp.float32),
        lax.psum_scatter(
            pieces[1].astype(jnp.bfloat16), "dp", scatter_dimension=0, tiled=True
        ).astype(jnp.float32),
        lax.psum_scatter(
            pieces[2].astype(jnp.bfloat16), "dp", scatter_dimension=0, tiled=True
        ).astype(jnp.float32),
        lax.psum_scatter(
            pieces[3].astype(jnp.bfloat16), "dp", scatter_dimension=1, tiled=True
        ).astype(jnp.float32),
        lax.psum_scatter(
            pieces[4].astype(jnp.bfloat16), "dp", scatter_dimension=0, tiled=True
        ).astype(jnp.float32),
        lax.psum_scatter(
            pieces[5].astype(jnp.bfloat16), "dp", scatter_dimension=0, tiled=True
        ).astype(jnp.float32),
        lax.psum_scatter(
            pieces[6].astype(jnp.bfloat16), "dp", scatter_dimension=1, tiled=True
        ).astype(jnp.float32),
        lax.psum_scatter(
            pieces[7].astype(jnp.bfloat16), "dp", scatter_dimension=0, tiled=True
        ).astype(jnp.float32),
        lax.psum_scatter(
            pieces[8].astype(jnp.bfloat16), "dp", scatter_dimension=0, tiled=True
        ).astype(jnp.float32),
    )


def general_shards(inputs, table, cotangent, wq, wk, wv, wo, w_gate, w_up, w_down, gain_attn, gain_mlp):
    groups = lax.axis_size("dp")
    parts = lax.axis_size("tensor")
    micro_count = inputs.shape[0]
    section = lax.axis_index("section")
    first_section = section == 0
    weights = (
        lax.all_gather(wq[0], "dp", axis=0, tiled=True),
        lax.all_gather(wk[0], "dp", axis=0, tiled=True),
        lax.all_gather(wv[0], "dp", axis=0, tiled=True),
        lax.all_gather(wo[0], "dp", axis=1, tiled=True),
        lax.all_gather(w_gate[0], "dp", axis=0, tiled=True),
        lax.all_gather(w_up[0], "dp", axis=0, tiled=True),
        lax.all_gather(w_down[0], "dp", axis=1, tiled=True),
        lax.all_gather(gain_attn[0], "dp", axis=0, tiled=True),
        lax.all_gather(gain_mlp[0], "dp", axis=0, tiled=True),
    )
    head = HEAD_SIZE
    heads_kv = wk.shape[2] // head
    received = jnp.zeros_like(inputs[0])
    produced = []
    saved = []
    for step in range(micro_count + 1):
        own_rows = inputs[step] if step < micro_count else jnp.zeros_like(inputs[0])
        start_rows = jnp.where(first_section, own_rows, received)
        micro = jnp.clip(step - section, 0, micro_count - 1)
        result, context = layer_forward(start_rows, table, micro, weights, groups, heads_kv, head)
        produced.append(result)
        saved.append(context)
        if step < micro_count:
            received = passed_along(result, "section", 1)
    stacked = jnp.stack(produced)
    outputs = jnp.where(first_section, stacked[:micro_count], stacked[1:])[None]
    returned = jnp.zeros_like(inputs[0])
    returned_list = []
    totals = None
    for step in range(micro_count + 1):
        index = micro_count - 1 - step
        given = cotangent[index] if index >= 0 else jnp.zeros_like(cotangent[0])
        start_grad = jnp.where(first_section, returned, given)
        din, pieces = layer_backward(
            start_grad, saved[micro_count - step], weights, groups, parts, heads_kv, head
        )
        returned_list.append(din)
        if step < micro_count:
            returned = passed_along(din.astype(jnp.bfloat16), "section", -1).astype(din.dtype)
        totals = (
            pieces
            if totals is None
            else tuple((left + right for left, right in zip(totals, pieces)))
        )
    totals = reduce_grads(totals)
    reverse_stack = jnp.stack(returned_list[::-1])
    input_grad = jnp.where(first_section, reverse_stack[:micro_count], reverse_stack[1:])[None]
    (
        grad_wq,
        grad_wk,
        grad_wv,
        grad_wo,
        grad_gate,
        grad_up,
        grad_down,
        gain_attn_sum,
        gain_mlp_sum,
    ) = totals
    width_piece = gain_attn_sum.shape[-1]
    return (
        outputs,
        input_grad,
        grad_wq[None],
        grad_wk[None],
        grad_wv[None],
        grad_wo[None],
        grad_gate[None],
        grad_up[None],
        grad_down[None],
        gain_attn_sum.reshape(1, width_piece),
        gain_mlp_sum.reshape(1, width_piece),
    )


MESH = pl.DeviceIdType.MESH
SUBS = 2


def taking(us):
    return pl.CostEstimate(flops=0, bytes_accessed=int(us * 3.69e6), transcendentals=0)


def ring_place(index, count):
    return jnp.where(lax.rem(index, 2) == 0, index // 2, count - (index + 1) // 2)


def ring_index(place, count):
    place = lax.rem(place + 2 * count, count)
    return jnp.where(place < count // 2, 2 * place, 2 * count - 1 - 2 * place)


def greet(others):
    barrier = pltpu.get_barrier_semaphore()
    for other in others:
        pl.semaphore_signal(barrier, inc=1, device_id=other, device_id_type=MESH)
    pl.semaphore_wait(barrier, len(others))


def remote(source, target, send, recv, device):
    return pltpu.make_async_remote_copy(
        source, target, send, recv, device_id=device, device_id_type=MESH
    )


def partners(me, count):
    half = count // 2
    side, inside = me // half, lax.rem(me, half)
    peers = [(1 - side) * half + lax.rem(inside + k, half) for k in range(half)]
    peers += [side * half + lax.rem(inside + k, half) for k in range(1, half)]
    origins = [(1 - side) * half + lax.rem(inside + half - k, half) for k in range(half)]
    origins += [side * half + lax.rem(inside + half - k, half) for k in range(1, half)]
    return peers, origins


def aligned(start, size):
    return pl.ds(pl.multiple_of(start, size), size)


class Ring:
    def __init__(self, count):
        self.count = count
        self.far = count // 2
        self.me = lax.axis_index("dp")
        self.core = lax.axis_index("tensor")
        self.place = ring_place(self.me, count)
        self.near = tuple({"dp": ring_index(self.place + step, count)} for step in (1, -1))
        self.side = {"tensor": 1 - self.core}

    def everyone(self):
        return [*self.near, self.side]

    def index(self, steps):
        return ring_index(self.place + steps, self.count)

    def orders(self):
        for k in range(SUBS):
            yield k, 0
            yield SUBS - 1 - k, 1


def gather_scratch(count):
    far = count // 2
    dma = pltpu.SemaphoreType.DMA
    return [dma((2, far, SUBS)), dma((2, far, SUBS)), dma((count, SUBS)), dma((count, SUBS)), dma]


class Gather:
    def __init__(self, ring, x_ref, o_ref, scratch):
        self.ring = ring
        self.x_ref, self.o_ref = x_ref, o_ref
        self.ring_send, self.ring_recv, self.side_send, self.side_recv, self.own_sem = scratch
        self.rows = x_ref.shape[0]
        self.piece = self.rows // SUBS
        self.sends = []

    def spot(self, steps, sub, core):
        start = (self.ring.index(steps) * 2 + core) * self.rows + sub * self.piece
        return self.o_ref.at[aligned(start, self.piece), :]

    def mine(self, steps, sub):
        if steps == 0:
            return self.x_ref.at[sub * self.piece : (sub + 1) * self.piece, :]
        return self.spot(steps, sub, self.ring.core)

    def travels(self, way, hop, sub):
        return hop < self.ring.far or (sub < SUBS // 2) == (way == 0)

    def go(self, copy):
        copy.start()
        self.sends.append(copy)

    def pass_on(self, way, hop, sub):
        steps = 1 - hop if way == 0 else hop - 1
        self.go(
            remote(
                self.mine(steps, sub),
                self.spot(steps, sub, self.ring.core),
                self.ring_send.at[way, hop - 1, sub],
                self.ring_recv.at[way, hop - 1, sub],
                self.ring.near[way],
            )
        )

    def hand_over(self, steps, sub, slot):
        self.go(
            remote(
                self.mine(steps, sub),
                self.spot(steps, sub, self.ring.core),
                self.side_send.at[slot, sub],
                self.side_recv.at[slot, sub],
                self.ring.side,
            )
        )

    def start(self):
        for sub, way in self.ring.orders():
            self.pass_on(way, 1, sub)
        for sub in range(SUBS):
            self.hand_over(0, sub, 0)
        self.own = pltpu.make_async_copy(
            self.x_ref,
            self.o_ref.at[aligned((self.ring.me * 2 + self.ring.core) * self.rows, self.rows), :],
            self.own_sem,
        )
        self.own.start()

    def hop(self, hop):
        far, count = self.ring.far, self.ring.count
        for sub, way in self.ring.orders():
            if not self.travels(way, hop, sub):
                continue
            steps = -hop if way == 0 else hop
            here = self.spot(steps, sub, self.ring.core)
            remote(
                here, here, self.ring_send.at[way, hop - 1, sub],
                self.ring_recv.at[way, hop - 1, sub], self.ring.near[way],
            ).wait_recv()
            if hop < far and self.travels(way, hop + 1, sub):
                self.pass_on(way, hop + 1, sub)
            self.hand_over(steps, sub, hop if way == 0 or hop == far else count - hop)

    def finish(self):
        for copy in self.sends:
            copy.wait_send()
        for slot in range(self.ring.count):
            steps = -slot if slot <= self.ring.far else self.ring.count - slot
            for sub in range(SUBS):
                there = self.spot(steps, sub, 1 - self.ring.core)
                remote(
                    there, there, self.side_send.at[slot, sub], self.side_recv.at[slot, sub],
                    self.ring.side,
                ).wait_recv()
        self.own.wait()


def gather_kernel(count, x_ref, o_ref, *scratch):
    ring = Ring(count)
    greet(ring.everyone())
    gather = Gather(ring, x_ref, o_ref, scratch)
    gather.start()
    for hop in range(1, ring.far + 1):
        gather.hop(hop)
    gather.finish()


def gather_rows(x, count, cid):
    rows, width = x.shape
    return pl.pallas_call(
        functools.partial(gather_kernel, count),
        out_shape=jax.ShapeDtypeStruct((count * 2 * rows, width), x.dtype),
        in_specs=[pl.BlockSpec(memory_space=pltpu.VMEM)],
        out_specs=pl.BlockSpec(memory_space=pltpu.VMEM),
        scratch_shapes=gather_scratch(count),
        compiler_params=pltpu.CompilerParams(collective_id=cid, has_side_effects=True),
        cost_estimate=taking(27),
        name="gather_rows",
    )(x)


def reduce_kernel(count, p_ref, o_ref, side_buf, send_buf, recv_buf, ring_send, ring_recv, side_send, side_recv):
    rows, width = o_ref.shape
    piece = rows // SUBS
    ring = Ring(count)
    far, core = ring.far, ring.core
    greet(ring.everyone())
    steps = [far]
    for k in range(far - 1, 0, -1):
        steps += [k, -k]
    steps += [0]
    sends = []

    def part(step_to, of_core):
        return pl.multiple_of((ring.index(step_to) * 2 + of_core) * rows, rows)

    side_copies = {}
    for slot, step_to in enumerate(steps):
        copy = remote(
            p_ref.at[pl.ds(part(step_to, 1 - core), rows), :], side_buf.at[slot],
            side_send.at[slot], side_recv.at[slot], ring.side,
        )
        copy.start()
        side_copies[step_to] = (slot, copy)

    def span(sub):
        return slice(sub * piece, (sub + 1) * piece)

    def mine(step_to, sub):
        slot, _ = side_copies[step_to]
        start = pl.multiple_of(part(step_to, core) + sub * piece, piece)
        return p_ref[pl.ds(start, piece), :].astype(jnp.float32) + side_buf[
            slot, span(sub), :
        ].astype(jnp.float32)

    def travels(way, step, sub):
        return step > 1 or (sub < SUBS // 2) == (way == 0)

    def ring_copy(way, step, sub):
        return remote(
            send_buf.at[way, step - 1, span(sub), :], recv_buf.at[way, step - 1, span(sub), :],
            ring_send.at[way, step - 1, sub], ring_recv.at[way, step - 1, sub], ring.near[way],
        )

    seen = set()
    for step in range(1, far + 1):
        for sub, way in ring.orders():
            if not travels(way, step, sub):
                continue
            step_to = far + 1 - step
            step_to = step_to if way == 0 or step_to == far else -step_to
            if step_to not in seen:
                side_copies[step_to][1].wait_recv()
                seen.add(step_to)
            value = mine(step_to, sub)
            if step > 1 and travels(way, step - 1, sub):
                ring_copy(way, step - 1, sub).wait_recv()
                value = value + recv_buf[way, step - 2, span(sub), :].astype(jnp.float32)
            send_buf[way, step - 1, span(sub), :] = value.astype(send_buf.dtype)
            copy = ring_copy(way, step, sub)
            copy.start()
            sends.append(copy)
    side_copies[0][1].wait_recv()
    for sub in range(SUBS):
        value = mine(0, sub)
        for way in range(2):
            ring_copy(way, far, sub).wait_recv()
            value = value + recv_buf[way, far - 1, span(sub), :].astype(jnp.float32)
        o_ref[span(sub), :] = value.astype(o_ref.dtype)
    for copy in sends:
        copy.wait_send()
    for _, copy in side_copies.values():
        copy.wait_send()


def reduce_rows(p, count, cid, dtype=jnp.float32):
    total, width = p.shape
    rows = total // (2 * count)
    far = count // 2
    dma = pltpu.SemaphoreType.DMA
    return pl.pallas_call(
        functools.partial(reduce_kernel, count),
        out_shape=jax.ShapeDtypeStruct((rows, width), dtype),
        in_specs=[pl.BlockSpec(memory_space=pltpu.VMEM)],
        out_specs=pl.BlockSpec(memory_space=pltpu.VMEM),
        scratch_shapes=[
            pltpu.VMEM((count, rows, width), p.dtype),
            pltpu.VMEM((2, far, rows, width), p.dtype),
            pltpu.VMEM((2, far, rows, width), p.dtype),
            dma((2, far, SUBS)), dma((2, far, SUBS)), dma((count,)), dma((count,)),
        ],
        compiler_params=pltpu.CompilerParams(collective_id=cid, has_side_effects=True),
        cost_estimate=taking(29),
        name="reduce_rows",
    )(p)


def weight_pieces(source, target, count, heads, srcs, dsts, layer):
    qkv, wo, gate, up, down = srcs
    out_qkv, out_wo, out_gu, out_down = dsts
    depth = gate.shape[0]
    hidden = gate.shape[1] // count
    q_rows = wo.shape[0] // count
    kv_rows = (qkv.shape[0] - wo.shape[0]) // 2
    shared = count * heads // kv_rows
    cols = aligned(source * depth, depth)
    k_from = pl.multiple_of(wo.shape[0] + target // shared * heads, heads)
    v_from = pl.multiple_of(wo.shape[0] + kv_rows + target // shared * heads, heads)
    mine = aligned(target * hidden, hidden)
    return (
        (qkv.at[aligned(target * q_rows, q_rows), :], out_qkv.at[layer, pl.ds(0, q_rows), cols]),
        (qkv.at[pl.ds(k_from, heads), :], out_qkv.at[layer, pl.ds(q_rows, heads), cols]),
        (qkv.at[pl.ds(v_from, heads), :], out_qkv.at[layer, pl.ds(q_rows + heads, heads), cols]),
        (wo.at[aligned(target * q_rows, q_rows), :], out_wo.at[layer, :, cols]),
        (gate.at[:, mine], out_gu.at[layer, cols, pl.ds(0, hidden)]),
        (up.at[:, mine], out_gu.at[layer, cols, pl.ds(hidden, hidden)]),
        (down.at[mine, :], out_down.at[layer, :, cols]),
    )


KINDS = 7


def spread_kernel(count, heads, *refs):
    srcs, gain_in, unit_ref, grad_ref = refs[:5], refs[5], refs[6], refs[7]
    dsts, all_gains, gathered = refs[8:12], refs[12], refs[13:15]
    normed, gain_send, gain_recv, gain_own = refs[15:19]
    send, recv, cross_send, cross_recv, own_sem = refs[19:24]
    ring = Ring(count)
    me = ring.me
    layer = lax.axis_index("section")
    peers, origins = partners(me, count)
    across = {"section": 1 - layer}
    holders = [{"dp": peer} for peer in peers] + [
        {"section": 1 - layer, "dp": peer} for peer in [*peers, me]
    ]
    greet([*holders, ring.side])
    gathers = [
        Gather(ring, source, gathered[k], refs[24 + 5 * k : 29 + 5 * k])
        for k, source in enumerate((normed, grad_ref))
    ]
    started = []
    local = []

    def go(copy):
        copy.start()
        started.append(copy)

    def gain_spot(at, source):
        depth = gain_in.shape[1]
        return all_gains.at[at, :, aligned(source * depth, depth)]

    def send_kind(kind):
        for k, peer in enumerate(peers):
            source, target = weight_pieces(me, peer, count, heads, srcs, dsts, layer)[kind]
            go(remote(source, target, send.at[kind, k], recv.at[kind, k], {"dp": peer}))

    def own_kind(kind):
        source, target = weight_pieces(me, me, count, heads, srcs, dsts, layer)[kind]
        go(remote(source, target, cross_send.at[kind, count - 1], cross_recv.at[kind, count - 1], across))
        copy = pltpu.make_async_copy(source, target, own_sem.at[kind])
        copy.start()
        local.append(copy)

    def forward(kind, k):
        here = weight_pieces(origins[k], me, count, heads, srcs, dsts, layer)[kind][1]
        remote(here, here, send.at[kind, k], recv.at[kind, k], {"dp": origins[k]}).wait_recv()
        go(remote(here, here, cross_send.at[kind, k], cross_recv.at[kind, k], across))

    sizes = [math.prod(there.shape) for _, there in weight_pieces(me, me, count, heads, srcs, dsts, layer)]
    arrivals = []
    for kind in range(KINDS):
        for k in range(count - 1):
            part = (k + 1) / (count // 2) if k < count // 2 else 1.0
            due = sum(sizes[:kind]) + part * sizes[kind]
            arrivals.append((due if k < count // 2 else due * 0.5, kind, k))
    arrivals.sort()

    for k, holder in enumerate(holders):
        go(remote(gain_in, gain_spot(layer, me), gain_send.at[k], gain_recv.at[k], holder))
    own_gains = pltpu.make_async_copy(gain_in, gain_spot(layer, me), gain_own)
    own_gains.start()
    gathers[1].start()
    for kind in range(KINDS):
        own_kind(kind)
    own_gains.wait()
    for k, holder in enumerate(holders):
        at, source = (layer, k) if k < count - 1 else (1 - layer, k - count + 1)
        spot = gain_spot(at, origins[source] if source < count - 1 else me)
        remote(spot, spot, gain_send.at[k], gain_recv.at[k], holder).wait_recv()
    normed[...] = (unit_ref[...] * all_gains[0, 0:1, :]).astype(normed.dtype)
    gathers[0].start()
    batches = [range(KINDS - 3), [KINDS - 3], [KINDS - 2, KINDS - 1]]
    for hop in range(1, ring.far + 1):
        gathers[1].hop(hop)
        gathers[0].hop(hop)
        if hop > ring.far - len(batches):
            for kind in batches[hop - 1 - ring.far + len(batches)]:
                send_kind(kind)
    for _, kind, k in arrivals:
        forward(kind, k)
    for gather in gathers:
        gather.finish()
    for copy in local:
        copy.wait()
    for copy in started:
        copy.wait_send()
    for kind in range(KINDS):
        for k in range(count):
            origin = origins[k] if k < count - 1 else me
            there = weight_pieces(origin, me, count, heads, srcs, dsts, 1 - layer)[kind][1]
            remote(there, there, cross_send.at[kind, k], cross_recv.at[kind, k], across).wait_recv()


def spread_weights(qkv, wo, gate, up, down, gains, unit, grads, count, heads, cid):
    depth = gate.shape[0]
    width = depth * count
    hidden = gate.shape[1] // count
    q_rows = wo.shape[0] // count
    shape = lambda *dims: jax.ShapeDtypeStruct((2, *dims), jnp.bfloat16)
    hbm = pl.BlockSpec(memory_space=pl.ANY)
    vmem = pl.BlockSpec(memory_space=pltpu.VMEM)
    dma = pltpu.SemaphoreType.DMA
    gathered = jax.ShapeDtypeStruct((count * 2 * grads.shape[0], width), grads.dtype)
    return pl.pallas_call(
        functools.partial(spread_kernel, count, heads),
        out_shape=(
            shape(q_rows + 2 * heads, width),
            shape(q_rows, width),
            shape(width, 2 * hidden),
            shape(hidden, width),
            jax.ShapeDtypeStruct((2, gains.shape[0], width), gains.dtype),
            gathered,
            gathered,
        ),
        in_specs=[hbm] * 5 + [vmem] * 3,
        out_specs=(hbm,) * 4 + (vmem,) * 3,
        scratch_shapes=[
            pltpu.VMEM(grads.shape, grads.dtype),
            dma((2 * count - 1,)), dma((2 * count - 1,)), dma,
            dma((KINDS, count - 1)), dma((KINDS, count - 1)),
            dma((KINDS, count)), dma((KINDS, count)), dma((KINDS,)),
            *gather_scratch(count), *gather_scratch(count),
        ],
        compiler_params=pltpu.CompilerParams(collective_id=cid, has_side_effects=True),
        cost_estimate=taking(220),
        name="spread_weights",
    )(qkv, wo, gate, up, down, gains, unit, grads)


def gradient_pieces(target, count, refs):
    down, gate, up, wo, qkv = refs
    depth = down.shape[1] // count
    cols = aligned(target * depth, depth)
    return (
        down.at[:, cols],
        gate.at[cols, :],
        up.at[cols, :],
        wo.at[:, cols],
        qkv.at[cols, :],
    )


def owned_pieces(source, refs, sizes):
    down, gate, up, wo, qkv = refs
    return (
        down.at[aligned(source * sizes[0][0], sizes[0][0]), :],
        gate.at[:, aligned(source * sizes[1][1], sizes[1][1])],
        up.at[:, aligned(source * sizes[2][1], sizes[2][1])],
        wo.at[aligned(source * sizes[3][0], sizes[3][0]), :],
        qkv.at[source],
    )


GRADS = 5


def return_kernel(count, *refs):
    partial = (refs[:5], refs[5:10])
    gain_in = refs[10]
    outs, gain_out = refs[11:16], refs[16]
    landed, mine = refs[17:22], refs[22:27]
    gain_landed, cross_send, cross_recv, load_sem, send, recv, own_sem, gain_send, gain_recv = refs[27:]
    ring = Ring(count)
    me, core = ring.me, ring.core
    layer = lax.axis_index("section")
    across = {"section": 1 - layer}
    sizes = [ref.shape[1:] for ref in mine]
    everyone = 4 * count
    this = (layer * count + me) * 2 + core

    def device(k):
        other = lax.rem(this + k, everyone)
        return {
            "section": other // (2 * count),
            "dp": lax.rem(other // 2, count),
            "tensor": lax.rem(other, 2),
        }

    greet([device(k) for k in range(1, everyone)])
    gain_copies = []
    for k in range(1, everyone):
        copy = remote(
            gain_in.at[lax.rem(this + k, everyone)], gain_landed.at[k - 1],
            gain_send.at[k - 1], gain_recv.at[k - 1], device(k),
        )
        copy.start()
        gain_copies.append(copy)
    peers, origins = partners(me, count)
    order = [*peers, me]
    crossing, loads, sends = {}, {}, []
    for kind in range(GRADS):
        for k, owner in enumerate(order):
            pieces = [gradient_pieces(owner, count, partial[at])[kind] for at in range(2)]
            for at in range(2):
                copy = remote(
                    pieces[1 - at], landed[kind].at[k],
                    cross_send.at[kind, k], cross_recv.at[kind, k], across,
                )
                load = pltpu.make_async_copy(pieces[at], mine[kind].at[k], load_sem.at[kind, k])

                @pl.when(layer == at)
                def _():
                    copy.start()
                    load.start()

            crossing[kind, k], loads[kind, k] = copy, load
    for kind in range(GRADS):
        for k, owner in enumerate(order):
            loads[kind, k].wait()
            crossing[kind, k].wait_recv()
            total = mine[kind][k].astype(jnp.float32) + landed[kind][k].astype(jnp.float32)
            mine[kind][k] = total.astype(jnp.bfloat16)
            target = owned_pieces(me, outs, sizes)[kind]
            if k < count - 1:
                copy = remote(
                    mine[kind].at[k], target, send.at[kind, k], recv.at[kind, k], {"dp": owner}
                )
            else:
                copy = pltpu.make_async_copy(mine[kind].at[k], target, own_sem.at[kind])
            copy.start()
            sends.append((k, copy))
    total = gain_in[this]
    for k, copy in enumerate(gain_copies):
        copy.wait_recv()
        total = total + gain_landed[k]
    gain_out[...] = total
    for copy in gain_copies:
        copy.wait_send()
    for copy in crossing.values():
        copy.wait_send()
    for k, copy in sends:
        if k < count - 1:
            copy.wait_send()
        else:
            copy.wait()
    for kind in range(GRADS):
        for k in range(count - 1):
            here = owned_pieces(origins[k], outs, sizes)[kind]
            remote(
                mine[kind].at[k], here, send.at[kind, k], recv.at[kind, k], {"dp": origins[k]}
            ).wait_recv()


def return_gradients(layer0, layer1, gains, count, cid):
    hidden, width = layer0[0].shape
    depth = width // count
    q_rows = layer0[3].shape[0]
    qkv_rows = layer0[4].shape[1]
    hbm = pl.BlockSpec(memory_space=pl.ANY)
    vmem = pl.BlockSpec(memory_space=pltpu.VMEM)
    dma = pltpu.SemaphoreType.DMA
    shape = lambda *dims: jax.ShapeDtypeStruct(dims, jnp.bfloat16)
    sizes = [(hidden, depth), (depth, hidden), (depth, hidden), (q_rows, depth), (depth, qkv_rows)]
    everyone, gain_rows, lanes = gains.shape
    return pl.pallas_call(
        functools.partial(return_kernel, count),
        out_shape=(
            shape(count * hidden, depth),
            shape(depth, count * hidden),
            shape(depth, count * hidden),
            shape(count * q_rows, depth),
            shape(count, depth, qkv_rows),
            jax.ShapeDtypeStruct((gain_rows, lanes), gains.dtype),
        ),
        in_specs=[hbm] * 10 + [vmem],
        out_specs=(hbm,) * 5 + (vmem,),
        scratch_shapes=[
            *(pltpu.VMEM((count, *size), jnp.bfloat16) for size in sizes),
            *(pltpu.VMEM((count, *size), jnp.bfloat16) for size in sizes),
            pltpu.VMEM((everyone - 1, gain_rows, lanes), gains.dtype),
            dma((GRADS, count)), dma((GRADS, count)), dma((GRADS, count)),
            dma((GRADS, count - 1)), dma((GRADS, count - 1)), dma((GRADS,)),
            dma((everyone - 1,)), dma((everyone - 1,)),
        ],
        compiler_params=pltpu.CompilerParams(collective_id=cid, has_side_effects=True),
        cost_estimate=taking(200),
        name="return_gradients",
    )(*layer0, *layer1, gains)


def swap_halves(rows, head):
    width = rows.shape[1]
    lane = lax.broadcasted_iota(jnp.int32, rows.shape, 1)
    half = head // 2
    return jnp.where(
        lax.rem(lane, head) < half, pltpu.roll(rows, width - half, 1), pltpu.roll(rows, half, 1)
    )


def low_lanes(shape, head):
    return lax.broadcasted_iota(jnp.int32, shape, 1) < head


def dot(left, right, contract):
    return lax.dot_general(
        left, right, (contract, ((), ())), preferred_element_type=jnp.float32
    )


def two_heads(rows, head):
    low = low_lanes(rows.shape, head)
    zero = jnp.zeros_like(rows)
    return jnp.concatenate([jnp.where(low, rows, zero), jnp.where(low, zero, rows)], axis=0)


def one_row(rows, head):
    half = rows.shape[0] // 2
    return jnp.where(low_lanes((half, rows.shape[1]), head), rows[:half], rows[half:])


def triangle(block, keys):
    row = lax.rem(lax.broadcasted_iota(jnp.int32, (2 * block, keys), 0), block)
    column = lax.broadcasted_iota(jnp.int32, (2 * block, keys), 1)
    return column <= row + (keys - block)


def attend_kernel(groups, head, slots, qkv_ref, cos_ref, sin_ref, mixed_ref, kept_ref, lse_ref, key2, value2):
    tokens = qkv_ref.shape[0]
    block = tokens // groups
    span = groups // 2
    wide = 2 * head
    scale = 1.0 / math.sqrt(head)
    for spot in range(groups):
        rows = pl.ds(pl.multiple_of(slots[spot] * block, block), block)
        cosine = cos_ref[rows, :]
        sine = sin_ref[rows, :]
        query = qkv_ref[rows, :wide]
        query = (query * cosine + swap_halves(query, head) * sine).astype(jnp.bfloat16)
        pair = qkv_ref[rows, wide:]
        low = low_lanes(pair.shape, head)
        pair = jnp.where(low, pair * cosine + swap_halves(pair, head) * sine, pair)
        turned = pltpu.roll(pair, head, 1)
        kept_ref[rows, :wide] = query
        kept_ref[rows, wide:] = pair.astype(jnp.bfloat16)
        here = slice(spot * block, (spot + 1) * block)
        key2[here, :] = jnp.where(low, pair, turned).astype(jnp.bfloat16)
        value2[here, :] = jnp.where(low, turned, pair).astype(jnp.bfloat16)
    for spot in range(groups):
        first = spot // span * span * block
        keys = (spot % span + 1) * block
        rows = pl.ds(pl.multiple_of(slots[spot] * block, block), block)
        query = two_heads(kept_ref[rows, :wide], head)
        score = dot(query, key2[first : first + keys, :], ((1,), (1,))) * scale
        power = jnp.where(triangle(block, keys), jnp.exp(score), 0.0)
        total = jnp.sum(power, axis=1, keepdims=True)
        lse = jnp.log(total)
        probs = jnp.where(triangle(block, keys), jnp.exp(score - lse), 0.0).astype(jnp.bfloat16)
        mixed = dot(probs, value2[first : first + keys, :], ((1,), (0,)))
        mixed_ref[rows, :] = one_row(mixed, head).astype(jnp.bfloat16)
        lse_ref[spot] = lse


def attend_blocks(slots, qkv, cosine, sine, groups, head):
    tokens = qkv.shape[0]
    block = tokens // groups
    vmem = pl.BlockSpec(memory_space=pltpu.VMEM)
    return pl.pallas_call(
        functools.partial(attend_kernel, groups, head),
        out_shape=(
            jax.ShapeDtypeStruct((tokens, 2 * head), jnp.bfloat16),
            jax.ShapeDtypeStruct((tokens, 4 * head), jnp.bfloat16),
            jax.ShapeDtypeStruct((groups, 2 * block, 1), jnp.float32),
        ),
        in_specs=[pl.BlockSpec(memory_space=pltpu.SMEM), vmem, vmem, vmem],
        out_specs=(vmem, vmem, vmem),
        scratch_shapes=[
            pltpu.VMEM((tokens, 2 * head), jnp.bfloat16),
            pltpu.VMEM((tokens, 2 * head), jnp.bfloat16),
        ],
        cost_estimate=taking(6),
        name="attend_blocks",
    )(slots, qkv, cosine, sine)


def attend_back_kernel(
    groups, head, slots, grad_ref, kept_ref, lse_ref, cos_ref, sin_ref, out_ref, key2, value2, key_sum, value_sum
):
    tokens = kept_ref.shape[0]
    block = tokens // groups
    span = groups // 2
    wide = 2 * head
    scale = 1.0 / math.sqrt(head)
    for spot in range(groups):
        rows = pl.ds(pl.multiple_of(slots[spot] * block, block), block)
        pair = kept_ref[rows, wide:].astype(jnp.float32)
        low = low_lanes(pair.shape, head)
        turned = pltpu.roll(pair, head, 1)
        here = slice(spot * block, (spot + 1) * block)
        key2[here, :] = jnp.where(low, pair, turned).astype(jnp.bfloat16)
        value2[here, :] = jnp.where(low, turned, pair).astype(jnp.bfloat16)
    for spot in range(groups - 1, -1, -1):
        place = spot % span
        first = spot // span * span * block
        keys = (place + 1) * block
        rows = pl.ds(pl.multiple_of(slots[spot] * block, block), block)
        query = two_heads(kept_ref[rows, :wide], head)
        grad = two_heads(grad_ref[rows, :], head)
        key = key2[first : first + keys, :]
        value = value2[first : first + keys, :]
        score = dot(query, key, ((1,), (1,))) * scale
        probs = jnp.where(triangle(block, keys), jnp.exp(score - lse_ref[spot]), 0.0)
        prob_grad = dot(grad, value, ((1,), (1,)))
        rowdot = jnp.sum(probs * prob_grad, axis=1, keepdims=True)
        score_grad = (probs * (prob_grad - rowdot) * scale).astype(jnp.bfloat16)
        value_part = dot(probs.astype(jnp.bfloat16), grad, ((0,), (0,)))
        key_part = dot(score_grad, query, ((0,), (0,)))
        if place == span - 1:
            value_sum[first : first + keys, :] = value_part
            key_sum[first : first + keys, :] = key_part
        else:
            value_sum[first : first + keys, :] += value_part
            key_sum[first : first + keys, :] += key_part
        query_grad = one_row(dot(score_grad, key, ((1,), (0,))), head)
        query_grad = query_grad * cos_ref[rows, :] - swap_halves(query_grad, head) * sin_ref[rows, :]
        out_ref[rows, :wide] = query_grad.astype(jnp.bfloat16)
    for spot in range(groups):
        rows = pl.ds(pl.multiple_of(slots[spot] * block, block), block)
        here = slice(spot * block, (spot + 1) * block)
        key = key_sum[here, :]
        key = key + pltpu.roll(key, head, 1)
        key = key * cos_ref[rows, :] - swap_halves(key, head) * sin_ref[rows, :]
        value = value_sum[here, :]
        value = value + pltpu.roll(value, head, 1)
        low = low_lanes(key.shape, head)
        out_ref[rows, wide:] = jnp.where(low, key, value).astype(jnp.bfloat16)


def attend_blocks_back(slots, grad, kept, lse, cosine, sine, groups, head):
    tokens = kept.shape[0]
    vmem = pl.BlockSpec(memory_space=pltpu.VMEM)
    return pl.pallas_call(
        functools.partial(attend_back_kernel, groups, head),
        out_shape=jax.ShapeDtypeStruct((tokens, 4 * head), jnp.bfloat16),
        in_specs=[pl.BlockSpec(memory_space=pltpu.SMEM)] + [vmem] * 5,
        out_specs=vmem,
        scratch_shapes=[
            pltpu.VMEM((tokens, 2 * head), jnp.bfloat16),
            pltpu.VMEM((tokens, 2 * head), jnp.bfloat16),
            pltpu.VMEM((tokens, 2 * head), jnp.float32),
            pltpu.VMEM((tokens, 2 * head), jnp.float32),
        ],
        cost_estimate=taking(8),
        name="attend_blocks_back",
    )(slots, grad, kept, lse, cosine, sine)


def rope_tables(table_row, block, head):
    groups = table_row.shape[0]
    place = table_row % (groups // 2)
    positions = (place[:, None] * block + jnp.arange(block, dtype=jnp.int32)).reshape(-1)
    angle = positions.astype(jnp.float32)[:, None] * rope_frequencies(head)[None, :]
    cosine = jnp.cos(angle)
    sine = jnp.sin(angle)
    return (
        jnp.concatenate([cosine] * 4, axis=1),
        jnp.concatenate([-sine, sine] * 2, axis=1),
    )


def matmul_nt(left, right):
    return dot(left, right, ((1,), (1,)))


def matmul_tn(left, right):
    return dot(left, right, ((0,), (0,)))


def section_swap(value):
    return lax.ppermute(value, "section", [(0, 1), (1, 0)])


def fast_forward(rows, normed1, weights, tools):
    qkv_w, wo_w, gu_w, down_w, gain_attn, gain_mlp = weights
    count, slots, cosine, sine, head = tools
    unit1, inverse1 = norm_stats(rows)
    if normed1 is None:
        normed1 = gather_rows((unit1 * gain_attn).astype(jnp.bfloat16), count, 1)
    qkv = matmul_nt(normed1, qkv_w)
    mixed, kept, lse = attend_blocks(slots, qkv, cosine, sine, count, head)
    second = rows + reduce_rows(matmul(mixed, wo_w).astype(jnp.bfloat16), count, 2)
    unit2, inverse2 = norm_stats(second)
    normed2 = gather_rows((unit2 * gain_mlp).astype(jnp.bfloat16), count, 1)
    gate_up = matmul(normed2, gu_w)
    gate, upper = jnp.split(gate_up, 2, axis=1)
    hidden = (jax.nn.silu(gate) * upper).astype(jnp.bfloat16)
    result = second + reduce_rows(matmul(hidden, down_w).astype(jnp.bfloat16), count, 2)
    return result, (unit1, inverse1, normed1, kept, lse, mixed, unit2, inverse2, normed2, gate_up, hidden)


def fast_backward(grad_rows, out_grad, context, weights, tools):
    qkv_w, wo_w, gu_w, down_w, gain_attn, gain_mlp = weights
    count, slots, cosine, sine, head = tools
    unit1, inverse1, normed1, kept, lse, mixed, unit2, inverse2, normed2, gate_up, hidden = context
    gate, upper = jnp.split(gate_up, 2, axis=1)
    if out_grad is None:
        out_grad = gather_rows(grad_rows.astype(jnp.bfloat16), count, 1)
    hidden_grad = matmul_nt(out_grad, down_w)
    grad_down = matmul_tn(hidden, out_grad).astype(jnp.bfloat16)
    sigma = jax.nn.sigmoid(gate)
    gate_grad = (hidden_grad * upper * sigma * (1.0 + gate * (1.0 - sigma))).astype(jnp.bfloat16)
    up_grad = (hidden_grad * gate * sigma).astype(jnp.bfloat16)
    gu_grad = jnp.concatenate([gate_grad, up_grad], axis=1)
    grad_gate = matmul_tn(normed2, gate_grad).astype(jnp.bfloat16)
    grad_up = matmul_tn(normed2, up_grad).astype(jnp.bfloat16)
    normed2_grad = reduce_rows(matmul_nt(gu_grad, gu_w).astype(jnp.bfloat16), count, 2)
    second_part, gain_mlp_part = norm_back(normed2_grad, unit2, inverse2, gain_mlp)
    second_grad = grad_rows + second_part
    attn_grad = gather_rows(second_grad.astype(jnp.bfloat16), count, 1)
    grad_wo = matmul_tn(mixed, attn_grad).astype(jnp.bfloat16)
    mixed_grad = matmul_nt(attn_grad, wo_w).astype(jnp.bfloat16)
    qkv_grad = attend_blocks_back(slots, mixed_grad, kept, lse, cosine, sine, count, head)
    grad_qkv = matmul_tn(normed1, qkv_grad).astype(jnp.bfloat16)
    normed1_grad = reduce_rows(matmul(qkv_grad, qkv_w).astype(jnp.bfloat16), count, 2)
    first_part, gain_attn_part = norm_back(normed1_grad, unit1, inverse1, gain_attn)
    return (
        second_grad + first_part,
        (grad_down, grad_gate, grad_up, grad_wo, grad_qkv),
        (gain_attn_part, gain_mlp_part),
    )


def fast_shards(inputs, table, cotangent, wq, wk, wv, wo, w_gate, w_up, w_down, gain_attn, gain_mlp):
    count = lax.axis_size("dp")
    parts = lax.axis_size("tensor")
    head = HEAD_SIZE
    section = lax.axis_index("section")
    first_section = section == 0
    block = inputs.shape[1] * parts
    depth = wq.shape[1]
    q_cols = wq.shape[2] // count

    rows = lax.dynamic_index_in_dim(inputs, section, 0, keepdims=False)
    given = lax.dynamic_index_in_dim(cotangent, section, 0, keepdims=False)
    table_row = lax.dynamic_index_in_dim(table, section, 0, keepdims=False)
    slot_ids = jnp.arange(count, dtype=jnp.int32)
    slots = jnp.sum(jnp.where(table_row[None, :] == slot_ids[:, None], slot_ids[None, :], 0), axis=1)
    cosine, sine = rope_tables(table_row, block, head)
    tools = (count, slots, cosine, sine, head)

    qkv_t = jnp.concatenate([wq[0], wk[0], wv[0]], axis=1).T
    gains = jnp.concatenate([gain_attn, gain_mlp], axis=0).astype(jnp.float32)
    gains = jnp.concatenate([gains] * 4, axis=0)
    unit1, _ = norm_stats(rows)
    qkv_w, wo_w, gu_w, down_w, all_gains, normed1, out_grad = spread_weights(
        qkv_t, wo[0], w_gate[0], w_up[0], w_down[0], gains,
        unit1, given.astype(jnp.bfloat16), count, head, 0,
    )
    weights = [
        (qkv_w[at], wo_w[at], gu_w[at], down_w[at], all_gains[at, 0], all_gains[at, 1])
        for at in range(2)
    ]

    result0, context0 = fast_forward(rows, normed1, weights[0], tools)
    result1, context1 = fast_forward(result0, None, weights[1], tools)
    din1, grads1, gains1 = fast_backward(given, out_grad, context1, weights[1], tools)
    din0, grads0, gains0 = fast_backward(din1, None, context0, weights[0], tools)

    def both(at0, at1):
        other = section_swap(jnp.where(first_section, at1, at0))
        return jnp.where(
            first_section, jnp.stack([at0, other]), jnp.stack([other, at1])
        )[None]

    outputs = both(result0, result1)
    input_grad = both(din0, din1)

    gain_rows = jnp.stack(gains0 + gains1).reshape(2, 2, count * parts, -1).transpose(0, 2, 1, 3)
    gain_rows = jnp.concatenate([gain_rows.reshape(2 * count * parts, 2, -1)] * 4, axis=1)
    grad_down, grad_gate, grad_up, grad_wo, qkv_own, gain_sums = return_gradients(
        grads0, grads1, gain_rows, count, 3
    )
    grad_wq = qkv_own[:, :, :q_cols].astype(jnp.float32).transpose(1, 0, 2).reshape(depth, -1)
    shared = count * head // wk.shape[2]
    joined = qkv_own[:, :, q_cols:].astype(jnp.float32).reshape(count // shared, shared, depth, 2, head)
    joined = jnp.sum(joined, axis=1)
    grad_wk = joined[:, :, 0].transpose(1, 0, 2).reshape(depth, -1)
    grad_wv = joined[:, :, 1].transpose(1, 0, 2).reshape(depth, -1)
    wide = lambda value: value.astype(jnp.float32)[None]
    return (
        outputs,
        input_grad,
        grad_wq[None],
        grad_wk[None],
        grad_wv[None],
        wide(grad_wo),
        wide(grad_gate),
        wide(grad_up),
        wide(grad_down),
        gain_sums[:1],
        gain_sums[1:2],
    )


def fits(mesh, inputs, table, cotangent, wq, wk, wv, wo, w_gate, w_up, w_down, gain_attn, gain_mlp):
    sections, count, parts = (mesh.shape[axis] for axis in ("section", "dp", "tensor"))
    head = HEAD_SIZE
    if sections != 2 or parts != 2 or inputs.shape[0] != sections or count % 4:
        return False
    devices = count * parts
    queries, keys = wq.shape[2] // head, wk.shape[2] // head
    if queries != 2 * devices or devices % keys or keys % parts or 4 * head != 256:
        return False
    return (
        wq.shape[1] % (128 * count) == 0
        and w_gate.shape[2] % (128 * devices) == 0
        and inputs.shape[1] % (64 * devices) == 0
    )


def shards(mesh, whole, *args):
    if fits(mesh, *whole):
        return fast_shards(*args)
    return general_shards(*args)


def solution(mesh):
    in_specs = (
        P(None, ("dp", "tensor"), None),
        P(),
        P(None, ("dp", "tensor"), None),
        P("section", "dp", "tensor"),
        P("section", "dp", "tensor"),
        P("section", "dp", "tensor"),
        P("section", "tensor", "dp"),
        P("section", "dp", "tensor"),
        P("section", "dp", "tensor"),
        P("section", "tensor", "dp"),
        P("section", "dp"),
        P("section", "dp"),
    )
    out_specs = (
        P("section", None, ("dp", "tensor"), None),
        P("section", None, ("dp", "tensor"), None),
        P("section", "dp", "tensor"),
        P("section", "dp", "tensor"),
        P("section", "dp", "tensor"),
        P("section", "tensor", "dp"),
        P("section", "dp", "tensor"),
        P("section", "dp", "tensor"),
        P("section", "tensor", "dp"),
        P("section", ("dp", "tensor")),
        P("section", ("dp", "tensor")),
    )

    def step(*args):
        return jax.shard_map(
            functools.partial(shards, mesh, args),
            mesh=mesh,
            in_specs=in_specs,
            out_specs=out_specs,
            check_vma=False,
        )(*args)

    return step
```

```python
import functools
import math

import jax
import jax.numpy as jnp
from jax import lax
from jax.experimental import pallas as pl
from jax.experimental.pallas import tpu as pltpu
from jax.sharding import PartitionSpec as P

HEAD_SIZE = 64
SECTION, DP, TENSOR = "section", "dp", "tensor"


epsilon = 1e-05


def passed_along(value, axis, steps):
    count = lax.axis_size(axis)
    initial, last = (max(0, -steps), min(count, count - steps))
    return lax.ppermute(value, axis, [(source, source + steps) for source in range(initial, last)])


def rope_frequencies(head):
    index = jnp.arange(head // 2, dtype=jnp.float32)
    base = 1.0 / 500000.0 ** (index * 2.0 / head)
    wavelength = 2.0 * math.pi / base
    blend = (8192.0 / wavelength - 1.0) / 3.0
    middle = (1.0 - blend) * base / 32.0 + blend * base
    return jnp.where(wavelength < 2048.0, base, jnp.where(wavelength > 8192.0, base / 32.0, middle))


def rotate(values, positions, head):
    step_count = values.shape[0]
    shaped = values.reshape(step_count, -1, head)
    angle = positions.astype(jnp.float32)[:, None] * rope_frequencies(head)[None, :]
    cosine = jnp.cos(angle)[:, None, :]
    sine = jnp.sin(angle)[:, None, :]
    first = shaped[:, :, : head // 2]
    second = shaped[:, :, head // 2 :]
    return jnp.concatenate(
        [first * cosine - second * sine, second * cosine + first * sine], axis=-1
    ).reshape(step_count, -1)


def unrotate(values, positions, head):
    step_count = values.shape[0]
    shaped = values.reshape(step_count, -1, head)
    angle = positions.astype(jnp.float32)[:, None] * rope_frequencies(head)[None, :]
    cosine = jnp.cos(angle)[:, None, :]
    sine = jnp.sin(angle)[:, None, :]
    first = shaped[:, :, : head // 2]
    second = shaped[:, :, head // 2 :]
    return jnp.concatenate(
        [first * cosine + second * sine, second * cosine - first * sine], axis=-1
    ).reshape(step_count, -1)


def norm_stats(rows):
    inverse = lax.rsqrt(jnp.mean(rows * rows, axis=-1, keepdims=True) + epsilon)
    return (rows * inverse, inverse)


def norm_back(grad, unit, inverse, gain):
    scaled = grad * gain
    inner = jnp.mean(scaled * unit, axis=-1, keepdims=True)
    return (inverse * (scaled - unit * inner), jnp.sum(grad * unit, axis=0))


def matmul(left, right):
    return jnp.dot(left, right, preferred_element_type=jnp.float32)


def block_layout(table, micro, groups, block):
    layout_row = lax.dynamic_index_in_dim(table, micro, 0, keepdims=False)
    span = groups // 2
    mine = lax.dynamic_index_in_dim(layout_row, lax.axis_index(DP), 0, keepdims=False)
    sequence = mine // span
    place = mine % span
    slot_ids = jnp.arange(groups, dtype=jnp.int32)
    holder = jnp.sum(
        jnp.where(layout_row[None, :] == slot_ids[:, None], slot_ids[None, :], 0), axis=1
    )
    slots = lax.dynamic_slice_in_dim(holder, sequence * span, span)
    positions = place * block + jnp.arange(block, dtype=jnp.int32)
    return (slots, positions)


def attend(query_rows, key_seq, value_seq, positions, heads_kv, head):
    step_count = query_rows.shape[0]
    keys_total = key_seq.shape[0]
    head_group = query_rows.shape[1] // (heads_kv * head)
    scale = 1.0 / math.sqrt(head)
    allowed = jnp.arange(keys_total, dtype=jnp.int32)[None, :] <= positions[:, None]
    query_layers = query_rows.reshape(step_count, heads_kv, head_group * head).transpose(1, 0, 2)
    key_layers = key_seq.reshape(keys_total, heads_kv, head).transpose(1, 0, 2)
    value_layers = value_seq.reshape(keys_total, heads_kv, head).transpose(1, 0, 2)

    def one_head(parts):
        q_head, k_head, v_head = parts
        q_three = q_head.reshape(step_count, head_group, head)
        scores = (
            jnp.einsum("qgd,kd->gqk", q_three, k_head, preferred_element_type=jnp.float32) * scale
        )
        total = jnp.sum(jnp.where(allowed, jnp.exp(scores), 0.0), axis=-1)
        log_total = jnp.log(total)
        probs = jnp.where(allowed, jnp.exp(scores - log_total[..., None]), 0.0).astype(jnp.bfloat16)
        mixed = jnp.einsum("gqk,kd->qgd", probs, v_head, preferred_element_type=jnp.float32).astype(
            jnp.bfloat16
        )
        return (mixed.reshape(step_count, head_group * head), log_total)

    mixed, log_total = lax.map(one_head, (query_layers, key_layers, value_layers))
    return (mixed.transpose(1, 0, 2).reshape(step_count, -1), log_total)


def attend_back(
    blended_gradient, query_rows, key_seq, value_seq, log_total, positions, heads_kv, head
):
    step_count = query_rows.shape[0]
    keys_total = key_seq.shape[0]
    head_group = query_rows.shape[1] // (heads_kv * head)
    scale = 1.0 / math.sqrt(head)
    allowed = jnp.arange(keys_total, dtype=jnp.int32)[None, :] <= positions[:, None]
    query_layers = query_rows.reshape(step_count, heads_kv, head_group * head).transpose(1, 0, 2)
    key_layers = key_seq.reshape(keys_total, heads_kv, head).transpose(1, 0, 2)
    value_layers = value_seq.reshape(keys_total, heads_kv, head).transpose(1, 0, 2)
    gain_layers = blended_gradient.reshape(step_count, heads_kv, head_group * head).transpose(
        1, 0, 2
    )

    def one_head(parts):
        q_head, k_head, v_head, g_head, l_head = parts
        q_three = q_head.reshape(step_count, head_group, head)
        g_three = g_head.reshape(step_count, head_group, head)
        scores = (
            jnp.einsum("qgd,kd->gqk", q_three, k_head, preferred_element_type=jnp.float32) * scale
        )
        probs = jnp.where(allowed, jnp.exp(scores - l_head[..., None]), 0.0)
        rounded = probs.astype(jnp.bfloat16)
        prob_grad = jnp.einsum("qgd,kd->gqk", g_three, v_head, preferred_element_type=jnp.float32)
        value_total_sum = jnp.einsum(
            "gqk,qgd->kd", rounded, g_three, preferred_element_type=jnp.float32
        )
        rowdot = jnp.sum(probs * prob_grad, axis=-1, keepdims=True)
        score_grad = (probs * (prob_grad - rowdot) * scale).astype(jnp.bfloat16)
        query_grad = jnp.einsum(
            "gqk,kd->qgd", score_grad, k_head, preferred_element_type=jnp.float32
        )
        key_gradient = jnp.einsum(
            "gqk,qgd->kd", score_grad, q_three, preferred_element_type=jnp.float32
        )
        return (query_grad.reshape(step_count, head_group * head), key_gradient, value_total_sum)

    query_grad, key_gradient, value_total_sum = lax.map(
        one_head, (query_layers, key_layers, value_layers, gain_layers, log_total)
    )
    query_grad = query_grad.transpose(1, 0, 2).reshape(step_count, -1)
    key_gradient = key_gradient.transpose(1, 0, 2).reshape(keys_total, -1)
    value_total_sum = value_total_sum.transpose(1, 0, 2).reshape(keys_total, -1)
    return (query_grad, key_gradient, value_total_sum)


def layer_forward(rows, table, micro, weights, groups, heads_kv, head):
    wq, wk, wv, wo, w_gate, w_up, w_down, gain_attn, gain_mlp = weights
    full = lax.all_gather(rows, TENSOR, axis=0, tiled=True)
    block = full.shape[0]
    slots, positions = block_layout(table, micro, groups, block)
    unit1, inverse1 = norm_stats(full)
    normed1 = (unit1 * gain_attn.astype(jnp.float32)).astype(jnp.bfloat16)
    query_rows = rotate(matmul(normed1, wq), positions, head).astype(jnp.bfloat16)
    key = rotate(matmul(normed1, wk), positions, head).astype(jnp.bfloat16)
    value_rows = matmul(normed1, wv).astype(jnp.bfloat16)
    key_all, value_all = (
        lax.all_gather(key, DP, axis=0, tiled=True),
        lax.all_gather(value_rows, DP, axis=0, tiled=True),
    )
    kv_width = key.shape[1]
    key_seq = key_all.reshape(groups, block, kv_width)[slots].reshape(-1, kv_width)
    value_seq = value_all.reshape(groups, block, kv_width)[slots].reshape(-1, kv_width)
    mixed, log_total = attend(query_rows, key_seq, value_seq, positions, heads_kv, head)
    second = rows + lax.psum_scatter(matmul(mixed, wo), TENSOR, scatter_dimension=0, tiled=True)
    full_second = lax.all_gather(second, TENSOR, axis=0, tiled=True)
    unit2, inverse2 = norm_stats(full_second)
    normed2 = (unit2 * gain_mlp.astype(jnp.float32)).astype(jnp.bfloat16)
    gate = matmul(normed2, w_gate)
    upper = matmul(normed2, w_up)
    hidden = (jax.nn.silu(gate) * upper).astype(jnp.bfloat16)
    result = second + lax.psum_scatter(
        matmul(hidden, w_down), TENSOR, scatter_dimension=0, tiled=True
    )
    return (
        result,
        (
            full,
            query_rows,
            key_seq,
            value_seq,
            mixed,
            log_total,
            full_second,
            gate,
            upper,
            hidden,
            slots,
            positions,
        ),
    )


def layer_backward(grad_rows, context, weights, groups, parts, heads_kv, head):
    wq, wk, wv, wo, w_gate, w_up, w_down, gain_attn, gain_mlp = weights
    (
        full,
        query_rows,
        key_seq,
        value_seq,
        mixed,
        log_total,
        full_second,
        gate,
        upper,
        hidden,
        slots,
        positions,
    ) = context
    block = full.shape[0]
    out_grad = lax.all_gather(grad_rows.astype(jnp.bfloat16), TENSOR, axis=0, tiled=True)
    grad_down = matmul(hidden.T, out_grad)
    hidden_grad = matmul(out_grad, w_down.T)
    sigma = jax.nn.sigmoid(gate)
    gate_grad = (hidden_grad * upper * sigma * (1.0 + gate * (1.0 - sigma))).astype(jnp.bfloat16)
    up_grad = (hidden_grad * gate * sigma).astype(jnp.bfloat16)
    unit2, inverse2 = norm_stats(full_second)
    normed2 = (unit2 * gain_mlp.astype(jnp.float32)).astype(jnp.bfloat16)
    grad_gate = matmul(normed2.T, gate_grad)
    grad_up = matmul(normed2.T, up_grad)
    normed2_grad = matmul(gate_grad, w_gate.T) + matmul(up_grad, w_up.T)
    second_terms, gain_mlp_terms = norm_back(
        normed2_grad, unit2, inverse2, gain_mlp.astype(jnp.float32)
    )
    piece_width = gain_mlp_terms.shape[0] // (groups * parts)
    second_part, gain_mlp_part = (
        lax.psum_scatter(
            second_terms.astype(jnp.bfloat16), TENSOR, scatter_dimension=0, tiled=True
        ).astype(jnp.float32),
        lax.psum_scatter(
            gain_mlp_terms.reshape(groups, parts, piece_width).astype(jnp.bfloat16),
            TENSOR,
            scatter_dimension=1,
            tiled=True,
        ).astype(jnp.float32),
    )
    second_grad = grad_rows + second_part
    attn_grad = lax.all_gather(second_grad.astype(jnp.bfloat16), TENSOR, axis=0, tiled=True)
    grad_wo = matmul(mixed.T, attn_grad)
    blended_gradient = matmul(attn_grad, wo.T).astype(jnp.bfloat16)
    query_grad, key_seq_grad, value_seq_grad = attend_back(
        blended_gradient, query_rows, key_seq, value_seq, log_total, positions, heads_kv, head
    )
    kv_width = key_seq.shape[1]
    key_spread = (
        jnp.zeros((groups, block, kv_width), jnp.float32)
        .at[slots]
        .set(key_seq_grad.reshape(-1, block, kv_width))
    )
    value_spread = (
        jnp.zeros((groups, block, kv_width), jnp.float32)
        .at[slots]
        .set(value_seq_grad.reshape(-1, block, kv_width))
    )
    key_own, value_own = (
        lax.psum_scatter(
            key_spread.astype(jnp.bfloat16), DP, scatter_dimension=0, tiled=True
        ).astype(jnp.float32),
        lax.psum_scatter(
            value_spread.astype(jnp.bfloat16), DP, scatter_dimension=0, tiled=True
        ).astype(jnp.float32),
    )
    query_round = unrotate(query_grad, positions, head).astype(jnp.bfloat16)
    key_round = unrotate(key_own.reshape(block, kv_width), positions, head).astype(jnp.bfloat16)
    value_round = value_own.reshape(block, kv_width).astype(jnp.bfloat16)
    unit1, inverse1 = norm_stats(full)
    normed1 = (unit1 * gain_attn.astype(jnp.float32)).astype(jnp.bfloat16)
    grad_wq = matmul(normed1.T, query_round)
    grad_wk = matmul(normed1.T, key_round)
    grad_wv = matmul(normed1.T, value_round)
    normed1_grad = matmul(query_round, wq.T) + matmul(key_round, wk.T) + matmul(value_round, wv.T)
    first_terms, gain_attn_terms = norm_back(
        normed1_grad, unit1, inverse1, gain_attn.astype(jnp.float32)
    )
    first_part, gain_attn_part = (
        lax.psum_scatter(first_terms, TENSOR, scatter_dimension=0, tiled=True),
        lax.psum_scatter(
            gain_attn_terms.reshape(groups, parts, piece_width),
            TENSOR,
            scatter_dimension=1,
            tiled=True,
        ),
    )
    input_grad = second_grad + first_part
    return (
        input_grad,
        (
            grad_wq,
            grad_wk,
            grad_wv,
            grad_wo,
            grad_gate,
            grad_up,
            grad_down,
            gain_attn_part,
            gain_mlp_part,
        ),
    )


def reduce_grads(pieces):
    return (
        lax.psum_scatter(
            pieces[0].astype(jnp.bfloat16), DP, scatter_dimension=0, tiled=True
        ).astype(jnp.float32),
        lax.psum_scatter(
            pieces[1].astype(jnp.bfloat16), DP, scatter_dimension=0, tiled=True
        ).astype(jnp.float32),
        lax.psum_scatter(
            pieces[2].astype(jnp.bfloat16), DP, scatter_dimension=0, tiled=True
        ).astype(jnp.float32),
        lax.psum_scatter(
            pieces[3].astype(jnp.bfloat16), DP, scatter_dimension=1, tiled=True
        ).astype(jnp.float32),
        lax.psum_scatter(
            pieces[4].astype(jnp.bfloat16), DP, scatter_dimension=0, tiled=True
        ).astype(jnp.float32),
        lax.psum_scatter(
            pieces[5].astype(jnp.bfloat16), DP, scatter_dimension=0, tiled=True
        ).astype(jnp.float32),
        lax.psum_scatter(
            pieces[6].astype(jnp.bfloat16), DP, scatter_dimension=1, tiled=True
        ).astype(jnp.float32),
        lax.psum_scatter(
            pieces[7].astype(jnp.bfloat16), DP, scatter_dimension=0, tiled=True
        ).astype(jnp.float32),
        lax.psum_scatter(
            pieces[8].astype(jnp.bfloat16), DP, scatter_dimension=0, tiled=True
        ).astype(jnp.float32),
    )


def general_shards(inputs, table, cotangent, wq, wk, wv, wo, w_gate, w_up, w_down, gain_attn, gain_mlp):
    groups = lax.axis_size(DP)
    parts = lax.axis_size(TENSOR)
    micro_count = inputs.shape[0]
    section = lax.axis_index(SECTION)
    first_section = section == 0
    weights = (
        lax.all_gather(wq[0], DP, axis=0, tiled=True),
        lax.all_gather(wk[0], DP, axis=0, tiled=True),
        lax.all_gather(wv[0], DP, axis=0, tiled=True),
        lax.all_gather(wo[0], DP, axis=1, tiled=True),
        lax.all_gather(w_gate[0], DP, axis=0, tiled=True),
        lax.all_gather(w_up[0], DP, axis=0, tiled=True),
        lax.all_gather(w_down[0], DP, axis=1, tiled=True),
        lax.all_gather(gain_attn[0], DP, axis=0, tiled=True),
        lax.all_gather(gain_mlp[0], DP, axis=0, tiled=True),
    )
    head = HEAD_SIZE
    heads_kv = wk.shape[2] // head
    received = jnp.zeros_like(inputs[0])
    produced = []
    saved = []
    for step in range(micro_count + 1):
        own_rows = inputs[step] if step < micro_count else jnp.zeros_like(inputs[0])
        start_rows = jnp.where(first_section, own_rows, received)
        micro = jnp.clip(step - section, 0, micro_count - 1)
        result, context = layer_forward(start_rows, table, micro, weights, groups, heads_kv, head)
        produced.append(result)
        saved.append(context)
        if step < micro_count:
            received = passed_along(result, SECTION, 1)
    stacked = jnp.stack(produced)
    outputs = jnp.where(first_section, stacked[:micro_count], stacked[1:])[None]
    returned = jnp.zeros_like(inputs[0])
    returned_list = []
    totals = None
    for step in range(micro_count + 1):
        index = micro_count - 1 - step
        given = cotangent[index] if index >= 0 else jnp.zeros_like(cotangent[0])
        start_grad = jnp.where(first_section, returned, given)
        din, pieces = layer_backward(
            start_grad, saved[micro_count - step], weights, groups, parts, heads_kv, head
        )
        returned_list.append(din)
        if step < micro_count:
            returned = passed_along(din.astype(jnp.bfloat16), SECTION, -1).astype(din.dtype)
        totals = (
            pieces
            if totals is None
            else tuple((left + right for left, right in zip(totals, pieces)))
        )
    totals = reduce_grads(totals)
    reverse_stack = jnp.stack(returned_list[::-1])
    input_grad = jnp.where(first_section, reverse_stack[:micro_count], reverse_stack[1:])[None]
    (
        grad_wq,
        grad_wk,
        grad_wv,
        grad_wo,
        grad_gate,
        grad_up,
        grad_down,
        gain_attn_sum,
        gain_mlp_sum,
    ) = totals
    width_piece = gain_attn_sum.shape[-1]
    return (
        outputs,
        input_grad,
        grad_wq[None],
        grad_wk[None],
        grad_wv[None],
        grad_wo[None],
        grad_gate[None],
        grad_up[None],
        grad_down[None],
        gain_attn_sum.reshape(1, width_piece),
        gain_mlp_sum.reshape(1, width_piece),
    )


MESH = pl.DeviceIdType.MESH
SUBS = 2
HBM = pl.BlockSpec(memory_space=pl.ANY)
VMEM = pl.BlockSpec(memory_space=pltpu.VMEM)
SMEM = pl.BlockSpec(memory_space=pltpu.SMEM)
NARROW, WIDE = jnp.bfloat16, jnp.float32


def ring_place(index, count):
    return jnp.where(lax.rem(index, 2) == 0, index // 2, count - (index + 1) // 2)


def ring_index(place, count):
    place = lax.rem(place + 2 * count, count)
    return jnp.where(place < count // 2, 2 * place, 2 * count - 1 - 2 * place)


def greet(others):
    barrier = pltpu.get_barrier_semaphore()
    for other in others:
        pl.semaphore_signal(barrier, inc=1, device_id=other, device_id_type=MESH)
    pl.semaphore_wait(barrier, len(others))


def remote(source, target, send, recv, device):
    return pltpu.make_async_remote_copy(
        source, target, send, recv, device_id=device, device_id_type=MESH
    )


def partners(me, count):
    half = count // 2
    side, inside = me // half, lax.rem(me, half)
    peers = [(1 - side) * half + lax.rem(inside + k, half) for k in range(half)]
    peers += [side * half + lax.rem(inside + k, half) for k in range(1, half)]
    origins = [(1 - side) * half + lax.rem(inside + half - k, half) for k in range(half)]
    origins += [side * half + lax.rem(inside + half - k, half) for k in range(1, half)]
    return peers, origins


def aligned(start, size):
    return pl.ds(pl.multiple_of(start, size), size)


def tiles(size, tile):
    return [slice(at, at + tile) for at in range(0, size, tile)]


def loop(start, stop, body):
    if stop - start == 1:
        body(start)
    elif stop > start:

        def step(at, carry):
            body(at)
            return carry

        lax.fori_loop(start, stop, step, 0)


def dot(left, right, contract):
    return lax.dot_general(
        left, right, (contract, ((), ())), preferred_element_type=jnp.float32
    )


class Names:
    def __init__(self, **values):
        self.__dict__.update(values)


class Work:
    def __init__(self):
        self.items = []

    def add(self, body, count=1):
        self.items.append((body, 0, count))

    def first(self, body):
        self.items.insert(0, (body, 0, 1))

    def do(self, some=1 << 20):
        while some > 0 and self.items:
            body, start, stop = self.items.pop(0)
            until = min(stop, start + some)
            loop(start, until, body)
            some -= until - start
            if until < stop:
                self.items.insert(0, (body, until, stop))


class Copies:
    def __init__(self, sem):
        self.sem = sem
        self.used = 0

    def __call__(self, source, target):
        copy = pltpu.make_async_copy(source, target, self.sem.at[self.used])
        self.used += 1
        copy.start()
        return copy


class Ring:
    def __init__(self):
        self.count = lax.axis_size(DP)
        self.far = self.count // 2
        self.me = lax.axis_index(DP)
        self.core = lax.axis_index(TENSOR)
        self.place = ring_place(self.me, self.count)
        self.near = tuple({DP: ring_index(self.place + step, self.count)} for step in (1, -1))
        self.side = {TENSOR: 1 - self.core}

    def everyone(self):
        return [*self.near, self.side]

    def index(self, steps):
        return ring_index(self.place + steps, self.count)

    def orders(self):
        for k in range(SUBS):
            yield k, 0
            yield SUBS - 1 - k, 1


def gather_scratch(count):
    far = count // 2
    dma = pltpu.SemaphoreType.DMA
    return [
        dma((2, far, SUBS)), dma((2, far, SUBS)), dma((count, SUBS)), dma((count, SUBS)), dma((1,))
    ]


class Gather:
    def __init__(self, ring, x_ref, o_ref, sems):
        self.ring = ring
        self.x_ref, self.o_ref = x_ref, o_ref
        self.ring_send, self.ring_recv, self.side_send, self.side_recv, self.own_sem = sems
        self.rows = x_ref.shape[0]
        self.piece = self.rows // SUBS
        self.sends = []

    def spot(self, steps, sub, core):
        start = (self.ring.index(steps) * 2 + core) * self.rows + sub * self.piece
        return self.o_ref.at[aligned(start, self.piece), :]

    def mine(self, steps, sub):
        if steps == 0:
            return self.x_ref.at[sub * self.piece : (sub + 1) * self.piece, :]
        return self.spot(steps, sub, self.ring.core)

    def travels(self, way, hop, sub):
        return hop < self.ring.far or (sub < SUBS // 2) == (way == 0)

    def go(self, copy):
        copy.start()
        self.sends.append(copy)

    def pass_on(self, way, hop, sub):
        steps = 1 - hop if way == 0 else hop - 1
        self.go(
            remote(
                self.mine(steps, sub),
                self.spot(steps, sub, self.ring.core),
                self.ring_send.at[way, hop - 1, sub],
                self.ring_recv.at[way, hop - 1, sub],
                self.ring.near[way],
            )
        )

    def hand_over(self, steps, sub, slot):
        self.go(
            remote(
                self.mine(steps, sub),
                self.spot(steps, sub, self.ring.core),
                self.side_send.at[slot, sub],
                self.side_recv.at[slot, sub],
                self.ring.side,
            )
        )

    def start(self):
        for sub, way in self.ring.orders():
            self.pass_on(way, 1, sub)
        for sub in range(SUBS):
            self.hand_over(0, sub, 0)
        self.own = pltpu.make_async_copy(
            self.x_ref,
            self.o_ref.at[aligned((self.ring.me * 2 + self.ring.core) * self.rows, self.rows), :],
            self.own_sem.at[0],
        )
        self.own.start()

    def hop(self, hop):
        far, count = self.ring.far, self.ring.count
        for sub, way in self.ring.orders():
            if not self.travels(way, hop, sub):
                continue
            steps = -hop if way == 0 else hop
            here = self.spot(steps, sub, self.ring.core)
            remote(
                here, here, self.ring_send.at[way, hop - 1, sub],
                self.ring_recv.at[way, hop - 1, sub], self.ring.near[way],
            ).wait_recv()
            if hop < far and self.travels(way, hop + 1, sub):
                self.pass_on(way, hop + 1, sub)
            self.hand_over(steps, sub, hop if way == 0 or hop == far else count - hop)

    def side_arrived(self, steps):
        slot = -steps if steps <= 0 else self.ring.count - steps
        slot = self.ring.far if abs(steps) == self.ring.far else slot
        for sub in range(SUBS):
            there = self.spot(steps, sub, 1 - self.ring.core)
            remote(
                there, there, self.side_send.at[slot, sub], self.side_recv.at[slot, sub],
                self.ring.side,
            ).wait_recv()

    def around(self, hop):
        return (-hop, hop) if hop < self.ring.far else (-hop,)

    def sent(self):
        for copy in self.sends:
            copy.wait_send()

    def finish(self):
        self.own.wait()
        self.side_arrived(0)
        for hop in range(1, self.ring.far + 1):
            for steps in self.around(hop):
                self.side_arrived(steps)
        self.sent()

    def run(self, use, work, some):
        self.start()
        self.own.wait()
        self.side_arrived(0)
        use([self.ring.index(0)])
        for hop in range(1, self.ring.far + 1):
            work.do(some)
            self.hop(hop)
            for steps in self.around(hop):
                self.side_arrived(steps)
            use([self.ring.index(steps) for steps in self.around(hop)])
        self.sent()


def chosen(at, indices):
    return indices[0] if len(indices) == 1 else indices[0] + (indices[1] - indices[0]) * at


def reduce_scratch(count, rows, width):
    far = count // 2
    dma = pltpu.SemaphoreType.DMA
    return [
        pltpu.VMEM((count * 2 * rows, width), NARROW),
        pltpu.VMEM((count, rows, width), NARROW),
        pltpu.VMEM((2, far, rows, width), NARROW),
        pltpu.VMEM((2, far, rows, width), NARROW),
        dma((2, far, SUBS)), dma((2, far, SUBS)), dma((count,)), dma((count,)),
    ]


class Reduce:
    def __init__(self, ring, scratch):
        self.ring = ring
        self.parts, self.beside, self.outgoing, self.incoming = scratch[:4]
        self.ring_send, self.ring_recv, self.side_send, self.side_recv = scratch[4:]
        self.rows = self.beside.shape[1]
        self.piece = self.rows // SUBS

    def span(self, sub):
        return slice(sub * self.piece, (sub + 1) * self.piece)

    def spot(self, steps, core, sub=None):
        start = (self.ring.index(steps) * 2 + core) * self.rows
        if sub is None:
            return aligned(start, self.rows)
        return aligned(start + sub * self.piece, self.piece)

    def make(self, *several):
        self.produce([self.ring.index(steps) for steps in several], self.parts)
        for steps in several:
            slot = len(self.slots)
            copy = remote(
                self.parts.at[self.spot(steps, 1 - self.ring.core), :], self.beside.at[slot],
                self.side_send.at[slot], self.side_recv.at[slot], self.ring.side,
            )
            copy.start()
            self.slots[steps] = (slot, copy)

    def mine(self, steps, sub):
        slot, copy = self.slots[steps]
        if steps not in self.joined:
            copy.wait_recv()
            self.joined.add(steps)
        return self.parts[self.spot(steps, self.ring.core, sub), :].astype(
            jnp.float32
        ) + self.beside[slot, self.span(sub), :].astype(jnp.float32)

    def travels(self, way, step, sub):
        return step > 1 or (sub < SUBS // 2) == (way == 0)

    def ring_copy(self, way, step, sub):
        return remote(
            self.outgoing.at[way, step - 1, self.span(sub), :],
            self.incoming.at[way, step - 1, self.span(sub), :],
            self.ring_send.at[way, step - 1, sub],
            self.ring_recv.at[way, step - 1, sub],
            self.ring.near[way],
        )

    def step(self, step):
        far = self.ring.far
        for sub, way in self.ring.orders():
            if not self.travels(way, step, sub):
                continue
            steps = far + 1 - step
            steps = steps if way == 0 or steps == far else -steps
            value = self.mine(steps, sub)
            if step > 1 and self.travels(way, step - 1, sub):
                self.ring_copy(way, step - 1, sub).wait_recv()
                value = value + self.incoming[way, step - 2, self.span(sub), :].astype(jnp.float32)
            self.outgoing[way, step - 1, self.span(sub), :] = value.astype(NARROW)
            copy = self.ring_copy(way, step, sub)
            copy.start()
            self.sends.append(copy)

    def begin(self, produce):
        self.produce = produce
        self.slots, self.joined, self.sends = {}, set(), []
        far = self.ring.far
        self.make(far)
        self.make(far - 1, 1 - far)

    def middle(self, step):
        left = self.ring.far - 1 - step
        self.step(step)
        if left > 0:
            self.make(left, -left)
        elif left == 0:
            self.make(0)

    def end(self, finish):
        far = self.ring.far
        for sub in range(SUBS):
            value = self.mine(0, sub)
            for way in range(2):
                self.ring_copy(way, far, sub).wait_recv()
                value = value + self.incoming[way, far - 1, self.span(sub), :].astype(jnp.float32)
            finish(self.span(sub), value)
        for copy in self.sends:
            copy.wait_send()
        for _, copy in self.slots.values():
            copy.wait_send()

    def run(self, produce, finish, work, some, beside=()):
        beside = list(beside)
        self.begin(produce)
        for step in range(1, self.ring.far + 1):
            self.middle(step)
            if beside:
                beside.pop(0)()
            work.do(some)
        self.end(finish)
        return beside


def products(left, right, transposed, tile=512):
    width = right.shape[0] if transposed else right.shape[1]
    number = width // tile

    def produce(indices, parts):
        block = parts.shape[0] // lax.axis_size(DP)

        def one(at):
            rows = aligned(chosen(at // number, indices) * block, block)
            cols = aligned(lax.rem(at, number) * tile, tile)
            if transposed:
                part = dot(left[rows, :], right[cols, :], ((1,), (1,)))
            else:
                part = dot(left[rows, :], right[:, cols], ((1,), (0,)))
            parts[rows, cols] = part.astype(NARROW)

        loop(0, number * len(indices), one)

    return produce


def add_gradient(work, left, right, out, tile=256):
    if out.shape[0] >= out.shape[1]:

        def piece(at):
            cols = aligned(at * tile, tile)
            out[cols, :] = dot(left[:, cols], right[...], ((0,), (0,))).astype(NARROW)

        work.add(piece, out.shape[0] // tile)
    else:

        def piece(at):
            cols = aligned(at * tile, tile)
            out[:, cols] = dot(left[...], right[:, cols], ((0,), (0,))).astype(NARROW)

        work.add(piece, out.shape[1] // tile)


def unit_rows(value):
    inverse = lax.rsqrt(jnp.mean(value * value, axis=-1, keepdims=True) + epsilon)
    return value * inverse, inverse


def through_norm(grad, value, gain):
    unit, inverse = unit_rows(value)
    scaled = grad * gain
    inner = jnp.mean(scaled * unit, axis=-1, keepdims=True)
    return inverse * (scaled - unit * inner), jnp.sum(grad * unit, axis=0, keepdims=True)


def shape_of(*dims, kind=NARROW):
    return jax.ShapeDtypeStruct(dims, kind)


def call_fused(name, body, cid, us, ins, outs, scratch):
    def kernel(*refs):
        refs = list(refs)
        named = {key: refs.pop(0) for key in [*ins, *outs]}
        for key, kind in scratch.items():
            named[key] = [refs.pop(0) for _ in kind] if isinstance(kind, list) else refs.pop(0)
        body(Names(**named))

    flat = []
    for kind in scratch.values():
        flat += kind if isinstance(kind, list) else [kind]
    result = pl.pallas_call(
        kernel,
        out_shape=tuple(shape for shape, _ in outs.values()),
        in_specs=[spec for _, spec in ins.values()],
        out_specs=tuple(spec for _, spec in outs.values()),
        scratch_shapes=flat,
        compiler_params=pltpu.CompilerParams(
            collective_id=cid, has_side_effects=True, vmem_limit_bytes=63 * 1024 * 1024
        ),
        cost_estimate=pl.CostEstimate(
            flops=0, bytes_accessed=int(us * 3.69e6), transcendentals=0
        ),
        name=name,
    )(*[value for value, _ in ins.values()])
    return Names(**dict(zip(outs, result)))


def swap_halves(rows, head):
    width = rows.shape[1]
    lane = lax.broadcasted_iota(jnp.int32, rows.shape, 1)
    half = head // 2
    return jnp.where(
        lax.rem(lane, head) < half, pltpu.roll(rows, width - half, 1), pltpu.roll(rows, half, 1)
    )


def low_lanes(shape, head):
    return lax.broadcasted_iota(jnp.int32, shape, 1) < head


def two_heads(rows, head):
    low = low_lanes(rows.shape, head)
    zero = jnp.zeros_like(rows)
    return jnp.concatenate([jnp.where(low, rows, zero), jnp.where(low, zero, rows)], axis=0)


def one_row(rows, head):
    half = rows.shape[0] // 2
    return jnp.where(low_lanes((half, rows.shape[1]), head), rows[:half], rows[half:])


def triangle(block, keys):
    row = lax.rem(lax.broadcasted_iota(jnp.int32, (2 * block, keys), 0), block)
    column = lax.broadcasted_iota(jnp.int32, (2 * block, keys), 1)
    return column <= row + (keys - block)


def in_order(ref, order, spot, block):
    value = ref[:block, :]
    for other in range(1, ref.shape[0] // block):
        there = order[spot] == other
        value = jnp.where(there, ref[other * block : (other + 1) * block, :], value)
    return value


def attend_here(slots, qkv, cosine, sine, kept, lse, mixed, key2, value2):
    groups = slots.shape[0]
    tokens = qkv.shape[0]
    block = tokens // groups
    span = groups // 2
    wide = qkv.shape[1] // 2
    head = wide // 2
    scale = 1.0 / math.sqrt(head)
    for spot in range(groups):
        here = slice(spot * block, (spot + 1) * block)
        turn_rows = slice(spot % span * block, (spot % span + 1) * block)
        turned_by, turned_sine = cosine[turn_rows, :], sine[turn_rows, :]
        rows = in_order(qkv, slots, spot, block)
        query, pair = rows[:, :wide], rows[:, wide:]
        low = low_lanes(pair.shape, head)
        query = query * turned_by + swap_halves(query, head) * turned_sine
        pair = jnp.where(low, pair * turned_by + swap_halves(pair, head) * turned_sine, pair)
        other = pltpu.roll(pair, head, 1)
        kept[here, :wide] = query.astype(kept.dtype)
        kept[here, wide:] = pair.astype(kept.dtype)
        key2[here, :] = jnp.where(low, pair, other).astype(key2.dtype)
        value2[here, :] = jnp.where(low, other, pair).astype(value2.dtype)
    for spot in range(groups):
        here = slice(spot * block, (spot + 1) * block)
        first = spot // span * span * block
        keys = (spot % span + 1) * block
        query = two_heads(kept[here, :wide], head)
        score = dot(query, key2[first : first + keys, :], ((1,), (1,))) * scale
        allowed = triangle(block, keys)
        total = jnp.sum(jnp.where(allowed, jnp.exp(score), 0.0), axis=1, keepdims=True)
        log_total = jnp.log(total)
        probs = jnp.where(allowed, jnp.exp(score - log_total), 0.0).astype(jnp.bfloat16)
        value = dot(probs, value2[first : first + keys, :], ((1,), (0,)))
        mixed[here, :] = one_row(value, head).astype(mixed.dtype)
        lse[spot] = log_total


def attend_back_here(slots, grad, kept, lse, cosine, sine, out, key2, value2, key_sum, value_sum):
    groups = slots.shape[0]
    tokens = kept.shape[0]
    block = tokens // groups
    span = groups // 2
    wide = kept.shape[1] // 2
    head = wide // 2
    scale = 1.0 / math.sqrt(head)
    for spot in range(groups):
        here = slice(spot * block, (spot + 1) * block)
        pair = kept[here, wide:].astype(jnp.float32)
        low = low_lanes(pair.shape, head)
        other = pltpu.roll(pair, head, 1)
        key2[here, :] = jnp.where(low, pair, other).astype(key2.dtype)
        value2[here, :] = jnp.where(low, other, pair).astype(value2.dtype)
    for spot in range(groups - 1, -1, -1):
        here = slice(spot * block, (spot + 1) * block)
        place = spot % span
        turn_rows = slice(place * block, (place + 1) * block)
        first = spot // span * span * block
        keys = (place + 1) * block
        query = two_heads(kept[here, :wide], head)
        given = two_heads(in_order(grad, slots, spot, block), head)
        key = key2[first : first + keys, :]
        value = value2[first : first + keys, :]
        score = dot(query, key, ((1,), (1,))) * scale
        probs = jnp.where(triangle(block, keys), jnp.exp(score - lse[spot]), 0.0)
        prob_grad = dot(given, value, ((1,), (1,)))
        rowdot = jnp.sum(probs * prob_grad, axis=1, keepdims=True)
        score_grad = (probs * (prob_grad - rowdot) * scale).astype(jnp.bfloat16)
        value_part = dot(probs.astype(jnp.bfloat16), given, ((0,), (0,)))
        key_part = dot(score_grad, query, ((0,), (0,)))
        if place == span - 1:
            value_sum[first : first + keys, :] = value_part
            key_sum[first : first + keys, :] = key_part
        else:
            value_sum[first : first + keys, :] += value_part
            key_sum[first : first + keys, :] += key_part
        query_grad = one_row(dot(score_grad, key, ((1,), (0,))), head)
        query_grad = query_grad * cosine[turn_rows, :] - swap_halves(query_grad, head) * sine[turn_rows, :]
        out[here, :wide] = query_grad.astype(out.dtype)
    for spot in range(groups):
        here = slice(spot * block, (spot + 1) * block)
        turn_rows = slice(spot % span * block, (spot % span + 1) * block)
        key = key_sum[here, :]
        key = key + pltpu.roll(key, head, 1)
        key = key * cosine[turn_rows, :] - swap_halves(key, head) * sine[turn_rows, :]
        value = value_sum[here, :]
        value = value + pltpu.roll(value, head, 1)
        out[here, wide:] = jnp.where(low_lanes(key.shape, head), key, value).astype(out.dtype)


def put_back(source, target, row):
    groups = row.shape[0]
    block = source.shape[0] // groups
    for spot in range(groups):
        target[spot * block : (spot + 1) * block, :] = in_order(source, row, spot, block)


def attend_scratch(tokens, head, back=False):
    vmem = pltpu.VMEM
    wide = 2 * head
    kinds = dict(
        key2=vmem((tokens, wide), jnp.bfloat16),
        value2=vmem((tokens, wide), jnp.bfloat16),
        by_number=vmem((tokens, 2 * wide if back else wide), jnp.bfloat16),
    )
    if back:
        kinds.update(
            key_sum=vmem((tokens, wide), jnp.float32), value_sum=vmem((tokens, wide), jnp.float32)
        )
    return kinds


def rope_tables(tokens, head):
    angle = jnp.arange(tokens, dtype=jnp.float32)[:, None] * rope_frequencies(head)[None, :]
    cosine = jnp.cos(angle)
    sine = jnp.sin(angle)
    return (
        jnp.concatenate([cosine] * 4, axis=1),
        jnp.concatenate([-sine, sine] * 2, axis=1),
    )


def weight_pieces(source, target, count, heads, srcs, dsts, layer):
    qkv, wo, gate, up, down = srcs
    out_qkv, out_wo, out_gu, out_down = dsts
    depth = gate.shape[1]
    hidden = gate.shape[2] // count
    q_rows = wo.shape[1] // count
    kv_rows = (qkv.shape[0] - wo.shape[1]) // 2
    shared = count * heads // kv_rows
    cols = aligned(source * depth, depth)
    k_from = pl.multiple_of(wo.shape[1] + target // shared * heads, heads)
    v_from = pl.multiple_of(wo.shape[1] + kv_rows + target // shared * heads, heads)
    mine = aligned(target * hidden, hidden)
    return (
        (qkv.at[aligned(target * q_rows, q_rows), :], out_qkv.at[layer, pl.ds(0, q_rows), cols]),
        (qkv.at[pl.ds(k_from, heads), :], out_qkv.at[layer, pl.ds(q_rows, heads), cols]),
        (qkv.at[pl.ds(v_from, heads), :], out_qkv.at[layer, pl.ds(q_rows + heads, heads), cols]),
        (wo.at[0, aligned(target * q_rows, q_rows), :], out_wo.at[layer, :, cols]),
        (gate.at[0, :, mine], out_gu.at[layer, cols, pl.ds(0, hidden)]),
        (up.at[0, :, mine], out_gu.at[layer, cols, pl.ds(hidden, hidden)]),
        (down.at[0, mine, :], out_down.at[layer, :, cols]),
    )


KINDS, ATTENTION_KINDS = 7, 4


class Spread:
    def __init__(self, ring, heads, srcs, dsts, sems):
        self.ring = ring
        self.layer = lax.axis_index(SECTION)
        self.across = {SECTION: 1 - self.layer}
        self.peers, self.origins = partners(ring.me, ring.count)
        self.send, self.recv, self.cross_send, self.cross_recv, self.own_sem = sems
        self.pieces = lambda source, target, layer: weight_pieces(
            source, target, ring.count, heads, srcs, dsts, layer
        )
        self.started, self.local = [], {}
        count = ring.count
        sizes = [math.prod(there.shape) for _, there in self.pieces(ring.me, ring.me, self.layer)]
        arrivals = []
        for kind in range(KINDS):
            for k in range(count - 1):
                part = (k + 1) / (count // 2) if k < count // 2 else 1.0
                due = sum(sizes[:kind]) + part * sizes[kind]
                arrivals.append((due if k < count // 2 else due * 0.5, kind, k))
        self.arrivals = sorted(arrivals)

    def go(self, copy):
        copy.start()
        self.started.append(copy)

    def own(self, kinds):
        last = self.ring.count - 1
        for kind in kinds:
            source, target = self.pieces(self.ring.me, self.ring.me, self.layer)[kind]
            self.go(
                remote(
                    source, target, self.cross_send.at[kind, last], self.cross_recv.at[kind, last],
                    self.across,
                )
            )
            self.local[kind] = pltpu.make_async_copy(source, target, self.own_sem.at[kind])
            self.local[kind].start()

    def out(self, kinds):
        for kind in kinds:
            for k, peer in enumerate(self.peers):
                source, target = self.pieces(self.ring.me, peer, self.layer)[kind]
                self.go(remote(source, target, self.send.at[kind, k], self.recv.at[kind, k], {DP: peer}))

    def pass_on(self, kinds):
        for _, kind, k in self.arrivals:
            if kind not in kinds:
                continue
            here = self.pieces(self.origins[k], self.ring.me, self.layer)[kind][1]
            remote(
                here, here, self.send.at[kind, k], self.recv.at[kind, k], {DP: self.origins[k]}
            ).wait_recv()
            self.go(
                remote(
                    here, here, self.cross_send.at[kind, k], self.cross_recv.at[kind, k], self.across
                )
            )

    def here(self, kinds):
        for kind in kinds:
            self.local[kind].wait()
            for k in range(self.ring.count):
                origin = self.origins[k] if k < self.ring.count - 1 else self.ring.me
                there = self.pieces(origin, self.ring.me, 1 - self.layer)[kind][1]
                remote(
                    there, there, self.cross_send.at[kind, k], self.cross_recv.at[kind, k], self.across
                ).wait_recv()

    def sent(self):
        for copy in self.started:
            copy.wait_send()


def chip_rows(index, local):
    return aligned(index * 2 * local, 2 * local)


def feed_forward_use(s, local, after):
    width = s.hidden.shape[1]
    tile = 256
    number = width // tile

    def use(indices):
        def one(at):
            rows = chip_rows(chosen(at // number, indices), local)
            start = lax.rem(at, number) * tile
            cols, right = aligned(start, tile), aligned(start + width, tile)
            value = s.normed2[rows, :]
            gate = dot(value, s.gu[:, cols], ((1,), (0,)))
            upper = dot(value, s.gu[:, right], ((1,), (0,)))
            s.hidden[rows, cols] = (gate * jax.nn.sigmoid(gate) * upper).astype(NARROW)
            after(rows, cols, right, gate, upper)

        loop(0, number * len(indices), one)

    return use


def feed_forward_back(s, rows, cols, right, gate, upper):
    hidden_grad = dot(s.out_grad[rows, :], s.down[cols, :], ((1,), (1,)))
    sigma = jax.nn.sigmoid(gate)
    gate_grad = hidden_grad * upper * sigma * (1.0 + gate * (1.0 - sigma))
    s.gu_grad[rows, cols] = gate_grad.astype(NARROW)
    s.gu_grad[rows, right] = (hidden_grad * gate * sigma).astype(NARROW)


def opening_body(s):
    ring = Ring()
    layer = lax.axis_index(SECTION)
    peers, origins = partners(ring.me, ring.count)
    holders = [{DP: peer} for peer in peers] + [
        {SECTION: 1 - layer, DP: peer} for peer in [*peers, ring.me]
    ]
    greet([*holders, ring.side])
    copies = Copies(s.copy_sem)
    rows_in = copies(s.inputs.at[layer], s.rows)
    given_in = copies(s.cotangent.at[layer], s.given)
    spread = Spread(
        ring, s.kept0.shape[1] // 4, (s.qkv, s.wo, s.gate, s.up, s.down_in),
        (s.out_qkv, s.out_wo, s.out_gu, s.out_down), s.spread_sems,
    )
    attention, feed = range(ATTENTION_KINDS), range(ATTENTION_KINDS, KINDS)
    local, depth = s.rows.shape[0], s.gain_attn.shape[1]

    s.gain_piece[...] = jnp.zeros_like(s.gain_piece)
    s.gain_piece[0:1, :] = s.gain_attn[...].astype(WIDE)
    s.gain_piece[1:2, :] = s.gain_mlp[...].astype(WIDE)
    gain_send, gain_recv = s.gain_sems
    spot = lambda at, source: s.gains.at[at, :, aligned(source * depth, depth)]
    for k, holder in enumerate(holders):
        spread.go(remote(s.gain_piece, spot(layer, ring.me), gain_send.at[k], gain_recv.at[k], holder))
    own_gains = copies(s.gain_piece, spot(layer, ring.me))
    spread.own(attention)
    own_gains.wait()
    for k, holder in enumerate(holders):
        at, place = (layer, k) if k < ring.count - 1 else (1 - layer, k - ring.count + 1)
        here = spot(at, origins[place] if place < ring.count - 1 else ring.me)
        remote(here, here, gain_send.at[k], gain_recv.at[k], holder).wait_recv()

    rows_in.wait()
    unit, _ = unit_rows(s.rows[...])
    s.shard0[...] = (unit * s.gains[0, 0:1, :]).astype(NARROW)
    first = Gather(ring, s.shard0, s.normed1, s.first_sems)
    first.start()
    spread.out(attention)
    for hop in range(1, ring.far + 1):
        first.hop(hop)
    given_in.wait()
    s.shard1[...] = s.given[...].astype(NARROW)
    grads = Gather(ring, s.shard1, s.out_grad, s.grads_sems)
    grads.start()
    spread.pass_on(attention)
    spread.out(feed)
    spread.own(feed)
    first.finish()
    spread.here(attention)
    loads = [
        copies(s.out_qkv.at[0], s.qkv_w), copies(s.out_qkv.at[1], s.next_qkv_w),
        copies(s.out_wo.at[0], s.wo_w),
    ]
    stores = [copies(s.normed1, s.normed1_out)]
    for load in loads:
        load.wait()
    tile = 2 * local

    def project(at):
        rows = aligned(at * tile, tile)
        s.projected[rows, :] = dot(s.normed1[rows, :], s.qkv_w[...], ((1,), (1,)))

    loop(0, s.projected.shape[0] // tile, project)
    attend_here(s.slots, s.projected, s.cosine, s.sine, s.kept0, s.lse0, s.by_number, s.key2, s.value2)
    put_back(s.by_number, s.mixed0, s.row)
    stores[0].wait()
    grads.hop(1)
    spread.pass_on(feed)

    reduce = Reduce(ring, s.reduce)
    none = Work()

    def second(span, value):
        s.second[span, :] = s.rows[span, :] + value

    loads = {}

    def gate_up_here():
        spread.here(feed[:2])
        loads[0] = copies(s.out_gu.at[0], s.gu)

    left = reduce.run(
        products(s.mixed0, s.wo_w, False), second, none, 0,
        [functools.partial(grads.hop, hop) for hop in range(2, ring.far + 1)] + [gate_up_here],
    )
    for do in left:
        do()
    unit, _ = unit_rows(s.second[...])
    s.shard2[...] = (unit * s.gains[0, 1:2, :]).astype(NARROW)
    loads[0].wait()
    spread.here(feed[2:])
    load = copies(s.out_down.at[0], s.down)

    def keep(rows, cols, right, gate, upper):
        s.gate_up[rows, cols] = gate
        s.gate_up[rows, right] = upper

    Gather(ring, s.shard2, s.normed2, s.gather_sems).run(feed_forward_use(s, local, keep), none, 0)
    grads.finish()
    stores += [
        copies(s.out_grad, s.out_grad_out), copies(s.normed2, s.normed2_out),
        copies(s.gate_up, s.gate_up_out),
    ]
    load.wait()

    def result(span, value):
        s.result[span, :] = s.second[span, :] + value

    reduce.run(products(s.hidden, s.down, False), result, none, 0)
    unit, _ = unit_rows(s.result[...])
    s.shard0[...] = (unit * s.gains[1, 0:1, :]).astype(NARROW)

    def use(indices):
        def one(at):
            rows = chip_rows(chosen(at, indices), local)
            s.projected[rows, :] = dot(s.normed1[rows, :], s.next_qkv_w[...], ((1,), (1,)))

        loop(0, len(indices), one)

    Gather(ring, s.shard0, s.normed1, s.first_sems).run(use, none, 0)
    stores.append(copies(s.normed1, s.next_normed1_out))
    attend_here(s.slots, s.projected, s.cosine, s.sine, s.kept1, s.lse1, s.by_number, s.key2, s.value2)
    put_back(s.by_number, s.mixed1, s.row)
    for store in stores[1:]:
        store.wait()
    spread.sent()


def opening(slots, row, cosine, sine, inputs, cotangent, qkv, wo, gate, up, down, gain_attn, gain_mlp, count, head):
    local, width = inputs.shape[1:]
    tokens = count * 2 * local
    depth = gate.shape[1]
    hidden = gate.shape[2] // count
    q_rows = wo.shape[1] // count
    vmem, dma = pltpu.VMEM, pltpu.SemaphoreType.DMA
    lse = shape_of(count, 2 * tokens // count, 1, kind=WIDE)
    return call_fused(
        "opening", opening_body, 0, 360,
        dict(
            slots=(slots, SMEM), row=(row, SMEM), cosine=(cosine, VMEM), sine=(sine, VMEM),
            inputs=(inputs, HBM), cotangent=(cotangent, HBM), qkv=(qkv, HBM), wo=(wo, HBM),
            gate=(gate, HBM), up=(up, HBM), down_in=(down, HBM),
            gain_attn=(gain_attn, VMEM), gain_mlp=(gain_mlp, VMEM),
        ),
        dict(
            out_qkv=(shape_of(2, q_rows + 2 * head, width), HBM),
            out_wo=(shape_of(2, q_rows, width), HBM),
            out_gu=(shape_of(2, width, 2 * hidden), HBM),
            out_down=(shape_of(2, hidden, width), HBM),
            gains=(shape_of(2, 8, width, kind=WIDE), VMEM),
            normed1_out=(shape_of(tokens, width), HBM),
            next_normed1_out=(shape_of(tokens, width), HBM),
            normed2_out=(shape_of(tokens, width), HBM),
            out_grad_out=(shape_of(tokens, width), HBM),
            gate_up_out=(shape_of(tokens, 2 * hidden, kind=WIDE), HBM),
            second=(shape_of(local, width, kind=WIDE), VMEM),
            result=(shape_of(local, width, kind=WIDE), VMEM),
            hidden=(shape_of(tokens, hidden), VMEM),
            mixed0=(shape_of(tokens, 2 * head), VMEM), mixed1=(shape_of(tokens, 2 * head), VMEM),
            kept0=(shape_of(tokens, 4 * head), VMEM), kept1=(shape_of(tokens, 4 * head), VMEM),
            lse0=(lse, VMEM), lse1=(lse, VMEM),
        ),
        dict(
            rows=vmem((local, width), WIDE), given=vmem((local, width), WIDE),
            gain_piece=vmem((8, depth), WIDE),
            shard0=vmem((local, width), NARROW), shard1=vmem((local, width), NARROW),
            shard2=vmem((local, width), NARROW),
            normed1=vmem((tokens, width), NARROW), normed2=vmem((tokens, width), NARROW),
            out_grad=vmem((tokens, width), NARROW), gate_up=vmem((tokens, 2 * hidden), WIDE),
            qkv_w=vmem((q_rows + 2 * head, width), NARROW),
            next_qkv_w=vmem((q_rows + 2 * head, width), NARROW),
            wo_w=vmem((q_rows, width), NARROW), gu=vmem((width, 2 * hidden), NARROW),
            down=vmem((hidden, width), NARROW), projected=vmem((tokens, 4 * head), WIDE),
            key2=vmem((tokens, 2 * head), NARROW), value2=vmem((tokens, 2 * head), NARROW),
            by_number=vmem((tokens, 2 * head), NARROW),
            reduce=reduce_scratch(count, local, width),
            first_sems=gather_scratch(count), grads_sems=gather_scratch(count),
            gather_sems=gather_scratch(count),
            gain_sems=[dma((2 * count - 1,)), dma((2 * count - 1,))],
            spread_sems=[
                dma((KINDS, count - 1)), dma((KINDS, count - 1)),
                dma((KINDS, count)), dma((KINDS, count)), dma((KINDS,)),
            ],
            copy_sem=dma((16,)),
        ),
    )


def back_through_feed_forward(at, s, ring, reduce, work, beside):
    local = s.given.shape[0]
    add_gradient(work, s.hidden, s.out_grad, s.grad_down)
    add_gradient(work, s.normed2, s.gu_grad, s.grad_gu)

    def keep(span, value):
        s.normed_grad[span, :] = value

    left = reduce.run(products(s.gu_grad, s.gu, True), keep, work, 3, beside)
    part, s.gain_mlp_grad[...] = through_norm(
        s.normed_grad[...], s.second[...], s.gains[at, 1:2, :]
    )
    s.second_grad[...] = s.given[...] + part
    s.shard2[...] = s.second_grad[...].astype(NARROW)

    def use(indices):
        def one(at):
            rows = chip_rows(chosen(at, indices), local)
            s.mixed_grad[rows, :] = dot(s.attn_grad[rows, :], s.wo[...], ((1,), (1,))).astype(NARROW)

        loop(0, len(indices), one)

    for do in reversed(left):
        work.first(lambda _, do=do: do())
    Gather(ring, s.shard2, s.attn_grad, s.gather_sems).run(use, work, 3)
    work.do()


def turn_body(at, s):
    ring = Ring()
    greet(ring.everyone())
    copies = Copies(s.copy_sem)
    wo_in = copies(s.wo_in.at[at], s.wo)
    ins = [
        copies(s.gu_in.at[at], s.gu), copies(s.down_in.at[at], s.down),
        copies(s.out_grad_in, s.out_grad), copies(s.cotangent.at[lax.axis_index(SECTION)], s.given),
    ]
    reduce, other = Reduce(ring, s.reduce), Reduce(ring, s.other)
    work = Work()

    def second(span, value):
        s.second[span, :] = s.rows[span, :] + value

    wo_in.wait()
    reduce.run(products(s.mixed, s.wo, False), second, work, 0)
    unit, _ = unit_rows(s.second[...])
    s.shard[...] = (unit * s.gains[at, 1:2, :]).astype(NARROW)
    for load in ins:
        load.wait()
    Gather(ring, s.shard, s.normed2, s.first_sems).run(
        feed_forward_use(s, s.rows.shape[0], functools.partial(feed_forward_back, s)), work, 0
    )

    def result(span, value):
        s.result[span, :] = s.second[span, :] + value

    beside = [lambda: other.begin(products(s.hidden, s.down, False))]
    beside += [functools.partial(other.middle, step) for step in range(1, ring.far + 1)]
    beside += [lambda: other.end(result)]
    back_through_feed_forward(at, s, ring, reduce, work, beside)
    stores = [
        copies(s.grad_down, s.grad_down_out), copies(s.grad_gu, s.grad_gu_out),
        copies(s.attn_grad, s.attn_grad_out),
    ]
    attend_back_here(
        s.slots, s.mixed_grad, s.kept, s.lse, s.cosine, s.sine, s.by_number, s.key2, s.value2,
        s.key_sum, s.value_sum,
    )
    put_back(s.by_number, s.qkv_grad, s.row)
    for store in stores:
        store.wait()


def turn(at, known, rows, mixed, kept, lse, out_grad, cotangent, weights, count):
    _, wo, gu, down, gains = weights
    local, width = rows.shape
    tokens = mixed.shape[0]
    hidden = down.shape[1]
    head = mixed.shape[1] // 2
    vmem, dma = pltpu.VMEM, pltpu.SemaphoreType.DMA
    return call_fused(
        "turn", functools.partial(turn_body, at), 1, 140,
        dict(
            **known, rows=(rows, VMEM), mixed=(mixed, VMEM), kept=(kept, VMEM), lse=(lse, VMEM),
            gains=(gains, VMEM), out_grad_in=(out_grad, HBM), cotangent=(cotangent, HBM),
            wo_in=(wo, HBM), gu_in=(gu, HBM), down_in=(down, HBM),
        ),
        dict(
            result=(shape_of(local, width, kind=WIDE), VMEM),
            second_grad=(shape_of(local, width, kind=WIDE), VMEM),
            qkv_grad=(shape_of(tokens, 4 * head), VMEM),
            attn_grad_out=(shape_of(tokens, width), HBM),
            gain_mlp_grad=(shape_of(1, width, kind=WIDE), VMEM),
            grad_down_out=(shape_of(hidden, width), HBM),
            grad_gu_out=(shape_of(width, 2 * hidden), HBM),
        ),
        dict(
            reduce=reduce_scratch(count, local, width), other=reduce_scratch(count, local, width),
            first_sems=gather_scratch(count), gather_sems=gather_scratch(count),
            gu=vmem(gu.shape[1:], NARROW), down=vmem(down.shape[1:], NARROW), wo=vmem(wo.shape[1:], NARROW),
            out_grad=vmem((tokens, width), NARROW), normed2=vmem((tokens, width), NARROW),
            attn_grad=vmem((tokens, width), NARROW), mixed_grad=vmem((tokens, 2 * head), NARROW),
            hidden=vmem((tokens, hidden), NARROW), gu_grad=vmem((tokens, 2 * hidden), NARROW),
            grad_down=vmem((hidden, width), NARROW), grad_gu=vmem((width, 2 * hidden), NARROW),
            given=vmem((local, width), WIDE), second=vmem((local, width), WIDE),
            normed_grad=vmem((local, width), WIDE),
            shard=vmem((local, width), NARROW), shard2=vmem((local, width), NARROW),
            **attend_scratch(tokens, head, True),
            copy_sem=dma((8,)),
        ),
    )


def attention_back(at, s, reduce, work, beside=()):
    def keep(span, value):
        s.normed_grad[span, :] = value

    reduce.run(products(s.qkv_grad, s.qkv_w, False), keep, work, 3, beside)
    part, s.gain_attn_grad[...] = through_norm(s.normed_grad[...], s.rows[...], s.gains[at, 0:1, :])
    s.input_grad[...] = s.second_grad_in[...] + part


def backward_body(upper, lower, s):
    ring = Ring()
    local = s.rows.shape[0]
    greet(ring.everyone())
    copies = Copies(s.copy_sem)
    qkv_in = copies(s.qkv_w_in.at[upper], s.qkv_w)
    upper_in = [copies(s.attn_grad_in, s.attn_grad), copies(s.normed1_in, s.normed2)]
    first_in = [copies(s.down_in.at[lower], s.down), copies(s.gate_up_in, s.gate_up)]
    then_in = [copies(s.gu_in.at[lower], s.gu), copies(s.wo_in.at[lower], s.wo)]
    reduce = Reduce(ring, s.reduce)
    work = Work()

    def wait(_):
        for load in upper_in:
            load.wait()

    work.add(wait)
    add_gradient(work, s.mixed, s.attn_grad, s.grad_wo)
    add_gradient(work, s.normed2, s.qkv_grad, s.grad_qkv)
    qkv_in.wait()
    attention_back(upper, s, reduce, work)
    work.do()
    then_in.append(copies(s.normed2_in, s.normed2))
    stores = [copies(s.grad_wo, s.grad_wo_out), copies(s.grad_qkv, s.grad_qkv_out)]
    s.shard[...] = s.input_grad[...].astype(NARROW)
    s.given[...] = s.input_grad[...]
    for load in first_in:
        load.wait()
    width = s.hidden.shape[1]
    tile = 256
    number = width // tile

    def use(indices):
        def one(at):
            rows = chip_rows(chosen(at // number, indices), local)
            start = lax.rem(at, number) * tile
            cols, right = aligned(start, tile), aligned(start + width, tile)
            feed_forward_back(s, rows, cols, right, s.gate_up[rows, cols], s.gate_up[rows, right])

        loop(0, number * len(indices), one)

    Gather(ring, s.shard, s.out_grad, s.first_sems).run(use, work, 0)
    for load in then_in:
        load.wait()
    back_through_feed_forward(lower, s, ring, reduce, work, [])
    stores += [
        copies(s.grad_down, s.grad_down_out), copies(s.grad_gu, s.grad_gu_out),
        copies(s.attn_grad, s.attn_grad_out),
    ]
    for store in stores:
        store.wait()


def backward_between(at, upper, lower, weights, count):
    qkv_w, wo, gu, down, gains = weights
    local, width = upper.rows.shape
    tokens = upper.mixed.shape[0]
    hidden = down.shape[1]
    q_rows = wo.shape[1]
    vmem, dma = pltpu.VMEM, pltpu.SemaphoreType.DMA
    return call_fused(
        "backward_between", functools.partial(backward_body, at, at - 1), 2, 115,
        dict(
            rows=(upper.rows, VMEM), second_grad_in=(upper.second_grad, VMEM),
            qkv_grad=(upper.qkv_grad, VMEM), mixed=(upper.mixed, VMEM), gains=(gains, VMEM),
            attn_grad_in=(upper.attn_grad, HBM), normed1_in=(upper.normed1, HBM),
            second=(lower.second, VMEM), hidden=(lower.hidden, VMEM),
            gate_up_in=(lower.gate_up, HBM), normed2_in=(lower.normed2, HBM),
            qkv_w_in=(qkv_w, HBM), wo_in=(wo, HBM), gu_in=(gu, HBM), down_in=(down, HBM),
        ),
        dict(
            input_grad=(shape_of(local, width, kind=WIDE), VMEM),
            second_grad=(shape_of(local, width, kind=WIDE), VMEM),
            mixed_grad=(shape_of(tokens, q_rows), VMEM),
            attn_grad_out=(shape_of(tokens, width), HBM),
            gain_attn_grad=(shape_of(1, width, kind=WIDE), VMEM),
            gain_mlp_grad=(shape_of(1, width, kind=WIDE), VMEM),
            grad_wo_out=(shape_of(q_rows, width), HBM),
            grad_qkv_out=(shape_of(width, qkv_w.shape[1]), HBM),
            grad_down_out=(shape_of(hidden, width), HBM),
            grad_gu_out=(shape_of(width, 2 * hidden), HBM),
        ),
        dict(
            reduce=reduce_scratch(count, local, width),
            first_sems=gather_scratch(count), gather_sems=gather_scratch(count),
            gu=vmem(gu.shape[1:], NARROW), down=vmem(down.shape[1:], NARROW), wo=vmem(wo.shape[1:], NARROW),
            qkv_w=vmem(qkv_w.shape[1:], NARROW), gate_up=vmem((tokens, 2 * hidden), WIDE),
            out_grad=vmem((tokens, width), NARROW), normed2=vmem((tokens, width), NARROW),
            attn_grad=vmem((tokens, width), NARROW), gu_grad=vmem((tokens, 2 * hidden), NARROW),
            grad_wo=vmem((q_rows, width), NARROW), grad_qkv=vmem((width, qkv_w.shape[1]), NARROW),
            grad_down=vmem((hidden, width), NARROW), grad_gu=vmem((width, 2 * hidden), NARROW),
            given=vmem((local, width), WIDE), normed_grad=vmem((local, width), WIDE),
            shard=vmem((local, width), NARROW), shard2=vmem((local, width), NARROW),
            copy_sem=dma((16,)),
        ),
    )


def gradient_pieces(target, count, refs):
    down, gu, wo, qkv = refs
    depth = down.shape[1] // count
    hidden = down.shape[0]
    cols = aligned(target * depth, depth)
    return (
        down.at[:, cols],
        gu.at[cols, pl.ds(0, hidden)],
        gu.at[cols, pl.ds(hidden, hidden)],
        wo.at[:, cols],
        qkv.at[cols, :],
    )


def owned_pieces(source, refs, sizes):
    down, gate, up, wo, qkv = refs
    return (
        down.at[aligned(source * sizes[0][0], sizes[0][0]), :],
        gate.at[:, aligned(source * sizes[1][1], sizes[1][1])],
        up.at[:, aligned(source * sizes[2][1], sizes[2][1])],
        wo.at[aligned(source * sizes[3][0], sizes[3][0]), :],
        qkv.at[source],
    )


GRADS, FEED_GRADS = 5, 3


class Return:
    def __init__(self, ring, partial, outs, landed, mine, sems):
        self.ring = ring
        self.layer = lax.axis_index(SECTION)
        self.across = {SECTION: 1 - self.layer}
        peers, self.origins = partners(ring.me, ring.count)
        self.order = [*peers, ring.me]
        self.partial, self.outs, self.landed, self.mine = partial, outs, landed, mine
        self.cross_send, self.cross_recv, self.load_sem, self.send, self.recv, self.own_sem = sems
        self.sizes = [ref.shape[1:] for ref in mine]
        self.crossing, self.loads, self.sends, self.events = {}, {}, [], []

    def cross(self, kinds):
        count = self.ring.count
        for kind in kinds:
            for k, owner in enumerate(self.order):
                pieces = [gradient_pieces(owner, count, refs)[kind] for refs in self.partial]
                for at in range(2):
                    copy = remote(
                        pieces[1 - at], self.landed[kind].at[k],
                        self.cross_send.at[kind, k], self.cross_recv.at[kind, k], self.across,
                    )
                    load = pltpu.make_async_copy(
                        pieces[at], self.mine[kind].at[k], self.load_sem.at[kind, k]
                    )

                    @pl.when(self.layer == at)
                    def _():
                        copy.start()
                        load.start()

                self.crossing[kind, k], self.loads[kind, k] = copy, load
                self.events.append((kind, k))

    def some(self, number):
        for kind, k in self.events[:number]:
            self.loads[kind, k].wait()
            self.crossing[kind, k].wait_recv()
            mine = self.mine[kind]
            total = mine[k].astype(WIDE) + self.landed[kind][k].astype(WIDE)
            mine[k] = total.astype(NARROW)
            target = owned_pieces(self.ring.me, self.outs, self.sizes)[kind]
            if k < self.ring.count - 1:
                copy = remote(
                    mine.at[k], target, self.send.at[kind, k], self.recv.at[kind, k],
                    {DP: self.order[k]},
                )
            else:
                copy = pltpu.make_async_copy(mine.at[k], target, self.own_sem.at[kind])
            copy.start()
            self.sends.append((k, copy))
        self.events = self.events[number:]

    def finish(self):
        for copy in self.crossing.values():
            copy.wait_send()
        for k, copy in self.sends:
            if k < self.ring.count - 1:
                copy.wait_send()
            else:
                copy.wait()
        for kind in range(GRADS):
            for k in range(self.ring.count - 1):
                here = owned_pieces(self.origins[k], self.outs, self.sizes)[kind]
                remote(
                    self.mine[kind].at[k], here, self.send.at[kind, k], self.recv.at[kind, k],
                    {DP: self.origins[k]},
                ).wait_recv()


def closing_body(at, s):
    ring = Ring()
    layer = lax.axis_index(SECTION)
    count = ring.count
    everyone = 4 * count
    this = (layer * count + ring.me) * 2 + ring.core

    def device(k):
        other = lax.rem(this + k, everyone)
        return {SECTION: other // (2 * count), DP: lax.rem(other // 2, count), TENSOR: lax.rem(other, 2)}

    greet([device(k) for k in range(1, everyone)])
    copies = Copies(s.copy_sem)
    qkv_in = copies(s.qkv_w_in.at[at], s.qkv_w)
    ins = [copies(s.attn_grad_in, s.attn_grad), copies(s.normed1_in, s.normed1)]
    rows_in = copies(s.inputs.at[layer], s.rows)
    back = Return(
        ring,
        ((s.down0, s.gu0, s.grad_wo, s.grad_qkv), (s.down1, s.gu1, s.wo1, s.qkv1)),
        (s.down_out, s.gate_out, s.up_out, s.wo_out, s.qkv_out), s.landed, s.mine, s.back_sems,
    )
    back.cross(range(FEED_GRADS))

    swap_send, swap_recv = s.swap_sems
    swaps = []

    def swap(which, out, values):
        for section in range(2):
            copy = remote(
                values[1 - section], out.at[section], swap_send.at[which], swap_recv.at[which],
                {SECTION: 1 - layer},
            )
            own = pltpu.make_async_copy(values[section], out.at[section], s.own_sems.at[which])

            @pl.when(layer == section)
            def _():
                copy.start()
                own.start()

        swaps.append((copy, own))

    swap(0, s.results, (s.result0, s.result1))
    attend_back_here(
        s.slots, s.mixed_grad, s.kept, s.lse, s.cosine, s.sine, s.by_number, s.key2, s.value2,
        s.key_sum, s.value_sum,
    )
    put_back(s.by_number, s.qkv_grad, s.row)
    work = Work()
    for load in ins:
        load.wait()
    add_gradient(work, s.mixed, s.attn_grad, s.grad_wo)
    add_gradient(work, s.normed1, s.qkv_grad, s.grad_qkv)
    qkv_in.wait()
    rows_in.wait()

    def rest():
        work.do()
        back.cross(range(FEED_GRADS, GRADS))
        back.some(1)

    beside = [functools.partial(back.some, 1)] * 2 + [rest] + [functools.partial(back.some, 1)] * (ring.far - 3)
    attention_back(at, s, Reduce(ring, s.reduce), work, beside)
    swap(1, s.input_grads, (s.input_grad, s.input_grad1))

    lanes = s.gain_out.shape[1]
    for section, (attn, mlp) in enumerate(((s.gain_attn_grad, s.gain_mlp0), (s.gain_attn1, s.gain_mlp1))):
        for owner in range(2 * count):
            s.gain_in[section * 2 * count + owner] = jnp.zeros_like(s.gain_out)
            cols = slice(owner * lanes, (owner + 1) * lanes)
            s.gain_in[section * 2 * count + owner, 0:1, :] = attn[:, cols]
            s.gain_in[section * 2 * count + owner, 1:2, :] = mlp[:, cols]
    gain_send, gain_recv = s.gain_sems
    gain_copies = []
    for k in range(1, everyone):
        copy = remote(
            s.gain_in.at[lax.rem(this + k, everyone)], s.gain_landed.at[k - 1],
            gain_send.at[k - 1], gain_recv.at[k - 1], device(k),
        )
        copy.start()
        gain_copies.append(copy)
    back.some(len(back.events))
    total = s.gain_in[this]
    for k, copy in enumerate(gain_copies):
        copy.wait_recv()
        total = total + s.gain_landed[k]
    s.gain_out[...] = total
    for copy in gain_copies:
        copy.wait_send()
    for copy, own in swaps:
        copy.wait()
        own.wait()
    back.finish()


def closing(at, known, inputs, first, last, feed0, grads1, gains_of, weights, count):
    qkv_w, _, _, _, gains = weights
    local, width = inputs.shape[1:]
    tokens = first.mixed.shape[0]
    head = first.mixed.shape[1] // 2
    down0, gu0 = feed0
    down1, gu1, wo1, qkv1 = grads1
    hidden, q_rows, qkv_rows = down0.shape[0], wo1.shape[0], qkv1.shape[1]
    depth = width // count
    sizes = [(hidden, depth), (depth, hidden), (depth, hidden), (q_rows, depth), (depth, qkv_rows)]
    everyone = 4 * count
    lanes = width // (2 * count)
    vmem, dma = pltpu.VMEM, pltpu.SemaphoreType.DMA
    pieces = lambda: [vmem((count, *size), NARROW) for size in sizes]
    return call_fused(
        "closing", functools.partial(closing_body, at), 3, 210,
        dict(
            **known, inputs=(inputs, HBM), gains=(gains, VMEM), qkv_w_in=(qkv_w, HBM),
            second_grad_in=(first.second_grad, VMEM), mixed_grad=(first.mixed_grad, VMEM),
            mixed=(first.mixed, VMEM), kept=(first.kept, VMEM), lse=(first.lse, VMEM),
            attn_grad_in=(first.attn_grad, HBM), normed1_in=(first.normed1, HBM),
            result0=(first.result, VMEM), result1=(last.result, VMEM),
            input_grad1=(last.input_grad, VMEM),
            down0=(down0, HBM), gu0=(gu0, HBM),
            down1=(down1, HBM), gu1=(gu1, HBM), wo1=(wo1, HBM), qkv1=(qkv1, HBM),
            gain_mlp0=(gains_of[0], VMEM), gain_attn1=(gains_of[1], VMEM), gain_mlp1=(gains_of[2], VMEM),
        ),
        dict(
            results=(shape_of(2, local, width, kind=WIDE), HBM),
            input_grads=(shape_of(2, local, width, kind=WIDE), HBM),
            down_out=(shape_of(count * hidden, depth), HBM),
            gate_out=(shape_of(depth, count * hidden), HBM),
            up_out=(shape_of(depth, count * hidden), HBM),
            wo_out=(shape_of(count * q_rows, depth), HBM),
            qkv_out=(shape_of(count, depth, qkv_rows), HBM),
            gain_out=(shape_of(8, lanes, kind=WIDE), VMEM),
        ),
        dict(
            reduce=reduce_scratch(count, local, width),
            qkv_w=vmem(qkv_w.shape[1:], NARROW), rows=vmem((local, width), WIDE),
            attn_grad=vmem((tokens, width), NARROW), normed1=vmem((tokens, width), NARROW),
            qkv_grad=vmem((tokens, 4 * head), NARROW),
            grad_wo=vmem((q_rows, width), NARROW), grad_qkv=vmem((width, qkv_rows), NARROW),
            normed_grad=vmem((local, width), WIDE), input_grad=vmem((local, width), WIDE),
            gain_attn_grad=vmem((1, width), WIDE),
            landed=pieces(), mine=pieces(),
            gain_in=vmem((everyone, 8, lanes), WIDE), gain_landed=vmem((everyone - 1, 8, lanes), WIDE),
            **attend_scratch(tokens, head, True),
            back_sems=[
                dma((GRADS, count)), dma((GRADS, count)), dma((GRADS, count)),
                dma((GRADS, count - 1)), dma((GRADS, count - 1)), dma((GRADS,)),
            ],
            gain_sems=[dma((everyone - 1,)), dma((everyone - 1,))],
            swap_sems=[dma((2,)), dma((2,))], own_sems=dma((2,)),
            copy_sem=dma((8,)),
        ),
    )


def fast_shards(inputs, table, cotangent, wq, wk, wv, wo, w_gate, w_up, w_down, gain_attn, gain_mlp):
    count = lax.axis_size(DP)
    parts = lax.axis_size(TENSOR)
    head = HEAD_SIZE
    section = lax.axis_index(SECTION)
    block = inputs.shape[1] * parts
    depth = wq.shape[1]
    q_cols = wq.shape[2] // count

    row = lax.dynamic_index_in_dim(table, section, 0, keepdims=False)
    ids = jnp.arange(count, dtype=jnp.int32)
    slots = jnp.sum(jnp.where(row[None, :] == ids[:, None], ids[None, :], 0), axis=1)
    cosine, sine = rope_tables(count // 2 * block, head)
    qkv_t = jnp.concatenate([wq[0], wk[0], wv[0]], axis=1).T
    s = opening(
        slots, row, cosine, sine, inputs, cotangent, qkv_t, wo, w_gate, w_up, w_down,
        gain_attn, gain_mlp, count, head,
    )
    weights = (s.out_qkv, s.out_wo, s.out_gu, s.out_down, s.gains)
    known = dict(
        slots=(slots, SMEM), row=(row, SMEM), cosine=(cosine, VMEM), sine=(sine, VMEM)
    )
    top = turn(
        1, known, s.result, s.mixed1, s.kept1, s.lse1, s.out_grad_out, cotangent, weights, count
    )
    upper = Names(
        rows=s.result, second_grad=top.second_grad, qkv_grad=top.qkv_grad, mixed=s.mixed1,
        attn_grad=top.attn_grad_out, normed1=s.next_normed1_out,
    )
    lower = Names(
        second=s.second, hidden=s.hidden, gate_up=s.gate_up_out, normed2=s.normed2_out
    )
    back = backward_between(1, upper, lower, weights, count)
    first = Names(
        second_grad=back.second_grad, mixed_grad=back.mixed_grad, mixed=s.mixed0, kept=s.kept0,
        lse=s.lse0, attn_grad=back.attn_grad_out, normed1=s.normed1_out, result=s.result,
    )
    last = Names(result=top.result, input_grad=back.input_grad)
    end = closing(
        0, known, inputs, first, last,
        (back.grad_down_out, back.grad_gu_out),
        (top.grad_down_out, top.grad_gu_out, back.grad_wo_out, back.grad_qkv_out),
        (back.gain_mlp_grad, back.gain_attn_grad, top.gain_mlp_grad),
        weights, count,
    )
    grad_wq = end.qkv_out[:, :, :q_cols].astype(WIDE).transpose(1, 0, 2).reshape(depth, -1)
    shared = count * head // wk.shape[2]
    joined = end.qkv_out[:, :, q_cols:].astype(WIDE).reshape(count // shared, shared, depth, 2, head)
    joined = jnp.sum(joined, axis=1)
    grad_wk = joined[:, :, 0].transpose(1, 0, 2).reshape(depth, -1)
    grad_wv = joined[:, :, 1].transpose(1, 0, 2).reshape(depth, -1)
    wide = lambda value: value.astype(WIDE)[None]
    return (
        end.results[None],
        end.input_grads[None],
        grad_wq[None],
        grad_wk[None],
        grad_wv[None],
        wide(end.wo_out),
        wide(end.gate_out),
        wide(end.up_out),
        wide(end.down_out),
        end.gain_out[:1],
        end.gain_out[1:2],
    )


def fits(mesh, inputs, table, cotangent, wq, wk, wv, wo, w_gate, w_up, w_down, gain_attn, gain_mlp):
    sections, count, parts = (mesh.shape[axis] for axis in (SECTION, DP, TENSOR))
    head = HEAD_SIZE
    if sections != 2 or parts != 2 or inputs.shape[0] != sections or count % 4 or count < 8:
        return False
    devices = count * parts
    queries, keys = wq.shape[2] // head, wk.shape[2] // head
    if queries != 2 * devices or devices % keys or keys % parts or 4 * head != 256:
        return False
    return (
        wq.shape[1] % (128 * count) == 0
        and wq.shape[1] % 512 == 0
        and w_gate.shape[2] % (256 * devices) == 0
        and inputs.shape[1] % (64 * devices) == 0
    )


def shards(mesh, whole, *args):
    if fits(mesh, *whole):
        return fast_shards(*args)
    return general_shards(*args)


def solution(mesh):
    in_specs = (
        P(None, (DP, TENSOR), None),
        P(),
        P(None, (DP, TENSOR), None),
        P(SECTION, DP, TENSOR),
        P(SECTION, DP, TENSOR),
        P(SECTION, DP, TENSOR),
        P(SECTION, TENSOR, DP),
        P(SECTION, DP, TENSOR),
        P(SECTION, DP, TENSOR),
        P(SECTION, TENSOR, DP),
        P(SECTION, DP),
        P(SECTION, DP),
    )
    out_specs = (
        P(SECTION, None, (DP, TENSOR), None),
        P(SECTION, None, (DP, TENSOR), None),
        P(SECTION, DP, TENSOR),
        P(SECTION, DP, TENSOR),
        P(SECTION, DP, TENSOR),
        P(SECTION, TENSOR, DP),
        P(SECTION, DP, TENSOR),
        P(SECTION, DP, TENSOR),
        P(SECTION, TENSOR, DP),
        P(SECTION, (DP, TENSOR)),
        P(SECTION, (DP, TENSOR)),
    )

    def step(*args):
        return jax.shard_map(
            functools.partial(shards, mesh, args),
            mesh=mesh,
            in_specs=in_specs,
            out_specs=out_specs,
            check_vma=False,
        )(*args)

    return step
```

```python
import functools
import math

import jax
import jax.numpy as jnp
from jax import lax
from jax.experimental import pallas as pl
from jax.experimental.pallas import tpu as pltpu
from jax.sharding import PartitionSpec as P

HEAD_SIZE = 64
SECTION, DP, TENSOR = "section", "dp", "tensor"


epsilon = 1e-05


def passed_along(value, axis, steps):
    count = lax.axis_size(axis)
    initial, last = (max(0, -steps), min(count, count - steps))
    return lax.ppermute(value, axis, [(source, source + steps) for source in range(initial, last)])


def rope_frequencies(head):
    index = jnp.arange(head // 2, dtype=jnp.float32)
    base = 1.0 / 500000.0 ** (index * 2.0 / head)
    wavelength = 2.0 * math.pi / base
    blend = (8192.0 / wavelength - 1.0) / 3.0
    middle = (1.0 - blend) * base / 32.0 + blend * base
    return jnp.where(wavelength < 2048.0, base, jnp.where(wavelength > 8192.0, base / 32.0, middle))


def rotate(values, positions, head):
    step_count = values.shape[0]
    shaped = values.reshape(step_count, -1, head)
    angle = positions.astype(jnp.float32)[:, None] * rope_frequencies(head)[None, :]
    cosine = jnp.cos(angle)[:, None, :]
    sine = jnp.sin(angle)[:, None, :]
    first = shaped[:, :, : head // 2]
    second = shaped[:, :, head // 2 :]
    return jnp.concatenate(
        [first * cosine - second * sine, second * cosine + first * sine], axis=-1
    ).reshape(step_count, -1)


def unrotate(values, positions, head):
    step_count = values.shape[0]
    shaped = values.reshape(step_count, -1, head)
    angle = positions.astype(jnp.float32)[:, None] * rope_frequencies(head)[None, :]
    cosine = jnp.cos(angle)[:, None, :]
    sine = jnp.sin(angle)[:, None, :]
    first = shaped[:, :, : head // 2]
    second = shaped[:, :, head // 2 :]
    return jnp.concatenate(
        [first * cosine + second * sine, second * cosine - first * sine], axis=-1
    ).reshape(step_count, -1)


def norm_stats(rows):
    inverse = lax.rsqrt(jnp.mean(rows * rows, axis=-1, keepdims=True) + epsilon)
    return (rows * inverse, inverse)


def norm_back(grad, unit, inverse, gain):
    scaled = grad * gain
    inner = jnp.mean(scaled * unit, axis=-1, keepdims=True)
    return (inverse * (scaled - unit * inner), jnp.sum(grad * unit, axis=0))


def matmul(left, right):
    return jnp.dot(left, right, preferred_element_type=jnp.float32)


def block_layout(table, micro, groups, block):
    layout_row = lax.dynamic_index_in_dim(table, micro, 0, keepdims=False)
    span = groups // 2
    mine = lax.dynamic_index_in_dim(layout_row, lax.axis_index(DP), 0, keepdims=False)
    sequence = mine // span
    place = mine % span
    slot_ids = jnp.arange(groups, dtype=jnp.int32)
    holder = jnp.sum(
        jnp.where(layout_row[None, :] == slot_ids[:, None], slot_ids[None, :], 0), axis=1
    )
    slots = lax.dynamic_slice_in_dim(holder, sequence * span, span)
    positions = place * block + jnp.arange(block, dtype=jnp.int32)
    return (slots, positions)


def attend(query_rows, key_seq, value_seq, positions, heads_kv, head):
    step_count = query_rows.shape[0]
    keys_total = key_seq.shape[0]
    head_group = query_rows.shape[1] // (heads_kv * head)
    scale = 1.0 / math.sqrt(head)
    allowed = jnp.arange(keys_total, dtype=jnp.int32)[None, :] <= positions[:, None]
    query_layers = query_rows.reshape(step_count, heads_kv, head_group * head).transpose(1, 0, 2)
    key_layers = key_seq.reshape(keys_total, heads_kv, head).transpose(1, 0, 2)
    value_layers = value_seq.reshape(keys_total, heads_kv, head).transpose(1, 0, 2)

    def one_head(parts):
        q_head, k_head, v_head = parts
        q_three = q_head.reshape(step_count, head_group, head)
        scores = (
            jnp.einsum("qgd,kd->gqk", q_three, k_head, preferred_element_type=jnp.float32) * scale
        )
        total = jnp.sum(jnp.where(allowed, jnp.exp(scores), 0.0), axis=-1)
        log_total = jnp.log(total)
        probs = jnp.where(allowed, jnp.exp(scores - log_total[..., None]), 0.0).astype(jnp.bfloat16)
        mixed = jnp.einsum("gqk,kd->qgd", probs, v_head, preferred_element_type=jnp.float32).astype(
            jnp.bfloat16
        )
        return (mixed.reshape(step_count, head_group * head), log_total)

    mixed, log_total = lax.map(one_head, (query_layers, key_layers, value_layers))
    return (mixed.transpose(1, 0, 2).reshape(step_count, -1), log_total)


def attend_back(
    blended_gradient, query_rows, key_seq, value_seq, log_total, positions, heads_kv, head
):
    step_count = query_rows.shape[0]
    keys_total = key_seq.shape[0]
    head_group = query_rows.shape[1] // (heads_kv * head)
    scale = 1.0 / math.sqrt(head)
    allowed = jnp.arange(keys_total, dtype=jnp.int32)[None, :] <= positions[:, None]
    query_layers = query_rows.reshape(step_count, heads_kv, head_group * head).transpose(1, 0, 2)
    key_layers = key_seq.reshape(keys_total, heads_kv, head).transpose(1, 0, 2)
    value_layers = value_seq.reshape(keys_total, heads_kv, head).transpose(1, 0, 2)
    gain_layers = blended_gradient.reshape(step_count, heads_kv, head_group * head).transpose(
        1, 0, 2
    )

    def one_head(parts):
        q_head, k_head, v_head, g_head, l_head = parts
        q_three = q_head.reshape(step_count, head_group, head)
        g_three = g_head.reshape(step_count, head_group, head)
        scores = (
            jnp.einsum("qgd,kd->gqk", q_three, k_head, preferred_element_type=jnp.float32) * scale
        )
        probs = jnp.where(allowed, jnp.exp(scores - l_head[..., None]), 0.0)
        rounded = probs.astype(jnp.bfloat16)
        prob_grad = jnp.einsum("qgd,kd->gqk", g_three, v_head, preferred_element_type=jnp.float32)
        value_total_sum = jnp.einsum(
            "gqk,qgd->kd", rounded, g_three, preferred_element_type=jnp.float32
        )
        rowdot = jnp.sum(probs * prob_grad, axis=-1, keepdims=True)
        score_grad = (probs * (prob_grad - rowdot) * scale).astype(jnp.bfloat16)
        query_grad = jnp.einsum(
            "gqk,kd->qgd", score_grad, k_head, preferred_element_type=jnp.float32
        )
        key_gradient = jnp.einsum(
            "gqk,qgd->kd", score_grad, q_three, preferred_element_type=jnp.float32
        )
        return (query_grad.reshape(step_count, head_group * head), key_gradient, value_total_sum)

    query_grad, key_gradient, value_total_sum = lax.map(
        one_head, (query_layers, key_layers, value_layers, gain_layers, log_total)
    )
    query_grad = query_grad.transpose(1, 0, 2).reshape(step_count, -1)
    key_gradient = key_gradient.transpose(1, 0, 2).reshape(keys_total, -1)
    value_total_sum = value_total_sum.transpose(1, 0, 2).reshape(keys_total, -1)
    return (query_grad, key_gradient, value_total_sum)


def layer_forward(rows, table, micro, weights, groups, heads_kv, head):
    wq, wk, wv, wo, w_gate, w_up, w_down, gain_attn, gain_mlp = weights
    full = lax.all_gather(rows, TENSOR, axis=0, tiled=True)
    block = full.shape[0]
    slots, positions = block_layout(table, micro, groups, block)
    unit1, inverse1 = norm_stats(full)
    normed1 = (unit1 * gain_attn.astype(jnp.float32)).astype(jnp.bfloat16)
    query_rows = rotate(matmul(normed1, wq), positions, head).astype(jnp.bfloat16)
    key = rotate(matmul(normed1, wk), positions, head).astype(jnp.bfloat16)
    value_rows = matmul(normed1, wv).astype(jnp.bfloat16)
    key_all, value_all = (
        lax.all_gather(key, DP, axis=0, tiled=True),
        lax.all_gather(value_rows, DP, axis=0, tiled=True),
    )
    kv_width = key.shape[1]
    key_seq = key_all.reshape(groups, block, kv_width)[slots].reshape(-1, kv_width)
    value_seq = value_all.reshape(groups, block, kv_width)[slots].reshape(-1, kv_width)
    mixed, log_total = attend(query_rows, key_seq, value_seq, positions, heads_kv, head)
    second = rows + lax.psum_scatter(matmul(mixed, wo), TENSOR, scatter_dimension=0, tiled=True)
    full_second = lax.all_gather(second, TENSOR, axis=0, tiled=True)
    unit2, inverse2 = norm_stats(full_second)
    normed2 = (unit2 * gain_mlp.astype(jnp.float32)).astype(jnp.bfloat16)
    gate = matmul(normed2, w_gate)
    upper = matmul(normed2, w_up)
    hidden = (jax.nn.silu(gate) * upper).astype(jnp.bfloat16)
    result = second + lax.psum_scatter(
        matmul(hidden, w_down), TENSOR, scatter_dimension=0, tiled=True
    )
    return (
        result,
        (
            full,
            query_rows,
            key_seq,
            value_seq,
            mixed,
            log_total,
            full_second,
            gate,
            upper,
            hidden,
            slots,
            positions,
        ),
    )


def layer_backward(grad_rows, context, weights, groups, parts, heads_kv, head):
    wq, wk, wv, wo, w_gate, w_up, w_down, gain_attn, gain_mlp = weights
    (
        full,
        query_rows,
        key_seq,
        value_seq,
        mixed,
        log_total,
        full_second,
        gate,
        upper,
        hidden,
        slots,
        positions,
    ) = context
    block = full.shape[0]
    out_grad = lax.all_gather(grad_rows.astype(jnp.bfloat16), TENSOR, axis=0, tiled=True)
    grad_down = matmul(hidden.T, out_grad)
    hidden_grad = matmul(out_grad, w_down.T)
    sigma = jax.nn.sigmoid(gate)
    gate_grad = (hidden_grad * upper * sigma * (1.0 + gate * (1.0 - sigma))).astype(jnp.bfloat16)
    up_grad = (hidden_grad * gate * sigma).astype(jnp.bfloat16)
    unit2, inverse2 = norm_stats(full_second)
    normed2 = (unit2 * gain_mlp.astype(jnp.float32)).astype(jnp.bfloat16)
    grad_gate = matmul(normed2.T, gate_grad)
    grad_up = matmul(normed2.T, up_grad)
    normed2_grad = matmul(gate_grad, w_gate.T) + matmul(up_grad, w_up.T)
    second_terms, gain_mlp_terms = norm_back(
        normed2_grad, unit2, inverse2, gain_mlp.astype(jnp.float32)
    )
    piece_width = gain_mlp_terms.shape[0] // (groups * parts)
    second_part, gain_mlp_part = (
        lax.psum_scatter(
            second_terms.astype(jnp.bfloat16), TENSOR, scatter_dimension=0, tiled=True
        ).astype(jnp.float32),
        lax.psum_scatter(
            gain_mlp_terms.reshape(groups, parts, piece_width).astype(jnp.bfloat16),
            TENSOR,
            scatter_dimension=1,
            tiled=True,
        ).astype(jnp.float32),
    )
    second_grad = grad_rows + second_part
    attn_grad = lax.all_gather(second_grad.astype(jnp.bfloat16), TENSOR, axis=0, tiled=True)
    grad_wo = matmul(mixed.T, attn_grad)
    blended_gradient = matmul(attn_grad, wo.T).astype(jnp.bfloat16)
    query_grad, key_seq_grad, value_seq_grad = attend_back(
        blended_gradient, query_rows, key_seq, value_seq, log_total, positions, heads_kv, head
    )
    kv_width = key_seq.shape[1]
    key_spread = (
        jnp.zeros((groups, block, kv_width), jnp.float32)
        .at[slots]
        .set(key_seq_grad.reshape(-1, block, kv_width))
    )
    value_spread = (
        jnp.zeros((groups, block, kv_width), jnp.float32)
        .at[slots]
        .set(value_seq_grad.reshape(-1, block, kv_width))
    )
    key_own, value_own = (
        lax.psum_scatter(
            key_spread.astype(jnp.bfloat16), DP, scatter_dimension=0, tiled=True
        ).astype(jnp.float32),
        lax.psum_scatter(
            value_spread.astype(jnp.bfloat16), DP, scatter_dimension=0, tiled=True
        ).astype(jnp.float32),
    )
    query_round = unrotate(query_grad, positions, head).astype(jnp.bfloat16)
    key_round = unrotate(key_own.reshape(block, kv_width), positions, head).astype(jnp.bfloat16)
    value_round = value_own.reshape(block, kv_width).astype(jnp.bfloat16)
    unit1, inverse1 = norm_stats(full)
    normed1 = (unit1 * gain_attn.astype(jnp.float32)).astype(jnp.bfloat16)
    grad_wq = matmul(normed1.T, query_round)
    grad_wk = matmul(normed1.T, key_round)
    grad_wv = matmul(normed1.T, value_round)
    normed1_grad = matmul(query_round, wq.T) + matmul(key_round, wk.T) + matmul(value_round, wv.T)
    first_terms, gain_attn_terms = norm_back(
        normed1_grad, unit1, inverse1, gain_attn.astype(jnp.float32)
    )
    first_part, gain_attn_part = (
        lax.psum_scatter(first_terms, TENSOR, scatter_dimension=0, tiled=True),
        lax.psum_scatter(
            gain_attn_terms.reshape(groups, parts, piece_width),
            TENSOR,
            scatter_dimension=1,
            tiled=True,
        ),
    )
    input_grad = second_grad + first_part
    return (
        input_grad,
        (
            grad_wq,
            grad_wk,
            grad_wv,
            grad_wo,
            grad_gate,
            grad_up,
            grad_down,
            gain_attn_part,
            gain_mlp_part,
        ),
    )


def reduce_grads(pieces):
    return (
        lax.psum_scatter(
            pieces[0].astype(jnp.bfloat16), DP, scatter_dimension=0, tiled=True
        ).astype(jnp.float32),
        lax.psum_scatter(
            pieces[1].astype(jnp.bfloat16), DP, scatter_dimension=0, tiled=True
        ).astype(jnp.float32),
        lax.psum_scatter(
            pieces[2].astype(jnp.bfloat16), DP, scatter_dimension=0, tiled=True
        ).astype(jnp.float32),
        lax.psum_scatter(
            pieces[3].astype(jnp.bfloat16), DP, scatter_dimension=1, tiled=True
        ).astype(jnp.float32),
        lax.psum_scatter(
            pieces[4].astype(jnp.bfloat16), DP, scatter_dimension=0, tiled=True
        ).astype(jnp.float32),
        lax.psum_scatter(
            pieces[5].astype(jnp.bfloat16), DP, scatter_dimension=0, tiled=True
        ).astype(jnp.float32),
        lax.psum_scatter(
            pieces[6].astype(jnp.bfloat16), DP, scatter_dimension=1, tiled=True
        ).astype(jnp.float32),
        lax.psum_scatter(
            pieces[7].astype(jnp.bfloat16), DP, scatter_dimension=0, tiled=True
        ).astype(jnp.float32),
        lax.psum_scatter(
            pieces[8].astype(jnp.bfloat16), DP, scatter_dimension=0, tiled=True
        ).astype(jnp.float32),
    )


def general_shards(inputs, table, cotangent, wq, wk, wv, wo, w_gate, w_up, w_down, gain_attn, gain_mlp):
    groups = lax.axis_size(DP)
    parts = lax.axis_size(TENSOR)
    micro_count = inputs.shape[0]
    section = lax.axis_index(SECTION)
    first_section = section == 0
    weights = (
        lax.all_gather(wq[0], DP, axis=0, tiled=True),
        lax.all_gather(wk[0], DP, axis=0, tiled=True),
        lax.all_gather(wv[0], DP, axis=0, tiled=True),
        lax.all_gather(wo[0], DP, axis=1, tiled=True),
        lax.all_gather(w_gate[0], DP, axis=0, tiled=True),
        lax.all_gather(w_up[0], DP, axis=0, tiled=True),
        lax.all_gather(w_down[0], DP, axis=1, tiled=True),
        lax.all_gather(gain_attn[0], DP, axis=0, tiled=True),
        lax.all_gather(gain_mlp[0], DP, axis=0, tiled=True),
    )
    head = HEAD_SIZE
    heads_kv = wk.shape[2] // head
    received = jnp.zeros_like(inputs[0])
    produced = []
    saved = []
    for step in range(micro_count + 1):
        own_rows = inputs[step] if step < micro_count else jnp.zeros_like(inputs[0])
        start_rows = jnp.where(first_section, own_rows, received)
        micro = jnp.clip(step - section, 0, micro_count - 1)
        result, context = layer_forward(start_rows, table, micro, weights, groups, heads_kv, head)
        produced.append(result)
        saved.append(context)
        if step < micro_count:
            received = passed_along(result, SECTION, 1)
    stacked = jnp.stack(produced)
    outputs = jnp.where(first_section, stacked[:micro_count], stacked[1:])[None]
    returned = jnp.zeros_like(inputs[0])
    returned_list = []
    totals = None
    for step in range(micro_count + 1):
        index = micro_count - 1 - step
        given = cotangent[index] if index >= 0 else jnp.zeros_like(cotangent[0])
        start_grad = jnp.where(first_section, returned, given)
        din, pieces = layer_backward(
            start_grad, saved[micro_count - step], weights, groups, parts, heads_kv, head
        )
        returned_list.append(din)
        if step < micro_count:
            returned = passed_along(din.astype(jnp.bfloat16), SECTION, -1).astype(din.dtype)
        totals = (
            pieces
            if totals is None
            else tuple((left + right for left, right in zip(totals, pieces)))
        )
    totals = reduce_grads(totals)
    reverse_stack = jnp.stack(returned_list[::-1])
    input_grad = jnp.where(first_section, reverse_stack[:micro_count], reverse_stack[1:])[None]
    (
        grad_wq,
        grad_wk,
        grad_wv,
        grad_wo,
        grad_gate,
        grad_up,
        grad_down,
        gain_attn_sum,
        gain_mlp_sum,
    ) = totals
    width_piece = gain_attn_sum.shape[-1]
    return (
        outputs,
        input_grad,
        grad_wq[None],
        grad_wk[None],
        grad_wv[None],
        grad_wo[None],
        grad_gate[None],
        grad_up[None],
        grad_down[None],
        gain_attn_sum.reshape(1, width_piece),
        gain_mlp_sum.reshape(1, width_piece),
    )


MESH = pl.DeviceIdType.MESH
SUBS = 4
HBM = pl.BlockSpec(memory_space=pl.ANY)
VMEM = pl.BlockSpec(memory_space=pltpu.VMEM)
SMEM = pl.BlockSpec(memory_space=pltpu.SMEM)
NARROW, WIDE = jnp.bfloat16, jnp.float32


def ring_place(index, count):
    return jnp.where(lax.rem(index, 2) == 0, index // 2, count - (index + 1) // 2)


def ring_index(place, count):
    place = lax.rem(place + 2 * count, count)
    return jnp.where(place < count // 2, 2 * place, 2 * count - 1 - 2 * place)


def greet(others):
    barrier = pltpu.get_barrier_semaphore()
    for other in others:
        pl.semaphore_signal(barrier, inc=1, device_id=other, device_id_type=MESH)
    pl.semaphore_wait(barrier, len(others))


def remote(source, target, send, recv, device):
    return pltpu.make_async_remote_copy(
        source, target, send, recv, device_id=device, device_id_type=MESH
    )


def partners(me, count):
    half = count // 2
    side, inside = me // half, lax.rem(me, half)
    peers = [(1 - side) * half + lax.rem(inside + k, half) for k in range(half)]
    peers += [side * half + lax.rem(inside + k, half) for k in range(1, half)]
    origins = [(1 - side) * half + lax.rem(inside + half - k, half) for k in range(half)]
    origins += [side * half + lax.rem(inside + half - k, half) for k in range(1, half)]
    return peers, origins


def aligned(start, size):
    return pl.ds(pl.multiple_of(start, size), size)


def tiles(size, tile):
    return [slice(at, at + tile) for at in range(0, size, tile)]


def loop(start, stop, body):
    if stop - start == 1:
        body(start)
    elif stop > start:

        def step(at, carry):
            body(at)
            return carry

        lax.fori_loop(start, stop, step, 0)


def dot(left, right, contract):
    return lax.dot_general(
        left, right, (contract, ((), ())), preferred_element_type=jnp.float32
    )


class Names:
    def __init__(self, **values):
        self.__dict__.update(values)


class Work:
    def __init__(self):
        self.items = []

    def add(self, body, count=1):
        self.items.append((body, 0, count))

    def first(self, body):
        self.items.insert(0, (body, 0, 1))

    def do(self, some=1 << 20):
        while some > 0 and self.items:
            body, start, stop = self.items.pop(0)
            until = min(stop, start + some)
            loop(start, until, body)
            some -= until - start
            if until < stop:
                self.items.insert(0, (body, until, stop))


class Copies:
    def __init__(self, sem):
        self.sem = sem
        self.used = 0

    def __call__(self, source, target):
        copy = pltpu.make_async_copy(source, target, self.sem.at[self.used])
        self.used += 1
        copy.start()
        return copy


class Ring:
    def __init__(self):
        self.count = lax.axis_size(DP)
        self.far = self.count // 2
        self.me = lax.axis_index(DP)
        self.core = lax.axis_index(TENSOR)
        self.place = ring_place(self.me, self.count)
        self.near = tuple({DP: ring_index(self.place + step, self.count)} for step in (1, -1))
        self.side = {TENSOR: 1 - self.core}

    def everyone(self):
        return [*self.near, self.side]

    def index(self, steps):
        return ring_index(self.place + steps, self.count)

    def orders(self):
        for k in range(SUBS):
            yield k, 0
            yield SUBS - 1 - k, 1


def gather_scratch(count):
    far = count // 2
    dma = pltpu.SemaphoreType.DMA
    return [
        dma((2, far, SUBS)), dma((2, far, SUBS)), dma((count, SUBS)), dma((count, SUBS)), dma((1,))
    ]


class Gather:
    def __init__(self, ring, x_ref, o_ref, sems):
        self.ring = ring
        self.x_ref, self.o_ref = x_ref, o_ref
        self.ring_send, self.ring_recv, self.side_send, self.side_recv, self.own_sem = sems
        self.rows = x_ref.shape[0]
        self.piece = self.rows // SUBS
        self.sends = []

    def spot(self, steps, sub, core):
        start = (self.ring.index(steps) * 2 + core) * self.rows + sub * self.piece
        return self.o_ref.at[aligned(start, self.piece), :]

    def mine(self, steps, sub):
        if steps == 0:
            return self.x_ref.at[sub * self.piece : (sub + 1) * self.piece, :]
        return self.spot(steps, sub, self.ring.core)

    def travels(self, way, hop, sub):
        return hop < self.ring.far or (sub < SUBS // 2) == (way == 0)

    def go(self, copy):
        copy.start()
        self.sends.append(copy)

    def pass_on(self, way, hop, sub):
        steps = 1 - hop if way == 0 else hop - 1
        self.go(
            remote(
                self.mine(steps, sub),
                self.spot(steps, sub, self.ring.core),
                self.ring_send.at[way, hop - 1, sub],
                self.ring_recv.at[way, hop - 1, sub],
                self.ring.near[way],
            )
        )

    def hand_over(self, steps, sub, slot):
        self.go(
            remote(
                self.mine(steps, sub),
                self.spot(steps, sub, self.ring.core),
                self.side_send.at[slot, sub],
                self.side_recv.at[slot, sub],
                self.ring.side,
            )
        )

    def start(self):
        for sub, way in self.ring.orders():
            self.pass_on(way, 1, sub)
        for sub in range(SUBS):
            self.hand_over(0, sub, 0)
        self.own = pltpu.make_async_copy(
            self.x_ref,
            self.o_ref.at[aligned((self.ring.me * 2 + self.ring.core) * self.rows, self.rows), :],
            self.own_sem.at[0],
        )
        self.own.start()

    def hop(self, hop, between=None):
        far, count = self.ring.far, self.ring.count
        for sub, way in self.ring.orders():
            if not self.travels(way, hop, sub):
                continue
            steps = -hop if way == 0 else hop
            here = self.spot(steps, sub, self.ring.core)
            remote(
                here, here, self.ring_send.at[way, hop - 1, sub],
                self.ring_recv.at[way, hop - 1, sub], self.ring.near[way],
            ).wait_recv()
            if hop < far and self.travels(way, hop + 1, sub):
                self.pass_on(way, hop + 1, sub)
            self.hand_over(steps, sub, hop if way == 0 or hop == far else count - hop)
            if way == 1 and between is not None:
                between()

    def side_arrived(self, steps):
        slot = -steps if steps <= 0 else self.ring.count - steps
        slot = self.ring.far if abs(steps) == self.ring.far else slot
        for sub in range(SUBS):
            there = self.spot(steps, sub, 1 - self.ring.core)
            remote(
                there, there, self.side_send.at[slot, sub], self.side_recv.at[slot, sub],
                self.ring.side,
            ).wait_recv()

    def around(self, hop):
        return (-hop, hop) if hop < self.ring.far else (-hop,)

    def sent(self):
        for copy in self.sends:
            copy.wait_send()

    def finish(self):
        self.own.wait()
        self.side_arrived(0)
        for hop in range(1, self.ring.far + 1):
            for steps in self.around(hop):
                self.side_arrived(steps)
        self.sent()

    def run(self, use, work):
        self.start()
        self.own.wait()
        waiting = [0]

        def between():
            if waiting:
                steps = waiting.pop(0)
                self.side_arrived(steps)
                use(self.ring.index(steps))
            else:
                work.do(1)

        for hop in range(1, self.ring.far + 1):
            self.hop(hop, between)
            waiting += self.around(hop)
        while waiting:
            between()
        self.sent()


def reduce_scratch(count, rows, width):
    far = count // 2
    dma = pltpu.SemaphoreType.DMA
    return [
        pltpu.VMEM((count * 2 * rows, width), NARROW),
        pltpu.VMEM((count, rows, width), NARROW),
        pltpu.VMEM((2, far, rows, width), NARROW),
        pltpu.VMEM((2, far, rows, width), NARROW),
        dma((2, far, SUBS)), dma((2, far, SUBS)), dma((count,)), dma((count,)),
    ]


class Reduce:
    def __init__(self, ring, scratch):
        self.ring = ring
        self.parts, self.beside, self.outgoing, self.incoming = scratch[:4]
        self.ring_send, self.ring_recv, self.side_send, self.side_recv = scratch[4:]
        self.rows = self.beside.shape[1]
        self.piece = self.rows // SUBS

    def span(self, sub):
        return slice(sub * self.piece, (sub + 1) * self.piece)

    def spot(self, steps, core, sub=None):
        start = (self.ring.index(steps) * 2 + core) * self.rows
        if sub is None:
            return aligned(start, self.rows)
        return aligned(start + sub * self.piece, self.piece)

    def make(self):
        steps = self.to_make.pop(0)
        self.produce(self.ring.index(steps), self.parts)
        slot = len(self.slots)
        copy = remote(
            self.parts.at[self.spot(steps, 1 - self.ring.core), :], self.beside.at[slot],
            self.side_send.at[slot], self.side_recv.at[slot], self.ring.side,
        )
        copy.start()
        self.slots[steps] = (slot, copy)

    def mine(self, steps, sub):
        while steps not in self.slots:
            self.make()
        slot, copy = self.slots[steps]
        if steps not in self.joined:
            copy.wait_recv()
            self.joined.add(steps)
        return self.parts[self.spot(steps, self.ring.core, sub), :].astype(
            jnp.float32
        ) + self.beside[slot, self.span(sub), :].astype(jnp.float32)

    def travels(self, way, step, sub):
        return step > 1 or (sub < SUBS // 2) == (way == 0)

    def ring_copy(self, way, step, sub):
        return remote(
            self.outgoing.at[way, step - 1, self.span(sub), :],
            self.incoming.at[way, step - 1, self.span(sub), :],
            self.ring_send.at[way, step - 1, sub],
            self.ring_recv.at[way, step - 1, sub],
            self.ring.near[way],
        )

    def step(self, step):
        far = self.ring.far
        for sub, way in self.ring.orders():
            if not self.travels(way, step, sub):
                continue
            steps = far + 1 - step
            steps = steps if way == 0 or steps == far else -steps
            value = self.mine(steps, sub)
            if step > 1 and self.travels(way, step - 1, sub):
                self.ring_copy(way, step - 1, sub).wait_recv()
                value = value + self.incoming[way, step - 2, self.span(sub), :].astype(jnp.float32)
            self.outgoing[way, step - 1, self.span(sub), :] = value.astype(NARROW)
            copy = self.ring_copy(way, step, sub)
            copy.start()
            self.sends.append(copy)
            if way == 1:
                if self.to_make:
                    self.make()
                else:
                    self.work.do(1)

    def begin(self, produce, work):
        self.produce, self.work = produce, work
        self.slots, self.joined, self.sends = {}, set(), []
        far = self.ring.far
        self.to_make = [far]
        for steps in range(far - 1, 0, -1):
            self.to_make += [steps, -steps]
        self.to_make.append(0)
        self.make()
        self.make()

    def end(self, finish):
        far = self.ring.far
        while self.to_make:
            self.make()
        for sub in range(SUBS):
            value = self.mine(0, sub)
            for way in range(2):
                self.ring_copy(way, far, sub).wait_recv()
                value = value + self.incoming[way, far - 1, self.span(sub), :].astype(jnp.float32)
            finish(self.span(sub), value)
        for copy in self.sends:
            copy.wait_send()
        for _, copy in self.slots.values():
            copy.wait_send()

    def run(self, produce, finish, work, beside=()):
        beside = list(beside)
        self.begin(produce, work)
        for step in range(1, self.ring.far + 1):
            self.step(step)
            if beside:
                beside.pop(0)()
        self.end(finish)
        return beside


def products(left, right, transposed, tile=512):
    width = right.shape[0] if transposed else right.shape[1]
    number = width // tile

    def produce(index, parts):
        block = parts.shape[0] // lax.axis_size(DP)
        rows = aligned(index * block, block)

        def one(at):
            cols = aligned(at * tile, tile)
            if transposed:
                part = dot(left[rows, :], right[cols, :], ((1,), (1,)))
            else:
                part = dot(left[rows, :], right[:, cols], ((1,), (0,)))
            parts[rows, cols] = part.astype(NARROW)

        loop(0, number, one)

    return produce


def add_gradient(work, left, right, out, tile=256):
    if out.shape[0] >= out.shape[1]:

        def piece(at):
            cols = aligned(at * tile, tile)
            out[cols, :] = dot(left[:, cols], right[...], ((0,), (0,))).astype(NARROW)

        work.add(piece, out.shape[0] // tile)
    else:

        def piece(at):
            cols = aligned(at * tile, tile)
            out[:, cols] = dot(left[...], right[:, cols], ((0,), (0,))).astype(NARROW)

        work.add(piece, out.shape[1] // tile)


def unit_rows(value):
    inverse = lax.rsqrt(jnp.mean(value * value, axis=-1, keepdims=True) + epsilon)
    return value * inverse, inverse


def through_norm(grad, value, gain):
    unit, inverse = unit_rows(value)
    scaled = grad * gain
    inner = jnp.mean(scaled * unit, axis=-1, keepdims=True)
    return inverse * (scaled - unit * inner), jnp.sum(grad * unit, axis=0, keepdims=True)


def shape_of(*dims, kind=NARROW):
    return jax.ShapeDtypeStruct(dims, kind)


def call_fused(name, body, cid, us, ins, outs, scratch):
    def kernel(*refs):
        refs = list(refs)
        named = {key: refs.pop(0) for key in [*ins, *outs]}
        for key, kind in scratch.items():
            named[key] = [refs.pop(0) for _ in kind] if isinstance(kind, list) else refs.pop(0)
        body(Names(**named))

    flat = []
    for kind in scratch.values():
        flat += kind if isinstance(kind, list) else [kind]
    result = pl.pallas_call(
        kernel,
        out_shape=tuple(shape for shape, _ in outs.values()),
        in_specs=[spec for _, spec in ins.values()],
        out_specs=tuple(spec for _, spec in outs.values()),
        scratch_shapes=flat,
        compiler_params=pltpu.CompilerParams(
            collective_id=cid, has_side_effects=True, vmem_limit_bytes=63 * 1024 * 1024
        ),
        cost_estimate=pl.CostEstimate(
            flops=0, bytes_accessed=int(us * 3.69e6), transcendentals=0
        ),
        name=name,
    )(*[value for value, _ in ins.values()])
    return Names(**dict(zip(outs, result)))


def swap_halves(rows, head):
    width = rows.shape[1]
    lane = lax.broadcasted_iota(jnp.int32, rows.shape, 1)
    half = head // 2
    return jnp.where(
        lax.rem(lane, head) < half, pltpu.roll(rows, width - half, 1), pltpu.roll(rows, half, 1)
    )


def low_lanes(shape, head):
    return lax.broadcasted_iota(jnp.int32, shape, 1) < head


def two_heads(rows, head):
    low = low_lanes(rows.shape, head)
    zero = jnp.zeros_like(rows)
    return jnp.concatenate([jnp.where(low, rows, zero), jnp.where(low, zero, rows)], axis=0)


def one_row(rows, head):
    half = rows.shape[0] // 2
    return jnp.where(low_lanes((half, rows.shape[1]), head), rows[:half], rows[half:])


def triangle(block, keys):
    row = lax.rem(lax.broadcasted_iota(jnp.int32, (2 * block, keys), 0), block)
    column = lax.broadcasted_iota(jnp.int32, (2 * block, keys), 1)
    return column <= row + (keys - block)


def in_order(ref, order, spot, block):
    value = ref[:block, :]
    for other in range(1, ref.shape[0] // block):
        there = order[spot] == other
        value = jnp.where(there, ref[other * block : (other + 1) * block, :], value)
    return value


def attend_here(slots, qkv, cosine, sine, kept, lse, mixed, key2, value2):
    groups = slots.shape[0]
    tokens = qkv.shape[0]
    block = tokens // groups
    span = groups // 2
    wide = qkv.shape[1] // 2
    head = wide // 2
    scale = 1.0 / math.sqrt(head)
    for spot in range(groups):
        here = slice(spot * block, (spot + 1) * block)
        turn_rows = slice(spot % span * block, (spot % span + 1) * block)
        turned_by, turned_sine = cosine[turn_rows, :], sine[turn_rows, :]
        rows = in_order(qkv, slots, spot, block)
        query, pair = rows[:, :wide], rows[:, wide:]
        low = low_lanes(pair.shape, head)
        query = query * turned_by + swap_halves(query, head) * turned_sine
        pair = jnp.where(low, pair * turned_by + swap_halves(pair, head) * turned_sine, pair)
        other = pltpu.roll(pair, head, 1)
        kept[here, :wide] = query.astype(kept.dtype)
        kept[here, wide:] = pair.astype(kept.dtype)
        key2[here, :] = jnp.where(low, pair, other).astype(key2.dtype)
        value2[here, :] = jnp.where(low, other, pair).astype(value2.dtype)
    for spot in range(groups):
        here = slice(spot * block, (spot + 1) * block)
        first = spot // span * span * block
        keys = (spot % span + 1) * block
        query = two_heads(kept[here, :wide], head)
        score = dot(query, key2[first : first + keys, :], ((1,), (1,))) * scale
        allowed = triangle(block, keys)
        total = jnp.sum(jnp.where(allowed, jnp.exp(score), 0.0), axis=1, keepdims=True)
        log_total = jnp.log(total)
        probs = jnp.where(allowed, jnp.exp(score - log_total), 0.0).astype(jnp.bfloat16)
        value = dot(probs, value2[first : first + keys, :], ((1,), (0,)))
        mixed[here, :] = one_row(value, head).astype(mixed.dtype)
        lse[spot] = log_total


def attend_back_here(slots, grad, kept, lse, cosine, sine, out, key2, value2, key_sum, value_sum):
    groups = slots.shape[0]
    tokens = kept.shape[0]
    block = tokens // groups
    span = groups // 2
    wide = kept.shape[1] // 2
    head = wide // 2
    scale = 1.0 / math.sqrt(head)
    for spot in range(groups):
        here = slice(spot * block, (spot + 1) * block)
        pair = kept[here, wide:].astype(jnp.float32)
        low = low_lanes(pair.shape, head)
        other = pltpu.roll(pair, head, 1)
        key2[here, :] = jnp.where(low, pair, other).astype(key2.dtype)
        value2[here, :] = jnp.where(low, other, pair).astype(value2.dtype)
    for spot in range(groups - 1, -1, -1):
        here = slice(spot * block, (spot + 1) * block)
        place = spot % span
        turn_rows = slice(place * block, (place + 1) * block)
        first = spot // span * span * block
        keys = (place + 1) * block
        query = two_heads(kept[here, :wide], head)
        given = two_heads(in_order(grad, slots, spot, block), head)
        key = key2[first : first + keys, :]
        value = value2[first : first + keys, :]
        score = dot(query, key, ((1,), (1,))) * scale
        probs = jnp.where(triangle(block, keys), jnp.exp(score - lse[spot]), 0.0)
        prob_grad = dot(given, value, ((1,), (1,)))
        rowdot = jnp.sum(probs * prob_grad, axis=1, keepdims=True)
        score_grad = (probs * (prob_grad - rowdot) * scale).astype(jnp.bfloat16)
        value_part = dot(probs.astype(jnp.bfloat16), given, ((0,), (0,)))
        key_part = dot(score_grad, query, ((0,), (0,)))
        if place == span - 1:
            value_sum[first : first + keys, :] = value_part
            key_sum[first : first + keys, :] = key_part
        else:
            value_sum[first : first + keys, :] += value_part
            key_sum[first : first + keys, :] += key_part
        query_grad = one_row(dot(score_grad, key, ((1,), (0,))), head)
        query_grad = query_grad * cosine[turn_rows, :] - swap_halves(query_grad, head) * sine[turn_rows, :]
        out[here, :wide] = query_grad.astype(out.dtype)
    for spot in range(groups):
        here = slice(spot * block, (spot + 1) * block)
        turn_rows = slice(spot % span * block, (spot % span + 1) * block)
        key = key_sum[here, :]
        key = key + pltpu.roll(key, head, 1)
        key = key * cosine[turn_rows, :] - swap_halves(key, head) * sine[turn_rows, :]
        value = value_sum[here, :]
        value = value + pltpu.roll(value, head, 1)
        out[here, wide:] = jnp.where(low_lanes(key.shape, head), key, value).astype(out.dtype)


def put_back(source, target, row):
    groups = row.shape[0]
    block = source.shape[0] // groups
    for spot in range(groups):
        target[spot * block : (spot + 1) * block, :] = in_order(source, row, spot, block)


def attend_scratch(tokens, head, back=False):
    vmem = pltpu.VMEM
    wide = 2 * head
    kinds = dict(
        key2=vmem((tokens, wide), jnp.bfloat16),
        value2=vmem((tokens, wide), jnp.bfloat16),
        by_number=vmem((tokens, 2 * wide if back else wide), jnp.bfloat16),
    )
    if back:
        kinds.update(
            key_sum=vmem((tokens, wide), jnp.float32), value_sum=vmem((tokens, wide), jnp.float32)
        )
    return kinds


def rope_tables(tokens, head):
    angle = jnp.arange(tokens, dtype=jnp.float32)[:, None] * rope_frequencies(head)[None, :]
    cosine = jnp.cos(angle)
    sine = jnp.sin(angle)
    return (
        jnp.concatenate([cosine] * 4, axis=1),
        jnp.concatenate([-sine, sine] * 2, axis=1),
    )


def weight_pieces(source, target, count, heads, srcs, dsts, layer):
    qkv, wo, gate, up, down = srcs
    out_qkv, out_wo, out_gu, out_down = dsts
    depth = gate.shape[1]
    hidden = gate.shape[2] // count
    q_rows = wo.shape[1] // count
    kv_rows = (qkv.shape[0] - wo.shape[1]) // 2
    shared = count * heads // kv_rows
    cols = aligned(source * depth, depth)
    k_from = pl.multiple_of(wo.shape[1] + target // shared * heads, heads)
    v_from = pl.multiple_of(wo.shape[1] + kv_rows + target // shared * heads, heads)
    mine = aligned(target * hidden, hidden)
    return (
        (qkv.at[aligned(target * q_rows, q_rows), :], out_qkv.at[layer, pl.ds(0, q_rows), cols]),
        (qkv.at[pl.ds(k_from, heads), :], out_qkv.at[layer, pl.ds(q_rows, heads), cols]),
        (qkv.at[pl.ds(v_from, heads), :], out_qkv.at[layer, pl.ds(q_rows + heads, heads), cols]),
        (wo.at[0, aligned(target * q_rows, q_rows), :], out_wo.at[layer, :, cols]),
        (gate.at[0, :, mine], out_gu.at[layer, cols, pl.ds(0, hidden)]),
        (up.at[0, :, mine], out_gu.at[layer, cols, pl.ds(hidden, hidden)]),
        (down.at[0, mine, :], out_down.at[layer, :, cols]),
    )


KINDS, ATTENTION_KINDS = 7, 4


class Spread:
    def __init__(self, ring, heads, srcs, dsts, sems):
        self.ring = ring
        self.layer = lax.axis_index(SECTION)
        self.across = {SECTION: 1 - self.layer}
        self.peers, self.origins = partners(ring.me, ring.count)
        self.send, self.recv, self.cross_send, self.cross_recv, self.own_sem = sems
        self.pieces = lambda source, target, layer: weight_pieces(
            source, target, ring.count, heads, srcs, dsts, layer
        )
        self.started, self.local = [], {}
        count = ring.count
        sizes = [math.prod(there.shape) for _, there in self.pieces(ring.me, ring.me, self.layer)]
        arrivals = []
        for kind in range(KINDS):
            for k in range(count - 1):
                part = (k + 1) / (count // 2) if k < count // 2 else 1.0
                due = sum(sizes[:kind]) + part * sizes[kind]
                arrivals.append((due if k < count // 2 else due * 0.5, kind, k))
        self.arrivals = sorted(arrivals)

    def go(self, copy):
        copy.start()
        self.started.append(copy)

    def own(self, kinds):
        last = self.ring.count - 1
        for kind in kinds:
            source, target = self.pieces(self.ring.me, self.ring.me, self.layer)[kind]
            self.go(
                remote(
                    source, target, self.cross_send.at[kind, last], self.cross_recv.at[kind, last],
                    self.across,
                )
            )
            self.local[kind] = pltpu.make_async_copy(source, target, self.own_sem.at[kind])
            self.local[kind].start()

    def out(self, kinds):
        for kind in kinds:
            for k, peer in enumerate(self.peers):
                source, target = self.pieces(self.ring.me, peer, self.layer)[kind]
                self.go(remote(source, target, self.send.at[kind, k], self.recv.at[kind, k], {DP: peer}))

    def pass_on(self, kinds):
        for _, kind, k in self.arrivals:
            if kind not in kinds:
                continue
            here = self.pieces(self.origins[k], self.ring.me, self.layer)[kind][1]
            remote(
                here, here, self.send.at[kind, k], self.recv.at[kind, k], {DP: self.origins[k]}
            ).wait_recv()
            self.go(
                remote(
                    here, here, self.cross_send.at[kind, k], self.cross_recv.at[kind, k], self.across
                )
            )

    def here(self, kinds):
        for kind in kinds:
            self.local[kind].wait()
            for k in range(self.ring.count):
                origin = self.origins[k] if k < self.ring.count - 1 else self.ring.me
                there = self.pieces(origin, self.ring.me, 1 - self.layer)[kind][1]
                remote(
                    there, there, self.cross_send.at[kind, k], self.cross_recv.at[kind, k], self.across
                ).wait_recv()

    def sent(self):
        for copy in self.started:
            copy.wait_send()


def chip_rows(index, local):
    return aligned(index * 2 * local, 2 * local)


def feed_forward_use(s, local, after):
    width = s.hidden.shape[1]
    tile = 256
    number = width // tile

    def use(index):
        rows = chip_rows(index, local)

        def one(at):
            start = at * tile
            cols, right = aligned(start, tile), aligned(start + width, tile)
            value = s.normed2[rows, :]
            gate = dot(value, s.gu[:, cols], ((1,), (0,)))
            upper = dot(value, s.gu[:, right], ((1,), (0,)))
            s.hidden[rows, cols] = (gate * jax.nn.sigmoid(gate) * upper).astype(NARROW)
            after(rows, cols, right, gate, upper)

        loop(0, number, one)

    return use


def feed_forward_back(s, rows, cols, right, gate, upper):
    hidden_grad = dot(s.out_grad[rows, :], s.down[cols, :], ((1,), (1,)))
    sigma = jax.nn.sigmoid(gate)
    gate_grad = hidden_grad * upper * sigma * (1.0 + gate * (1.0 - sigma))
    s.gu_grad[rows, cols] = gate_grad.astype(NARROW)
    s.gu_grad[rows, right] = (hidden_grad * gate * sigma).astype(NARROW)


def opening_body(s):
    ring = Ring()
    layer = lax.axis_index(SECTION)
    peers, origins = partners(ring.me, ring.count)
    holders = [{DP: peer} for peer in peers] + [
        {SECTION: 1 - layer, DP: peer} for peer in [*peers, ring.me]
    ]
    greet([*holders, ring.side])
    copies = Copies(s.copy_sem)
    rows_in = copies(s.inputs.at[layer], s.rows)
    given_in = copies(s.cotangent.at[layer], s.given)
    spread = Spread(
        ring, s.kept0.shape[1] // 4, (s.qkv, s.wo, s.gate, s.up, s.down_in),
        (s.out_qkv, s.out_wo, s.out_gu, s.out_down), s.spread_sems,
    )
    attention, feed = range(ATTENTION_KINDS), range(ATTENTION_KINDS, KINDS)
    local, depth = s.rows.shape[0], s.gain_attn.shape[1]

    s.gain_piece[...] = jnp.zeros_like(s.gain_piece)
    s.gain_piece[0:1, :] = s.gain_attn[...].astype(WIDE)
    s.gain_piece[1:2, :] = s.gain_mlp[...].astype(WIDE)
    gain_send, gain_recv = s.gain_sems
    spot = lambda at, source: s.gains.at[at, :, aligned(source * depth, depth)]
    for k, holder in enumerate(holders):
        spread.go(remote(s.gain_piece, spot(layer, ring.me), gain_send.at[k], gain_recv.at[k], holder))
    own_gains = copies(s.gain_piece, spot(layer, ring.me))
    spread.own(attention)
    own_gains.wait()
    for k, holder in enumerate(holders):
        at, place = (layer, k) if k < ring.count - 1 else (1 - layer, k - ring.count + 1)
        here = spot(at, origins[place] if place < ring.count - 1 else ring.me)
        remote(here, here, gain_send.at[k], gain_recv.at[k], holder).wait_recv()

    rows_in.wait()
    unit, _ = unit_rows(s.rows[...])
    s.shard0[...] = (unit * s.gains[0, 0:1, :]).astype(NARROW)
    first = Gather(ring, s.shard0, s.normed1, s.first_sems)
    first.start()
    spread.out(attention)
    for hop in range(1, ring.far + 1):
        first.hop(hop)
    given_in.wait()
    s.shard1[...] = s.given[...].astype(NARROW)
    grads = Gather(ring, s.shard1, s.out_grad, s.grads_sems)
    grads.start()
    spread.pass_on(attention)
    spread.out(feed)
    spread.own(feed)
    first.finish()
    spread.here(attention)
    loads = [
        copies(s.out_qkv.at[0], s.qkv_w), copies(s.out_qkv.at[1], s.next_qkv_w),
        copies(s.out_wo.at[0], s.wo_w),
    ]
    stores = [copies(s.normed1, s.normed1_out)]
    for load in loads:
        load.wait()
    tile = 2 * local

    def project(at):
        rows = aligned(at * tile, tile)
        s.projected[rows, :] = dot(s.normed1[rows, :], s.qkv_w[...], ((1,), (1,)))

    loop(0, s.projected.shape[0] // tile, project)
    attend_here(s.slots, s.projected, s.cosine, s.sine, s.kept0, s.lse0, s.by_number, s.key2, s.value2)
    put_back(s.by_number, s.mixed0, s.row)
    stores[0].wait()
    grads.hop(1)
    spread.pass_on(feed)

    reduce = Reduce(ring, s.reduce)
    none = Work()

    def second(span, value):
        s.second[span, :] = s.rows[span, :] + value

    loads = {}

    def gate_up_here():
        spread.here(feed[:2])
        loads[0] = copies(s.out_gu.at[0], s.gu)

    left = reduce.run(
        products(s.mixed0, s.wo_w, False), second, none,
        [functools.partial(grads.hop, hop) for hop in range(2, ring.far + 1)] + [gate_up_here],
    )
    for do in left:
        do()
    unit, _ = unit_rows(s.second[...])
    s.shard2[...] = (unit * s.gains[0, 1:2, :]).astype(NARROW)
    loads[0].wait()
    spread.here(feed[2:])
    load = copies(s.out_down.at[0], s.down)

    def keep(rows, cols, right, gate, upper):
        s.gate_up[rows, cols] = gate
        s.gate_up[rows, right] = upper

    Gather(ring, s.shard2, s.normed2, s.gather_sems).run(feed_forward_use(s, local, keep), none)
    grads.finish()
    stores += [
        copies(s.out_grad, s.out_grad_out), copies(s.normed2, s.normed2_out),
        copies(s.gate_up, s.gate_up_out),
    ]
    load.wait()

    def result(span, value):
        s.result[span, :] = s.second[span, :] + value

    reduce.run(products(s.hidden, s.down, False), result, none)
    unit, _ = unit_rows(s.result[...])
    s.shard0[...] = (unit * s.gains[1, 0:1, :]).astype(NARROW)

    def use(index):
        rows = chip_rows(index, local)
        s.projected[rows, :] = dot(s.normed1[rows, :], s.next_qkv_w[...], ((1,), (1,)))

    Gather(ring, s.shard0, s.normed1, s.first_sems).run(use, none)
    stores.append(copies(s.normed1, s.next_normed1_out))
    attend_here(s.slots, s.projected, s.cosine, s.sine, s.kept1, s.lse1, s.by_number, s.key2, s.value2)
    put_back(s.by_number, s.mixed1, s.row)
    for store in stores[1:]:
        store.wait()
    spread.sent()


def opening(slots, row, cosine, sine, inputs, cotangent, qkv, wo, gate, up, down, gain_attn, gain_mlp, count, head):
    local, width = inputs.shape[1:]
    tokens = count * 2 * local
    depth = gate.shape[1]
    hidden = gate.shape[2] // count
    q_rows = wo.shape[1] // count
    vmem, dma = pltpu.VMEM, pltpu.SemaphoreType.DMA
    lse = shape_of(count, 2 * tokens // count, 1, kind=WIDE)
    return call_fused(
        "opening", opening_body, 0, 360,
        dict(
            slots=(slots, SMEM), row=(row, SMEM), cosine=(cosine, VMEM), sine=(sine, VMEM),
            inputs=(inputs, HBM), cotangent=(cotangent, HBM), qkv=(qkv, HBM), wo=(wo, HBM),
            gate=(gate, HBM), up=(up, HBM), down_in=(down, HBM),
            gain_attn=(gain_attn, VMEM), gain_mlp=(gain_mlp, VMEM),
        ),
        dict(
            out_qkv=(shape_of(2, q_rows + 2 * head, width), HBM),
            out_wo=(shape_of(2, q_rows, width), HBM),
            out_gu=(shape_of(2, width, 2 * hidden), HBM),
            out_down=(shape_of(2, hidden, width), HBM),
            gains=(shape_of(2, 8, width, kind=WIDE), VMEM),
            normed1_out=(shape_of(tokens, width), HBM),
            next_normed1_out=(shape_of(tokens, width), HBM),
            normed2_out=(shape_of(tokens, width), HBM),
            out_grad_out=(shape_of(tokens, width), HBM),
            gate_up_out=(shape_of(tokens, 2 * hidden, kind=WIDE), HBM),
            second=(shape_of(local, width, kind=WIDE), VMEM),
            result=(shape_of(local, width, kind=WIDE), VMEM),
            hidden=(shape_of(tokens, hidden), VMEM),
            mixed0=(shape_of(tokens, 2 * head), VMEM), mixed1=(shape_of(tokens, 2 * head), VMEM),
            kept0=(shape_of(tokens, 4 * head), VMEM), kept1=(shape_of(tokens, 4 * head), VMEM),
            lse0=(lse, VMEM), lse1=(lse, VMEM),
        ),
        dict(
            rows=vmem((local, width), WIDE), given=vmem((local, width), WIDE),
            gain_piece=vmem((8, depth), WIDE),
            shard0=vmem((local, width), NARROW), shard1=vmem((local, width), NARROW),
            shard2=vmem((local, width), NARROW),
            normed1=vmem((tokens, width), NARROW), normed2=vmem((tokens, width), NARROW),
            out_grad=vmem((tokens, width), NARROW), gate_up=vmem((tokens, 2 * hidden), WIDE),
            qkv_w=vmem((q_rows + 2 * head, width), NARROW),
            next_qkv_w=vmem((q_rows + 2 * head, width), NARROW),
            wo_w=vmem((q_rows, width), NARROW), gu=vmem((width, 2 * hidden), NARROW),
            down=vmem((hidden, width), NARROW), projected=vmem((tokens, 4 * head), WIDE),
            key2=vmem((tokens, 2 * head), NARROW), value2=vmem((tokens, 2 * head), NARROW),
            by_number=vmem((tokens, 2 * head), NARROW),
            reduce=reduce_scratch(count, local, width),
            first_sems=gather_scratch(count), grads_sems=gather_scratch(count),
            gather_sems=gather_scratch(count),
            gain_sems=[dma((2 * count - 1,)), dma((2 * count - 1,))],
            spread_sems=[
                dma((KINDS, count - 1)), dma((KINDS, count - 1)),
                dma((KINDS, count)), dma((KINDS, count)), dma((KINDS,)),
            ],
            copy_sem=dma((16,)),
        ),
    )


def back_through_feed_forward(at, s, ring, reduce, work, beside):
    local = s.given.shape[0]
    add_gradient(work, s.hidden, s.out_grad, s.grad_down)
    add_gradient(work, s.normed2, s.gu_grad, s.grad_gu)

    def keep(span, value):
        s.normed_grad[span, :] = value

    left = reduce.run(products(s.gu_grad, s.gu, True), keep, work, beside)
    part, s.gain_mlp_grad[...] = through_norm(
        s.normed_grad[...], s.second[...], s.gains[at, 1:2, :]
    )
    s.second_grad[...] = s.given[...] + part
    s.shard2[...] = s.second_grad[...].astype(NARROW)

    def use(index):
        rows = chip_rows(index, local)
        s.mixed_grad[rows, :] = dot(s.attn_grad[rows, :], s.wo[...], ((1,), (1,))).astype(NARROW)

    for do in reversed(left):
        work.first(lambda _, do=do: do())
    Gather(ring, s.shard2, s.attn_grad, s.gather_sems).run(use, work)
    work.do()


def turn_body(at, s):
    ring = Ring()
    greet(ring.everyone())
    copies = Copies(s.copy_sem)
    wo_in = copies(s.wo_in.at[at], s.wo)
    ins = [
        copies(s.gu_in.at[at], s.gu), copies(s.down_in.at[at], s.down),
        copies(s.out_grad_in, s.out_grad), copies(s.cotangent.at[lax.axis_index(SECTION)], s.given),
    ]
    reduce, other = Reduce(ring, s.reduce), Reduce(ring, s.other)
    work = Work()

    def second(span, value):
        s.second[span, :] = s.rows[span, :] + value

    wo_in.wait()
    reduce.run(products(s.mixed, s.wo, False), second, work)
    unit, _ = unit_rows(s.second[...])
    s.shard[...] = (unit * s.gains[at, 1:2, :]).astype(NARROW)
    for load in ins:
        load.wait()
    Gather(ring, s.shard, s.normed2, s.first_sems).run(
        feed_forward_use(s, s.rows.shape[0], functools.partial(feed_forward_back, s)), work
    )

    def result(span, value):
        s.result[span, :] = s.second[span, :] + value

    beside = [lambda: other.begin(products(s.hidden, s.down, False), Work())]
    beside += [functools.partial(other.step, step) for step in range(1, ring.far + 1)]
    beside += [lambda: other.end(result)]
    back_through_feed_forward(at, s, ring, reduce, work, beside)
    stores = [
        copies(s.grad_down, s.grad_down_out), copies(s.grad_gu, s.grad_gu_out),
        copies(s.attn_grad, s.attn_grad_out),
    ]
    attend_back_here(
        s.slots, s.mixed_grad, s.kept, s.lse, s.cosine, s.sine, s.by_number, s.key2, s.value2,
        s.key_sum, s.value_sum,
    )
    put_back(s.by_number, s.qkv_grad, s.row)
    for store in stores:
        store.wait()


def turn(at, known, rows, mixed, kept, lse, out_grad, cotangent, weights, count):
    _, wo, gu, down, gains = weights
    local, width = rows.shape
    tokens = mixed.shape[0]
    hidden = down.shape[1]
    head = mixed.shape[1] // 2
    vmem, dma = pltpu.VMEM, pltpu.SemaphoreType.DMA
    return call_fused(
        "turn", functools.partial(turn_body, at), 1, 140,
        dict(
            **known, rows=(rows, VMEM), mixed=(mixed, VMEM), kept=(kept, VMEM), lse=(lse, VMEM),
            gains=(gains, VMEM), out_grad_in=(out_grad, HBM), cotangent=(cotangent, HBM),
            wo_in=(wo, HBM), gu_in=(gu, HBM), down_in=(down, HBM),
        ),
        dict(
            result=(shape_of(local, width, kind=WIDE), VMEM),
            second_grad=(shape_of(local, width, kind=WIDE), VMEM),
            qkv_grad=(shape_of(tokens, 4 * head), VMEM),
            attn_grad_out=(shape_of(tokens, width), HBM),
            gain_mlp_grad=(shape_of(1, width, kind=WIDE), VMEM),
            grad_down_out=(shape_of(hidden, width), HBM),
            grad_gu_out=(shape_of(width, 2 * hidden), HBM),
        ),
        dict(
            reduce=reduce_scratch(count, local, width), other=reduce_scratch(count, local, width),
            first_sems=gather_scratch(count), gather_sems=gather_scratch(count),
            gu=vmem(gu.shape[1:], NARROW), down=vmem(down.shape[1:], NARROW), wo=vmem(wo.shape[1:], NARROW),
            out_grad=vmem((tokens, width), NARROW), normed2=vmem((tokens, width), NARROW),
            attn_grad=vmem((tokens, width), NARROW), mixed_grad=vmem((tokens, 2 * head), NARROW),
            hidden=vmem((tokens, hidden), NARROW), gu_grad=vmem((tokens, 2 * hidden), NARROW),
            grad_down=vmem((hidden, width), NARROW), grad_gu=vmem((width, 2 * hidden), NARROW),
            given=vmem((local, width), WIDE), second=vmem((local, width), WIDE),
            normed_grad=vmem((local, width), WIDE),
            shard=vmem((local, width), NARROW), shard2=vmem((local, width), NARROW),
            **attend_scratch(tokens, head, True),
            copy_sem=dma((8,)),
        ),
    )


def attention_back(at, s, reduce, work, beside=()):
    def keep(span, value):
        s.normed_grad[span, :] = value

    reduce.run(products(s.qkv_grad, s.qkv_w, False), keep, work, beside)
    part, s.gain_attn_grad[...] = through_norm(s.normed_grad[...], s.rows[...], s.gains[at, 0:1, :])
    s.input_grad[...] = s.second_grad_in[...] + part


def backward_body(upper, lower, s):
    ring = Ring()
    local = s.rows.shape[0]
    greet(ring.everyone())
    copies = Copies(s.copy_sem)
    qkv_in = copies(s.qkv_w_in.at[upper], s.qkv_w)
    upper_in = [copies(s.attn_grad_in, s.attn_grad), copies(s.normed1_in, s.normed2)]
    first_in = [copies(s.down_in.at[lower], s.down), copies(s.gate_up_in, s.gate_up)]
    then_in = [copies(s.gu_in.at[lower], s.gu), copies(s.wo_in.at[lower], s.wo)]
    reduce = Reduce(ring, s.reduce)
    work = Work()

    def wait(_):
        for load in upper_in:
            load.wait()

    work.add(wait)
    add_gradient(work, s.mixed, s.attn_grad, s.grad_wo)
    add_gradient(work, s.normed2, s.qkv_grad, s.grad_qkv)
    qkv_in.wait()
    attention_back(upper, s, reduce, work)
    work.do()
    then_in.append(copies(s.normed2_in, s.normed2))
    stores = [copies(s.grad_wo, s.grad_wo_out), copies(s.grad_qkv, s.grad_qkv_out)]
    s.shard[...] = s.input_grad[...].astype(NARROW)
    s.given[...] = s.input_grad[...]
    for load in first_in:
        load.wait()
    width = s.hidden.shape[1]
    tile = 256
    number = width // tile

    def use(index):
        rows = chip_rows(index, local)

        def one(at):
            start = at * tile
            cols, right = aligned(start, tile), aligned(start + width, tile)
            feed_forward_back(s, rows, cols, right, s.gate_up[rows, cols], s.gate_up[rows, right])

        loop(0, number, one)

    Gather(ring, s.shard, s.out_grad, s.first_sems).run(use, work)
    for load in then_in:
        load.wait()
    back_through_feed_forward(lower, s, ring, reduce, work, [])
    stores += [
        copies(s.grad_down, s.grad_down_out), copies(s.grad_gu, s.grad_gu_out),
        copies(s.attn_grad, s.attn_grad_out),
    ]
    for store in stores:
        store.wait()


def backward_between(at, upper, lower, weights, count):
    qkv_w, wo, gu, down, gains = weights
    local, width = upper.rows.shape
    tokens = upper.mixed.shape[0]
    hidden = down.shape[1]
    q_rows = wo.shape[1]
    vmem, dma = pltpu.VMEM, pltpu.SemaphoreType.DMA
    return call_fused(
        "backward_between", functools.partial(backward_body, at, at - 1), 2, 115,
        dict(
            rows=(upper.rows, VMEM), second_grad_in=(upper.second_grad, VMEM),
            qkv_grad=(upper.qkv_grad, VMEM), mixed=(upper.mixed, VMEM), gains=(gains, VMEM),
            attn_grad_in=(upper.attn_grad, HBM), normed1_in=(upper.normed1, HBM),
            second=(lower.second, VMEM), hidden=(lower.hidden, VMEM),
            gate_up_in=(lower.gate_up, HBM), normed2_in=(lower.normed2, HBM),
            qkv_w_in=(qkv_w, HBM), wo_in=(wo, HBM), gu_in=(gu, HBM), down_in=(down, HBM),
        ),
        dict(
            input_grad=(shape_of(local, width, kind=WIDE), VMEM),
            second_grad=(shape_of(local, width, kind=WIDE), VMEM),
            mixed_grad=(shape_of(tokens, q_rows), VMEM),
            attn_grad_out=(shape_of(tokens, width), HBM),
            gain_attn_grad=(shape_of(1, width, kind=WIDE), VMEM),
            gain_mlp_grad=(shape_of(1, width, kind=WIDE), VMEM),
            grad_wo_out=(shape_of(q_rows, width), HBM),
            grad_qkv_out=(shape_of(width, qkv_w.shape[1]), HBM),
            grad_down_out=(shape_of(hidden, width), HBM),
            grad_gu_out=(shape_of(width, 2 * hidden), HBM),
        ),
        dict(
            reduce=reduce_scratch(count, local, width),
            first_sems=gather_scratch(count), gather_sems=gather_scratch(count),
            gu=vmem(gu.shape[1:], NARROW), down=vmem(down.shape[1:], NARROW), wo=vmem(wo.shape[1:], NARROW),
            qkv_w=vmem(qkv_w.shape[1:], NARROW), gate_up=vmem((tokens, 2 * hidden), WIDE),
            out_grad=vmem((tokens, width), NARROW), normed2=vmem((tokens, width), NARROW),
            attn_grad=vmem((tokens, width), NARROW), gu_grad=vmem((tokens, 2 * hidden), NARROW),
            grad_wo=vmem((q_rows, width), NARROW), grad_qkv=vmem((width, qkv_w.shape[1]), NARROW),
            grad_down=vmem((hidden, width), NARROW), grad_gu=vmem((width, 2 * hidden), NARROW),
            given=vmem((local, width), WIDE), normed_grad=vmem((local, width), WIDE),
            shard=vmem((local, width), NARROW), shard2=vmem((local, width), NARROW),
            copy_sem=dma((16,)),
        ),
    )


def gradient_pieces(target, count, refs):
    down, gu, wo, qkv = refs
    depth = down.shape[1] // count
    hidden = down.shape[0]
    cols = aligned(target * depth, depth)
    return (
        down.at[:, cols],
        gu.at[cols, pl.ds(0, hidden)],
        gu.at[cols, pl.ds(hidden, hidden)],
        wo.at[:, cols],
        qkv.at[cols, :],
    )


def owned_pieces(source, refs, sizes):
    down, gate, up, wo, qkv = refs
    return (
        down.at[aligned(source * sizes[0][0], sizes[0][0]), :],
        gate.at[:, aligned(source * sizes[1][1], sizes[1][1])],
        up.at[:, aligned(source * sizes[2][1], sizes[2][1])],
        wo.at[aligned(source * sizes[3][0], sizes[3][0]), :],
        qkv.at[source],
    )


GRADS, FEED_GRADS = 5, 3


class Return:
    def __init__(self, ring, partial, outs, landed, mine, sems):
        self.ring = ring
        self.layer = lax.axis_index(SECTION)
        self.across = {SECTION: 1 - self.layer}
        peers, self.origins = partners(ring.me, ring.count)
        self.order = [*peers, ring.me]
        self.partial, self.outs, self.landed, self.mine = partial, outs, landed, mine
        self.cross_send, self.cross_recv, self.load_sem, self.send, self.recv, self.own_sem = sems
        self.sizes = [ref.shape[1:] for ref in mine]
        self.crossing, self.loads, self.sends, self.events = {}, {}, [], []

    def cross(self, kinds):
        count = self.ring.count
        for kind in kinds:
            for k, owner in enumerate(self.order):
                pieces = [gradient_pieces(owner, count, refs)[kind] for refs in self.partial]
                for at in range(2):
                    copy = remote(
                        pieces[1 - at], self.landed[kind].at[k],
                        self.cross_send.at[kind, k], self.cross_recv.at[kind, k], self.across,
                    )
                    load = pltpu.make_async_copy(
                        pieces[at], self.mine[kind].at[k], self.load_sem.at[kind, k]
                    )

                    @pl.when(self.layer == at)
                    def _():
                        copy.start()
                        load.start()

                self.crossing[kind, k], self.loads[kind, k] = copy, load
                self.events.append((kind, k))

    def some(self, number):
        for kind, k in self.events[:number]:
            self.loads[kind, k].wait()
            self.crossing[kind, k].wait_recv()
            mine, theirs = self.mine[kind], self.landed[kind]
            tile = 64

            def add(at):
                rows = aligned(at * tile, tile)
                total = mine[k, rows, :].astype(WIDE) + theirs[k, rows, :].astype(WIDE)
                mine[k, rows, :] = total.astype(NARROW)

            loop(0, mine.shape[1] // tile, add)
            target = owned_pieces(self.ring.me, self.outs, self.sizes)[kind]
            if k < self.ring.count - 1:
                copy = remote(
                    mine.at[k], target, self.send.at[kind, k], self.recv.at[kind, k],
                    {DP: self.order[k]},
                )
            else:
                copy = pltpu.make_async_copy(mine.at[k], target, self.own_sem.at[kind])
            copy.start()
            self.sends.append((k, copy))
        self.events = self.events[number:]

    def finish(self):
        for copy in self.crossing.values():
            copy.wait_send()
        for k, copy in self.sends:
            if k < self.ring.count - 1:
                copy.wait_send()
            else:
                copy.wait()
        for kind in range(GRADS):
            for k in range(self.ring.count - 1):
                here = owned_pieces(self.origins[k], self.outs, self.sizes)[kind]
                remote(
                    self.mine[kind].at[k], here, self.send.at[kind, k], self.recv.at[kind, k],
                    {DP: self.origins[k]},
                ).wait_recv()


def closing_body(at, s):
    ring = Ring()
    layer = lax.axis_index(SECTION)
    count = ring.count
    everyone = 4 * count
    this = (layer * count + ring.me) * 2 + ring.core

    def device(k):
        other = lax.rem(this + k, everyone)
        return {SECTION: other // (2 * count), DP: lax.rem(other // 2, count), TENSOR: lax.rem(other, 2)}

    greet([device(k) for k in range(1, everyone)])
    copies = Copies(s.copy_sem)
    qkv_in = copies(s.qkv_w_in.at[at], s.qkv_w)
    ins = [copies(s.attn_grad_in, s.attn_grad), copies(s.normed1_in, s.normed1)]
    rows_in = copies(s.inputs.at[layer], s.rows)
    back = Return(
        ring,
        ((s.down0, s.gu0, s.grad_wo, s.grad_qkv), (s.down1, s.gu1, s.wo1, s.qkv1)),
        (s.down_out, s.gate_out, s.up_out, s.wo_out, s.qkv_out), s.landed, s.mine, s.back_sems,
    )
    back.cross(range(FEED_GRADS))

    swap_send, swap_recv = s.swap_sems
    swaps = []

    def swap(which, out, values):
        for section in range(2):
            copy = remote(
                values[1 - section], out.at[section], swap_send.at[which], swap_recv.at[which],
                {SECTION: 1 - layer},
            )
            own = pltpu.make_async_copy(values[section], out.at[section], s.own_sems.at[which])

            @pl.when(layer == section)
            def _():
                copy.start()
                own.start()

        swaps.append((copy, own))

    swap(0, s.results, (s.result0, s.result1))
    attend_back_here(
        s.slots, s.mixed_grad, s.kept, s.lse, s.cosine, s.sine, s.by_number, s.key2, s.value2,
        s.key_sum, s.value_sum,
    )
    put_back(s.by_number, s.qkv_grad, s.row)
    work = Work()
    for load in ins:
        load.wait()
    add_gradient(work, s.mixed, s.attn_grad, s.grad_wo)
    add_gradient(work, s.normed1, s.qkv_grad, s.grad_qkv)
    qkv_in.wait()
    rows_in.wait()

    def rest():
        work.do()
        back.cross(range(FEED_GRADS, GRADS))
        back.some(1)

    beside = [functools.partial(back.some, 1)] * 2 + [rest] + [functools.partial(back.some, 1)] * (ring.far - 3)
    attention_back(at, s, Reduce(ring, s.reduce), work, beside)
    swap(1, s.input_grads, (s.input_grad, s.input_grad1))

    lanes = s.gain_out.shape[1]
    for section, (attn, mlp) in enumerate(((s.gain_attn_grad, s.gain_mlp0), (s.gain_attn1, s.gain_mlp1))):
        for owner in range(2 * count):
            s.gain_in[section * 2 * count + owner] = jnp.zeros_like(s.gain_out)
            cols = slice(owner * lanes, (owner + 1) * lanes)
            s.gain_in[section * 2 * count + owner, 0:1, :] = attn[:, cols]
            s.gain_in[section * 2 * count + owner, 1:2, :] = mlp[:, cols]
    gain_send, gain_recv = s.gain_sems
    gain_copies = []
    for k in range(1, everyone):
        copy = remote(
            s.gain_in.at[lax.rem(this + k, everyone)], s.gain_landed.at[k - 1],
            gain_send.at[k - 1], gain_recv.at[k - 1], device(k),
        )
        copy.start()
        gain_copies.append(copy)
    back.some(len(back.events))
    total = s.gain_in[this]
    for k, copy in enumerate(gain_copies):
        copy.wait_recv()
        total = total + s.gain_landed[k]
    s.gain_out[...] = total
    for copy in gain_copies:
        copy.wait_send()
    for copy, own in swaps:
        copy.wait()
        own.wait()
    back.finish()


def closing(at, known, inputs, first, last, feed0, grads1, gains_of, weights, count):
    qkv_w, _, _, _, gains = weights
    local, width = inputs.shape[1:]
    tokens = first.mixed.shape[0]
    head = first.mixed.shape[1] // 2
    down0, gu0 = feed0
    down1, gu1, wo1, qkv1 = grads1
    hidden, q_rows, qkv_rows = down0.shape[0], wo1.shape[0], qkv1.shape[1]
    depth = width // count
    sizes = [(hidden, depth), (depth, hidden), (depth, hidden), (q_rows, depth), (depth, qkv_rows)]
    everyone = 4 * count
    lanes = width // (2 * count)
    vmem, dma = pltpu.VMEM, pltpu.SemaphoreType.DMA
    pieces = lambda: [vmem((count, *size), NARROW) for size in sizes]
    return call_fused(
        "closing", functools.partial(closing_body, at), 3, 210,
        dict(
            **known, inputs=(inputs, HBM), gains=(gains, VMEM), qkv_w_in=(qkv_w, HBM),
            second_grad_in=(first.second_grad, VMEM), mixed_grad=(first.mixed_grad, VMEM),
            mixed=(first.mixed, VMEM), kept=(first.kept, VMEM), lse=(first.lse, VMEM),
            attn_grad_in=(first.attn_grad, HBM), normed1_in=(first.normed1, HBM),
            result0=(first.result, VMEM), result1=(last.result, VMEM),
            input_grad1=(last.input_grad, VMEM),
            down0=(down0, HBM), gu0=(gu0, HBM),
            down1=(down1, HBM), gu1=(gu1, HBM), wo1=(wo1, HBM), qkv1=(qkv1, HBM),
            gain_mlp0=(gains_of[0], VMEM), gain_attn1=(gains_of[1], VMEM), gain_mlp1=(gains_of[2], VMEM),
        ),
        dict(
            results=(shape_of(2, local, width, kind=WIDE), HBM),
            input_grads=(shape_of(2, local, width, kind=WIDE), HBM),
            down_out=(shape_of(count * hidden, depth), HBM),
            gate_out=(shape_of(depth, count * hidden), HBM),
            up_out=(shape_of(depth, count * hidden), HBM),
            wo_out=(shape_of(count * q_rows, depth), HBM),
            qkv_out=(shape_of(count, depth, qkv_rows), HBM),
            gain_out=(shape_of(8, lanes, kind=WIDE), VMEM),
        ),
        dict(
            reduce=reduce_scratch(count, local, width),
            qkv_w=vmem(qkv_w.shape[1:], NARROW), rows=vmem((local, width), WIDE),
            attn_grad=vmem((tokens, width), NARROW), normed1=vmem((tokens, width), NARROW),
            qkv_grad=vmem((tokens, 4 * head), NARROW),
            grad_wo=vmem((q_rows, width), NARROW), grad_qkv=vmem((width, qkv_rows), NARROW),
            normed_grad=vmem((local, width), WIDE), input_grad=vmem((local, width), WIDE),
            gain_attn_grad=vmem((1, width), WIDE),
            landed=pieces(), mine=pieces(),
            gain_in=vmem((everyone, 8, lanes), WIDE), gain_landed=vmem((everyone - 1, 8, lanes), WIDE),
            **attend_scratch(tokens, head, True),
            back_sems=[
                dma((GRADS, count)), dma((GRADS, count)), dma((GRADS, count)),
                dma((GRADS, count - 1)), dma((GRADS, count - 1)), dma((GRADS,)),
            ],
            gain_sems=[dma((everyone - 1,)), dma((everyone - 1,))],
            swap_sems=[dma((2,)), dma((2,))], own_sems=dma((2,)),
            copy_sem=dma((8,)),
        ),
    )


def widen_kernel(heads, down, gate, up, wo, qkv, every, gain, *outs):
    down_out, gate_out, up_out, wo_out, wq_out, wk_out, wv_out, attn_out, mlp_out = outs
    for source, out in ((down, down_out), (gate, gate_out), (up, up_out), (wo, wo_out)):
        out[0] = source[...].astype(WIDE)
    queries = wq_out.shape[2]
    wq_out[0] = qkv[0, :, :queries].astype(WIDE)

    @pl.when(pl.program_id(0) == 0)
    def _():
        attn_out[...] = gain[0:1, :]
        mlp_out[...] = gain[1:2, :]
        width = 2 * heads
        shared = every.shape[0] * heads // wk_out.shape[2]

        def one(head):
            chips = range(head * shared, (head + 1) * shared)
            return sum(every[chip, :, queries:].astype(WIDE) for chip in chips)

        for pair in range(wk_out.shape[2] // width):
            left, right = one(2 * pair), one(2 * pair + 1)
            low = low_lanes(left.shape, heads)
            cols = slice(pair * width, (pair + 1) * width)
            wk_out[0, :, cols] = jnp.where(low, left, pltpu.roll(right, heads, 1))
            wv_out[0, :, cols] = jnp.where(low, pltpu.roll(left, heads, 1), right)


def widen(end, kv_cols, count, head):
    depth = end.gate_out.shape[0]
    hidden = end.gate_out.shape[1] // count
    q_rows = end.wo_out.shape[0] // count
    lanes = end.gain_out.shape[1]
    down = (hidden, depth)
    across = (depth, hidden)
    result = lambda *dims: shape_of(1, *dims, kind=WIDE)
    by_rows = lambda at: (at, 0)
    by_cols = lambda at: (0, at)
    none = lambda at: (0, 0)
    flat = lambda index: lambda at: (0, *index(at))
    return pl.pallas_call(
        functools.partial(widen_kernel, head),
        grid=(count,),
        out_shape=(
            result(count * hidden, depth), result(depth, count * hidden), result(depth, count * hidden),
            result(count * q_rows, depth), result(depth, count * q_rows),
            result(depth, kv_cols), result(depth, kv_cols), result(lanes), result(lanes),
        ),
        in_specs=[
            pl.BlockSpec(down, by_rows), pl.BlockSpec(across, by_cols), pl.BlockSpec(across, by_cols),
            pl.BlockSpec((q_rows, depth), by_rows),
            pl.BlockSpec((1, *end.qkv_out.shape[1:]), lambda at: (at, 0, 0)),
            pl.BlockSpec(end.qkv_out.shape, lambda at: (0, 0, 0)),
            pl.BlockSpec(end.gain_out.shape, none),
        ],
        out_specs=(
            pl.BlockSpec((1, *down), flat(by_rows)), pl.BlockSpec((1, *across), flat(by_cols)),
            pl.BlockSpec((1, *across), flat(by_cols)), pl.BlockSpec((1, q_rows, depth), flat(by_rows)),
            pl.BlockSpec((1, depth, q_rows), flat(by_cols)),
            pl.BlockSpec((1, depth, kv_cols), flat(none)), pl.BlockSpec((1, depth, kv_cols), flat(none)),
            pl.BlockSpec((1, lanes), none), pl.BlockSpec((1, lanes), none),
        ),
        name="widen",
    )(end.down_out, end.gate_out, end.up_out, end.wo_out, end.qkv_out, end.qkv_out, end.gain_out)


def fast_shards(inputs, table, cotangent, wq, wk, wv, wo, w_gate, w_up, w_down, gain_attn, gain_mlp):
    count = lax.axis_size(DP)
    parts = lax.axis_size(TENSOR)
    head = HEAD_SIZE
    section = lax.axis_index(SECTION)
    block = inputs.shape[1] * parts

    row = lax.dynamic_index_in_dim(table, section, 0, keepdims=False)
    ids = jnp.arange(count, dtype=jnp.int32)
    slots = jnp.sum(jnp.where(row[None, :] == ids[:, None], ids[None, :], 0), axis=1)
    cosine, sine = rope_tables(count // 2 * block, head)
    qkv_t = jnp.concatenate([wq[0], wk[0], wv[0]], axis=1).T
    s = opening(
        slots, row, cosine, sine, inputs, cotangent, qkv_t, wo, w_gate, w_up, w_down,
        gain_attn, gain_mlp, count, head,
    )
    weights = (s.out_qkv, s.out_wo, s.out_gu, s.out_down, s.gains)
    known = dict(
        slots=(slots, SMEM), row=(row, SMEM), cosine=(cosine, VMEM), sine=(sine, VMEM)
    )
    top = turn(
        1, known, s.result, s.mixed1, s.kept1, s.lse1, s.out_grad_out, cotangent, weights, count
    )
    upper = Names(
        rows=s.result, second_grad=top.second_grad, qkv_grad=top.qkv_grad, mixed=s.mixed1,
        attn_grad=top.attn_grad_out, normed1=s.next_normed1_out,
    )
    lower = Names(
        second=s.second, hidden=s.hidden, gate_up=s.gate_up_out, normed2=s.normed2_out
    )
    back = backward_between(1, upper, lower, weights, count)
    first = Names(
        second_grad=back.second_grad, mixed_grad=back.mixed_grad, mixed=s.mixed0, kept=s.kept0,
        lse=s.lse0, attn_grad=back.attn_grad_out, normed1=s.normed1_out, result=s.result,
    )
    last = Names(result=top.result, input_grad=back.input_grad)
    end = closing(
        0, known, inputs, first, last,
        (back.grad_down_out, back.grad_gu_out),
        (top.grad_down_out, top.grad_gu_out, back.grad_wo_out, back.grad_qkv_out),
        (back.gain_mlp_grad, back.gain_attn_grad, top.gain_mlp_grad),
        weights, count,
    )
    grad_down, grad_gate, grad_up, grad_wo, grad_wq, grad_wk, grad_wv, sum_attn, sum_mlp = widen(
        end, wk.shape[2], count, head
    )
    return (
        end.results[None],
        end.input_grads[None],
        grad_wq,
        grad_wk,
        grad_wv,
        grad_wo,
        grad_gate,
        grad_up,
        grad_down,
        sum_attn,
        sum_mlp,
    )


def fits(mesh, inputs, table, cotangent, wq, wk, wv, wo, w_gate, w_up, w_down, gain_attn, gain_mlp):
    sections, count, parts = (mesh.shape[axis] for axis in (SECTION, DP, TENSOR))
    head = HEAD_SIZE
    if sections != 2 or parts != 2 or inputs.shape[0] != sections or count % 4 or count < 8:
        return False
    devices = count * parts
    queries, keys = wq.shape[2] // head, wk.shape[2] // head
    if queries != 2 * devices or devices % keys or keys % parts or 4 * head != 256:
        return False
    return (
        wq.shape[1] % (128 * count) == 0
        and wq.shape[1] % 512 == 0
        and w_gate.shape[2] % (256 * devices) == 0
        and inputs.shape[1] % (64 * devices) == 0
    )


def shards(mesh, whole, *args):
    if fits(mesh, *whole):
        return fast_shards(*args)
    return general_shards(*args)


def solution(mesh):
    in_specs = (
        P(None, (DP, TENSOR), None),
        P(),
        P(None, (DP, TENSOR), None),
        P(SECTION, DP, TENSOR),
        P(SECTION, DP, TENSOR),
        P(SECTION, DP, TENSOR),
        P(SECTION, TENSOR, DP),
        P(SECTION, DP, TENSOR),
        P(SECTION, DP, TENSOR),
        P(SECTION, TENSOR, DP),
        P(SECTION, DP),
        P(SECTION, DP),
    )
    out_specs = (
        P(SECTION, None, (DP, TENSOR), None),
        P(SECTION, None, (DP, TENSOR), None),
        P(SECTION, DP, TENSOR),
        P(SECTION, DP, TENSOR),
        P(SECTION, DP, TENSOR),
        P(SECTION, TENSOR, DP),
        P(SECTION, DP, TENSOR),
        P(SECTION, DP, TENSOR),
        P(SECTION, TENSOR, DP),
        P(SECTION, (DP, TENSOR)),
        P(SECTION, (DP, TENSOR)),
    )

    def step(*args):
        return jax.shard_map(
            functools.partial(shards, mesh, args),
            mesh=mesh,
            in_specs=in_specs,
            out_specs=out_specs,
            check_vma=False,
        )(*args)

    return step
```

```python
import functools
import math

import jax
import jax.numpy as jnp
from jax import lax
from jax.experimental import pallas as pl
from jax.experimental.pallas import tpu as pltpu
from jax.sharding import PartitionSpec as P

HEAD_SIZE = 64
SECTION, DP, TENSOR = "section", "dp", "tensor"


epsilon = 1e-05


def passed_along(value, axis, steps):
    count = lax.axis_size(axis)
    initial, last = (max(0, -steps), min(count, count - steps))
    return lax.ppermute(value, axis, [(source, source + steps) for source in range(initial, last)])


def rope_frequencies(head):
    index = jnp.arange(head // 2, dtype=jnp.float32)
    base = 1.0 / 500000.0 ** (index * 2.0 / head)
    wavelength = 2.0 * math.pi / base
    blend = (8192.0 / wavelength - 1.0) / 3.0
    middle = (1.0 - blend) * base / 32.0 + blend * base
    return jnp.where(wavelength < 2048.0, base, jnp.where(wavelength > 8192.0, base / 32.0, middle))


def rotate(values, positions, head):
    step_count = values.shape[0]
    shaped = values.reshape(step_count, -1, head)
    angle = positions.astype(jnp.float32)[:, None] * rope_frequencies(head)[None, :]
    cosine = jnp.cos(angle)[:, None, :]
    sine = jnp.sin(angle)[:, None, :]
    first = shaped[:, :, : head // 2]
    second = shaped[:, :, head // 2 :]
    return jnp.concatenate(
        [first * cosine - second * sine, second * cosine + first * sine], axis=-1
    ).reshape(step_count, -1)


def unrotate(values, positions, head):
    step_count = values.shape[0]
    shaped = values.reshape(step_count, -1, head)
    angle = positions.astype(jnp.float32)[:, None] * rope_frequencies(head)[None, :]
    cosine = jnp.cos(angle)[:, None, :]
    sine = jnp.sin(angle)[:, None, :]
    first = shaped[:, :, : head // 2]
    second = shaped[:, :, head // 2 :]
    return jnp.concatenate(
        [first * cosine + second * sine, second * cosine - first * sine], axis=-1
    ).reshape(step_count, -1)


def norm_stats(rows):
    inverse = lax.rsqrt(jnp.mean(rows * rows, axis=-1, keepdims=True) + epsilon)
    return (rows * inverse, inverse)


def norm_back(grad, unit, inverse, gain):
    scaled = grad * gain
    inner = jnp.mean(scaled * unit, axis=-1, keepdims=True)
    return (inverse * (scaled - unit * inner), jnp.sum(grad * unit, axis=0))


def matmul(left, right):
    return jnp.dot(left, right, preferred_element_type=jnp.float32)


def block_layout(table, micro, groups, block):
    layout_row = lax.dynamic_index_in_dim(table, micro, 0, keepdims=False)
    span = groups // 2
    mine = lax.dynamic_index_in_dim(layout_row, lax.axis_index(DP), 0, keepdims=False)
    sequence = mine // span
    place = mine % span
    slot_ids = jnp.arange(groups, dtype=jnp.int32)
    holder = jnp.sum(
        jnp.where(layout_row[None, :] == slot_ids[:, None], slot_ids[None, :], 0), axis=1
    )
    slots = lax.dynamic_slice_in_dim(holder, sequence * span, span)
    positions = place * block + jnp.arange(block, dtype=jnp.int32)
    return (slots, positions)


def attend(query_rows, key_seq, value_seq, positions, heads_kv, head):
    step_count = query_rows.shape[0]
    keys_total = key_seq.shape[0]
    head_group = query_rows.shape[1] // (heads_kv * head)
    scale = 1.0 / math.sqrt(head)
    allowed = jnp.arange(keys_total, dtype=jnp.int32)[None, :] <= positions[:, None]
    query_layers = query_rows.reshape(step_count, heads_kv, head_group * head).transpose(1, 0, 2)
    key_layers = key_seq.reshape(keys_total, heads_kv, head).transpose(1, 0, 2)
    value_layers = value_seq.reshape(keys_total, heads_kv, head).transpose(1, 0, 2)

    def one_head(parts):
        q_head, k_head, v_head = parts
        q_three = q_head.reshape(step_count, head_group, head)
        scores = (
            jnp.einsum("qgd,kd->gqk", q_three, k_head, preferred_element_type=jnp.float32) * scale
        )
        total = jnp.sum(jnp.where(allowed, jnp.exp(scores), 0.0), axis=-1)
        log_total = jnp.log(total)
        probs = jnp.where(allowed, jnp.exp(scores - log_total[..., None]), 0.0).astype(jnp.bfloat16)
        mixed = jnp.einsum("gqk,kd->qgd", probs, v_head, preferred_element_type=jnp.float32).astype(
            jnp.bfloat16
        )
        return (mixed.reshape(step_count, head_group * head), log_total)

    mixed, log_total = lax.map(one_head, (query_layers, key_layers, value_layers))
    return (mixed.transpose(1, 0, 2).reshape(step_count, -1), log_total)


def attend_back(
    blended_gradient, query_rows, key_seq, value_seq, log_total, positions, heads_kv, head
):
    step_count = query_rows.shape[0]
    keys_total = key_seq.shape[0]
    head_group = query_rows.shape[1] // (heads_kv * head)
    scale = 1.0 / math.sqrt(head)
    allowed = jnp.arange(keys_total, dtype=jnp.int32)[None, :] <= positions[:, None]
    query_layers = query_rows.reshape(step_count, heads_kv, head_group * head).transpose(1, 0, 2)
    key_layers = key_seq.reshape(keys_total, heads_kv, head).transpose(1, 0, 2)
    value_layers = value_seq.reshape(keys_total, heads_kv, head).transpose(1, 0, 2)
    gain_layers = blended_gradient.reshape(step_count, heads_kv, head_group * head).transpose(
        1, 0, 2
    )

    def one_head(parts):
        q_head, k_head, v_head, g_head, l_head = parts
        q_three = q_head.reshape(step_count, head_group, head)
        g_three = g_head.reshape(step_count, head_group, head)
        scores = (
            jnp.einsum("qgd,kd->gqk", q_three, k_head, preferred_element_type=jnp.float32) * scale
        )
        probs = jnp.where(allowed, jnp.exp(scores - l_head[..., None]), 0.0)
        rounded = probs.astype(jnp.bfloat16)
        prob_grad = jnp.einsum("qgd,kd->gqk", g_three, v_head, preferred_element_type=jnp.float32)
        value_total_sum = jnp.einsum(
            "gqk,qgd->kd", rounded, g_three, preferred_element_type=jnp.float32
        )
        rowdot = jnp.sum(probs * prob_grad, axis=-1, keepdims=True)
        score_grad = (probs * (prob_grad - rowdot) * scale).astype(jnp.bfloat16)
        query_grad = jnp.einsum(
            "gqk,kd->qgd", score_grad, k_head, preferred_element_type=jnp.float32
        )
        key_gradient = jnp.einsum(
            "gqk,qgd->kd", score_grad, q_three, preferred_element_type=jnp.float32
        )
        return (query_grad.reshape(step_count, head_group * head), key_gradient, value_total_sum)

    query_grad, key_gradient, value_total_sum = lax.map(
        one_head, (query_layers, key_layers, value_layers, gain_layers, log_total)
    )
    query_grad = query_grad.transpose(1, 0, 2).reshape(step_count, -1)
    key_gradient = key_gradient.transpose(1, 0, 2).reshape(keys_total, -1)
    value_total_sum = value_total_sum.transpose(1, 0, 2).reshape(keys_total, -1)
    return (query_grad, key_gradient, value_total_sum)


def layer_forward(rows, table, micro, weights, groups, heads_kv, head):
    wq, wk, wv, wo, w_gate, w_up, w_down, gain_attn, gain_mlp = weights
    full = lax.all_gather(rows, TENSOR, axis=0, tiled=True)
    block = full.shape[0]
    slots, positions = block_layout(table, micro, groups, block)
    unit1, inverse1 = norm_stats(full)
    normed1 = (unit1 * gain_attn.astype(jnp.float32)).astype(jnp.bfloat16)
    query_rows = rotate(matmul(normed1, wq), positions, head).astype(jnp.bfloat16)
    key = rotate(matmul(normed1, wk), positions, head).astype(jnp.bfloat16)
    value_rows = matmul(normed1, wv).astype(jnp.bfloat16)
    key_all, value_all = (
        lax.all_gather(key, DP, axis=0, tiled=True),
        lax.all_gather(value_rows, DP, axis=0, tiled=True),
    )
    kv_width = key.shape[1]
    key_seq = key_all.reshape(groups, block, kv_width)[slots].reshape(-1, kv_width)
    value_seq = value_all.reshape(groups, block, kv_width)[slots].reshape(-1, kv_width)
    mixed, log_total = attend(query_rows, key_seq, value_seq, positions, heads_kv, head)
    second = rows + lax.psum_scatter(matmul(mixed, wo), TENSOR, scatter_dimension=0, tiled=True)
    full_second = lax.all_gather(second, TENSOR, axis=0, tiled=True)
    unit2, inverse2 = norm_stats(full_second)
    normed2 = (unit2 * gain_mlp.astype(jnp.float32)).astype(jnp.bfloat16)
    gate = matmul(normed2, w_gate)
    upper = matmul(normed2, w_up)
    hidden = (jax.nn.silu(gate) * upper).astype(jnp.bfloat16)
    result = second + lax.psum_scatter(
        matmul(hidden, w_down), TENSOR, scatter_dimension=0, tiled=True
    )
    return (
        result,
        (
            full,
            query_rows,
            key_seq,
            value_seq,
            mixed,
            log_total,
            full_second,
            gate,
            upper,
            hidden,
            slots,
            positions,
        ),
    )


def layer_backward(grad_rows, context, weights, groups, parts, heads_kv, head):
    wq, wk, wv, wo, w_gate, w_up, w_down, gain_attn, gain_mlp = weights
    (
        full,
        query_rows,
        key_seq,
        value_seq,
        mixed,
        log_total,
        full_second,
        gate,
        upper,
        hidden,
        slots,
        positions,
    ) = context
    block = full.shape[0]
    out_grad = lax.all_gather(grad_rows.astype(jnp.bfloat16), TENSOR, axis=0, tiled=True)
    grad_down = matmul(hidden.T, out_grad)
    hidden_grad = matmul(out_grad, w_down.T)
    sigma = jax.nn.sigmoid(gate)
    gate_grad = (hidden_grad * upper * sigma * (1.0 + gate * (1.0 - sigma))).astype(jnp.bfloat16)
    up_grad = (hidden_grad * gate * sigma).astype(jnp.bfloat16)
    unit2, inverse2 = norm_stats(full_second)
    normed2 = (unit2 * gain_mlp.astype(jnp.float32)).astype(jnp.bfloat16)
    grad_gate = matmul(normed2.T, gate_grad)
    grad_up = matmul(normed2.T, up_grad)
    normed2_grad = matmul(gate_grad, w_gate.T) + matmul(up_grad, w_up.T)
    second_terms, gain_mlp_terms = norm_back(
        normed2_grad, unit2, inverse2, gain_mlp.astype(jnp.float32)
    )
    piece_width = gain_mlp_terms.shape[0] // (groups * parts)
    second_part, gain_mlp_part = (
        lax.psum_scatter(
            second_terms.astype(jnp.bfloat16), TENSOR, scatter_dimension=0, tiled=True
        ).astype(jnp.float32),
        lax.psum_scatter(
            gain_mlp_terms.reshape(groups, parts, piece_width).astype(jnp.bfloat16),
            TENSOR,
            scatter_dimension=1,
            tiled=True,
        ).astype(jnp.float32),
    )
    second_grad = grad_rows + second_part
    attn_grad = lax.all_gather(second_grad.astype(jnp.bfloat16), TENSOR, axis=0, tiled=True)
    grad_wo = matmul(mixed.T, attn_grad)
    blended_gradient = matmul(attn_grad, wo.T).astype(jnp.bfloat16)
    query_grad, key_seq_grad, value_seq_grad = attend_back(
        blended_gradient, query_rows, key_seq, value_seq, log_total, positions, heads_kv, head
    )
    kv_width = key_seq.shape[1]
    key_spread = (
        jnp.zeros((groups, block, kv_width), jnp.float32)
        .at[slots]
        .set(key_seq_grad.reshape(-1, block, kv_width))
    )
    value_spread = (
        jnp.zeros((groups, block, kv_width), jnp.float32)
        .at[slots]
        .set(value_seq_grad.reshape(-1, block, kv_width))
    )
    key_own, value_own = (
        lax.psum_scatter(
            key_spread.astype(jnp.bfloat16), DP, scatter_dimension=0, tiled=True
        ).astype(jnp.float32),
        lax.psum_scatter(
            value_spread.astype(jnp.bfloat16), DP, scatter_dimension=0, tiled=True
        ).astype(jnp.float32),
    )
    query_round = unrotate(query_grad, positions, head).astype(jnp.bfloat16)
    key_round = unrotate(key_own.reshape(block, kv_width), positions, head).astype(jnp.bfloat16)
    value_round = value_own.reshape(block, kv_width).astype(jnp.bfloat16)
    unit1, inverse1 = norm_stats(full)
    normed1 = (unit1 * gain_attn.astype(jnp.float32)).astype(jnp.bfloat16)
    grad_wq = matmul(normed1.T, query_round)
    grad_wk = matmul(normed1.T, key_round)
    grad_wv = matmul(normed1.T, value_round)
    normed1_grad = matmul(query_round, wq.T) + matmul(key_round, wk.T) + matmul(value_round, wv.T)
    first_terms, gain_attn_terms = norm_back(
        normed1_grad, unit1, inverse1, gain_attn.astype(jnp.float32)
    )
    first_part, gain_attn_part = (
        lax.psum_scatter(first_terms, TENSOR, scatter_dimension=0, tiled=True),
        lax.psum_scatter(
            gain_attn_terms.reshape(groups, parts, piece_width),
            TENSOR,
            scatter_dimension=1,
            tiled=True,
        ),
    )
    input_grad = second_grad + first_part
    return (
        input_grad,
        (
            grad_wq,
            grad_wk,
            grad_wv,
            grad_wo,
            grad_gate,
            grad_up,
            grad_down,
            gain_attn_part,
            gain_mlp_part,
        ),
    )


def reduce_grads(pieces):
    return (
        lax.psum_scatter(
            pieces[0].astype(jnp.bfloat16), DP, scatter_dimension=0, tiled=True
        ).astype(jnp.float32),
        lax.psum_scatter(
            pieces[1].astype(jnp.bfloat16), DP, scatter_dimension=0, tiled=True
        ).astype(jnp.float32),
        lax.psum_scatter(
            pieces[2].astype(jnp.bfloat16), DP, scatter_dimension=0, tiled=True
        ).astype(jnp.float32),
        lax.psum_scatter(
            pieces[3].astype(jnp.bfloat16), DP, scatter_dimension=1, tiled=True
        ).astype(jnp.float32),
        lax.psum_scatter(
            pieces[4].astype(jnp.bfloat16), DP, scatter_dimension=0, tiled=True
        ).astype(jnp.float32),
        lax.psum_scatter(
            pieces[5].astype(jnp.bfloat16), DP, scatter_dimension=0, tiled=True
        ).astype(jnp.float32),
        lax.psum_scatter(
            pieces[6].astype(jnp.bfloat16), DP, scatter_dimension=1, tiled=True
        ).astype(jnp.float32),
        lax.psum_scatter(
            pieces[7].astype(jnp.bfloat16), DP, scatter_dimension=0, tiled=True
        ).astype(jnp.float32),
        lax.psum_scatter(
            pieces[8].astype(jnp.bfloat16), DP, scatter_dimension=0, tiled=True
        ).astype(jnp.float32),
    )


def general_shards(inputs, table, cotangent, wq, wk, wv, wo, w_gate, w_up, w_down, gain_attn, gain_mlp):
    groups = lax.axis_size(DP)
    parts = lax.axis_size(TENSOR)
    micro_count = inputs.shape[0]
    section = lax.axis_index(SECTION)
    first_section = section == 0
    weights = (
        lax.all_gather(wq[0], DP, axis=0, tiled=True),
        lax.all_gather(wk[0], DP, axis=0, tiled=True),
        lax.all_gather(wv[0], DP, axis=0, tiled=True),
        lax.all_gather(wo[0], DP, axis=1, tiled=True),
        lax.all_gather(w_gate[0], DP, axis=0, tiled=True),
        lax.all_gather(w_up[0], DP, axis=0, tiled=True),
        lax.all_gather(w_down[0], DP, axis=1, tiled=True),
        lax.all_gather(gain_attn[0], DP, axis=0, tiled=True),
        lax.all_gather(gain_mlp[0], DP, axis=0, tiled=True),
    )
    head = HEAD_SIZE
    heads_kv = wk.shape[2] // head
    received = jnp.zeros_like(inputs[0])
    produced = []
    saved = []
    for step in range(micro_count + 1):
        own_rows = inputs[step] if step < micro_count else jnp.zeros_like(inputs[0])
        start_rows = jnp.where(first_section, own_rows, received)
        micro = jnp.clip(step - section, 0, micro_count - 1)
        result, context = layer_forward(start_rows, table, micro, weights, groups, heads_kv, head)
        produced.append(result)
        saved.append(context)
        if step < micro_count:
            received = passed_along(result, SECTION, 1)
    stacked = jnp.stack(produced)
    outputs = jnp.where(first_section, stacked[:micro_count], stacked[1:])[None]
    returned = jnp.zeros_like(inputs[0])
    returned_list = []
    totals = None
    for step in range(micro_count + 1):
        index = micro_count - 1 - step
        given = cotangent[index] if index >= 0 else jnp.zeros_like(cotangent[0])
        start_grad = jnp.where(first_section, returned, given)
        din, pieces = layer_backward(
            start_grad, saved[micro_count - step], weights, groups, parts, heads_kv, head
        )
        returned_list.append(din)
        if step < micro_count:
            returned = passed_along(din.astype(jnp.bfloat16), SECTION, -1).astype(din.dtype)
        totals = (
            pieces
            if totals is None
            else tuple((left + right for left, right in zip(totals, pieces)))
        )
    totals = reduce_grads(totals)
    reverse_stack = jnp.stack(returned_list[::-1])
    input_grad = jnp.where(first_section, reverse_stack[:micro_count], reverse_stack[1:])[None]
    (
        grad_wq,
        grad_wk,
        grad_wv,
        grad_wo,
        grad_gate,
        grad_up,
        grad_down,
        gain_attn_sum,
        gain_mlp_sum,
    ) = totals
    width_piece = gain_attn_sum.shape[-1]
    return (
        outputs,
        input_grad,
        grad_wq[None],
        grad_wk[None],
        grad_wv[None],
        grad_wo[None],
        grad_gate[None],
        grad_up[None],
        grad_down[None],
        gain_attn_sum.reshape(1, width_piece),
        gain_mlp_sum.reshape(1, width_piece),
    )


MESH = pl.DeviceIdType.MESH
SUBS = 4
HBM = pl.BlockSpec(memory_space=pl.ANY)
VMEM = pl.BlockSpec(memory_space=pltpu.VMEM)
SMEM = pl.BlockSpec(memory_space=pltpu.SMEM)
NARROW, WIDE = jnp.bfloat16, jnp.float32


def ring_place(index, count):
    return jnp.where(lax.rem(index, 2) == 0, index // 2, count - (index + 1) // 2)


def ring_index(place, count):
    place = lax.rem(place + 2 * count, count)
    return jnp.where(place < count // 2, 2 * place, 2 * count - 1 - 2 * place)


def greet(others):
    barrier = pltpu.get_barrier_semaphore()
    for other in others:
        pl.semaphore_signal(barrier, inc=1, device_id=other, device_id_type=MESH)
    pl.semaphore_wait(barrier, len(others))


def remote(source, target, send, recv, device):
    return pltpu.make_async_remote_copy(
        source, target, send, recv, device_id=device, device_id_type=MESH
    )


def partners(me, count):
    half = count // 2
    side, inside = me // half, lax.rem(me, half)
    peers = [(1 - side) * half + lax.rem(inside + k, half) for k in range(half)]
    peers += [side * half + lax.rem(inside + k, half) for k in range(1, half)]
    origins = [(1 - side) * half + lax.rem(inside + half - k, half) for k in range(half)]
    origins += [side * half + lax.rem(inside + half - k, half) for k in range(1, half)]
    return peers, origins


def aligned(start, size):
    return pl.ds(pl.multiple_of(start, size), size)


def tiles(size, tile):
    return [slice(at, at + tile) for at in range(0, size, tile)]


def loop(start, stop, body):
    if stop - start == 1:
        body(start)
    elif stop > start:

        def step(at, carry):
            body(at)
            return carry

        lax.fori_loop(start, stop, step, 0)


def dot(left, right, contract):
    return lax.dot_general(
        left, right, (contract, ((), ())), preferred_element_type=jnp.float32
    )


class Names:
    def __init__(self, **values):
        self.__dict__.update(values)


class Work:
    def __init__(self):
        self.items = []

    def add(self, body, count=1):
        self.items.append((body, 0, count))

    def first(self, body):
        self.items.insert(0, (body, 0, 1))

    def do(self, some=1 << 20):
        while some > 0 and self.items:
            body, start, stop = self.items.pop(0)
            until = min(stop, start + some)
            loop(start, until, body)
            some -= until - start
            if until < stop:
                self.items.insert(0, (body, until, stop))


class Copies:
    def __init__(self, sem):
        self.sem = sem
        self.used = 0

    def __call__(self, source, target):
        copy = pltpu.make_async_copy(source, target, self.sem.at[self.used])
        self.used += 1
        copy.start()
        return copy


class Ring:
    def __init__(self):
        self.count = lax.axis_size(DP)
        self.far = self.count // 2
        self.me = lax.axis_index(DP)
        self.core = lax.axis_index(TENSOR)
        self.place = ring_place(self.me, self.count)
        self.near = tuple({DP: ring_index(self.place + step, self.count)} for step in (1, -1))
        self.side = {TENSOR: 1 - self.core}

    def everyone(self):
        return [*self.near, self.side]

    def index(self, steps):
        return ring_index(self.place + steps, self.count)

    def orders(self):
        half = SUBS // 2
        for k in range(half):
            for sub in (k, k + half):
                yield sub, 0
                yield sub, 1


def gather_scratch(count):
    far = count // 2
    dma = pltpu.SemaphoreType.DMA
    return [
        dma((2, far, SUBS)), dma((2, far, SUBS)), dma((count, SUBS)), dma((count, SUBS)), dma((1,))
    ]


class Gather:
    def __init__(self, ring, x_ref, o_ref, sems):
        self.ring = ring
        self.x_ref, self.o_ref = x_ref, o_ref
        self.ring_send, self.ring_recv, self.side_send, self.side_recv, self.own_sem = sems
        self.rows = x_ref.shape[0]
        self.piece = self.rows // SUBS
        self.sends = []

    def spot(self, steps, sub, core):
        start = (self.ring.index(steps) * 2 + core) * self.rows + sub * self.piece
        return self.o_ref.at[aligned(start, self.piece), :]

    def mine(self, steps, sub):
        if steps == 0:
            return self.x_ref.at[sub * self.piece : (sub + 1) * self.piece, :]
        return self.spot(steps, sub, self.ring.core)

    def travels(self, way, hop, sub):
        return hop < self.ring.far or (sub < SUBS // 2) == (way == 0)

    def go(self, copy):
        copy.start()
        self.sends.append(copy)

    def pass_on(self, way, hop, sub):
        steps = 1 - hop if way == 0 else hop - 1
        self.go(
            remote(
                self.mine(steps, sub),
                self.spot(steps, sub, self.ring.core),
                self.ring_send.at[way, hop - 1, sub],
                self.ring_recv.at[way, hop - 1, sub],
                self.ring.near[way],
            )
        )

    def hand_over(self, steps, sub, slot):
        self.go(
            remote(
                self.mine(steps, sub),
                self.spot(steps, sub, self.ring.core),
                self.side_send.at[slot, sub],
                self.side_recv.at[slot, sub],
                self.ring.side,
            )
        )

    def start_piece(self, sub):
        for way in range(2):
            self.pass_on(way, 1, sub)
        self.hand_over(0, sub, 0)

    def start(self):
        for sub, way in self.ring.orders():
            if way == 0:
                self.start_piece(sub)
        self.started()

    def started(self):
        self.own = pltpu.make_async_copy(
            self.x_ref,
            self.o_ref.at[aligned((self.ring.me * 2 + self.ring.core) * self.rows, self.rows), :],
            self.own_sem.at[0],
        )
        self.own.start()

    def hop(self, hop, between=None):
        far, count = self.ring.far, self.ring.count
        for sub, way in self.ring.orders():
            if not self.travels(way, hop, sub):
                continue
            steps = -hop if way == 0 else hop
            here = self.spot(steps, sub, self.ring.core)
            remote(
                here, here, self.ring_send.at[way, hop - 1, sub],
                self.ring_recv.at[way, hop - 1, sub], self.ring.near[way],
            ).wait_recv()
            if hop < far and self.travels(way, hop + 1, sub):
                self.pass_on(way, hop + 1, sub)
            self.hand_over(steps, sub, hop if way == 0 or hop == far else count - hop)
            if way == 1 and between is not None:
                between()

    def side_arrived(self, steps):
        slot = -steps if steps <= 0 else self.ring.count - steps
        slot = self.ring.far if abs(steps) == self.ring.far else slot
        for sub in range(SUBS):
            there = self.spot(steps, sub, 1 - self.ring.core)
            remote(
                there, there, self.side_send.at[slot, sub], self.side_recv.at[slot, sub],
                self.ring.side,
            ).wait_recv()

    def around(self, hop):
        return (-hop, hop) if hop < self.ring.far else (-hop,)

    def sent(self):
        for copy in self.sends:
            copy.wait_send()

    def finish(self):
        self.own.wait()
        self.side_arrived(0)
        for hop in range(1, self.ring.far + 1):
            for steps in self.around(hop):
                self.side_arrived(steps)
        self.sent()

    def run(self, use, work):
        self.started()
        self.own.wait()
        waiting = [0]

        def between():
            if waiting:
                steps = waiting.pop(0)
                self.side_arrived(steps)
                use(self.ring.index(steps))
            else:
                work.do(1)

        for hop in range(1, self.ring.far + 1):
            self.hop(hop, between)
            waiting += self.around(hop)
        while waiting:
            between()
        self.sent()


def line_scratch(count):
    lines = count // 2
    dma = pltpu.SemaphoreType.DMA
    return [
        dma((2, lines)), dma((2, lines)), dma((2 * lines,)), dma((2 * lines,)),
        dma((2, 2 * lines)), dma((2, 2 * lines)), dma((1,)),
    ]


class LineGather:
    def __init__(self, ring, x_ref, o_ref, sems):
        self.ring = ring
        self.x_ref, self.o_ref = x_ref, o_ref
        self.lines = ring.count // 2
        self.line, self.column = ring.me // 2, lax.rem(ring.me, 2)
        self.next = {DP: ring.me + 1 - 2 * self.column}
        self.send, self.recv, self.next_send, self.next_recv = sems[:4]
        self.side_send, self.side_recv, self.own_sem = sems[4:]
        self.rows = x_ref.shape[0]
        self.sends = []

    def spot(self, steps, core, column):
        index = (self.line + steps) * 2 + column
        return self.o_ref.at[aligned((index * 2 + core) * self.rows, self.rows), :]

    def there(self, steps):
        if steps == 0:
            return None
        return self.line >= -steps if steps < 0 else self.line + steps < self.lines

    def if_there(self, condition, do):
        if condition is None:
            do()
        else:
            pl.when(condition)(do)

    def go(self, condition, copy):
        self.if_there(condition, copy.start)
        self.sends.append((condition, copy))

    def spread(self, steps):
        ring, slot = self.ring, steps + self.lines
        source = self.x_ref if steps == 0 else self.spot(steps, ring.core, self.column)
        target = self.spot(steps, ring.core, self.column)
        here = self.there(steps)
        both = lambda other: other if here is None else jnp.logical_and(here, other)
        for way, ahead in enumerate((self.line + 1 < self.lines, self.line > 0)):
            passed = -steps if way == 0 else steps
            if passed >= 0 and passed < self.lines - 1:
                self.go(
                    both(ahead),
                    remote(
                        source, target, self.send.at[way, passed], self.recv.at[way, passed],
                        {DP: ring.me + 2 - 4 * way},
                    ),
                )
        self.go(
            here, remote(source, target, self.next_send.at[slot], self.next_recv.at[slot], self.next)
        )
        self.go(
            here,
            remote(source, target, self.side_send.at[0, slot], self.side_recv.at[0, slot], ring.side),
        )

    def start(self):
        self.spread(0)
        self.own = pltpu.make_async_copy(
            self.x_ref, self.spot(0, self.ring.core, self.column), self.own_sem.at[0]
        )
        self.own.start()

    def hop(self, hop):
        for way, steps in enumerate((-hop, hop)):
            here = self.spot(steps, self.ring.core, self.column)
            copy = remote(
                here, here, self.send.at[way, hop - 1], self.recv.at[way, hop - 1], self.next
            )
            self.if_there(self.there(steps), copy.wait_recv)
            self.spread(steps)

    def finish(self):
        ring = self.ring
        every = range(1 - self.lines, self.lines)
        for steps in every:
            slot = steps + self.lines
            here = self.spot(steps, ring.core, 1 - self.column)
            copy = remote(here, here, self.next_send.at[slot], self.next_recv.at[slot], self.next)
            self.if_there(self.there(steps), copy.wait_recv)
            self.go(
                self.there(steps),
                remote(here, here, self.side_send.at[1, slot], self.side_recv.at[1, slot], ring.side),
            )
        for which, column in enumerate((self.column, 1 - self.column)):
            for steps in every:
                slot = steps + self.lines
                here = self.spot(steps, 1 - ring.core, column)
                copy = remote(
                    here, here, self.side_send.at[which, slot], self.side_recv.at[which, slot], ring.side
                )
                self.if_there(self.there(steps), copy.wait_recv)
        for condition, copy in self.sends:
            self.if_there(condition, copy.wait_send)
        self.own.wait()


def reduce_scratch(count, rows, width):
    far = count // 2
    dma = pltpu.SemaphoreType.DMA
    return [
        pltpu.VMEM((count * 2 * rows, width), NARROW),
        pltpu.VMEM((count, rows, width), NARROW),
        pltpu.VMEM((2, far, rows, width), NARROW),
        pltpu.VMEM((2, far, rows, width), NARROW),
        dma((2, far, SUBS)), dma((2, far, SUBS)), dma((count,)), dma((count,)),
    ]


class Reduce:
    def __init__(self, ring, scratch):
        self.ring = ring
        self.parts, self.beside, self.outgoing, self.incoming = scratch[:4]
        self.ring_send, self.ring_recv, self.side_send, self.side_recv = scratch[4:]
        self.rows = self.beside.shape[1]
        self.piece = self.rows // SUBS

    def span(self, sub):
        return slice(sub * self.piece, (sub + 1) * self.piece)

    def spot(self, steps, core, sub=None):
        start = (self.ring.index(steps) * 2 + core) * self.rows
        if sub is None:
            return aligned(start, self.rows)
        return aligned(start + sub * self.piece, self.piece)

    def make(self):
        steps = self.to_make.pop(0)
        self.produce(self.ring.index(steps), self.parts)
        slot = len(self.slots)
        copy = remote(
            self.parts.at[self.spot(steps, 1 - self.ring.core), :], self.beside.at[slot],
            self.side_send.at[slot], self.side_recv.at[slot], self.ring.side,
        )
        copy.start()
        self.slots[steps] = (slot, copy)

    def mine(self, steps, sub):
        while steps not in self.slots:
            self.make()
        slot, copy = self.slots[steps]
        if steps not in self.joined:
            copy.wait_recv()
            self.joined.add(steps)
        return self.parts[self.spot(steps, self.ring.core, sub), :].astype(
            jnp.float32
        ) + self.beside[slot, self.span(sub), :].astype(jnp.float32)

    def travels(self, way, step, sub):
        return step > 1 or (sub < SUBS // 2) == (way == 0)

    def ring_copy(self, way, step, sub):
        return remote(
            self.outgoing.at[way, step - 1, self.span(sub), :],
            self.incoming.at[way, step - 1, self.span(sub), :],
            self.ring_send.at[way, step - 1, sub],
            self.ring_recv.at[way, step - 1, sub],
            self.ring.near[way],
        )

    def step(self, step):
        far = self.ring.far
        for sub, way in self.ring.orders():
            if not self.travels(way, step, sub):
                continue
            steps = far + 1 - step
            steps = steps if way == 0 or steps == far else -steps
            value = self.mine(steps, sub)
            if step > 1 and self.travels(way, step - 1, sub):
                self.ring_copy(way, step - 1, sub).wait_recv()
                value = value + self.incoming[way, step - 2, self.span(sub), :].astype(jnp.float32)
            self.outgoing[way, step - 1, self.span(sub), :] = value.astype(NARROW)
            copy = self.ring_copy(way, step, sub)
            copy.start()
            self.sends.append(copy)
            if way == 1:
                if self.to_make:
                    self.make()
                else:
                    self.work.do(1)

    def begin(self, produce, work):
        self.produce, self.work = produce, work
        self.slots, self.joined, self.sends = {}, set(), []
        far = self.ring.far
        self.to_make = [far]
        for steps in range(far - 1, 0, -1):
            self.to_make += [steps, -steps]
        self.to_make.append(0)
        self.make()
        self.make()

    def end(self, finish):
        far = self.ring.far
        while self.to_make:
            self.make()
        for sub, way in self.ring.orders():
            if way == 1:
                continue
            value = self.mine(0, sub)
            for way in range(2):
                self.ring_copy(way, far, sub).wait_recv()
                value = value + self.incoming[way, far - 1, self.span(sub), :].astype(jnp.float32)
            finish(sub, self.span(sub), value)
        for copy in self.sends:
            copy.wait_send()
        for _, copy in self.slots.values():
            copy.wait_send()

    def run(self, produce, finish, work, beside=()):
        beside = list(beside)
        self.begin(produce, work)
        for step in range(1, self.ring.far + 1):
            self.step(step)
            if beside:
                beside.pop(0)()
        self.end(finish)
        return beside


def products(left, right, transposed, tile=512):
    width = right.shape[0] if transposed else right.shape[1]
    number = width // tile

    def produce(index, parts):
        block = parts.shape[0] // lax.axis_size(DP)
        rows = aligned(index * block, block)

        def one(at):
            cols = aligned(at * tile, tile)
            if transposed:
                part = dot(left[rows, :], right[cols, :], ((1,), (1,)))
            else:
                part = dot(left[rows, :], right[:, cols], ((1,), (0,)))
            parts[rows, cols] = part.astype(NARROW)

        loop(0, number, one)

    return produce


def add_gradient(work, left, right, out, tile=256):
    if out.shape[0] >= out.shape[1]:

        def piece(at):
            cols = aligned(at * tile, tile)
            out[cols, :] = dot(left[:, cols], right[...], ((0,), (0,))).astype(NARROW)

        work.add(piece, out.shape[0] // tile)
    else:

        def piece(at):
            cols = aligned(at * tile, tile)
            out[:, cols] = dot(left[...], right[:, cols], ((0,), (0,))).astype(NARROW)

        work.add(piece, out.shape[1] // tile)


def unit_rows(value):
    inverse = lax.rsqrt(jnp.mean(value * value, axis=-1, keepdims=True) + epsilon)
    return value * inverse, inverse


def through_norm(grad, value, gain):
    unit, inverse = unit_rows(value)
    scaled = grad * gain
    inner = jnp.mean(scaled * unit, axis=-1, keepdims=True)
    return inverse * (scaled - unit * inner), jnp.sum(grad * unit, axis=0, keepdims=True)


def shape_of(*dims, kind=NARROW):
    return jax.ShapeDtypeStruct(dims, kind)


def call_fused(name, body, cid, us, ins, outs, scratch):
    def kernel(*refs):
        refs = list(refs)
        named = {key: refs.pop(0) for key in [*ins, *outs]}
        for key, kind in scratch.items():
            named[key] = [refs.pop(0) for _ in kind] if isinstance(kind, list) else refs.pop(0)
        body(Names(**named))

    flat = []
    for kind in scratch.values():
        flat += kind if isinstance(kind, list) else [kind]
    result = pl.pallas_call(
        kernel,
        out_shape=tuple(shape for shape, _ in outs.values()),
        in_specs=[spec for _, spec in ins.values()],
        out_specs=tuple(spec for _, spec in outs.values()),
        scratch_shapes=flat,
        compiler_params=pltpu.CompilerParams(
            collective_id=cid, has_side_effects=True, vmem_limit_bytes=63 * 1024 * 1024
        ),
        cost_estimate=pl.CostEstimate(
            flops=0, bytes_accessed=int(us * 3.69e6), transcendentals=0
        ),
        name=name,
    )(*[value for value, _ in ins.values()])
    return Names(**dict(zip(outs, result)))


def swap_halves(rows, head):
    width = rows.shape[1]
    lane = lax.broadcasted_iota(jnp.int32, rows.shape, 1)
    half = head // 2
    return jnp.where(
        lax.rem(lane, head) < half, pltpu.roll(rows, width - half, 1), pltpu.roll(rows, half, 1)
    )


def low_lanes(shape, head):
    return lax.broadcasted_iota(jnp.int32, shape, 1) < head


def two_heads(rows, head):
    low = low_lanes(rows.shape, head)
    zero = jnp.zeros_like(rows)
    return jnp.concatenate([jnp.where(low, rows, zero), jnp.where(low, zero, rows)], axis=0)


def one_row(rows, head):
    half = rows.shape[0] // 2
    return jnp.where(low_lanes((half, rows.shape[1]), head), rows[:half], rows[half:])


def triangle(block, keys):
    row = lax.rem(lax.broadcasted_iota(jnp.int32, (2 * block, keys), 0), block)
    column = lax.broadcasted_iota(jnp.int32, (2 * block, keys), 1)
    return column <= row + (keys - block)


def in_order(ref, order, spot, block):
    value = ref[:block, :]
    for other in range(1, ref.shape[0] // block):
        there = order[spot] == other
        value = jnp.where(there, ref[other * block : (other + 1) * block, :], value)
    return value


def attend_here(slots, qkv, cosine, sine, kept, lse, mixed, key2, value2):
    groups = slots.shape[0]
    tokens = qkv.shape[0]
    block = tokens // groups
    span = groups // 2
    wide = qkv.shape[1] // 2
    head = wide // 2
    scale = 1.0 / math.sqrt(head)
    for spot in range(groups):
        here = slice(spot * block, (spot + 1) * block)
        turn_rows = slice(spot % span * block, (spot % span + 1) * block)
        turned_by, turned_sine = cosine[turn_rows, :], sine[turn_rows, :]
        rows = in_order(qkv, slots, spot, block)
        query, pair = rows[:, :wide], rows[:, wide:]
        low = low_lanes(pair.shape, head)
        query = query * turned_by + swap_halves(query, head) * turned_sine
        pair = jnp.where(low, pair * turned_by + swap_halves(pair, head) * turned_sine, pair)
        other = pltpu.roll(pair, head, 1)
        kept[here, :wide] = query.astype(kept.dtype)
        kept[here, wide:] = pair.astype(kept.dtype)
        key2[here, :] = jnp.where(low, pair, other).astype(key2.dtype)
        value2[here, :] = jnp.where(low, other, pair).astype(value2.dtype)
    for spot in range(groups):
        here = slice(spot * block, (spot + 1) * block)
        first = spot // span * span * block
        keys = (spot % span + 1) * block
        query = two_heads(kept[here, :wide], head)
        score = dot(query, key2[first : first + keys, :], ((1,), (1,))) * scale
        allowed = triangle(block, keys)
        power = jnp.where(allowed, jnp.exp(score), 0.0)
        total = jnp.sum(power, axis=1, keepdims=True)
        log_total = jnp.log(total)
        probs = (power * (1.0 / total)).astype(jnp.bfloat16)
        value = dot(probs, value2[first : first + keys, :], ((1,), (0,)))
        mixed[here, :] = one_row(value, head).astype(mixed.dtype)
        lse[spot] = log_total


def attend_back_here(
    slots, grad, kept, lse, cosine, sine, out, key2, value2, key_sum, value_sum, between=None
):
    groups = slots.shape[0]
    tokens = kept.shape[0]
    block = tokens // groups
    span = groups // 2
    wide = kept.shape[1] // 2
    head = wide // 2
    scale = 1.0 / math.sqrt(head)
    for spot in range(groups):
        here = slice(spot * block, (spot + 1) * block)
        pair = kept[here, wide:].astype(jnp.float32)
        low = low_lanes(pair.shape, head)
        other = pltpu.roll(pair, head, 1)
        key2[here, :] = jnp.where(low, pair, other).astype(key2.dtype)
        value2[here, :] = jnp.where(low, other, pair).astype(value2.dtype)
    for spot in range(groups - 1, -1, -1):
        here = slice(spot * block, (spot + 1) * block)
        place = spot % span
        turn_rows = slice(place * block, (place + 1) * block)
        first = spot // span * span * block
        keys = (place + 1) * block
        query = two_heads(kept[here, :wide], head)
        given = two_heads(in_order(grad, slots, spot, block), head)
        key = key2[first : first + keys, :]
        value = value2[first : first + keys, :]
        score = dot(query, key, ((1,), (1,))) * scale
        probs = jnp.where(triangle(block, keys), jnp.exp(score - lse[spot]), 0.0)
        prob_grad = dot(given, value, ((1,), (1,)))
        rowdot = jnp.sum(probs * prob_grad, axis=1, keepdims=True)
        score_grad = (probs * (prob_grad - rowdot) * scale).astype(jnp.bfloat16)
        value_part = dot(probs.astype(jnp.bfloat16), given, ((0,), (0,)))
        key_part = dot(score_grad, query, ((0,), (0,)))
        if place == span - 1:
            value_sum[first : first + keys, :] = value_part
            key_sum[first : first + keys, :] = key_part
        else:
            value_sum[first : first + keys, :] += value_part
            key_sum[first : first + keys, :] += key_part
        query_grad = one_row(dot(score_grad, key, ((1,), (0,))), head)
        query_grad = query_grad * cosine[turn_rows, :] - swap_halves(query_grad, head) * sine[turn_rows, :]
        out[here, :wide] = query_grad.astype(out.dtype)
        if between is not None:
            between(spot)
    for spot in range(groups):
        here = slice(spot * block, (spot + 1) * block)
        turn_rows = slice(spot % span * block, (spot % span + 1) * block)
        key = key_sum[here, :]
        key = key + pltpu.roll(key, head, 1)
        key = key * cosine[turn_rows, :] - swap_halves(key, head) * sine[turn_rows, :]
        value = value_sum[here, :]
        value = value + pltpu.roll(value, head, 1)
        out[here, wide:] = jnp.where(low_lanes(key.shape, head), key, value).astype(out.dtype)


def put_back(source, target, row):
    groups = row.shape[0]
    block = source.shape[0] // groups
    for spot in range(groups):
        target[spot * block : (spot + 1) * block, :] = in_order(source, row, spot, block)


def attend_scratch(tokens, head, back=False):
    vmem = pltpu.VMEM
    wide = 2 * head
    kinds = dict(
        key2=vmem((tokens, wide), jnp.bfloat16),
        value2=vmem((tokens, wide), jnp.bfloat16),
        by_number=vmem((tokens, 2 * wide if back else wide), jnp.bfloat16),
    )
    if back:
        kinds.update(
            key_sum=vmem((tokens, wide), jnp.float32), value_sum=vmem((tokens, wide), jnp.float32)
        )
    return kinds


def rope_tables(tokens, head):
    angle = jnp.arange(tokens, dtype=jnp.float32)[:, None] * rope_frequencies(head)[None, :]
    cosine = jnp.cos(angle)
    sine = jnp.sin(angle)
    return (
        jnp.concatenate([cosine] * 4, axis=1),
        jnp.concatenate([-sine, sine] * 2, axis=1),
    )


def weight_pieces(source, target, count, heads, srcs, dsts, layer):
    qkv, wo, gate, up, down = srcs
    out_qkv, out_wo, out_gu, out_down = dsts
    depth = gate.shape[1]
    hidden = gate.shape[2] // count
    q_rows = wo.shape[1] // count
    kv_rows = (qkv.shape[0] - wo.shape[1]) // 2
    shared = count * heads // kv_rows
    cols = aligned(source * depth, depth)
    k_from = pl.multiple_of(wo.shape[1] + target // shared * heads, heads)
    v_from = pl.multiple_of(wo.shape[1] + kv_rows + target // shared * heads, heads)
    mine = aligned(target * hidden, hidden)
    return (
        (qkv.at[aligned(target * q_rows, q_rows), :], out_qkv.at[layer, pl.ds(0, q_rows), cols]),
        (qkv.at[pl.ds(k_from, heads), :], out_qkv.at[layer, pl.ds(q_rows, heads), cols]),
        (qkv.at[pl.ds(v_from, heads), :], out_qkv.at[layer, pl.ds(q_rows + heads, heads), cols]),
        (wo.at[0, aligned(target * q_rows, q_rows), :], out_wo.at[layer, :, cols]),
        (gate.at[0, :, mine], out_gu.at[layer, cols, pl.ds(0, hidden)]),
        (up.at[0, :, mine], out_gu.at[layer, cols, pl.ds(hidden, hidden)]),
        (down.at[0, mine, :], out_down.at[layer, :, cols]),
    )


KINDS, ATTENTION_KINDS = 7, 4


class Spread:
    def __init__(self, ring, heads, srcs, dsts, sems):
        self.ring = ring
        self.layer = lax.axis_index(SECTION)
        self.across = {SECTION: 1 - self.layer}
        self.peers, self.origins = partners(ring.me, ring.count)
        self.send, self.recv, self.cross_send, self.cross_recv, self.own_sem = sems
        self.pieces = lambda source, target, layer: weight_pieces(
            source, target, ring.count, heads, srcs, dsts, layer
        )
        self.started, self.local = [], {}
        half = ring.count // 2
        self.near, self.far = list(range(half, ring.count - 1)), list(range(half))

    def go(self, copy):
        copy.start()
        self.started.append(copy)

    def own(self, kinds):
        last = self.ring.count - 1
        for kind in kinds:
            source, target = self.pieces(self.ring.me, self.ring.me, self.layer)[kind]
            self.go(
                remote(
                    source, target, self.cross_send.at[kind, last], self.cross_recv.at[kind, last],
                    self.across,
                )
            )
            self.local[kind] = pltpu.make_async_copy(source, target, self.own_sem.at[kind])
            self.local[kind].start()

    def out(self, kind, places):
        for k in places:
            source, target = self.pieces(self.ring.me, self.peers[k], self.layer)[kind]
            self.go(
                remote(
                    source, target, self.send.at[kind, k], self.recv.at[kind, k],
                    {DP: self.peers[k]},
                )
            )

    def pass_on(self, kind, places):
        for k in places:
            here = self.pieces(self.origins[k], self.ring.me, self.layer)[kind][1]
            remote(
                here, here, self.send.at[kind, k], self.recv.at[kind, k], {DP: self.origins[k]}
            ).wait_recv()
            self.go(
                remote(
                    here, here, self.cross_send.at[kind, k], self.cross_recv.at[kind, k], self.across
                )
            )

    def here(self, kinds):
        for kind in kinds:
            self.local[kind].wait()
            for k in range(self.ring.count):
                origin = self.origins[k] if k < self.ring.count - 1 else self.ring.me
                there = self.pieces(origin, self.ring.me, 1 - self.layer)[kind][1]
                remote(
                    there, there, self.cross_send.at[kind, k], self.cross_recv.at[kind, k], self.across
                ).wait_recv()

    def sent(self):
        for copy in self.started:
            copy.wait_send()


def chip_rows(index, local):
    return aligned(index * 2 * local, 2 * local)


def feed_forward_use(s, local, after):
    width = s.hidden.shape[1]
    tile = 256
    number = width // tile

    def use(index):
        rows = chip_rows(index, local)

        def one(at):
            start = at * tile
            cols, right = aligned(start, tile), aligned(start + width, tile)
            value = s.normed2[rows, :]
            gate = dot(value, s.gu[:, cols], ((1,), (0,)))
            upper = dot(value, s.gu[:, right], ((1,), (0,)))
            s.hidden[rows, cols] = (gate * jax.nn.sigmoid(gate) * upper).astype(NARROW)
            after(rows, cols, right, gate, upper)

        loop(0, number, one)

    return use


def feed_forward_back(s, rows, cols, right, gate, upper):
    hidden_grad = dot(s.out_grad[rows, :], s.down[cols, :], ((1,), (1,)))
    sigma = jax.nn.sigmoid(gate)
    gate_grad = hidden_grad * upper * sigma * (1.0 + gate * (1.0 - sigma))
    s.gu_grad[rows, cols] = gate_grad.astype(NARROW)
    s.gu_grad[rows, right] = (hidden_grad * gate * sigma).astype(NARROW)


def opening_body(s):
    ring = Ring()
    layer = lax.axis_index(SECTION)
    peers, origins = partners(ring.me, ring.count)
    holders = [{DP: peer} for peer in peers] + [
        {SECTION: 1 - layer, DP: peer} for peer in [*peers, ring.me]
    ]
    greet([*holders, ring.side])
    copies = Copies(s.copy_sem)
    rows_in = copies(s.inputs.at[layer], s.rows)
    given_in = copies(s.cotangent.at[layer], s.given)
    spread = Spread(
        ring, s.kept0.shape[1] // 4, (s.qkv, s.wo, s.gate, s.up, s.down_in),
        (s.out_qkv, s.out_wo, s.out_gu, s.out_down), s.spread_sems,
    )
    attention, feed = range(ATTENTION_KINDS), range(ATTENTION_KINDS, KINDS)
    local, depth = s.rows.shape[0], s.gain_attn.shape[1]

    s.gain_piece[...] = jnp.zeros_like(s.gain_piece)
    s.gain_piece[0:1, :] = s.gain_attn[...].astype(WIDE)
    s.gain_piece[1:2, :] = s.gain_mlp[...].astype(WIDE)
    gain_send, gain_recv = s.gain_sems
    spot = lambda at, source: s.gains.at[at, :, aligned(source * depth, depth)]
    for k, holder in enumerate(holders):
        spread.go(remote(s.gain_piece, spot(layer, ring.me), gain_send.at[k], gain_recv.at[k], holder))
    own_gains = copies(s.gain_piece, spot(layer, ring.me))
    spread.own(attention)
    own_gains.wait()
    for k, holder in enumerate(holders):
        at, place = (layer, k) if k < ring.count - 1 else (1 - layer, k - ring.count + 1)
        here = spot(at, origins[place] if place < ring.count - 1 else ring.me)
        remote(here, here, gain_send.at[k], gain_recv.at[k], holder).wait_recv()

    rows_in.wait()
    unit, _ = unit_rows(s.rows[...])
    s.shard0[...] = (unit * s.gains[0, 0:1, :]).astype(NARROW)
    first = LineGather(ring, s.shard0, s.normed1, s.line_sems)
    first.start()
    for kind in attention:
        spread.out(kind, spread.far + spread.near)
    for hop in range(1, ring.far):
        first.hop(hop)
    given_in.wait()
    s.shard1[...] = s.given[...].astype(NARROW)
    grads = LineGather(ring, s.shard1, s.out_grad, s.grads_sems)
    grads.start()
    for kind in attention:
        spread.pass_on(kind, spread.near + spread.far)
    gate, up, down = feed
    spread.out(gate, spread.far + spread.near)
    spread.own(feed)
    first.finish()
    spread.here(attention)
    loads = [
        copies(s.out_qkv.at[0], s.qkv_w), copies(s.out_qkv.at[1], s.next_qkv_w),
        copies(s.out_wo.at[0], s.wo_w),
    ]
    stores = [copies(s.normed1, s.normed1_out)]
    for load in loads:
        load.wait()
    tile = 2 * local

    def project(at):
        rows = aligned(at * tile, tile)
        s.projected[rows, :] = dot(s.normed1[rows, :], s.qkv_w[...], ((1,), (1,)))

    loop(0, s.projected.shape[0] // tile, project)
    attend_here(s.slots, s.projected, s.cosine, s.sine, s.kept0, s.lse0, s.by_number, s.key2, s.value2)
    put_back(s.by_number, s.mixed0, s.row)
    stores[0].wait()
    grads.hop(1)

    reduce = Reduce(ring, s.reduce)
    none = Work()

    second_rows = Gather(ring, s.shard2, s.normed2, s.gather_sems)
    next_rows = Gather(ring, s.shard0, s.normed1, s.first_sems)

    def second(sub, span, value):
        value = s.rows[span, :] + value
        s.second[span, :] = value
        unit, _ = unit_rows(value)
        s.shard2[span, :] = (unit * s.gains[0, 1:2, :]).astype(NARROW)
        second_rows.start_piece(sub)

    middle = len(spread.far) // 2
    early, late = spread.near + spread.far[:middle], spread.far[middle:]

    def stage(number):
        kind, places = ((up, early), (up, late), (down, early), (down, late))[number]
        spread.out(kind, places)
        if number == 0:
            spread.pass_on(gate, spread.near + spread.far)
        else:
            kind, places = ((up, early), (up, late), (down, early))[number - 1]
            spread.pass_on(kind, places)
        if number + 2 < ring.far:
            grads.hop(number + 2)

    left = reduce.run(
        products(s.mixed0, s.wo_w, False), second, none,
        [functools.partial(stage, number) for number in range(4)],
    )
    for do in left:
        do()
    spread.pass_on(down, late)
    spread.here((gate, up))
    copies(s.out_gu.at[0], s.gu).wait()

    def keep(rows, cols, right, gate, upper):
        s.gate_up[rows, cols] = gate
        s.gate_up[rows, right] = upper

    second_rows.run(feed_forward_use(s, local, keep), none)
    spread.here((down,))
    load = copies(s.out_down.at[0], s.down)
    grads.finish()
    stores += [
        copies(s.out_grad, s.out_grad_out), copies(s.normed2, s.normed2_out),
        copies(s.gate_up, s.gate_up_out),
    ]
    load.wait()

    def result(sub, span, value):
        value = s.second[span, :] + value
        s.result[span, :] = value
        unit, _ = unit_rows(value)
        s.shard0[span, :] = (unit * s.gains[1, 0:1, :]).astype(NARROW)
        next_rows.start_piece(sub)

    reduce.run(products(s.hidden, s.down, False), result, none)

    def use(index):
        rows = chip_rows(index, local)
        s.projected[rows, :] = dot(s.normed1[rows, :], s.next_qkv_w[...], ((1,), (1,)))

    next_rows.run(use, none)
    stores.append(copies(s.normed1, s.next_normed1_out))
    attend_here(s.slots, s.projected, s.cosine, s.sine, s.kept1, s.lse1, s.by_number, s.key2, s.value2)
    put_back(s.by_number, s.mixed1, s.row)
    for store in stores[1:]:
        store.wait()
    spread.sent()


def opening(slots, row, cosine, sine, inputs, cotangent, qkv, wo, gate, up, down, gain_attn, gain_mlp, count, head):
    local, width = inputs.shape[1:]
    tokens = count * 2 * local
    depth = gate.shape[1]
    hidden = gate.shape[2] // count
    q_rows = wo.shape[1] // count
    vmem, dma = pltpu.VMEM, pltpu.SemaphoreType.DMA
    lse = shape_of(count, 2 * tokens // count, 1, kind=WIDE)
    return call_fused(
        "opening", opening_body, 0, 360,
        dict(
            slots=(slots, SMEM), row=(row, SMEM), cosine=(cosine, VMEM), sine=(sine, VMEM),
            inputs=(inputs, HBM), cotangent=(cotangent, HBM), qkv=(qkv, HBM), wo=(wo, HBM),
            gate=(gate, HBM), up=(up, HBM), down_in=(down, HBM),
            gain_attn=(gain_attn, VMEM), gain_mlp=(gain_mlp, VMEM),
        ),
        dict(
            out_qkv=(shape_of(2, q_rows + 2 * head, width), HBM),
            out_wo=(shape_of(2, q_rows, width), HBM),
            out_gu=(shape_of(2, width, 2 * hidden), HBM),
            out_down=(shape_of(2, hidden, width), HBM),
            gains=(shape_of(2, 8, width, kind=WIDE), VMEM),
            normed1_out=(shape_of(tokens, width), HBM),
            next_normed1_out=(shape_of(tokens, width), HBM),
            normed2_out=(shape_of(tokens, width), HBM),
            out_grad_out=(shape_of(tokens, width), HBM),
            gate_up_out=(shape_of(tokens, 2 * hidden, kind=WIDE), HBM),
            second=(shape_of(local, width, kind=WIDE), VMEM),
            result=(shape_of(local, width, kind=WIDE), VMEM),
            hidden=(shape_of(tokens, hidden), VMEM),
            mixed0=(shape_of(tokens, 2 * head), VMEM), mixed1=(shape_of(tokens, 2 * head), VMEM),
            kept0=(shape_of(tokens, 4 * head), VMEM), kept1=(shape_of(tokens, 4 * head), VMEM),
            lse0=(lse, VMEM), lse1=(lse, VMEM),
        ),
        dict(
            rows=vmem((local, width), WIDE), given=vmem((local, width), WIDE),
            gain_piece=vmem((8, depth), WIDE),
            shard0=vmem((local, width), NARROW), shard1=vmem((local, width), NARROW),
            shard2=vmem((local, width), NARROW),
            normed1=vmem((tokens, width), NARROW), normed2=vmem((tokens, width), NARROW),
            out_grad=vmem((tokens, width), NARROW), gate_up=vmem((tokens, 2 * hidden), WIDE),
            qkv_w=vmem((q_rows + 2 * head, width), NARROW),
            next_qkv_w=vmem((q_rows + 2 * head, width), NARROW),
            wo_w=vmem((q_rows, width), NARROW), gu=vmem((width, 2 * hidden), NARROW),
            down=vmem((hidden, width), NARROW), projected=vmem((tokens, 4 * head), WIDE),
            key2=vmem((tokens, 2 * head), NARROW), value2=vmem((tokens, 2 * head), NARROW),
            by_number=vmem((tokens, 2 * head), NARROW),
            reduce=reduce_scratch(count, local, width),
            first_sems=gather_scratch(count), gather_sems=gather_scratch(count),
            line_sems=line_scratch(count), grads_sems=line_scratch(count),
            gain_sems=[dma((2 * count - 1,)), dma((2 * count - 1,))],
            spread_sems=[
                dma((KINDS, count - 1)), dma((KINDS, count - 1)),
                dma((KINDS, count)), dma((KINDS, count)), dma((KINDS,)),
            ],
            copy_sem=dma((16,)),
        ),
    )


def back_through_feed_forward(at, s, ring, reduce, work, beside):
    local = s.given.shape[0]
    add_gradient(work, s.hidden, s.out_grad, s.grad_down)
    add_gradient(work, s.normed2, s.gu_grad, s.grad_gu)

    gather = Gather(ring, s.shard2, s.attn_grad, s.gather_sems)
    s.gain_mlp_grad[...] = jnp.zeros_like(s.gain_mlp_grad)

    def through(sub, span, value):
        part, gain_part = through_norm(value, s.second[span, :], s.gains[at, 1:2, :])
        value = s.given[span, :] + part
        s.second_grad[span, :] = value
        s.shard2[span, :] = value.astype(NARROW)
        gather.start_piece(sub)
        s.gain_mlp_grad[...] += gain_part

    left = reduce.run(products(s.gu_grad, s.gu, True), through, work, beside)

    def use(index):
        rows = chip_rows(index, local)
        s.mixed_grad[rows, :] = dot(s.attn_grad[rows, :], s.wo[...], ((1,), (1,))).astype(NARROW)

    for do in reversed(left):
        work.first(lambda _, do=do: do())
    gather.run(use, work)
    work.do()


def turn_body(at, s):
    ring = Ring()
    greet(ring.everyone())
    copies = Copies(s.copy_sem)
    wo_in = copies(s.wo_in.at[at], s.wo)
    ins = [
        copies(s.gu_in.at[at], s.gu), copies(s.down_in.at[at], s.down),
        copies(s.out_grad_in, s.out_grad), copies(s.cotangent.at[lax.axis_index(SECTION)], s.given),
    ]
    reduce, other = Reduce(ring, s.reduce), Reduce(ring, s.other)
    work = Work()

    second_rows = Gather(ring, s.shard, s.normed2, s.first_sems)

    def second(sub, span, value):
        value = s.rows[span, :] + value
        s.second[span, :] = value
        unit, _ = unit_rows(value)
        s.shard[span, :] = (unit * s.gains[at, 1:2, :]).astype(NARROW)
        second_rows.start_piece(sub)

    wo_in.wait()
    reduce.run(products(s.mixed, s.wo, False), second, work)
    for load in ins:
        load.wait()
    second_rows.run(
        feed_forward_use(s, s.rows.shape[0], functools.partial(feed_forward_back, s)), work
    )

    def result(sub, span, value):
        s.result[span, :] = s.second[span, :] + value

    beside = [lambda: other.begin(products(s.hidden, s.down, False), Work())]
    beside += [functools.partial(other.step, step) for step in range(1, ring.far + 1)]
    beside += [lambda: other.end(result)]
    back_through_feed_forward(at, s, ring, reduce, work, beside)
    stores = [
        copies(s.grad_down, s.grad_down_out), copies(s.grad_gu, s.grad_gu_out),
        copies(s.attn_grad, s.attn_grad_out),
    ]
    attend_back_here(
        s.slots, s.mixed_grad, s.kept, s.lse, s.cosine, s.sine, s.by_number, s.key2, s.value2,
        s.key_sum, s.value_sum,
    )
    put_back(s.by_number, s.qkv_grad, s.row)
    for store in stores:
        store.wait()


def turn(at, known, rows, mixed, kept, lse, out_grad, cotangent, weights, count):
    _, wo, gu, down, gains = weights
    local, width = rows.shape
    tokens = mixed.shape[0]
    hidden = down.shape[1]
    head = mixed.shape[1] // 2
    vmem, dma = pltpu.VMEM, pltpu.SemaphoreType.DMA
    return call_fused(
        "turn", functools.partial(turn_body, at), 1, 140,
        dict(
            **known, rows=(rows, VMEM), mixed=(mixed, VMEM), kept=(kept, VMEM), lse=(lse, VMEM),
            gains=(gains, VMEM), out_grad_in=(out_grad, HBM), cotangent=(cotangent, HBM),
            wo_in=(wo, HBM), gu_in=(gu, HBM), down_in=(down, HBM),
        ),
        dict(
            result=(shape_of(local, width, kind=WIDE), VMEM),
            second_grad=(shape_of(local, width, kind=WIDE), VMEM),
            qkv_grad=(shape_of(tokens, 4 * head), VMEM),
            attn_grad_out=(shape_of(tokens, width), HBM),
            gain_mlp_grad=(shape_of(1, width, kind=WIDE), VMEM),
            grad_down_out=(shape_of(hidden, width), HBM),
            grad_gu_out=(shape_of(width, 2 * hidden), HBM),
        ),
        dict(
            reduce=reduce_scratch(count, local, width), other=reduce_scratch(count, local, width),
            first_sems=gather_scratch(count), gather_sems=gather_scratch(count),
            gu=vmem(gu.shape[1:], NARROW), down=vmem(down.shape[1:], NARROW), wo=vmem(wo.shape[1:], NARROW),
            out_grad=vmem((tokens, width), NARROW), normed2=vmem((tokens, width), NARROW),
            attn_grad=vmem((tokens, width), NARROW), mixed_grad=vmem((tokens, 2 * head), NARROW),
            hidden=vmem((tokens, hidden), NARROW), gu_grad=vmem((tokens, 2 * hidden), NARROW),
            grad_down=vmem((hidden, width), NARROW), grad_gu=vmem((width, 2 * hidden), NARROW),
            given=vmem((local, width), WIDE), second=vmem((local, width), WIDE),
            shard=vmem((local, width), NARROW), shard2=vmem((local, width), NARROW),
            **attend_scratch(tokens, head, True),
            copy_sem=dma((8,)),
        ),
    )


def attention_back(at, s, reduce, work, then, beside=()):
    s.gain_attn_grad[...] = jnp.zeros_like(s.gain_attn_grad)

    def through(sub, span, value):
        part, gain_part = through_norm(value, s.rows[span, :], s.gains[at, 0:1, :])
        value = s.second_grad_in[span, :] + part
        s.input_grad[span, :] = value
        then(sub, span, value)
        s.gain_attn_grad[...] += gain_part

    reduce.run(products(s.qkv_grad, s.qkv_w, False), through, work, beside)


def backward_body(upper, lower, s):
    ring = Ring()
    local = s.rows.shape[0]
    greet(ring.everyone())
    copies = Copies(s.copy_sem)
    qkv_in = copies(s.qkv_w_in.at[upper], s.qkv_w)
    upper_in = [copies(s.attn_grad_in, s.attn_grad), copies(s.normed1_in, s.normed2)]
    first_in = [copies(s.down_in.at[lower], s.down), copies(s.gate_up_in, s.gate_up)]
    then_in = [copies(s.gu_in.at[lower], s.gu), copies(s.wo_in.at[lower], s.wo)]
    reduce = Reduce(ring, s.reduce)
    work = Work()

    def wait(_):
        for load in upper_in:
            load.wait()

    work.add(wait)
    add_gradient(work, s.mixed, s.attn_grad, s.grad_wo)
    add_gradient(work, s.normed2, s.qkv_grad, s.grad_qkv)
    qkv_in.wait()
    gather = Gather(ring, s.shard, s.out_grad, s.first_sems)

    def go_on(sub, span, value):
        s.shard[span, :] = value.astype(NARROW)
        s.given[span, :] = value
        gather.start_piece(sub)

    attention_back(upper, s, reduce, work, go_on)
    work.do()
    then_in.append(copies(s.normed2_in, s.normed2))
    stores = [copies(s.grad_wo, s.grad_wo_out), copies(s.grad_qkv, s.grad_qkv_out)]
    for load in first_in:
        load.wait()
    width = s.hidden.shape[1]
    tile = 256
    number = width // tile

    def use(index):
        rows = chip_rows(index, local)

        def one(at):
            start = at * tile
            cols, right = aligned(start, tile), aligned(start + width, tile)
            feed_forward_back(s, rows, cols, right, s.gate_up[rows, cols], s.gate_up[rows, right])

        loop(0, number, one)

    gather.run(use, work)
    for load in then_in:
        load.wait()
    back_through_feed_forward(lower, s, ring, reduce, work, [])
    stores += [
        copies(s.grad_down, s.grad_down_out), copies(s.grad_gu, s.grad_gu_out),
        copies(s.attn_grad, s.attn_grad_out),
    ]
    for store in stores:
        store.wait()


def backward_between(at, upper, lower, weights, count):
    qkv_w, wo, gu, down, gains = weights
    local, width = upper.rows.shape
    tokens = upper.mixed.shape[0]
    hidden = down.shape[1]
    q_rows = wo.shape[1]
    vmem, dma = pltpu.VMEM, pltpu.SemaphoreType.DMA
    return call_fused(
        "backward_between", functools.partial(backward_body, at, at - 1), 2, 115,
        dict(
            rows=(upper.rows, VMEM), second_grad_in=(upper.second_grad, VMEM),
            qkv_grad=(upper.qkv_grad, VMEM), mixed=(upper.mixed, VMEM), gains=(gains, VMEM),
            attn_grad_in=(upper.attn_grad, HBM), normed1_in=(upper.normed1, HBM),
            second=(lower.second, VMEM), hidden=(lower.hidden, VMEM),
            gate_up_in=(lower.gate_up, HBM), normed2_in=(lower.normed2, HBM),
            qkv_w_in=(qkv_w, HBM), wo_in=(wo, HBM), gu_in=(gu, HBM), down_in=(down, HBM),
        ),
        dict(
            input_grad=(shape_of(local, width, kind=WIDE), VMEM),
            second_grad=(shape_of(local, width, kind=WIDE), VMEM),
            mixed_grad=(shape_of(tokens, q_rows), VMEM),
            attn_grad_out=(shape_of(tokens, width), HBM),
            gain_attn_grad=(shape_of(1, width, kind=WIDE), VMEM),
            gain_mlp_grad=(shape_of(1, width, kind=WIDE), VMEM),
            grad_wo_out=(shape_of(q_rows, width), HBM),
            grad_qkv_out=(shape_of(width, qkv_w.shape[1]), HBM),
            grad_down_out=(shape_of(hidden, width), HBM),
            grad_gu_out=(shape_of(width, 2 * hidden), HBM),
        ),
        dict(
            reduce=reduce_scratch(count, local, width),
            first_sems=gather_scratch(count), gather_sems=gather_scratch(count),
            gu=vmem(gu.shape[1:], NARROW), down=vmem(down.shape[1:], NARROW), wo=vmem(wo.shape[1:], NARROW),
            qkv_w=vmem(qkv_w.shape[1:], NARROW), gate_up=vmem((tokens, 2 * hidden), WIDE),
            out_grad=vmem((tokens, width), NARROW), normed2=vmem((tokens, width), NARROW),
            attn_grad=vmem((tokens, width), NARROW), gu_grad=vmem((tokens, 2 * hidden), NARROW),
            grad_wo=vmem((q_rows, width), NARROW), grad_qkv=vmem((width, qkv_w.shape[1]), NARROW),
            grad_down=vmem((hidden, width), NARROW), grad_gu=vmem((width, 2 * hidden), NARROW),
            given=vmem((local, width), WIDE),
            shard=vmem((local, width), NARROW), shard2=vmem((local, width), NARROW),
            copy_sem=dma((16,)),
        ),
    )


def gradient_pieces(target, count, refs):
    down, gu, wo, qkv = refs
    depth = down.shape[1] // count
    hidden = down.shape[0]
    cols = aligned(target * depth, depth)
    return (
        down.at[:, cols],
        gu.at[cols, pl.ds(0, hidden)],
        gu.at[cols, pl.ds(hidden, hidden)],
        wo.at[:, cols],
        qkv.at[cols, :],
    )


def owned_pieces(source, refs, sizes):
    down, gate, up, wo, qkv = refs
    return (
        down.at[aligned(source * sizes[0][0], sizes[0][0]), :],
        gate.at[:, aligned(source * sizes[1][1], sizes[1][1])],
        up.at[:, aligned(source * sizes[2][1], sizes[2][1])],
        wo.at[aligned(source * sizes[3][0], sizes[3][0]), :],
        qkv.at[source],
    )


GRADS, FEED_GRADS = 5, 3


class Return:
    def __init__(self, ring, partial, outs, landed, mine, sems):
        self.ring = ring
        self.layer = lax.axis_index(SECTION)
        self.across = {SECTION: 1 - self.layer}
        peers, self.origins = partners(ring.me, ring.count)
        self.order = [*peers, ring.me]
        self.partial, self.outs, self.landed, self.mine = partial, outs, landed, mine
        self.cross_send, self.cross_recv, self.load_sem, self.send, self.recv, self.own_sem = sems
        self.sizes = [ref.shape[1:] for ref in mine]
        self.crossing, self.loads, self.sends, self.events = {}, {}, [], []

    def cross(self, kinds):
        count = self.ring.count
        for kind in kinds:
            for k, owner in enumerate(self.order):
                pieces = [gradient_pieces(owner, count, refs)[kind] for refs in self.partial]
                for at in range(2):
                    copy = remote(
                        pieces[1 - at], self.landed[kind].at[k],
                        self.cross_send.at[kind, k], self.cross_recv.at[kind, k], self.across,
                    )
                    load = pltpu.make_async_copy(
                        pieces[at], self.mine[kind].at[k], self.load_sem.at[kind, k]
                    )

                    @pl.when(self.layer == at)
                    def _():
                        copy.start()
                        load.start()

                self.crossing[kind, k], self.loads[kind, k] = copy, load
                self.events.append((kind, k))

    def some(self, number):
        for kind, k in self.events[:number]:
            self.loads[kind, k].wait()
            self.crossing[kind, k].wait_recv()
            mine, theirs = self.mine[kind], self.landed[kind]
            tile = 64

            def add(at):
                rows = aligned(at * tile, tile)
                total = mine[k, rows, :].astype(WIDE) + theirs[k, rows, :].astype(WIDE)
                mine[k, rows, :] = total.astype(NARROW)

            loop(0, mine.shape[1] // tile, add)
            target = owned_pieces(self.ring.me, self.outs, self.sizes)[kind]
            if k < self.ring.count - 1:
                copy = remote(
                    mine.at[k], target, self.send.at[kind, k], self.recv.at[kind, k],
                    {DP: self.order[k]},
                )
            else:
                copy = pltpu.make_async_copy(mine.at[k], target, self.own_sem.at[kind])
            copy.start()
            self.sends.append((k, copy))
        self.events = self.events[number:]

    def finish(self):
        for copy in self.crossing.values():
            copy.wait_send()
        for k, copy in self.sends:
            if k < self.ring.count - 1:
                copy.wait_send()
            else:
                copy.wait()
        for kind in range(GRADS):
            for k in range(self.ring.count - 1):
                here = owned_pieces(self.origins[k], self.outs, self.sizes)[kind]
                remote(
                    self.mine[kind].at[k], here, self.send.at[kind, k], self.recv.at[kind, k],
                    {DP: self.origins[k]},
                ).wait_recv()


def closing_body(at, s):
    ring = Ring()
    layer = lax.axis_index(SECTION)
    count = ring.count
    everyone = 4 * count
    this = (layer * count + ring.me) * 2 + ring.core

    def device(k):
        other = lax.rem(this + k, everyone)
        return {SECTION: other // (2 * count), DP: lax.rem(other // 2, count), TENSOR: lax.rem(other, 2)}

    greet([device(k) for k in range(1, everyone)])
    copies = Copies(s.copy_sem)
    qkv_in = copies(s.qkv_w_in.at[at], s.qkv_w)
    ins = [copies(s.attn_grad_in, s.attn_grad), copies(s.normed1_in, s.normed1)]
    rows_in = copies(s.inputs.at[layer], s.rows)
    back = Return(
        ring,
        ((s.down0, s.gu0, s.grad_wo, s.grad_qkv), (s.down1, s.gu1, s.wo1, s.qkv1)),
        (s.down_out, s.gate_out, s.up_out, s.wo_out, s.qkv_out), s.landed, s.mine, s.back_sems,
    )
    back.cross(range(FEED_GRADS))

    swap_send, swap_recv = s.swap_sems
    swaps = []

    def swap(which, out, values):
        for section in range(2):
            copy = remote(
                values[1 - section], out.at[section], swap_send.at[which], swap_recv.at[which],
                {SECTION: 1 - layer},
            )
            own = pltpu.make_async_copy(values[section], out.at[section], s.own_sems.at[which])

            @pl.when(layer == section)
            def _():
                copy.start()
                own.start()

        swaps.append((copy, own))

    swap(0, s.results, (s.result0, s.result1))
    attend_back_here(
        s.slots, s.mixed_grad, s.kept, s.lse, s.cosine, s.sine, s.by_number, s.key2, s.value2,
        s.key_sum, s.value_sum, lambda spot: back.some(1) if spot == 1 else None,
    )
    put_back(s.by_number, s.qkv_grad, s.row)
    work = Work()
    for load in ins:
        load.wait()
    add_gradient(work, s.mixed, s.attn_grad, s.grad_wo)
    add_gradient(work, s.normed1, s.qkv_grad, s.grad_qkv)
    qkv_in.wait()
    rows_in.wait()

    def rest():
        work.do()
        back.cross(range(FEED_GRADS, GRADS))
        back.some(1)

    beside = [functools.partial(back.some, 1)] * 2 + [rest] + [functools.partial(back.some, 1)] * (ring.far - 3)
    attention_back(at, s, Reduce(ring, s.reduce), work, lambda *_: None, beside)
    swap(1, s.input_grads, (s.input_grad, s.input_grad1))

    lanes = s.gain_out.shape[1]
    for section, (attn, mlp) in enumerate(((s.gain_attn_grad, s.gain_mlp0), (s.gain_attn1, s.gain_mlp1))):
        for owner in range(2 * count):
            s.gain_in[section * 2 * count + owner] = jnp.zeros_like(s.gain_out)
            cols = slice(owner * lanes, (owner + 1) * lanes)
            s.gain_in[section * 2 * count + owner, 0:1, :] = attn[:, cols]
            s.gain_in[section * 2 * count + owner, 1:2, :] = mlp[:, cols]
    gain_send, gain_recv = s.gain_sems
    gain_copies = []
    for k in range(1, everyone):
        copy = remote(
            s.gain_in.at[lax.rem(this + k, everyone)], s.gain_landed.at[k - 1],
            gain_send.at[k - 1], gain_recv.at[k - 1], device(k),
        )
        copy.start()
        gain_copies.append(copy)
    back.some(len(back.events))
    total = s.gain_in[this]
    for k, copy in enumerate(gain_copies):
        copy.wait_recv()
        total = total + s.gain_landed[k]
    s.gain_out[...] = total
    for copy in gain_copies:
        copy.wait_send()
    for copy, own in swaps:
        copy.wait()
        own.wait()
    back.finish()


def closing(at, known, inputs, first, last, feed0, grads1, gains_of, weights, count):
    qkv_w, _, _, _, gains = weights
    local, width = inputs.shape[1:]
    tokens = first.mixed.shape[0]
    head = first.mixed.shape[1] // 2
    down0, gu0 = feed0
    down1, gu1, wo1, qkv1 = grads1
    hidden, q_rows, qkv_rows = down0.shape[0], wo1.shape[0], qkv1.shape[1]
    depth = width // count
    sizes = [(hidden, depth), (depth, hidden), (depth, hidden), (q_rows, depth), (depth, qkv_rows)]
    everyone = 4 * count
    lanes = width // (2 * count)
    vmem, dma = pltpu.VMEM, pltpu.SemaphoreType.DMA
    pieces = lambda: [vmem((count, *size), NARROW) for size in sizes]
    return call_fused(
        "closing", functools.partial(closing_body, at), 3, 210,
        dict(
            **known, inputs=(inputs, HBM), gains=(gains, VMEM), qkv_w_in=(qkv_w, HBM),
            second_grad_in=(first.second_grad, VMEM), mixed_grad=(first.mixed_grad, VMEM),
            mixed=(first.mixed, VMEM), kept=(first.kept, VMEM), lse=(first.lse, VMEM),
            attn_grad_in=(first.attn_grad, HBM), normed1_in=(first.normed1, HBM),
            result0=(first.result, VMEM), result1=(last.result, VMEM),
            input_grad1=(last.input_grad, VMEM),
            down0=(down0, HBM), gu0=(gu0, HBM),
            down1=(down1, HBM), gu1=(gu1, HBM), wo1=(wo1, HBM), qkv1=(qkv1, HBM),
            gain_mlp0=(gains_of[0], VMEM), gain_attn1=(gains_of[1], VMEM), gain_mlp1=(gains_of[2], VMEM),
        ),
        dict(
            results=(shape_of(2, local, width, kind=WIDE), HBM),
            input_grads=(shape_of(2, local, width, kind=WIDE), HBM),
            down_out=(shape_of(count * hidden, depth), HBM),
            gate_out=(shape_of(depth, count * hidden), HBM),
            up_out=(shape_of(depth, count * hidden), HBM),
            wo_out=(shape_of(count * q_rows, depth), HBM),
            qkv_out=(shape_of(count, depth, qkv_rows), HBM),
            gain_out=(shape_of(8, lanes, kind=WIDE), VMEM),
        ),
        dict(
            reduce=reduce_scratch(count, local, width),
            qkv_w=vmem(qkv_w.shape[1:], NARROW), rows=vmem((local, width), WIDE),
            attn_grad=vmem((tokens, width), NARROW), normed1=vmem((tokens, width), NARROW),
            qkv_grad=vmem((tokens, 4 * head), NARROW),
            grad_wo=vmem((q_rows, width), NARROW), grad_qkv=vmem((width, qkv_rows), NARROW),
            input_grad=vmem((local, width), WIDE),
            gain_attn_grad=vmem((1, width), WIDE),
            landed=pieces(), mine=pieces(),
            gain_in=vmem((everyone, 8, lanes), WIDE), gain_landed=vmem((everyone - 1, 8, lanes), WIDE),
            **attend_scratch(tokens, head, True),
            back_sems=[
                dma((GRADS, count)), dma((GRADS, count)), dma((GRADS, count)),
                dma((GRADS, count - 1)), dma((GRADS, count - 1)), dma((GRADS,)),
            ],
            gain_sems=[dma((everyone - 1,)), dma((everyone - 1,))],
            swap_sems=[dma((2,)), dma((2,))], own_sems=dma((2,)),
            copy_sem=dma((8,)),
        ),
    )


def widen_kernel(heads, down, gate, up, wo, qkv, every, gain, *outs):
    down_out, gate_out, up_out, wo_out, wq_out, wk_out, wv_out, attn_out, mlp_out = outs
    for source, out in ((down, down_out), (gate, gate_out), (up, up_out), (wo, wo_out)):
        out[0] = source[...].astype(WIDE)
    queries = wq_out.shape[2]
    wq_out[0] = qkv[0, :, :queries].astype(WIDE)

    @pl.when(pl.program_id(0) == 0)
    def _():
        attn_out[...] = gain[0:1, :]
        mlp_out[...] = gain[1:2, :]
        width = 2 * heads
        shared = every.shape[0] * heads // wk_out.shape[2]

        def one(head):
            chips = range(head * shared, (head + 1) * shared)
            return sum(every[chip, :, queries:].astype(WIDE) for chip in chips)

        for pair in range(wk_out.shape[2] // width):
            left, right = one(2 * pair), one(2 * pair + 1)
            low = low_lanes(left.shape, heads)
            cols = slice(pair * width, (pair + 1) * width)
            wk_out[0, :, cols] = jnp.where(low, left, pltpu.roll(right, heads, 1))
            wv_out[0, :, cols] = jnp.where(low, pltpu.roll(left, heads, 1), right)


def widen(end, kv_cols, count, head):
    depth = end.gate_out.shape[0]
    hidden = end.gate_out.shape[1] // count
    q_rows = end.wo_out.shape[0] // count
    lanes = end.gain_out.shape[1]
    down = (hidden, depth)
    across = (depth, hidden)
    result = lambda *dims: shape_of(1, *dims, kind=WIDE)
    by_rows = lambda at: (at, 0)
    by_cols = lambda at: (0, at)
    none = lambda at: (0, 0)
    flat = lambda index: lambda at: (0, *index(at))
    return pl.pallas_call(
        functools.partial(widen_kernel, head),
        grid=(count,),
        out_shape=(
            result(count * hidden, depth), result(depth, count * hidden), result(depth, count * hidden),
            result(count * q_rows, depth), result(depth, count * q_rows),
            result(depth, kv_cols), result(depth, kv_cols), result(lanes), result(lanes),
        ),
        in_specs=[
            pl.BlockSpec(down, by_rows), pl.BlockSpec(across, by_cols), pl.BlockSpec(across, by_cols),
            pl.BlockSpec((q_rows, depth), by_rows),
            pl.BlockSpec((1, *end.qkv_out.shape[1:]), lambda at: (at, 0, 0)),
            pl.BlockSpec(end.qkv_out.shape, lambda at: (0, 0, 0)),
            pl.BlockSpec(end.gain_out.shape, none),
        ],
        out_specs=(
            pl.BlockSpec((1, *down), flat(by_rows)), pl.BlockSpec((1, *across), flat(by_cols)),
            pl.BlockSpec((1, *across), flat(by_cols)), pl.BlockSpec((1, q_rows, depth), flat(by_rows)),
            pl.BlockSpec((1, depth, q_rows), flat(by_cols)),
            pl.BlockSpec((1, depth, kv_cols), flat(none)), pl.BlockSpec((1, depth, kv_cols), flat(none)),
            pl.BlockSpec((1, lanes), none), pl.BlockSpec((1, lanes), none),
        ),
        name="widen",
    )(end.down_out, end.gate_out, end.up_out, end.wo_out, end.qkv_out, end.qkv_out, end.gain_out)


def fast_shards(inputs, table, cotangent, wq, wk, wv, wo, w_gate, w_up, w_down, gain_attn, gain_mlp):
    count = lax.axis_size(DP)
    parts = lax.axis_size(TENSOR)
    head = HEAD_SIZE
    section = lax.axis_index(SECTION)
    block = inputs.shape[1] * parts

    row = lax.dynamic_index_in_dim(table, section, 0, keepdims=False)
    ids = jnp.arange(count, dtype=jnp.int32)
    slots = jnp.sum(jnp.where(row[None, :] == ids[:, None], ids[None, :], 0), axis=1)
    cosine, sine = rope_tables(count // 2 * block, head)
    qkv_t = jnp.concatenate([wq[0], wk[0], wv[0]], axis=1).T
    s = opening(
        slots, row, cosine, sine, inputs, cotangent, qkv_t, wo, w_gate, w_up, w_down,
        gain_attn, gain_mlp, count, head,
    )
    weights = (s.out_qkv, s.out_wo, s.out_gu, s.out_down, s.gains)
    known = dict(
        slots=(slots, SMEM), row=(row, SMEM), cosine=(cosine, VMEM), sine=(sine, VMEM)
    )
    top = turn(
        1, known, s.result, s.mixed1, s.kept1, s.lse1, s.out_grad_out, cotangent, weights, count
    )
    upper = Names(
        rows=s.result, second_grad=top.second_grad, qkv_grad=top.qkv_grad, mixed=s.mixed1,
        attn_grad=top.attn_grad_out, normed1=s.next_normed1_out,
    )
    lower = Names(
        second=s.second, hidden=s.hidden, gate_up=s.gate_up_out, normed2=s.normed2_out
    )
    back = backward_between(1, upper, lower, weights, count)
    first = Names(
        second_grad=back.second_grad, mixed_grad=back.mixed_grad, mixed=s.mixed0, kept=s.kept0,
        lse=s.lse0, attn_grad=back.attn_grad_out, normed1=s.normed1_out, result=s.result,
    )
    last = Names(result=top.result, input_grad=back.input_grad)
    end = closing(
        0, known, inputs, first, last,
        (back.grad_down_out, back.grad_gu_out),
        (top.grad_down_out, top.grad_gu_out, back.grad_wo_out, back.grad_qkv_out),
        (back.gain_mlp_grad, back.gain_attn_grad, top.gain_mlp_grad),
        weights, count,
    )
    grad_down, grad_gate, grad_up, grad_wo, grad_wq, grad_wk, grad_wv, sum_attn, sum_mlp = widen(
        end, wk.shape[2], count, head
    )
    return (
        end.results[None],
        end.input_grads[None],
        grad_wq,
        grad_wk,
        grad_wv,
        grad_wo,
        grad_gate,
        grad_up,
        grad_down,
        sum_attn,
        sum_mlp,
    )


def fits(mesh, inputs, table, cotangent, wq, wk, wv, wo, w_gate, w_up, w_down, gain_attn, gain_mlp):
    sections, count, parts = (mesh.shape[axis] for axis in (SECTION, DP, TENSOR))
    head = HEAD_SIZE
    if sections != 2 or parts != 2 or inputs.shape[0] != sections or count % 4 or count < 8:
        return False
    devices = count * parts
    queries, keys = wq.shape[2] // head, wk.shape[2] // head
    if queries != 2 * devices or devices % keys or keys % parts or 4 * head != 256:
        return False
    return (
        wq.shape[1] % (128 * count) == 0
        and wq.shape[1] % 512 == 0
        and w_gate.shape[2] % (256 * devices) == 0
        and inputs.shape[1] % (64 * devices) == 0
    )


def shards(mesh, whole, *args):
    if fits(mesh, *whole):
        return fast_shards(*args)
    return general_shards(*args)


def solution(mesh):
    in_specs = (
        P(None, (DP, TENSOR), None),
        P(),
        P(None, (DP, TENSOR), None),
        P(SECTION, DP, TENSOR),
        P(SECTION, DP, TENSOR),
        P(SECTION, DP, TENSOR),
        P(SECTION, TENSOR, DP),
        P(SECTION, DP, TENSOR),
        P(SECTION, DP, TENSOR),
        P(SECTION, TENSOR, DP),
        P(SECTION, DP),
        P(SECTION, DP),
    )
    out_specs = (
        P(SECTION, None, (DP, TENSOR), None),
        P(SECTION, None, (DP, TENSOR), None),
        P(SECTION, DP, TENSOR),
        P(SECTION, DP, TENSOR),
        P(SECTION, DP, TENSOR),
        P(SECTION, TENSOR, DP),
        P(SECTION, DP, TENSOR),
        P(SECTION, DP, TENSOR),
        P(SECTION, TENSOR, DP),
        P(SECTION, (DP, TENSOR)),
        P(SECTION, (DP, TENSOR)),
    )

    def step(*args):
        return jax.shard_map(
            functools.partial(shards, mesh, args),
            mesh=mesh,
            in_specs=in_specs,
            out_specs=out_specs,
            check_vma=False,
        )(*args)

    return step
```

```python
import functools
import math

import jax
import jax.numpy as jnp
import numpy as np
from jax import lax
from jax.experimental import pallas as pl
from jax.experimental.pallas import tpu as pltpu
from jax.sharding import PartitionSpec as P

HEAD_SIZE = 64
SECTION, DP, TENSOR = "section", "dp", "tensor"


epsilon = 1e-05


def passed_along(value, axis, steps):
    count = lax.axis_size(axis)
    initial, last = (max(0, -steps), min(count, count - steps))
    return lax.ppermute(value, axis, [(source, source + steps) for source in range(initial, last)])


def rope_frequencies(head):
    index = jnp.arange(head // 2, dtype=jnp.float32)
    base = 1.0 / 500000.0 ** (index * 2.0 / head)
    wavelength = 2.0 * math.pi / base
    blend = (8192.0 / wavelength - 1.0) / 3.0
    middle = (1.0 - blend) * base / 32.0 + blend * base
    return jnp.where(wavelength < 2048.0, base, jnp.where(wavelength > 8192.0, base / 32.0, middle))


def rotate(values, positions, head):
    step_count = values.shape[0]
    shaped = values.reshape(step_count, -1, head)
    angle = positions.astype(jnp.float32)[:, None] * rope_frequencies(head)[None, :]
    cosine = jnp.cos(angle)[:, None, :]
    sine = jnp.sin(angle)[:, None, :]
    first = shaped[:, :, : head // 2]
    second = shaped[:, :, head // 2 :]
    return jnp.concatenate(
        [first * cosine - second * sine, second * cosine + first * sine], axis=-1
    ).reshape(step_count, -1)


def unrotate(values, positions, head):
    step_count = values.shape[0]
    shaped = values.reshape(step_count, -1, head)
    angle = positions.astype(jnp.float32)[:, None] * rope_frequencies(head)[None, :]
    cosine = jnp.cos(angle)[:, None, :]
    sine = jnp.sin(angle)[:, None, :]
    first = shaped[:, :, : head // 2]
    second = shaped[:, :, head // 2 :]
    return jnp.concatenate(
        [first * cosine + second * sine, second * cosine - first * sine], axis=-1
    ).reshape(step_count, -1)


def norm_stats(rows):
    inverse = lax.rsqrt(jnp.mean(rows * rows, axis=-1, keepdims=True) + epsilon)
    return (rows * inverse, inverse)


def norm_back(grad, unit, inverse, gain):
    scaled = grad * gain
    inner = jnp.mean(scaled * unit, axis=-1, keepdims=True)
    return (inverse * (scaled - unit * inner), jnp.sum(grad * unit, axis=0))


def matmul(left, right):
    return jnp.dot(left, right, preferred_element_type=jnp.float32)


def block_layout(table, micro, groups, block):
    layout_row = lax.dynamic_index_in_dim(table, micro, 0, keepdims=False)
    span = groups // 2
    mine = lax.dynamic_index_in_dim(layout_row, lax.axis_index(DP), 0, keepdims=False)
    sequence = mine // span
    place = mine % span
    slot_ids = jnp.arange(groups, dtype=jnp.int32)
    holder = jnp.sum(
        jnp.where(layout_row[None, :] == slot_ids[:, None], slot_ids[None, :], 0), axis=1
    )
    slots = lax.dynamic_slice_in_dim(holder, sequence * span, span)
    positions = place * block + jnp.arange(block, dtype=jnp.int32)
    return (slots, positions)


def attend(query_rows, key_seq, value_seq, positions, heads_kv, head):
    step_count = query_rows.shape[0]
    keys_total = key_seq.shape[0]
    head_group = query_rows.shape[1] // (heads_kv * head)
    scale = 1.0 / math.sqrt(head)
    allowed = jnp.arange(keys_total, dtype=jnp.int32)[None, :] <= positions[:, None]
    query_layers = query_rows.reshape(step_count, heads_kv, head_group * head).transpose(1, 0, 2)
    key_layers = key_seq.reshape(keys_total, heads_kv, head).transpose(1, 0, 2)
    value_layers = value_seq.reshape(keys_total, heads_kv, head).transpose(1, 0, 2)

    def one_head(parts):
        q_head, k_head, v_head = parts
        q_three = q_head.reshape(step_count, head_group, head)
        scores = (
            jnp.einsum("qgd,kd->gqk", q_three, k_head, preferred_element_type=jnp.float32) * scale
        )
        total = jnp.sum(jnp.where(allowed, jnp.exp(scores), 0.0), axis=-1)
        log_total = jnp.log(total)
        probs = jnp.where(allowed, jnp.exp(scores - log_total[..., None]), 0.0).astype(jnp.bfloat16)
        mixed = jnp.einsum("gqk,kd->qgd", probs, v_head, preferred_element_type=jnp.float32).astype(
            jnp.bfloat16
        )
        return (mixed.reshape(step_count, head_group * head), log_total)

    mixed, log_total = lax.map(one_head, (query_layers, key_layers, value_layers))
    return (mixed.transpose(1, 0, 2).reshape(step_count, -1), log_total)


def attend_back(
    blended_gradient, query_rows, key_seq, value_seq, log_total, positions, heads_kv, head
):
    step_count = query_rows.shape[0]
    keys_total = key_seq.shape[0]
    head_group = query_rows.shape[1] // (heads_kv * head)
    scale = 1.0 / math.sqrt(head)
    allowed = jnp.arange(keys_total, dtype=jnp.int32)[None, :] <= positions[:, None]
    query_layers = query_rows.reshape(step_count, heads_kv, head_group * head).transpose(1, 0, 2)
    key_layers = key_seq.reshape(keys_total, heads_kv, head).transpose(1, 0, 2)
    value_layers = value_seq.reshape(keys_total, heads_kv, head).transpose(1, 0, 2)
    gain_layers = blended_gradient.reshape(step_count, heads_kv, head_group * head).transpose(
        1, 0, 2
    )

    def one_head(parts):
        q_head, k_head, v_head, g_head, l_head = parts
        q_three = q_head.reshape(step_count, head_group, head)
        g_three = g_head.reshape(step_count, head_group, head)
        scores = (
            jnp.einsum("qgd,kd->gqk", q_three, k_head, preferred_element_type=jnp.float32) * scale
        )
        probs = jnp.where(allowed, jnp.exp(scores - l_head[..., None]), 0.0)
        rounded = probs.astype(jnp.bfloat16)
        prob_grad = jnp.einsum("qgd,kd->gqk", g_three, v_head, preferred_element_type=jnp.float32)
        value_total_sum = jnp.einsum(
            "gqk,qgd->kd", rounded, g_three, preferred_element_type=jnp.float32
        )
        rowdot = jnp.sum(probs * prob_grad, axis=-1, keepdims=True)
        score_grad = (probs * (prob_grad - rowdot) * scale).astype(jnp.bfloat16)
        query_grad = jnp.einsum(
            "gqk,kd->qgd", score_grad, k_head, preferred_element_type=jnp.float32
        )
        key_gradient = jnp.einsum(
            "gqk,qgd->kd", score_grad, q_three, preferred_element_type=jnp.float32
        )
        return (query_grad.reshape(step_count, head_group * head), key_gradient, value_total_sum)

    query_grad, key_gradient, value_total_sum = lax.map(
        one_head, (query_layers, key_layers, value_layers, gain_layers, log_total)
    )
    query_grad = query_grad.transpose(1, 0, 2).reshape(step_count, -1)
    key_gradient = key_gradient.transpose(1, 0, 2).reshape(keys_total, -1)
    value_total_sum = value_total_sum.transpose(1, 0, 2).reshape(keys_total, -1)
    return (query_grad, key_gradient, value_total_sum)


def layer_forward(rows, table, micro, weights, groups, heads_kv, head):
    wq, wk, wv, wo, w_gate, w_up, w_down, gain_attn, gain_mlp = weights
    full = lax.all_gather(rows, TENSOR, axis=0, tiled=True)
    block = full.shape[0]
    slots, positions = block_layout(table, micro, groups, block)
    unit1, inverse1 = norm_stats(full)
    normed1 = (unit1 * gain_attn.astype(jnp.float32)).astype(jnp.bfloat16)
    query_rows = rotate(matmul(normed1, wq), positions, head).astype(jnp.bfloat16)
    key = rotate(matmul(normed1, wk), positions, head).astype(jnp.bfloat16)
    value_rows = matmul(normed1, wv).astype(jnp.bfloat16)
    key_all, value_all = (
        lax.all_gather(key, DP, axis=0, tiled=True),
        lax.all_gather(value_rows, DP, axis=0, tiled=True),
    )
    kv_width = key.shape[1]
    key_seq = key_all.reshape(groups, block, kv_width)[slots].reshape(-1, kv_width)
    value_seq = value_all.reshape(groups, block, kv_width)[slots].reshape(-1, kv_width)
    mixed, log_total = attend(query_rows, key_seq, value_seq, positions, heads_kv, head)
    second = rows + lax.psum_scatter(matmul(mixed, wo), TENSOR, scatter_dimension=0, tiled=True)
    full_second = lax.all_gather(second, TENSOR, axis=0, tiled=True)
    unit2, inverse2 = norm_stats(full_second)
    normed2 = (unit2 * gain_mlp.astype(jnp.float32)).astype(jnp.bfloat16)
    gate = matmul(normed2, w_gate)
    upper = matmul(normed2, w_up)
    hidden = (jax.nn.silu(gate) * upper).astype(jnp.bfloat16)
    result = second + lax.psum_scatter(
        matmul(hidden, w_down), TENSOR, scatter_dimension=0, tiled=True
    )
    return (
        result,
        (
            full,
            query_rows,
            key_seq,
            value_seq,
            mixed,
            log_total,
            full_second,
            gate,
            upper,
            hidden,
            slots,
            positions,
        ),
    )


def layer_backward(grad_rows, context, weights, groups, parts, heads_kv, head):
    wq, wk, wv, wo, w_gate, w_up, w_down, gain_attn, gain_mlp = weights
    (
        full,
        query_rows,
        key_seq,
        value_seq,
        mixed,
        log_total,
        full_second,
        gate,
        upper,
        hidden,
        slots,
        positions,
    ) = context
    block = full.shape[0]
    out_grad = lax.all_gather(grad_rows.astype(jnp.bfloat16), TENSOR, axis=0, tiled=True)
    grad_down = matmul(hidden.T, out_grad)
    hidden_grad = matmul(out_grad, w_down.T)
    sigma = jax.nn.sigmoid(gate)
    gate_grad = (hidden_grad * upper * sigma * (1.0 + gate * (1.0 - sigma))).astype(jnp.bfloat16)
    up_grad = (hidden_grad * gate * sigma).astype(jnp.bfloat16)
    unit2, inverse2 = norm_stats(full_second)
    normed2 = (unit2 * gain_mlp.astype(jnp.float32)).astype(jnp.bfloat16)
    grad_gate = matmul(normed2.T, gate_grad)
    grad_up = matmul(normed2.T, up_grad)
    normed2_grad = matmul(gate_grad, w_gate.T) + matmul(up_grad, w_up.T)
    second_terms, gain_mlp_terms = norm_back(
        normed2_grad, unit2, inverse2, gain_mlp.astype(jnp.float32)
    )
    piece_width = gain_mlp_terms.shape[0] // (groups * parts)
    second_part, gain_mlp_part = (
        lax.psum_scatter(
            second_terms.astype(jnp.bfloat16), TENSOR, scatter_dimension=0, tiled=True
        ).astype(jnp.float32),
        lax.psum_scatter(
            gain_mlp_terms.reshape(groups, parts, piece_width).astype(jnp.bfloat16),
            TENSOR,
            scatter_dimension=1,
            tiled=True,
        ).astype(jnp.float32),
    )
    second_grad = grad_rows + second_part
    attn_grad = lax.all_gather(second_grad.astype(jnp.bfloat16), TENSOR, axis=0, tiled=True)
    grad_wo = matmul(mixed.T, attn_grad)
    blended_gradient = matmul(attn_grad, wo.T).astype(jnp.bfloat16)
    query_grad, key_seq_grad, value_seq_grad = attend_back(
        blended_gradient, query_rows, key_seq, value_seq, log_total, positions, heads_kv, head
    )
    kv_width = key_seq.shape[1]
    key_spread = (
        jnp.zeros((groups, block, kv_width), jnp.float32)
        .at[slots]
        .set(key_seq_grad.reshape(-1, block, kv_width))
    )
    value_spread = (
        jnp.zeros((groups, block, kv_width), jnp.float32)
        .at[slots]
        .set(value_seq_grad.reshape(-1, block, kv_width))
    )
    key_own, value_own = (
        lax.psum_scatter(
            key_spread.astype(jnp.bfloat16), DP, scatter_dimension=0, tiled=True
        ).astype(jnp.float32),
        lax.psum_scatter(
            value_spread.astype(jnp.bfloat16), DP, scatter_dimension=0, tiled=True
        ).astype(jnp.float32),
    )
    query_round = unrotate(query_grad, positions, head).astype(jnp.bfloat16)
    key_round = unrotate(key_own.reshape(block, kv_width), positions, head).astype(jnp.bfloat16)
    value_round = value_own.reshape(block, kv_width).astype(jnp.bfloat16)
    unit1, inverse1 = norm_stats(full)
    normed1 = (unit1 * gain_attn.astype(jnp.float32)).astype(jnp.bfloat16)
    grad_wq = matmul(normed1.T, query_round)
    grad_wk = matmul(normed1.T, key_round)
    grad_wv = matmul(normed1.T, value_round)
    normed1_grad = matmul(query_round, wq.T) + matmul(key_round, wk.T) + matmul(value_round, wv.T)
    first_terms, gain_attn_terms = norm_back(
        normed1_grad, unit1, inverse1, gain_attn.astype(jnp.float32)
    )
    first_part, gain_attn_part = (
        lax.psum_scatter(first_terms, TENSOR, scatter_dimension=0, tiled=True),
        lax.psum_scatter(
            gain_attn_terms.reshape(groups, parts, piece_width),
            TENSOR,
            scatter_dimension=1,
            tiled=True,
        ),
    )
    input_grad = second_grad + first_part
    return (
        input_grad,
        (
            grad_wq,
            grad_wk,
            grad_wv,
            grad_wo,
            grad_gate,
            grad_up,
            grad_down,
            gain_attn_part,
            gain_mlp_part,
        ),
    )


def reduce_grads(pieces):
    return (
        lax.psum_scatter(
            pieces[0].astype(jnp.bfloat16), DP, scatter_dimension=0, tiled=True
        ).astype(jnp.float32),
        lax.psum_scatter(
            pieces[1].astype(jnp.bfloat16), DP, scatter_dimension=0, tiled=True
        ).astype(jnp.float32),
        lax.psum_scatter(
            pieces[2].astype(jnp.bfloat16), DP, scatter_dimension=0, tiled=True
        ).astype(jnp.float32),
        lax.psum_scatter(
            pieces[3].astype(jnp.bfloat16), DP, scatter_dimension=1, tiled=True
        ).astype(jnp.float32),
        lax.psum_scatter(
            pieces[4].astype(jnp.bfloat16), DP, scatter_dimension=0, tiled=True
        ).astype(jnp.float32),
        lax.psum_scatter(
            pieces[5].astype(jnp.bfloat16), DP, scatter_dimension=0, tiled=True
        ).astype(jnp.float32),
        lax.psum_scatter(
            pieces[6].astype(jnp.bfloat16), DP, scatter_dimension=1, tiled=True
        ).astype(jnp.float32),
        lax.psum_scatter(
            pieces[7].astype(jnp.bfloat16), DP, scatter_dimension=0, tiled=True
        ).astype(jnp.float32),
        lax.psum_scatter(
            pieces[8].astype(jnp.bfloat16), DP, scatter_dimension=0, tiled=True
        ).astype(jnp.float32),
    )


def general_shards(inputs, table, cotangent, wq, wk, wv, wo, w_gate, w_up, w_down, gain_attn, gain_mlp):
    groups = lax.axis_size(DP)
    parts = lax.axis_size(TENSOR)
    micro_count = inputs.shape[0]
    section = lax.axis_index(SECTION)
    first_section = section == 0
    weights = (
        lax.all_gather(wq[0], DP, axis=0, tiled=True),
        lax.all_gather(wk[0], DP, axis=0, tiled=True),
        lax.all_gather(wv[0], DP, axis=0, tiled=True),
        lax.all_gather(wo[0], DP, axis=1, tiled=True),
        lax.all_gather(w_gate[0], DP, axis=0, tiled=True),
        lax.all_gather(w_up[0], DP, axis=0, tiled=True),
        lax.all_gather(w_down[0], DP, axis=1, tiled=True),
        lax.all_gather(gain_attn[0], DP, axis=0, tiled=True),
        lax.all_gather(gain_mlp[0], DP, axis=0, tiled=True),
    )
    head = HEAD_SIZE
    heads_kv = wk.shape[2] // head
    received = jnp.zeros_like(inputs[0])
    produced = []
    saved = []
    for step in range(micro_count + 1):
        own_rows = inputs[step] if step < micro_count else jnp.zeros_like(inputs[0])
        start_rows = jnp.where(first_section, own_rows, received)
        micro = jnp.clip(step - section, 0, micro_count - 1)
        result, context = layer_forward(start_rows, table, micro, weights, groups, heads_kv, head)
        produced.append(result)
        saved.append(context)
        if step < micro_count:
            received = passed_along(result, SECTION, 1)
    stacked = jnp.stack(produced)
    outputs = jnp.where(first_section, stacked[:micro_count], stacked[1:])[None]
    returned = jnp.zeros_like(inputs[0])
    returned_list = []
    totals = None
    for step in range(micro_count + 1):
        index = micro_count - 1 - step
        given = cotangent[index] if index >= 0 else jnp.zeros_like(cotangent[0])
        start_grad = jnp.where(first_section, returned, given)
        din, pieces = layer_backward(
            start_grad, saved[micro_count - step], weights, groups, parts, heads_kv, head
        )
        returned_list.append(din)
        if step < micro_count:
            returned = passed_along(din.astype(jnp.bfloat16), SECTION, -1).astype(din.dtype)
        totals = (
            pieces
            if totals is None
            else tuple((left + right for left, right in zip(totals, pieces)))
        )
    totals = reduce_grads(totals)
    reverse_stack = jnp.stack(returned_list[::-1])
    input_grad = jnp.where(first_section, reverse_stack[:micro_count], reverse_stack[1:])[None]
    (
        grad_wq,
        grad_wk,
        grad_wv,
        grad_wo,
        grad_gate,
        grad_up,
        grad_down,
        gain_attn_sum,
        gain_mlp_sum,
    ) = totals
    width_piece = gain_attn_sum.shape[-1]
    return (
        outputs,
        input_grad,
        grad_wq[None],
        grad_wk[None],
        grad_wv[None],
        grad_wo[None],
        grad_gate[None],
        grad_up[None],
        grad_down[None],
        gain_attn_sum.reshape(1, width_piece),
        gain_mlp_sum.reshape(1, width_piece),
    )


MESH = pl.DeviceIdType.MESH
SUBS = 4
HBM = pl.BlockSpec(memory_space=pl.ANY)
VMEM = pl.BlockSpec(memory_space=pltpu.VMEM)
SMEM = pl.BlockSpec(memory_space=pltpu.SMEM)
NARROW, WIDE = jnp.bfloat16, jnp.float32


def ring_place(index, count):
    return jnp.where(lax.rem(index, 2) == 0, index // 2, count - (index + 1) // 2)


def ring_index(place, count):
    place = lax.rem(place + 2 * count, count)
    return jnp.where(place < count // 2, 2 * place, 2 * count - 1 - 2 * place)


def greet(others):
    barrier = pltpu.get_barrier_semaphore()
    for other in others:
        pl.semaphore_signal(barrier, inc=1, device_id=other, device_id_type=MESH)
    pl.semaphore_wait(barrier, len(others))


def remote(source, target, send, recv, device):
    return pltpu.make_async_remote_copy(
        source, target, send, recv, device_id=device, device_id_type=MESH
    )


def partners(me, count):
    half = count // 2
    side, inside = me // half, lax.rem(me, half)
    peers = [(1 - side) * half + lax.rem(inside + k, half) for k in range(half)]
    peers += [side * half + lax.rem(inside + k, half) for k in range(1, half)]
    origins = [(1 - side) * half + lax.rem(inside + half - k, half) for k in range(half)]
    origins += [side * half + lax.rem(inside + half - k, half) for k in range(1, half)]
    return peers, origins


def aligned(start, size):
    return pl.ds(pl.multiple_of(start, size), size)


def tiles(size, tile):
    return [slice(at, at + tile) for at in range(0, size, tile)]


def loop(start, stop, body):
    if stop - start == 1:
        body(start)
    elif stop > start:

        def step(at, carry):
            body(at)
            return carry

        lax.fori_loop(start, stop, step, 0)


def dot(left, right, contract):
    return lax.dot_general(
        left, right, (contract, ((), ())), preferred_element_type=jnp.float32
    )


class Names:
    def __init__(self, **values):
        self.__dict__.update(values)


class Work:
    def __init__(self):
        self.items = []

    def add(self, body, count=1):
        self.items.append((body, 0, count))

    def first(self, body):
        self.items.insert(0, (body, 0, 1))

    def do(self, some=1 << 20):
        while some > 0 and self.items:
            body, start, stop = self.items.pop(0)
            until = min(stop, start + some)
            loop(start, until, body)
            some -= until - start
            if until < stop:
                self.items.insert(0, (body, until, stop))


class Copies:
    def __init__(self, sem):
        self.sem = sem
        self.used = 0

    def __call__(self, source, target):
        copy = pltpu.make_async_copy(source, target, self.sem.at[self.used])
        self.used += 1
        copy.start()
        return copy


class Ring:
    def __init__(self):
        self.count = lax.axis_size(DP)
        self.far = self.count // 2
        self.me = lax.axis_index(DP)
        self.core = lax.axis_index(TENSOR)
        self.place = ring_place(self.me, self.count)
        self.near = tuple({DP: ring_index(self.place + step, self.count)} for step in (1, -1))
        self.side = {TENSOR: 1 - self.core}

    def everyone(self):
        return [*self.near, self.side]

    def index(self, steps):
        return ring_index(self.place + steps, self.count)

    def orders(self):
        half = SUBS // 2
        for k in range(half):
            for sub in (k, k + half):
                yield sub, 0
                yield sub, 1


def gather_scratch(count):
    far = count // 2
    dma = pltpu.SemaphoreType.DMA
    return [
        dma((2, far, SUBS)), dma((2, far, SUBS)), dma((count, SUBS)), dma((count, SUBS)), dma((1,))
    ]


class Gather:
    def __init__(self, ring, x_ref, o_ref, sems):
        self.ring = ring
        self.x_ref, self.o_ref = x_ref, o_ref
        self.ring_send, self.ring_recv, self.side_send, self.side_recv, self.own_sem = sems
        self.rows = x_ref.shape[0]
        self.piece = self.rows // SUBS
        self.sends = []

    def spot(self, steps, sub, core):
        start = (self.ring.index(steps) * 2 + core) * self.rows + sub * self.piece
        return self.o_ref.at[aligned(start, self.piece), :]

    def mine(self, steps, sub):
        if steps == 0:
            return self.x_ref.at[sub * self.piece : (sub + 1) * self.piece, :]
        return self.spot(steps, sub, self.ring.core)

    def travels(self, way, hop, sub):
        return hop < self.ring.far or (sub < SUBS // 2) == (way == 0)

    def go(self, copy):
        copy.start()
        self.sends.append(copy)

    def pass_on(self, way, hop, sub):
        steps = 1 - hop if way == 0 else hop - 1
        self.go(
            remote(
                self.mine(steps, sub),
                self.spot(steps, sub, self.ring.core),
                self.ring_send.at[way, hop - 1, sub],
                self.ring_recv.at[way, hop - 1, sub],
                self.ring.near[way],
            )
        )

    def hand_over(self, steps, sub, slot):
        self.go(
            remote(
                self.mine(steps, sub),
                self.spot(steps, sub, self.ring.core),
                self.side_send.at[slot, sub],
                self.side_recv.at[slot, sub],
                self.ring.side,
            )
        )

    def start_piece(self, sub):
        for way in range(2):
            self.pass_on(way, 1, sub)
        self.hand_over(0, sub, 0)

    def start(self):
        for sub, way in self.ring.orders():
            if way == 0:
                self.start_piece(sub)
        self.started()

    def started(self):
        self.own = pltpu.make_async_copy(
            self.x_ref,
            self.o_ref.at[aligned((self.ring.me * 2 + self.ring.core) * self.rows, self.rows), :],
            self.own_sem.at[0],
        )
        self.own.start()

    def hop(self, hop, between=None):
        far, count = self.ring.far, self.ring.count
        for sub, way in self.ring.orders():
            if not self.travels(way, hop, sub):
                continue
            steps = -hop if way == 0 else hop
            here = self.spot(steps, sub, self.ring.core)
            remote(
                here, here, self.ring_send.at[way, hop - 1, sub],
                self.ring_recv.at[way, hop - 1, sub], self.ring.near[way],
            ).wait_recv()
            if hop < far and self.travels(way, hop + 1, sub):
                self.pass_on(way, hop + 1, sub)
            self.hand_over(steps, sub, hop if way == 0 or hop == far else count - hop)
            if way == 1 and between is not None:
                between()

    def side_arrived(self, steps):
        slot = -steps if steps <= 0 else self.ring.count - steps
        slot = self.ring.far if abs(steps) == self.ring.far else slot
        for sub in range(SUBS):
            there = self.spot(steps, sub, 1 - self.ring.core)
            remote(
                there, there, self.side_send.at[slot, sub], self.side_recv.at[slot, sub],
                self.ring.side,
            ).wait_recv()

    def around(self, hop):
        return (-hop, hop) if hop < self.ring.far else (-hop,)

    def sent(self):
        for copy in self.sends:
            copy.wait_send()

    def finish(self):
        self.own.wait()
        self.side_arrived(0)
        for hop in range(1, self.ring.far + 1):
            for steps in self.around(hop):
                self.side_arrived(steps)
        self.sent()

    def run(self, use, work):
        self.started()
        self.own.wait()
        waiting = [0]

        def between():
            if waiting:
                steps = waiting.pop(0)
                self.side_arrived(steps)
                use(self.ring.index(steps))
            else:
                work.do(1)

        for hop in range(1, self.ring.far + 1):
            self.hop(hop, between)
            waiting += self.around(hop)
        while waiting:
            between()
        self.sent()


def line_scratch(count):
    lines = count // 2
    dma = pltpu.SemaphoreType.DMA
    return [
        dma((2, lines)), dma((2, lines)), dma((2 * lines,)), dma((2 * lines,)),
        dma((2, 2 * lines)), dma((2, 2 * lines)), dma((1,)),
    ]


class LineGather:
    def __init__(self, ring, x_ref, o_ref, sems):
        self.ring = ring
        self.x_ref, self.o_ref = x_ref, o_ref
        self.lines = ring.count // 2
        self.line, self.column = ring.me // 2, lax.rem(ring.me, 2)
        self.next = {DP: ring.me + 1 - 2 * self.column}
        self.send, self.recv, self.next_send, self.next_recv = sems[:4]
        self.side_send, self.side_recv, self.own_sem = sems[4:]
        self.rows = x_ref.shape[0]
        self.sends = []

    def spot(self, steps, core, column):
        index = (self.line + steps) * 2 + column
        return self.o_ref.at[aligned((index * 2 + core) * self.rows, self.rows), :]

    def there(self, steps):
        if steps == 0:
            return None
        return self.line >= -steps if steps < 0 else self.line + steps < self.lines

    def if_there(self, condition, do):
        if condition is None:
            do()
        else:
            pl.when(condition)(do)

    def go(self, condition, copy):
        self.if_there(condition, copy.start)
        self.sends.append((condition, copy))

    def spread(self, steps):
        ring, slot = self.ring, steps + self.lines
        source = self.x_ref if steps == 0 else self.spot(steps, ring.core, self.column)
        target = self.spot(steps, ring.core, self.column)
        here = self.there(steps)
        both = lambda other: other if here is None else jnp.logical_and(here, other)
        for way, ahead in enumerate((self.line + 1 < self.lines, self.line > 0)):
            passed = -steps if way == 0 else steps
            if passed >= 0 and passed < self.lines - 1:
                self.go(
                    both(ahead),
                    remote(
                        source, target, self.send.at[way, passed], self.recv.at[way, passed],
                        {DP: ring.me + 2 - 4 * way},
                    ),
                )
        self.go(
            here, remote(source, target, self.next_send.at[slot], self.next_recv.at[slot], self.next)
        )
        self.go(
            here,
            remote(source, target, self.side_send.at[0, slot], self.side_recv.at[0, slot], ring.side),
        )

    def start(self):
        self.spread(0)
        self.own = pltpu.make_async_copy(
            self.x_ref, self.spot(0, self.ring.core, self.column), self.own_sem.at[0]
        )
        self.own.start()

    def hop(self, hop):
        for way, steps in enumerate((-hop, hop)):
            here = self.spot(steps, self.ring.core, self.column)
            copy = remote(
                here, here, self.send.at[way, hop - 1], self.recv.at[way, hop - 1], self.next
            )
            self.if_there(self.there(steps), copy.wait_recv)
            self.spread(steps)

    def finish(self):
        ring = self.ring
        every = range(1 - self.lines, self.lines)
        for steps in every:
            slot = steps + self.lines
            here = self.spot(steps, ring.core, 1 - self.column)
            copy = remote(here, here, self.next_send.at[slot], self.next_recv.at[slot], self.next)
            self.if_there(self.there(steps), copy.wait_recv)
            self.go(
                self.there(steps),
                remote(here, here, self.side_send.at[1, slot], self.side_recv.at[1, slot], ring.side),
            )
        for which, column in enumerate((self.column, 1 - self.column)):
            for steps in every:
                slot = steps + self.lines
                here = self.spot(steps, 1 - ring.core, column)
                copy = remote(
                    here, here, self.side_send.at[which, slot], self.side_recv.at[which, slot], ring.side
                )
                self.if_there(self.there(steps), copy.wait_recv)
        for condition, copy in self.sends:
            self.if_there(condition, copy.wait_send)
        self.own.wait()


def reduce_scratch(count, rows, width):
    far = count // 2
    dma = pltpu.SemaphoreType.DMA
    return [
        pltpu.VMEM((count * 2 * rows, width), NARROW),
        pltpu.VMEM((count, rows, width), NARROW),
        pltpu.VMEM((2, far, rows, width), NARROW),
        pltpu.VMEM((2, far, rows, width), NARROW),
        dma((2, far, SUBS)), dma((2, far, SUBS)), dma((count,)), dma((count,)),
    ]


class Reduce:
    def __init__(self, ring, scratch):
        self.ring = ring
        self.parts, self.beside, self.outgoing, self.incoming = scratch[:4]
        self.ring_send, self.ring_recv, self.side_send, self.side_recv = scratch[4:]
        self.rows = self.beside.shape[1]
        self.piece = self.rows // SUBS

    def span(self, sub):
        return slice(sub * self.piece, (sub + 1) * self.piece)

    def spot(self, steps, core, sub=None):
        start = (self.ring.index(steps) * 2 + core) * self.rows
        if sub is None:
            return aligned(start, self.rows)
        return aligned(start + sub * self.piece, self.piece)

    def make(self):
        steps = self.to_make.pop(0)
        self.produce(self.ring.index(steps), self.parts)
        slot = len(self.slots)
        copy = remote(
            self.parts.at[self.spot(steps, 1 - self.ring.core), :], self.beside.at[slot],
            self.side_send.at[slot], self.side_recv.at[slot], self.ring.side,
        )
        copy.start()
        self.slots[steps] = (slot, copy)

    def mine(self, steps, sub):
        while steps not in self.slots:
            self.make()
        slot, copy = self.slots[steps]
        if steps not in self.joined:
            copy.wait_recv()
            self.joined.add(steps)
        return self.parts[self.spot(steps, self.ring.core, sub), :].astype(
            jnp.float32
        ) + self.beside[slot, self.span(sub), :].astype(jnp.float32)

    def travels(self, way, step, sub):
        return step > 1 or (sub < SUBS // 2) == (way == 0)

    def ring_copy(self, way, step, sub):
        return remote(
            self.outgoing.at[way, step - 1, self.span(sub), :],
            self.incoming.at[way, step - 1, self.span(sub), :],
            self.ring_send.at[way, step - 1, sub],
            self.ring_recv.at[way, step - 1, sub],
            self.ring.near[way],
        )

    def step(self, step):
        far = self.ring.far
        for sub, way in self.ring.orders():
            if not self.travels(way, step, sub):
                continue
            steps = far + 1 - step
            steps = steps if way == 0 or steps == far else -steps
            value = self.mine(steps, sub)
            if step > 1 and self.travels(way, step - 1, sub):
                self.ring_copy(way, step - 1, sub).wait_recv()
                value = value + self.incoming[way, step - 2, self.span(sub), :].astype(jnp.float32)
            self.outgoing[way, step - 1, self.span(sub), :] = value.astype(NARROW)
            copy = self.ring_copy(way, step, sub)
            copy.start()
            self.sends.append(copy)
            if way == 1:
                if self.to_make:
                    self.make()
                else:
                    self.work.do(1)

    def begin(self, produce, work):
        self.produce, self.work = produce, work
        self.slots, self.joined, self.sends = {}, set(), []
        far = self.ring.far
        self.to_make = [far]
        for steps in range(far - 1, 0, -1):
            self.to_make += [steps, -steps]
        self.to_make.append(0)
        self.make()
        self.make()

    def end(self, finish):
        far = self.ring.far
        while self.to_make:
            self.make()
        for sub, way in self.ring.orders():
            if way == 1:
                continue
            value = self.mine(0, sub)
            for way in range(2):
                self.ring_copy(way, far, sub).wait_recv()
                value = value + self.incoming[way, far - 1, self.span(sub), :].astype(jnp.float32)
            finish(sub, self.span(sub), value)
        for copy in self.sends:
            copy.wait_send()
        for _, copy in self.slots.values():
            copy.wait_send()

    def run(self, produce, finish, work, beside=()):
        beside = list(beside)
        self.begin(produce, work)
        for step in range(1, self.ring.far + 1):
            self.step(step)
            if beside:
                beside.pop(0)()
        self.end(finish)
        return beside


def products(left, right, transposed, tile=512):
    width = right.shape[0] if transposed else right.shape[1]
    number = width // tile

    def produce(index, parts):
        block = parts.shape[0] // lax.axis_size(DP)
        rows = aligned(index * block, block)

        def one(at):
            cols = aligned(at * tile, tile)
            if transposed:
                part = dot(left[rows, :], right[cols, :], ((1,), (1,)))
            else:
                part = dot(left[rows, :], right[:, cols], ((1,), (0,)))
            parts[rows, cols] = part.astype(NARROW)

        loop(0, number, one)

    return produce


def add_gradient(work, left, right, out, tile=256):
    if out.shape[0] >= out.shape[1]:

        def piece(at):
            cols = aligned(at * tile, tile)
            out[cols, :] = dot(left[:, cols], right[...], ((0,), (0,))).astype(NARROW)

        work.add(piece, out.shape[0] // tile)
    else:

        def piece(at):
            cols = aligned(at * tile, tile)
            out[:, cols] = dot(left[...], right[:, cols], ((0,), (0,))).astype(NARROW)

        work.add(piece, out.shape[1] // tile)


def unit_rows(value):
    inverse = lax.rsqrt(jnp.mean(value * value, axis=-1, keepdims=True) + epsilon)
    return value * inverse, inverse


def through_norm(grad, value, gain):
    unit, inverse = unit_rows(value)
    scaled = grad * gain
    inner = jnp.mean(scaled * unit, axis=-1, keepdims=True)
    return inverse * (scaled - unit * inner), jnp.sum(grad * unit, axis=0, keepdims=True)


def shape_of(*dims, kind=NARROW):
    return jax.ShapeDtypeStruct(dims, kind)


def call_fused(name, body, cid, us, ins, outs, scratch):
    def kernel(*refs):
        refs = list(refs)
        named = {key: refs.pop(0) for key in [*ins, *outs]}
        for key, kind in scratch.items():
            named[key] = [refs.pop(0) for _ in kind] if isinstance(kind, list) else refs.pop(0)
        body(Names(**named))

    flat = []
    for kind in scratch.values():
        flat += kind if isinstance(kind, list) else [kind]
    result = pl.pallas_call(
        kernel,
        out_shape=tuple(shape for shape, _ in outs.values()),
        in_specs=[spec for _, spec in ins.values()],
        out_specs=tuple(spec for _, spec in outs.values()),
        scratch_shapes=flat,
        compiler_params=pltpu.CompilerParams(
            collective_id=cid, has_side_effects=True, vmem_limit_bytes=63 * 1024 * 1024
        ),
        cost_estimate=pl.CostEstimate(
            flops=0, bytes_accessed=int(us * 3.69e6), transcendentals=0
        ),
        name=name,
    )(*[value for value, _ in ins.values()])
    return Names(**dict(zip(outs, result)))


def swap_halves(rows, head):
    width = rows.shape[1]
    lane = lax.broadcasted_iota(jnp.int32, rows.shape, 1)
    half = head // 2
    return jnp.where(
        lax.rem(lane, head) < half, pltpu.roll(rows, width - half, 1), pltpu.roll(rows, half, 1)
    )


def low_lanes(shape, head):
    return lax.broadcasted_iota(jnp.int32, shape, 1) < head


def two_heads(rows, head):
    low = low_lanes(rows.shape, head)
    zero = jnp.zeros_like(rows)
    return jnp.concatenate([jnp.where(low, rows, zero), jnp.where(low, zero, rows)], axis=0)


def one_row(rows, head):
    half = rows.shape[0] // 2
    return jnp.where(low_lanes((half, rows.shape[1]), head), rows[:half], rows[half:])


def triangle(block, keys):
    row = lax.rem(lax.broadcasted_iota(jnp.int32, (2 * block, keys), 0), block)
    column = lax.broadcasted_iota(jnp.int32, (2 * block, keys), 1)
    return column <= row + (keys - block)


def in_order(ref, order, spot, block):
    value = ref[:block, :]
    for other in range(1, ref.shape[0] // block):
        there = order[spot] == other
        value = jnp.where(there, ref[other * block : (other + 1) * block, :], value)
    return value


def attend_here(slots, qkv, cosine, sine, kept, lse, mixed, key2, value2):
    groups = slots.shape[0]
    tokens = qkv.shape[0]
    block = tokens // groups
    span = groups // 2
    wide = qkv.shape[1] // 2
    head = wide // 2
    scale = 1.0 / math.sqrt(head)
    for spot in range(groups):
        here = slice(spot * block, (spot + 1) * block)
        turn_rows = slice(spot % span * block, (spot % span + 1) * block)
        turned_by, turned_sine = cosine[turn_rows, :], sine[turn_rows, :]
        rows = in_order(qkv, slots, spot, block)
        query, pair = rows[:, :wide], rows[:, wide:]
        low = low_lanes(pair.shape, head)
        query = query * turned_by + swap_halves(query, head) * turned_sine
        pair = jnp.where(low, pair * turned_by + swap_halves(pair, head) * turned_sine, pair)
        other = pltpu.roll(pair, head, 1)
        kept[here, :wide] = query.astype(kept.dtype)
        kept[here, wide:] = pair.astype(kept.dtype)
        key2[here, :] = jnp.where(low, pair, other).astype(key2.dtype)
        value2[here, :] = jnp.where(low, other, pair).astype(value2.dtype)
    for spot in range(groups):
        here = slice(spot * block, (spot + 1) * block)
        first = spot // span * span * block
        keys = (spot % span + 1) * block
        query = two_heads(kept[here, :wide], head)
        score = dot(query, key2[first : first + keys, :], ((1,), (1,))) * scale
        allowed = triangle(block, keys)
        power = jnp.where(allowed, jnp.exp(score), 0.0)
        total = jnp.sum(power, axis=1, keepdims=True)
        log_total = jnp.log(total)
        probs = (power * (1.0 / total)).astype(jnp.bfloat16)
        value = dot(probs, value2[first : first + keys, :], ((1,), (0,)))
        mixed[here, :] = one_row(value, head).astype(mixed.dtype)
        lse[spot] = log_total


def attend_back_here(
    slots, grad, kept, lse, cosine, sine, out, key2, value2, key_sum, value_sum, between=None
):
    groups = slots.shape[0]
    tokens = kept.shape[0]
    block = tokens // groups
    span = groups // 2
    wide = kept.shape[1] // 2
    head = wide // 2
    scale = 1.0 / math.sqrt(head)
    for spot in range(groups):
        here = slice(spot * block, (spot + 1) * block)
        pair = kept[here, wide:].astype(jnp.float32)
        low = low_lanes(pair.shape, head)
        other = pltpu.roll(pair, head, 1)
        key2[here, :] = jnp.where(low, pair, other).astype(key2.dtype)
        value2[here, :] = jnp.where(low, other, pair).astype(value2.dtype)
    for spot in range(groups - 1, -1, -1):
        here = slice(spot * block, (spot + 1) * block)
        place = spot % span
        turn_rows = slice(place * block, (place + 1) * block)
        first = spot // span * span * block
        keys = (place + 1) * block
        query = two_heads(kept[here, :wide], head)
        given = two_heads(in_order(grad, slots, spot, block), head)
        key = key2[first : first + keys, :]
        value = value2[first : first + keys, :]
        score = dot(query, key, ((1,), (1,))) * scale
        probs = jnp.where(triangle(block, keys), jnp.exp(score - lse[spot]), 0.0)
        prob_grad = dot(given, value, ((1,), (1,)))
        rowdot = jnp.sum(probs * prob_grad, axis=1, keepdims=True)
        score_grad = (probs * (prob_grad - rowdot) * scale).astype(jnp.bfloat16)
        value_part = dot(probs.astype(jnp.bfloat16), given, ((0,), (0,)))
        key_part = dot(score_grad, query, ((0,), (0,)))
        if place == span - 1:
            value_sum[first : first + keys, :] = value_part
            key_sum[first : first + keys, :] = key_part
        else:
            value_sum[first : first + keys, :] += value_part
            key_sum[first : first + keys, :] += key_part
        query_grad = one_row(dot(score_grad, key, ((1,), (0,))), head)
        query_grad = query_grad * cosine[turn_rows, :] - swap_halves(query_grad, head) * sine[turn_rows, :]
        out[here, :wide] = query_grad.astype(out.dtype)
        if between is not None:
            between(spot)
    for spot in range(groups):
        here = slice(spot * block, (spot + 1) * block)
        turn_rows = slice(spot % span * block, (spot % span + 1) * block)
        key = key_sum[here, :]
        key = key + pltpu.roll(key, head, 1)
        key = key * cosine[turn_rows, :] - swap_halves(key, head) * sine[turn_rows, :]
        value = value_sum[here, :]
        value = value + pltpu.roll(value, head, 1)
        out[here, wide:] = jnp.where(low_lanes(key.shape, head), key, value).astype(out.dtype)


def put_back(source, target, row):
    groups = row.shape[0]
    block = source.shape[0] // groups
    for spot in range(groups):
        target[spot * block : (spot + 1) * block, :] = in_order(source, row, spot, block)


def attend_scratch(tokens, head, back=False):
    vmem = pltpu.VMEM
    wide = 2 * head
    kinds = dict(
        key2=vmem((tokens, wide), jnp.bfloat16),
        value2=vmem((tokens, wide), jnp.bfloat16),
        by_number=vmem((tokens, 2 * wide if back else wide), jnp.bfloat16),
    )
    if back:
        kinds.update(
            key_sum=vmem((tokens, wide), jnp.float32), value_sum=vmem((tokens, wide), jnp.float32)
        )
    return kinds


def rope_tables(tokens, head):
    index = np.arange(head // 2, dtype=np.float32)
    base = (1.0 / np.float32(500000.0) ** (index * 2.0 / head)).astype(np.float32)
    wavelength = 2.0 * math.pi / base
    blend = (8192.0 / wavelength - 1.0) / 3.0
    middle = (1.0 - blend) * base / 32.0 + blend * base
    slow = np.where(wavelength > 8192.0, base / 32.0, middle)
    frequencies = np.where(wavelength < 2048.0, base, slow).astype(np.float32)
    angle = np.arange(tokens, dtype=np.float32)[:, None] * frequencies[None, :]
    cosine, sine = np.cos(angle), np.sin(angle)
    return (
        jnp.asarray(np.concatenate([cosine] * 4, axis=1)),
        jnp.asarray(np.concatenate([-sine, sine] * 2, axis=1)),
    )


def weight_pieces(source, target, count, heads, srcs, dsts, layer):
    qkv, wo, gate, up, down = srcs
    out_qkv, out_wo, out_gu, out_down = dsts
    depth = gate.shape[1]
    hidden = gate.shape[2] // count
    q_rows = wo.shape[1] // count
    kv_rows = (qkv.shape[0] - wo.shape[1]) // 2
    shared = count * heads // kv_rows
    cols = aligned(source * depth, depth)
    k_from = pl.multiple_of(wo.shape[1] + target // shared * heads, heads)
    v_from = pl.multiple_of(wo.shape[1] + kv_rows + target // shared * heads, heads)
    mine = aligned(target * hidden, hidden)
    return (
        (qkv.at[aligned(target * q_rows, q_rows), :], out_qkv.at[layer, pl.ds(0, q_rows), cols]),
        (qkv.at[pl.ds(k_from, heads), :], out_qkv.at[layer, pl.ds(q_rows, heads), cols]),
        (qkv.at[pl.ds(v_from, heads), :], out_qkv.at[layer, pl.ds(q_rows + heads, heads), cols]),
        (wo.at[0, aligned(target * q_rows, q_rows), :], out_wo.at[layer, :, cols]),
        (gate.at[0, :, mine], out_gu.at[layer, cols, pl.ds(0, hidden)]),
        (up.at[0, :, mine], out_gu.at[layer, cols, pl.ds(hidden, hidden)]),
        (down.at[0, mine, :], out_down.at[layer, :, cols]),
    )


KINDS, ATTENTION_KINDS = 7, 4


class Spread:
    def __init__(self, ring, heads, srcs, dsts, sems):
        self.ring = ring
        self.layer = lax.axis_index(SECTION)
        self.across = {SECTION: 1 - self.layer}
        self.peers, self.origins = partners(ring.me, ring.count)
        self.send, self.recv, self.cross_send, self.cross_recv, self.own_sem = sems
        self.pieces = lambda source, target, layer: weight_pieces(
            source, target, ring.count, heads, srcs, dsts, layer
        )
        self.started, self.local = [], {}
        half = ring.count // 2
        self.near, self.far = list(range(half, ring.count - 1)), list(range(half))

    def go(self, copy):
        copy.start()
        self.started.append(copy)

    def own(self, kinds):
        last = self.ring.count - 1
        for kind in kinds:
            source, target = self.pieces(self.ring.me, self.ring.me, self.layer)[kind]
            self.go(
                remote(
                    source, target, self.cross_send.at[kind, last], self.cross_recv.at[kind, last],
                    self.across,
                )
            )
            self.local[kind] = pltpu.make_async_copy(source, target, self.own_sem.at[kind])
            self.local[kind].start()

    def out(self, kind, places):
        for k in places:
            source, target = self.pieces(self.ring.me, self.peers[k], self.layer)[kind]
            self.go(
                remote(
                    source, target, self.send.at[kind, k], self.recv.at[kind, k],
                    {DP: self.peers[k]},
                )
            )

    def pass_on(self, kind, places):
        for k in places:
            here = self.pieces(self.origins[k], self.ring.me, self.layer)[kind][1]
            remote(
                here, here, self.send.at[kind, k], self.recv.at[kind, k], {DP: self.origins[k]}
            ).wait_recv()
            self.go(
                remote(
                    here, here, self.cross_send.at[kind, k], self.cross_recv.at[kind, k], self.across
                )
            )

    def here(self, kinds):
        for kind in kinds:
            self.local[kind].wait()
            for k in range(self.ring.count):
                origin = self.origins[k] if k < self.ring.count - 1 else self.ring.me
                there = self.pieces(origin, self.ring.me, 1 - self.layer)[kind][1]
                remote(
                    there, there, self.cross_send.at[kind, k], self.cross_recv.at[kind, k], self.across
                ).wait_recv()

    def sent(self):
        for copy in self.started:
            copy.wait_send()


def chip_rows(index, local):
    return aligned(index * 2 * local, 2 * local)


def feed_forward_use(s, local, after):
    width = s.hidden.shape[1]
    tile = 256
    number = width // tile

    def use(index):
        rows = chip_rows(index, local)

        def one(at):
            start = at * tile
            cols, right = aligned(start, tile), aligned(start + width, tile)
            value = s.normed2[rows, :]
            gate = dot(value, s.gu[:, cols], ((1,), (0,)))
            upper = dot(value, s.gu[:, right], ((1,), (0,)))
            s.hidden[rows, cols] = (gate * jax.nn.sigmoid(gate) * upper).astype(NARROW)
            after(rows, cols, right, gate, upper)

        loop(0, number, one)

    return use


def feed_forward_back(s, rows, cols, right, gate, upper):
    hidden_grad = dot(s.out_grad[rows, :], s.down[cols, :], ((1,), (1,)))
    sigma = jax.nn.sigmoid(gate)
    gate_grad = hidden_grad * upper * sigma * (1.0 + gate * (1.0 - sigma))
    s.gu_grad[rows, cols] = gate_grad.astype(NARROW)
    s.gu_grad[rows, right] = (hidden_grad * gate * sigma).astype(NARROW)


def opening_body(s):
    ring = Ring()
    layer = lax.axis_index(SECTION)
    peers, origins = partners(ring.me, ring.count)
    holders = [{DP: peer} for peer in peers] + [
        {SECTION: 1 - layer, DP: peer} for peer in [*peers, ring.me]
    ]
    greet([*holders, ring.side])
    copies = Copies(s.copy_sem)
    rows_in = copies(s.inputs.at[layer], s.rows)
    given_in = copies(s.cotangent.at[layer], s.given)
    spread = Spread(
        ring, s.kept0.shape[1] // 4, (s.qkv, s.wo, s.gate, s.up, s.down_in),
        (s.out_qkv, s.out_wo, s.out_gu, s.out_down), s.spread_sems,
    )
    attention, feed = range(ATTENTION_KINDS), range(ATTENTION_KINDS, KINDS)
    local, depth = s.rows.shape[0], s.gain_attn.shape[1]

    s.gain_piece[...] = jnp.zeros_like(s.gain_piece)
    s.gain_piece[0:1, :] = s.gain_attn[...].astype(WIDE)
    s.gain_piece[1:2, :] = s.gain_mlp[...].astype(WIDE)
    gain_send, gain_recv = s.gain_sems
    spot = lambda at, source: s.gains.at[at, :, aligned(source * depth, depth)]
    for k, holder in enumerate(holders):
        spread.go(remote(s.gain_piece, spot(layer, ring.me), gain_send.at[k], gain_recv.at[k], holder))
    own_gains = copies(s.gain_piece, spot(layer, ring.me))
    spread.own(attention)
    own_gains.wait()
    for k, holder in enumerate(holders):
        at, place = (layer, k) if k < ring.count - 1 else (1 - layer, k - ring.count + 1)
        here = spot(at, origins[place] if place < ring.count - 1 else ring.me)
        remote(here, here, gain_send.at[k], gain_recv.at[k], holder).wait_recv()

    rows_in.wait()
    unit, _ = unit_rows(s.rows[...])
    s.shard0[...] = (unit * s.gains[0, 0:1, :]).astype(NARROW)
    first = LineGather(ring, s.shard0, s.normed1, s.line_sems)
    first.start()
    for kind in attention:
        spread.out(kind, spread.far + spread.near)
    for hop in range(1, ring.far):
        first.hop(hop)
    given_in.wait()
    s.shard1[...] = s.given[...].astype(NARROW)
    grads = LineGather(ring, s.shard1, s.out_grad, s.grads_sems)
    grads.start()
    for kind in attention:
        spread.pass_on(kind, spread.near + spread.far)
    gate, up, down = feed
    spread.out(gate, spread.far + spread.near)
    spread.own(feed)
    first.finish()
    spread.here(attention)
    loads = [
        copies(s.out_qkv.at[0], s.qkv_w), copies(s.out_qkv.at[1], s.next_qkv_w),
        copies(s.out_wo.at[0], s.wo_w),
    ]
    stores = [copies(s.normed1, s.normed1_out)]
    for load in loads:
        load.wait()
    tile = 2 * local

    def project(at):
        rows = aligned(at * tile, tile)
        s.projected[rows, :] = dot(s.normed1[rows, :], s.qkv_w[...], ((1,), (1,)))

    loop(0, s.projected.shape[0] // tile, project)
    attend_here(s.slots, s.projected, s.cosine, s.sine, s.kept0, s.lse0, s.by_number, s.key2, s.value2)
    put_back(s.by_number, s.mixed0, s.row)
    stores[0].wait()
    grads.hop(1)

    reduce = Reduce(ring, s.reduce)
    none = Work()

    second_rows = Gather(ring, s.shard2, s.normed2, s.gather_sems)
    next_rows = Gather(ring, s.shard0, s.normed1, s.first_sems)

    def second(sub, span, value):
        value = s.rows[span, :] + value
        s.second[span, :] = value
        unit, _ = unit_rows(value)
        s.shard2[span, :] = (unit * s.gains[0, 1:2, :]).astype(NARROW)
        second_rows.start_piece(sub)

    middle = len(spread.far) // 2
    early, late = spread.near + spread.far[:middle], spread.far[middle:]

    def stage(number):
        kind, places = ((up, early), (up, late), (down, early), (down, late))[number]
        spread.out(kind, places)
        if number == 0:
            spread.pass_on(gate, spread.near + spread.far)
        else:
            kind, places = ((up, early), (up, late), (down, early))[number - 1]
            spread.pass_on(kind, places)
        if number + 2 < ring.far:
            grads.hop(number + 2)

    left = reduce.run(
        products(s.mixed0, s.wo_w, False), second, none,
        [functools.partial(stage, number) for number in range(4)],
    )
    for do in left:
        do()
    spread.pass_on(down, late)
    spread.here((gate, up))
    copies(s.out_gu.at[0], s.gu).wait()

    def keep(rows, cols, right, gate, upper):
        s.gate_up[rows, cols] = gate
        s.gate_up[rows, right] = upper

    second_rows.run(feed_forward_use(s, local, keep), none)
    spread.here((down,))
    load = copies(s.out_down.at[0], s.down)
    grads.finish()
    stores += [
        copies(s.out_grad, s.out_grad_out), copies(s.normed2, s.normed2_out),
        copies(s.gate_up, s.gate_up_out),
    ]
    load.wait()

    def result(sub, span, value):
        value = s.second[span, :] + value
        s.result[span, :] = value
        unit, _ = unit_rows(value)
        s.shard0[span, :] = (unit * s.gains[1, 0:1, :]).astype(NARROW)
        next_rows.start_piece(sub)

    reduce.run(products(s.hidden, s.down, False), result, none)

    def use(index):
        rows = chip_rows(index, local)
        s.projected[rows, :] = dot(s.normed1[rows, :], s.next_qkv_w[...], ((1,), (1,)))

    next_rows.run(use, none)
    stores.append(copies(s.normed1, s.next_normed1_out))
    attend_here(s.slots, s.projected, s.cosine, s.sine, s.kept1, s.lse1, s.by_number, s.key2, s.value2)
    put_back(s.by_number, s.mixed1, s.row)
    for store in stores[1:]:
        store.wait()
    spread.sent()


def opening(slots, row, cosine, sine, inputs, cotangent, qkv, wo, gate, up, down, gain_attn, gain_mlp, count, head):
    local, width = inputs.shape[1:]
    tokens = count * 2 * local
    depth = gate.shape[1]
    hidden = gate.shape[2] // count
    q_rows = wo.shape[1] // count
    vmem, dma = pltpu.VMEM, pltpu.SemaphoreType.DMA
    lse = shape_of(count, 2 * tokens // count, 1, kind=WIDE)
    return call_fused(
        "opening", opening_body, 0, 360,
        dict(
            slots=(slots, SMEM), row=(row, SMEM), cosine=(cosine, VMEM), sine=(sine, VMEM),
            inputs=(inputs, HBM), cotangent=(cotangent, HBM), qkv=(qkv, HBM), wo=(wo, HBM),
            gate=(gate, HBM), up=(up, HBM), down_in=(down, HBM),
            gain_attn=(gain_attn, VMEM), gain_mlp=(gain_mlp, VMEM),
        ),
        dict(
            out_qkv=(shape_of(2, q_rows + 2 * head, width), HBM),
            out_wo=(shape_of(2, q_rows, width), HBM),
            out_gu=(shape_of(2, width, 2 * hidden), HBM),
            out_down=(shape_of(2, hidden, width), HBM),
            gains=(shape_of(2, 8, width, kind=WIDE), VMEM),
            normed1_out=(shape_of(tokens, width), HBM),
            next_normed1_out=(shape_of(tokens, width), HBM),
            normed2_out=(shape_of(tokens, width), HBM),
            out_grad_out=(shape_of(tokens, width), HBM),
            gate_up_out=(shape_of(tokens, 2 * hidden, kind=WIDE), HBM),
            second=(shape_of(local, width, kind=WIDE), VMEM),
            result=(shape_of(local, width, kind=WIDE), VMEM),
            hidden=(shape_of(tokens, hidden), VMEM),
            mixed0=(shape_of(tokens, 2 * head), VMEM), mixed1=(shape_of(tokens, 2 * head), VMEM),
            kept0=(shape_of(tokens, 4 * head), VMEM), kept1=(shape_of(tokens, 4 * head), VMEM),
            lse0=(lse, VMEM), lse1=(lse, VMEM),
        ),
        dict(
            rows=vmem((local, width), WIDE), given=vmem((local, width), WIDE),
            gain_piece=vmem((8, depth), WIDE),
            shard0=vmem((local, width), NARROW), shard1=vmem((local, width), NARROW),
            shard2=vmem((local, width), NARROW),
            normed1=vmem((tokens, width), NARROW), normed2=vmem((tokens, width), NARROW),
            out_grad=vmem((tokens, width), NARROW), gate_up=vmem((tokens, 2 * hidden), WIDE),
            qkv_w=vmem((q_rows + 2 * head, width), NARROW),
            next_qkv_w=vmem((q_rows + 2 * head, width), NARROW),
            wo_w=vmem((q_rows, width), NARROW), gu=vmem((width, 2 * hidden), NARROW),
            down=vmem((hidden, width), NARROW), projected=vmem((tokens, 4 * head), WIDE),
            key2=vmem((tokens, 2 * head), NARROW), value2=vmem((tokens, 2 * head), NARROW),
            by_number=vmem((tokens, 2 * head), NARROW),
            reduce=reduce_scratch(count, local, width),
            first_sems=gather_scratch(count), gather_sems=gather_scratch(count),
            line_sems=line_scratch(count), grads_sems=line_scratch(count),
            gain_sems=[dma((2 * count - 1,)), dma((2 * count - 1,))],
            spread_sems=[
                dma((KINDS, count - 1)), dma((KINDS, count - 1)),
                dma((KINDS, count)), dma((KINDS, count)), dma((KINDS,)),
            ],
            copy_sem=dma((16,)),
        ),
    )


def back_through_feed_forward(at, s, ring, reduce, work, beside):
    local = s.given.shape[0]
    add_gradient(work, s.hidden, s.out_grad, s.grad_down)
    add_gradient(work, s.normed2, s.gu_grad, s.grad_gu)

    gather = Gather(ring, s.shard2, s.attn_grad, s.gather_sems)
    s.gain_mlp_grad[...] = jnp.zeros_like(s.gain_mlp_grad)

    def through(sub, span, value):
        part, gain_part = through_norm(value, s.second[span, :], s.gains[at, 1:2, :])
        value = s.given[span, :] + part
        s.second_grad[span, :] = value
        s.shard2[span, :] = value.astype(NARROW)
        gather.start_piece(sub)
        s.gain_mlp_grad[...] += gain_part

    left = reduce.run(products(s.gu_grad, s.gu, True), through, work, beside)

    def use(index):
        rows = chip_rows(index, local)
        s.mixed_grad[rows, :] = dot(s.attn_grad[rows, :], s.wo[...], ((1,), (1,))).astype(NARROW)

    for do in left:
        do()
    gather.run(use, work)
    work.do()


def turn_body(at, s):
    ring = Ring()
    greet(ring.everyone())
    copies = Copies(s.copy_sem)
    wo_in = copies(s.wo_in.at[at], s.wo)
    ins = [
        copies(s.gu_in.at[at], s.gu), copies(s.down_in.at[at], s.down),
        copies(s.out_grad_in, s.out_grad), copies(s.cotangent.at[lax.axis_index(SECTION)], s.given),
    ]
    reduce, other = Reduce(ring, s.reduce), Reduce(ring, s.other)
    work = Work()

    second_rows = Gather(ring, s.shard, s.normed2, s.first_sems)

    def second(sub, span, value):
        value = s.rows[span, :] + value
        s.second[span, :] = value
        unit, _ = unit_rows(value)
        s.shard[span, :] = (unit * s.gains[at, 1:2, :]).astype(NARROW)
        second_rows.start_piece(sub)

    wo_in.wait()
    reduce.run(products(s.mixed, s.wo, False), second, work)
    for load in ins:
        load.wait()
    second_rows.run(
        feed_forward_use(s, s.rows.shape[0], functools.partial(feed_forward_back, s)), work
    )

    def result(sub, span, value):
        s.result[span, :] = s.second[span, :] + value

    beside = [lambda: other.begin(products(s.hidden, s.down, False), Work())]
    beside += [functools.partial(other.step, step) for step in range(1, ring.far + 1)]
    beside += [lambda: other.end(result)]
    early = ring.far - 1
    back_through_feed_forward(at, s, ring, reduce, work, beside[:early])
    beside = beside[early:]

    def between(spot):
        if beside and spot % 2:
            beside.pop(0)()

    stores = [
        copies(s.grad_down, s.grad_down_out), copies(s.grad_gu, s.grad_gu_out),
        copies(s.attn_grad, s.attn_grad_out),
    ]
    attend_back_here(
        s.slots, s.mixed_grad, s.kept, s.lse, s.cosine, s.sine, s.by_number, s.key2, s.value2,
        s.key_sum, s.value_sum, between,
    )
    for do in beside:
        do()
    put_back(s.by_number, s.qkv_grad, s.row)
    for store in stores:
        store.wait()


def turn(at, known, rows, mixed, kept, lse, out_grad, cotangent, weights, count):
    _, wo, gu, down, gains = weights
    local, width = rows.shape
    tokens = mixed.shape[0]
    hidden = down.shape[1]
    head = mixed.shape[1] // 2
    vmem, dma = pltpu.VMEM, pltpu.SemaphoreType.DMA
    return call_fused(
        "turn", functools.partial(turn_body, at), 1, 140,
        dict(
            **known, rows=(rows, VMEM), mixed=(mixed, VMEM), kept=(kept, VMEM), lse=(lse, VMEM),
            gains=(gains, VMEM), out_grad_in=(out_grad, HBM), cotangent=(cotangent, HBM),
            wo_in=(wo, HBM), gu_in=(gu, HBM), down_in=(down, HBM),
        ),
        dict(
            result=(shape_of(local, width, kind=WIDE), VMEM),
            second_grad=(shape_of(local, width, kind=WIDE), VMEM),
            qkv_grad=(shape_of(tokens, 4 * head), VMEM),
            attn_grad_out=(shape_of(tokens, width), HBM),
            gain_mlp_grad=(shape_of(1, width, kind=WIDE), VMEM),
            grad_down_out=(shape_of(hidden, width), HBM),
            grad_gu_out=(shape_of(width, 2 * hidden), HBM),
        ),
        dict(
            reduce=reduce_scratch(count, local, width), other=reduce_scratch(count, local, width),
            first_sems=gather_scratch(count), gather_sems=gather_scratch(count),
            gu=vmem(gu.shape[1:], NARROW), down=vmem(down.shape[1:], NARROW), wo=vmem(wo.shape[1:], NARROW),
            out_grad=vmem((tokens, width), NARROW), normed2=vmem((tokens, width), NARROW),
            attn_grad=vmem((tokens, width), NARROW), mixed_grad=vmem((tokens, 2 * head), NARROW),
            hidden=vmem((tokens, hidden), NARROW), gu_grad=vmem((tokens, 2 * hidden), NARROW),
            grad_down=vmem((hidden, width), NARROW), grad_gu=vmem((width, 2 * hidden), NARROW),
            given=vmem((local, width), WIDE), second=vmem((local, width), WIDE),
            shard=vmem((local, width), NARROW), shard2=vmem((local, width), NARROW),
            **attend_scratch(tokens, head, True),
            copy_sem=dma((8,)),
        ),
    )


def attention_back(at, s, reduce, work, then, beside=()):
    s.gain_attn_grad[...] = jnp.zeros_like(s.gain_attn_grad)

    def through(sub, span, value):
        part, gain_part = through_norm(value, s.rows[span, :], s.gains[at, 0:1, :])
        value = s.second_grad_in[span, :] + part
        s.input_grad[span, :] = value
        then(sub, span, value)
        s.gain_attn_grad[...] += gain_part

    reduce.run(products(s.qkv_grad, s.qkv_w, False), through, work, beside)


def backward_body(upper, lower, s):
    ring = Ring()
    local = s.rows.shape[0]
    greet(ring.everyone())
    copies = Copies(s.copy_sem)
    qkv_in = copies(s.qkv_w_in.at[upper], s.qkv_w)
    upper_in = [copies(s.attn_grad_in, s.attn_grad), copies(s.normed1_in, s.normed2)]
    first_in = [copies(s.down_in.at[lower], s.down), copies(s.gate_up_in, s.gate_up)]
    then_in = [copies(s.gu_in.at[lower], s.gu), copies(s.wo_in.at[lower], s.wo)]
    reduce = Reduce(ring, s.reduce)
    work = Work()

    def wait(_):
        for load in upper_in:
            load.wait()

    work.add(wait)
    add_gradient(work, s.mixed, s.attn_grad, s.grad_wo)
    add_gradient(work, s.normed2, s.qkv_grad, s.grad_qkv)
    qkv_in.wait()
    gather = Gather(ring, s.shard, s.out_grad, s.first_sems)

    def go_on(sub, span, value):
        s.shard[span, :] = value.astype(NARROW)
        s.given[span, :] = value
        gather.start_piece(sub)

    attention_back(upper, s, reduce, work, go_on)
    work.do()
    then_in.append(copies(s.normed2_in, s.normed2))
    stores = [copies(s.grad_wo, s.grad_wo_out), copies(s.grad_qkv, s.grad_qkv_out)]
    for load in first_in:
        load.wait()
    width = s.hidden.shape[1]
    tile = 256
    number = width // tile

    def use(index):
        rows = chip_rows(index, local)

        def one(at):
            start = at * tile
            cols, right = aligned(start, tile), aligned(start + width, tile)
            feed_forward_back(s, rows, cols, right, s.gate_up[rows, cols], s.gate_up[rows, right])

        loop(0, number, one)

    gather.run(use, work)
    for load in then_in:
        load.wait()
    back_through_feed_forward(lower, s, ring, reduce, work, [])
    stores += [
        copies(s.grad_down, s.grad_down_out), copies(s.grad_gu, s.grad_gu_out),
        copies(s.attn_grad, s.attn_grad_out),
    ]
    for store in stores:
        store.wait()


def backward_between(at, upper, lower, weights, count):
    qkv_w, wo, gu, down, gains = weights
    local, width = upper.rows.shape
    tokens = upper.mixed.shape[0]
    hidden = down.shape[1]
    q_rows = wo.shape[1]
    vmem, dma = pltpu.VMEM, pltpu.SemaphoreType.DMA
    return call_fused(
        "backward_between", functools.partial(backward_body, at, at - 1), 2, 115,
        dict(
            rows=(upper.rows, VMEM), second_grad_in=(upper.second_grad, VMEM),
            qkv_grad=(upper.qkv_grad, VMEM), mixed=(upper.mixed, VMEM), gains=(gains, VMEM),
            attn_grad_in=(upper.attn_grad, HBM), normed1_in=(upper.normed1, HBM),
            second=(lower.second, VMEM), hidden=(lower.hidden, VMEM),
            gate_up_in=(lower.gate_up, HBM), normed2_in=(lower.normed2, HBM),
            qkv_w_in=(qkv_w, HBM), wo_in=(wo, HBM), gu_in=(gu, HBM), down_in=(down, HBM),
        ),
        dict(
            input_grad=(shape_of(local, width, kind=WIDE), VMEM),
            second_grad=(shape_of(local, width, kind=WIDE), VMEM),
            mixed_grad=(shape_of(tokens, q_rows), VMEM),
            attn_grad_out=(shape_of(tokens, width), HBM),
            gain_attn_grad=(shape_of(1, width, kind=WIDE), VMEM),
            gain_mlp_grad=(shape_of(1, width, kind=WIDE), VMEM),
            grad_wo_out=(shape_of(q_rows, width), HBM),
            grad_qkv_out=(shape_of(width, qkv_w.shape[1]), HBM),
            grad_down_out=(shape_of(hidden, width), HBM),
            grad_gu_out=(shape_of(width, 2 * hidden), HBM),
        ),
        dict(
            reduce=reduce_scratch(count, local, width),
            first_sems=gather_scratch(count), gather_sems=gather_scratch(count),
            gu=vmem(gu.shape[1:], NARROW), down=vmem(down.shape[1:], NARROW), wo=vmem(wo.shape[1:], NARROW),
            qkv_w=vmem(qkv_w.shape[1:], NARROW), gate_up=vmem((tokens, 2 * hidden), WIDE),
            out_grad=vmem((tokens, width), NARROW), normed2=vmem((tokens, width), NARROW),
            attn_grad=vmem((tokens, width), NARROW), gu_grad=vmem((tokens, 2 * hidden), NARROW),
            grad_wo=vmem((q_rows, width), NARROW), grad_qkv=vmem((width, qkv_w.shape[1]), NARROW),
            grad_down=vmem((hidden, width), NARROW), grad_gu=vmem((width, 2 * hidden), NARROW),
            given=vmem((local, width), WIDE),
            shard=vmem((local, width), NARROW), shard2=vmem((local, width), NARROW),
            copy_sem=dma((16,)),
        ),
    )


def gradient_pieces(target, count, refs):
    down, gu, wo, qkv = refs
    depth = down.shape[1] // count
    hidden = down.shape[0]
    cols = aligned(target * depth, depth)
    return (
        down.at[:, cols],
        gu.at[cols, pl.ds(0, hidden)],
        gu.at[cols, pl.ds(hidden, hidden)],
        wo.at[:, cols],
        qkv.at[cols, :],
    )


def owned_pieces(source, refs, sizes):
    down, gate, up, wo, qkv = refs
    return (
        down.at[aligned(source * sizes[0][0], sizes[0][0]), :],
        gate.at[:, aligned(source * sizes[1][1], sizes[1][1])],
        up.at[:, aligned(source * sizes[2][1], sizes[2][1])],
        wo.at[aligned(source * sizes[3][0], sizes[3][0]), :],
        qkv.at[source],
    )


GRADS, FEED_GRADS = 5, 3


class Return:
    def __init__(self, ring, partial, outs, landed, mine, sems):
        self.ring = ring
        self.layer = lax.axis_index(SECTION)
        self.across = {SECTION: 1 - self.layer}
        peers, self.origins = partners(ring.me, ring.count)
        self.order = [*peers, ring.me]
        self.partial, self.outs, self.landed, self.mine = partial, outs, landed, mine
        self.cross_send, self.cross_recv, self.load_sem, self.send, self.recv, self.own_sem = sems
        self.sizes = [ref.shape[1:] for ref in mine]
        self.crossing, self.loads, self.sends, self.events = {}, {}, [], []

    def cross(self, kinds):
        count = self.ring.count
        for kind in kinds:
            for k, owner in enumerate(self.order):
                pieces = [gradient_pieces(owner, count, refs)[kind] for refs in self.partial]
                for at in range(2):
                    copy = remote(
                        pieces[1 - at], self.landed[kind].at[k],
                        self.cross_send.at[kind, k], self.cross_recv.at[kind, k], self.across,
                    )
                    load = pltpu.make_async_copy(
                        pieces[at], self.mine[kind].at[k], self.load_sem.at[kind, k]
                    )

                    @pl.when(self.layer == at)
                    def _():
                        copy.start()
                        load.start()

                self.crossing[kind, k], self.loads[kind, k] = copy, load
                self.events.append((kind, k))

    def some(self, number):
        for kind, k in self.events[:number]:
            self.loads[kind, k].wait()
            self.crossing[kind, k].wait_recv()
            mine, theirs = self.mine[kind], self.landed[kind]
            tile = 64

            def add(at):
                rows = aligned(at * tile, tile)
                total = mine[k, rows, :].astype(WIDE) + theirs[k, rows, :].astype(WIDE)
                mine[k, rows, :] = total.astype(NARROW)

            loop(0, mine.shape[1] // tile, add)
            target = owned_pieces(self.ring.me, self.outs, self.sizes)[kind]
            if k < self.ring.count - 1:
                copy = remote(
                    mine.at[k], target, self.send.at[kind, k], self.recv.at[kind, k],
                    {DP: self.order[k]},
                )
            else:
                copy = pltpu.make_async_copy(mine.at[k], target, self.own_sem.at[kind])
            copy.start()
            self.sends.append((k, copy))
        self.events = self.events[number:]

    def finish(self):
        for copy in self.crossing.values():
            copy.wait_send()
        for k, copy in self.sends:
            if k < self.ring.count - 1:
                copy.wait_send()
            else:
                copy.wait()
        for kind in range(GRADS):
            for k in range(self.ring.count - 1):
                here = owned_pieces(self.origins[k], self.outs, self.sizes)[kind]
                remote(
                    self.mine[kind].at[k], here, self.send.at[kind, k], self.recv.at[kind, k],
                    {DP: self.origins[k]},
                ).wait_recv()


def closing_body(at, s):
    ring = Ring()
    layer = lax.axis_index(SECTION)
    count = ring.count
    everyone = 4 * count
    this = (layer * count + ring.me) * 2 + ring.core

    def device(k):
        other = lax.rem(this + k, everyone)
        return {SECTION: other // (2 * count), DP: lax.rem(other // 2, count), TENSOR: lax.rem(other, 2)}

    greet([device(k) for k in range(1, everyone)])
    copies = Copies(s.copy_sem)
    qkv_in = copies(s.qkv_w_in.at[at], s.qkv_w)
    ins = [copies(s.attn_grad_in, s.attn_grad), copies(s.normed1_in, s.normed1)]
    rows_in = copies(s.inputs.at[layer], s.rows)
    back = Return(
        ring,
        ((s.down0, s.gu0, s.grad_wo, s.grad_qkv), (s.down1, s.gu1, s.wo1, s.qkv1)),
        (s.down_out, s.gate_out, s.up_out, s.wo_out, s.qkv_out), s.landed, s.mine, s.back_sems,
    )
    back.cross(range(FEED_GRADS))

    swap_send, swap_recv = s.swap_sems
    swaps = []

    def swap(which, out, values):
        for section in range(2):
            copy = remote(
                values[1 - section], out.at[section], swap_send.at[which], swap_recv.at[which],
                {SECTION: 1 - layer},
            )
            own = pltpu.make_async_copy(values[section], out.at[section], s.own_sems.at[which])

            @pl.when(layer == section)
            def _():
                copy.start()
                own.start()

        swaps.append((copy, own))

    swap(0, s.results, (s.result0, s.result1))
    attend_back_here(
        s.slots, s.mixed_grad, s.kept, s.lse, s.cosine, s.sine, s.by_number, s.key2, s.value2,
        s.key_sum, s.value_sum, lambda spot: back.some(1) if spot == 1 else None,
    )
    put_back(s.by_number, s.qkv_grad, s.row)
    work = Work()
    for load in ins:
        load.wait()
    add_gradient(work, s.mixed, s.attn_grad, s.grad_wo)
    add_gradient(work, s.normed1, s.qkv_grad, s.grad_qkv)
    qkv_in.wait()
    rows_in.wait()

    def rest():
        work.do()
        back.cross(range(FEED_GRADS, GRADS))
        back.some(1)

    beside = [functools.partial(back.some, 1)] * 2 + [rest] + [functools.partial(back.some, 1)] * (ring.far - 3)
    attention_back(at, s, Reduce(ring, s.reduce), work, lambda *_: None, beside)
    swap(1, s.input_grads, (s.input_grad, s.input_grad1))

    lanes = s.gain_out.shape[1]
    for section, (attn, mlp) in enumerate(((s.gain_attn_grad, s.gain_mlp0), (s.gain_attn1, s.gain_mlp1))):
        for owner in range(2 * count):
            s.gain_in[section * 2 * count + owner] = jnp.zeros_like(s.gain_out)
            cols = slice(owner * lanes, (owner + 1) * lanes)
            s.gain_in[section * 2 * count + owner, 0:1, :] = attn[:, cols]
            s.gain_in[section * 2 * count + owner, 1:2, :] = mlp[:, cols]
    gain_send, gain_recv = s.gain_sems
    gain_copies = []
    for k in range(1, everyone):
        copy = remote(
            s.gain_in.at[lax.rem(this + k, everyone)], s.gain_landed.at[k - 1],
            gain_send.at[k - 1], gain_recv.at[k - 1], device(k),
        )
        copy.start()
        gain_copies.append(copy)
    back.some(len(back.events))
    total = s.gain_in[this]
    for k, copy in enumerate(gain_copies):
        copy.wait_recv()
        total = total + s.gain_landed[k]
    s.gain_out[...] = total
    for copy in gain_copies:
        copy.wait_send()
    for copy, own in swaps:
        copy.wait()
        own.wait()
    back.finish()


def closing(at, known, inputs, first, last, feed0, grads1, gains_of, weights, count):
    qkv_w, _, _, _, gains = weights
    local, width = inputs.shape[1:]
    tokens = first.mixed.shape[0]
    head = first.mixed.shape[1] // 2
    down0, gu0 = feed0
    down1, gu1, wo1, qkv1 = grads1
    hidden, q_rows, qkv_rows = down0.shape[0], wo1.shape[0], qkv1.shape[1]
    depth = width // count
    sizes = [(hidden, depth), (depth, hidden), (depth, hidden), (q_rows, depth), (depth, qkv_rows)]
    everyone = 4 * count
    lanes = width // (2 * count)
    vmem, dma = pltpu.VMEM, pltpu.SemaphoreType.DMA
    pieces = lambda: [vmem((count, *size), NARROW) for size in sizes]
    return call_fused(
        "closing", functools.partial(closing_body, at), 3, 210,
        dict(
            **known, inputs=(inputs, HBM), gains=(gains, VMEM), qkv_w_in=(qkv_w, HBM),
            second_grad_in=(first.second_grad, VMEM), mixed_grad=(first.mixed_grad, VMEM),
            mixed=(first.mixed, VMEM), kept=(first.kept, VMEM), lse=(first.lse, VMEM),
            attn_grad_in=(first.attn_grad, HBM), normed1_in=(first.normed1, HBM),
            result0=(first.result, VMEM), result1=(last.result, VMEM),
            input_grad1=(last.input_grad, VMEM),
            down0=(down0, HBM), gu0=(gu0, HBM),
            down1=(down1, HBM), gu1=(gu1, HBM), wo1=(wo1, HBM), qkv1=(qkv1, HBM),
            gain_mlp0=(gains_of[0], VMEM), gain_attn1=(gains_of[1], VMEM), gain_mlp1=(gains_of[2], VMEM),
        ),
        dict(
            results=(shape_of(2, local, width, kind=WIDE), HBM),
            input_grads=(shape_of(2, local, width, kind=WIDE), HBM),
            down_out=(shape_of(count * hidden, depth), HBM),
            gate_out=(shape_of(depth, count * hidden), HBM),
            up_out=(shape_of(depth, count * hidden), HBM),
            wo_out=(shape_of(count * q_rows, depth), HBM),
            qkv_out=(shape_of(count, depth, qkv_rows), HBM),
            gain_out=(shape_of(8, lanes, kind=WIDE), VMEM),
        ),
        dict(
            reduce=reduce_scratch(count, local, width),
            qkv_w=vmem(qkv_w.shape[1:], NARROW), rows=vmem((local, width), WIDE),
            attn_grad=vmem((tokens, width), NARROW), normed1=vmem((tokens, width), NARROW),
            qkv_grad=vmem((tokens, 4 * head), NARROW),
            grad_wo=vmem((q_rows, width), NARROW), grad_qkv=vmem((width, qkv_rows), NARROW),
            input_grad=vmem((local, width), WIDE),
            gain_attn_grad=vmem((1, width), WIDE),
            landed=pieces(), mine=pieces(),
            gain_in=vmem((everyone, 8, lanes), WIDE), gain_landed=vmem((everyone - 1, 8, lanes), WIDE),
            **attend_scratch(tokens, head, True),
            back_sems=[
                dma((GRADS, count)), dma((GRADS, count)), dma((GRADS, count)),
                dma((GRADS, count - 1)), dma((GRADS, count - 1)), dma((GRADS,)),
            ],
            gain_sems=[dma((everyone - 1,)), dma((everyone - 1,))],
            swap_sems=[dma((2,)), dma((2,))], own_sems=dma((2,)),
            copy_sem=dma((8,)),
        ),
    )


def widen_kernel(heads, down, gate, up, wo, qkv, every, gain, *outs):
    down_out, gate_out, up_out, wo_out, wq_out, wk_out, wv_out, attn_out, mlp_out = outs
    for source, out in ((down, down_out), (gate, gate_out), (up, up_out), (wo, wo_out)):
        out[0] = source[...].astype(WIDE)
    queries = wq_out.shape[2]
    wq_out[0] = qkv[0, :, :queries].astype(WIDE)

    @pl.when(pl.program_id(0) == 0)
    def _():
        attn_out[...] = gain[0:1, :]
        mlp_out[...] = gain[1:2, :]
        width = 2 * heads
        shared = every.shape[0] * heads // wk_out.shape[2]

        def one(head):
            chips = range(head * shared, (head + 1) * shared)
            return sum(every[chip, :, queries:].astype(WIDE) for chip in chips)

        for pair in range(wk_out.shape[2] // width):
            left, right = one(2 * pair), one(2 * pair + 1)
            low = low_lanes(left.shape, heads)
            cols = slice(pair * width, (pair + 1) * width)
            wk_out[0, :, cols] = jnp.where(low, left, pltpu.roll(right, heads, 1))
            wv_out[0, :, cols] = jnp.where(low, pltpu.roll(left, heads, 1), right)


def widen(end, kv_cols, count, head):
    depth = end.gate_out.shape[0]
    hidden = end.gate_out.shape[1] // count
    q_rows = end.wo_out.shape[0] // count
    lanes = end.gain_out.shape[1]
    down = (hidden, depth)
    across = (depth, hidden)
    result = lambda *dims: shape_of(1, *dims, kind=WIDE)
    by_rows = lambda at: (at, 0)
    by_cols = lambda at: (0, at)
    none = lambda at: (0, 0)
    flat = lambda index: lambda at: (0, *index(at))
    return pl.pallas_call(
        functools.partial(widen_kernel, head),
        grid=(count,),
        out_shape=(
            result(count * hidden, depth), result(depth, count * hidden), result(depth, count * hidden),
            result(count * q_rows, depth), result(depth, count * q_rows),
            result(depth, kv_cols), result(depth, kv_cols), result(lanes), result(lanes),
        ),
        in_specs=[
            pl.BlockSpec(down, by_rows), pl.BlockSpec(across, by_cols), pl.BlockSpec(across, by_cols),
            pl.BlockSpec((q_rows, depth), by_rows),
            pl.BlockSpec((1, *end.qkv_out.shape[1:]), lambda at: (at, 0, 0)),
            pl.BlockSpec(end.qkv_out.shape, lambda at: (0, 0, 0)),
            pl.BlockSpec(end.gain_out.shape, none),
        ],
        out_specs=(
            pl.BlockSpec((1, *down), flat(by_rows)), pl.BlockSpec((1, *across), flat(by_cols)),
            pl.BlockSpec((1, *across), flat(by_cols)), pl.BlockSpec((1, q_rows, depth), flat(by_rows)),
            pl.BlockSpec((1, depth, q_rows), flat(by_cols)),
            pl.BlockSpec((1, depth, kv_cols), flat(none)), pl.BlockSpec((1, depth, kv_cols), flat(none)),
            pl.BlockSpec((1, lanes), none), pl.BlockSpec((1, lanes), none),
        ),
        name="widen",
    )(end.down_out, end.gate_out, end.up_out, end.wo_out, end.qkv_out, end.qkv_out, end.gain_out)


def fast_shards(inputs, table, cotangent, wq, wk, wv, wo, w_gate, w_up, w_down, gain_attn, gain_mlp):
    count = lax.axis_size(DP)
    parts = lax.axis_size(TENSOR)
    head = HEAD_SIZE
    section = lax.axis_index(SECTION)
    block = inputs.shape[1] * parts

    row = lax.dynamic_index_in_dim(table, section, 0, keepdims=False)
    ids = jnp.arange(count, dtype=jnp.int32)
    slots = jnp.sum(jnp.where(row[None, :] == ids[:, None], ids[None, :], 0), axis=1)
    cosine, sine = rope_tables(count // 2 * block, head)
    qkv_t = jnp.concatenate([wq[0], wk[0], wv[0]], axis=1).T
    s = opening(
        slots, row, cosine, sine, inputs, cotangent, qkv_t, wo, w_gate, w_up, w_down,
        gain_attn, gain_mlp, count, head,
    )
    weights = (s.out_qkv, s.out_wo, s.out_gu, s.out_down, s.gains)
    known = dict(
        slots=(slots, SMEM), row=(row, SMEM), cosine=(cosine, VMEM), sine=(sine, VMEM)
    )
    top = turn(
        1, known, s.result, s.mixed1, s.kept1, s.lse1, s.out_grad_out, cotangent, weights, count
    )
    upper = Names(
        rows=s.result, second_grad=top.second_grad, qkv_grad=top.qkv_grad, mixed=s.mixed1,
        attn_grad=top.attn_grad_out, normed1=s.next_normed1_out,
    )
    lower = Names(
        second=s.second, hidden=s.hidden, gate_up=s.gate_up_out, normed2=s.normed2_out
    )
    back = backward_between(1, upper, lower, weights, count)
    first = Names(
        second_grad=back.second_grad, mixed_grad=back.mixed_grad, mixed=s.mixed0, kept=s.kept0,
        lse=s.lse0, attn_grad=back.attn_grad_out, normed1=s.normed1_out, result=s.result,
    )
    last = Names(result=top.result, input_grad=back.input_grad)
    end = closing(
        0, known, inputs, first, last,
        (back.grad_down_out, back.grad_gu_out),
        (top.grad_down_out, top.grad_gu_out, back.grad_wo_out, back.grad_qkv_out),
        (back.gain_mlp_grad, back.gain_attn_grad, top.gain_mlp_grad),
        weights, count,
    )
    grad_down, grad_gate, grad_up, grad_wo, grad_wq, grad_wk, grad_wv, sum_attn, sum_mlp = widen(
        end, wk.shape[2], count, head
    )
    return (
        end.results[None],
        end.input_grads[None],
        grad_wq,
        grad_wk,
        grad_wv,
        grad_wo,
        grad_gate,
        grad_up,
        grad_down,
        sum_attn,
        sum_mlp,
    )


def fits(mesh, inputs, table, cotangent, wq, wk, wv, wo, w_gate, w_up, w_down, gain_attn, gain_mlp):
    sections, count, parts = (mesh.shape[axis] for axis in (SECTION, DP, TENSOR))
    head = HEAD_SIZE
    if sections != 2 or parts != 2 or inputs.shape[0] != sections or count % 4 or count < 8:
        return False
    devices = count * parts
    queries, keys = wq.shape[2] // head, wk.shape[2] // head
    if queries != 2 * devices or devices % keys or keys % parts or 4 * head != 256:
        return False
    return (
        wq.shape[1] % (128 * count) == 0
        and wq.shape[1] % 512 == 0
        and w_gate.shape[2] % (256 * devices) == 0
        and inputs.shape[1] % (64 * devices) == 0
    )


def shards(mesh, whole, *args):
    if fits(mesh, *whole):
        return fast_shards(*args)
    return general_shards(*args)


def solution(mesh):
    in_specs = (
        P(None, (DP, TENSOR), None),
        P(),
        P(None, (DP, TENSOR), None),
        P(SECTION, DP, TENSOR),
        P(SECTION, DP, TENSOR),
        P(SECTION, DP, TENSOR),
        P(SECTION, TENSOR, DP),
        P(SECTION, DP, TENSOR),
        P(SECTION, DP, TENSOR),
        P(SECTION, TENSOR, DP),
        P(SECTION, DP),
        P(SECTION, DP),
    )
    out_specs = (
        P(SECTION, None, (DP, TENSOR), None),
        P(SECTION, None, (DP, TENSOR), None),
        P(SECTION, DP, TENSOR),
        P(SECTION, DP, TENSOR),
        P(SECTION, DP, TENSOR),
        P(SECTION, TENSOR, DP),
        P(SECTION, DP, TENSOR),
        P(SECTION, DP, TENSOR),
        P(SECTION, TENSOR, DP),
        P(SECTION, (DP, TENSOR)),
        P(SECTION, (DP, TENSOR)),
    )

    def step(*args):
        return jax.shard_map(
            functools.partial(shards, mesh, args),
            mesh=mesh,
            in_specs=in_specs,
            out_specs=out_specs,
            check_vma=False,
        )(*args)

    return step
```

```python
import functools
import math

import jax
import jax.numpy as jnp
import numpy as np
from jax import lax
from jax.experimental import pallas as pl
from jax.experimental.pallas import tpu as pltpu
from jax.sharding import PartitionSpec as P

HEAD_SIZE = 64
SECTION, DP, TENSOR = "section", "dp", "tensor"


epsilon = 1e-05


def passed_along(value, axis, steps):
    count = lax.axis_size(axis)
    initial, last = (max(0, -steps), min(count, count - steps))
    return lax.ppermute(value, axis, [(source, source + steps) for source in range(initial, last)])


def rope_frequencies(head):
    index = jnp.arange(head // 2, dtype=jnp.float32)
    base = 1.0 / 500000.0 ** (index * 2.0 / head)
    wavelength = 2.0 * math.pi / base
    blend = (8192.0 / wavelength - 1.0) / 3.0
    middle = (1.0 - blend) * base / 32.0 + blend * base
    return jnp.where(wavelength < 2048.0, base, jnp.where(wavelength > 8192.0, base / 32.0, middle))


def rotate(values, positions, head):
    step_count = values.shape[0]
    shaped = values.reshape(step_count, -1, head)
    angle = positions.astype(jnp.float32)[:, None] * rope_frequencies(head)[None, :]
    cosine = jnp.cos(angle)[:, None, :]
    sine = jnp.sin(angle)[:, None, :]
    first = shaped[:, :, : head // 2]
    second = shaped[:, :, head // 2 :]
    return jnp.concatenate(
        [first * cosine - second * sine, second * cosine + first * sine], axis=-1
    ).reshape(step_count, -1)


def unrotate(values, positions, head):
    step_count = values.shape[0]
    shaped = values.reshape(step_count, -1, head)
    angle = positions.astype(jnp.float32)[:, None] * rope_frequencies(head)[None, :]
    cosine = jnp.cos(angle)[:, None, :]
    sine = jnp.sin(angle)[:, None, :]
    first = shaped[:, :, : head // 2]
    second = shaped[:, :, head // 2 :]
    return jnp.concatenate(
        [first * cosine + second * sine, second * cosine - first * sine], axis=-1
    ).reshape(step_count, -1)


def norm_stats(rows):
    inverse = lax.rsqrt(jnp.mean(rows * rows, axis=-1, keepdims=True) + epsilon)
    return (rows * inverse, inverse)


def norm_back(grad, unit, inverse, gain):
    scaled = grad * gain
    inner = jnp.mean(scaled * unit, axis=-1, keepdims=True)
    return (inverse * (scaled - unit * inner), jnp.sum(grad * unit, axis=0))


def matmul(left, right):
    return jnp.dot(left, right, preferred_element_type=jnp.float32)


def block_layout(table, micro, groups, block):
    layout_row = lax.dynamic_index_in_dim(table, micro, 0, keepdims=False)
    span = groups // 2
    mine = lax.dynamic_index_in_dim(layout_row, lax.axis_index(DP), 0, keepdims=False)
    sequence = mine // span
    place = mine % span
    slot_ids = jnp.arange(groups, dtype=jnp.int32)
    holder = jnp.sum(
        jnp.where(layout_row[None, :] == slot_ids[:, None], slot_ids[None, :], 0), axis=1
    )
    slots = lax.dynamic_slice_in_dim(holder, sequence * span, span)
    positions = place * block + jnp.arange(block, dtype=jnp.int32)
    return (slots, positions)


def attend(query_rows, key_seq, value_seq, positions, heads_kv, head):
    step_count = query_rows.shape[0]
    keys_total = key_seq.shape[0]
    head_group = query_rows.shape[1] // (heads_kv * head)
    scale = 1.0 / math.sqrt(head)
    allowed = jnp.arange(keys_total, dtype=jnp.int32)[None, :] <= positions[:, None]
    query_layers = query_rows.reshape(step_count, heads_kv, head_group * head).transpose(1, 0, 2)
    key_layers = key_seq.reshape(keys_total, heads_kv, head).transpose(1, 0, 2)
    value_layers = value_seq.reshape(keys_total, heads_kv, head).transpose(1, 0, 2)

    def one_head(parts):
        q_head, k_head, v_head = parts
        q_three = q_head.reshape(step_count, head_group, head)
        scores = (
            jnp.einsum("qgd,kd->gqk", q_three, k_head, preferred_element_type=jnp.float32) * scale
        )
        total = jnp.sum(jnp.where(allowed, jnp.exp(scores), 0.0), axis=-1)
        log_total = jnp.log(total)
        probs = jnp.where(allowed, jnp.exp(scores - log_total[..., None]), 0.0).astype(jnp.bfloat16)
        mixed = jnp.einsum("gqk,kd->qgd", probs, v_head, preferred_element_type=jnp.float32).astype(
            jnp.bfloat16
        )
        return (mixed.reshape(step_count, head_group * head), log_total)

    mixed, log_total = lax.map(one_head, (query_layers, key_layers, value_layers))
    return (mixed.transpose(1, 0, 2).reshape(step_count, -1), log_total)


def attend_back(
    blended_gradient, query_rows, key_seq, value_seq, log_total, positions, heads_kv, head
):
    step_count = query_rows.shape[0]
    keys_total = key_seq.shape[0]
    head_group = query_rows.shape[1] // (heads_kv * head)
    scale = 1.0 / math.sqrt(head)
    allowed = jnp.arange(keys_total, dtype=jnp.int32)[None, :] <= positions[:, None]
    query_layers = query_rows.reshape(step_count, heads_kv, head_group * head).transpose(1, 0, 2)
    key_layers = key_seq.reshape(keys_total, heads_kv, head).transpose(1, 0, 2)
    value_layers = value_seq.reshape(keys_total, heads_kv, head).transpose(1, 0, 2)
    gain_layers = blended_gradient.reshape(step_count, heads_kv, head_group * head).transpose(
        1, 0, 2
    )

    def one_head(parts):
        q_head, k_head, v_head, g_head, l_head = parts
        q_three = q_head.reshape(step_count, head_group, head)
        g_three = g_head.reshape(step_count, head_group, head)
        scores = (
            jnp.einsum("qgd,kd->gqk", q_three, k_head, preferred_element_type=jnp.float32) * scale
        )
        probs = jnp.where(allowed, jnp.exp(scores - l_head[..., None]), 0.0)
        rounded = probs.astype(jnp.bfloat16)
        prob_grad = jnp.einsum("qgd,kd->gqk", g_three, v_head, preferred_element_type=jnp.float32)
        value_total_sum = jnp.einsum(
            "gqk,qgd->kd", rounded, g_three, preferred_element_type=jnp.float32
        )
        rowdot = jnp.sum(probs * prob_grad, axis=-1, keepdims=True)
        score_grad = (probs * (prob_grad - rowdot) * scale).astype(jnp.bfloat16)
        query_grad = jnp.einsum(
            "gqk,kd->qgd", score_grad, k_head, preferred_element_type=jnp.float32
        )
        key_gradient = jnp.einsum(
            "gqk,qgd->kd", score_grad, q_three, preferred_element_type=jnp.float32
        )
        return (query_grad.reshape(step_count, head_group * head), key_gradient, value_total_sum)

    query_grad, key_gradient, value_total_sum = lax.map(
        one_head, (query_layers, key_layers, value_layers, gain_layers, log_total)
    )
    query_grad = query_grad.transpose(1, 0, 2).reshape(step_count, -1)
    key_gradient = key_gradient.transpose(1, 0, 2).reshape(keys_total, -1)
    value_total_sum = value_total_sum.transpose(1, 0, 2).reshape(keys_total, -1)
    return (query_grad, key_gradient, value_total_sum)


def layer_forward(rows, table, micro, weights, groups, heads_kv, head):
    wq, wk, wv, wo, w_gate, w_up, w_down, gain_attn, gain_mlp = weights
    full = lax.all_gather(rows, TENSOR, axis=0, tiled=True)
    block = full.shape[0]
    slots, positions = block_layout(table, micro, groups, block)
    unit1, inverse1 = norm_stats(full)
    normed1 = (unit1 * gain_attn.astype(jnp.float32)).astype(jnp.bfloat16)
    query_rows = rotate(matmul(normed1, wq), positions, head).astype(jnp.bfloat16)
    key = rotate(matmul(normed1, wk), positions, head).astype(jnp.bfloat16)
    value_rows = matmul(normed1, wv).astype(jnp.bfloat16)
    key_all, value_all = (
        lax.all_gather(key, DP, axis=0, tiled=True),
        lax.all_gather(value_rows, DP, axis=0, tiled=True),
    )
    kv_width = key.shape[1]
    key_seq = key_all.reshape(groups, block, kv_width)[slots].reshape(-1, kv_width)
    value_seq = value_all.reshape(groups, block, kv_width)[slots].reshape(-1, kv_width)
    mixed, log_total = attend(query_rows, key_seq, value_seq, positions, heads_kv, head)
    second = rows + lax.psum_scatter(matmul(mixed, wo), TENSOR, scatter_dimension=0, tiled=True)
    full_second = lax.all_gather(second, TENSOR, axis=0, tiled=True)
    unit2, inverse2 = norm_stats(full_second)
    normed2 = (unit2 * gain_mlp.astype(jnp.float32)).astype(jnp.bfloat16)
    gate = matmul(normed2, w_gate)
    upper = matmul(normed2, w_up)
    hidden = (jax.nn.silu(gate) * upper).astype(jnp.bfloat16)
    result = second + lax.psum_scatter(
        matmul(hidden, w_down), TENSOR, scatter_dimension=0, tiled=True
    )
    return (
        result,
        (
            full,
            query_rows,
            key_seq,
            value_seq,
            mixed,
            log_total,
            full_second,
            gate,
            upper,
            hidden,
            slots,
            positions,
        ),
    )


def layer_backward(grad_rows, context, weights, groups, parts, heads_kv, head):
    wq, wk, wv, wo, w_gate, w_up, w_down, gain_attn, gain_mlp = weights
    (
        full,
        query_rows,
        key_seq,
        value_seq,
        mixed,
        log_total,
        full_second,
        gate,
        upper,
        hidden,
        slots,
        positions,
    ) = context
    block = full.shape[0]
    out_grad = lax.all_gather(grad_rows.astype(jnp.bfloat16), TENSOR, axis=0, tiled=True)
    grad_down = matmul(hidden.T, out_grad)
    hidden_grad = matmul(out_grad, w_down.T)
    sigma = jax.nn.sigmoid(gate)
    gate_grad = (hidden_grad * upper * sigma * (1.0 + gate * (1.0 - sigma))).astype(jnp.bfloat16)
    up_grad = (hidden_grad * gate * sigma).astype(jnp.bfloat16)
    unit2, inverse2 = norm_stats(full_second)
    normed2 = (unit2 * gain_mlp.astype(jnp.float32)).astype(jnp.bfloat16)
    grad_gate = matmul(normed2.T, gate_grad)
    grad_up = matmul(normed2.T, up_grad)
    normed2_grad = matmul(gate_grad, w_gate.T) + matmul(up_grad, w_up.T)
    second_terms, gain_mlp_terms = norm_back(
        normed2_grad, unit2, inverse2, gain_mlp.astype(jnp.float32)
    )
    piece_width = gain_mlp_terms.shape[0] // (groups * parts)
    second_part, gain_mlp_part = (
        lax.psum_scatter(
            second_terms.astype(jnp.bfloat16), TENSOR, scatter_dimension=0, tiled=True
        ).astype(jnp.float32),
        lax.psum_scatter(
            gain_mlp_terms.reshape(groups, parts, piece_width).astype(jnp.bfloat16),
            TENSOR,
            scatter_dimension=1,
            tiled=True,
        ).astype(jnp.float32),
    )
    second_grad = grad_rows + second_part
    attn_grad = lax.all_gather(second_grad.astype(jnp.bfloat16), TENSOR, axis=0, tiled=True)
    grad_wo = matmul(mixed.T, attn_grad)
    blended_gradient = matmul(attn_grad, wo.T).astype(jnp.bfloat16)
    query_grad, key_seq_grad, value_seq_grad = attend_back(
        blended_gradient, query_rows, key_seq, value_seq, log_total, positions, heads_kv, head
    )
    kv_width = key_seq.shape[1]
    key_spread = (
        jnp.zeros((groups, block, kv_width), jnp.float32)
        .at[slots]
        .set(key_seq_grad.reshape(-1, block, kv_width))
    )
    value_spread = (
        jnp.zeros((groups, block, kv_width), jnp.float32)
        .at[slots]
        .set(value_seq_grad.reshape(-1, block, kv_width))
    )
    key_own, value_own = (
        lax.psum_scatter(
            key_spread.astype(jnp.bfloat16), DP, scatter_dimension=0, tiled=True
        ).astype(jnp.float32),
        lax.psum_scatter(
            value_spread.astype(jnp.bfloat16), DP, scatter_dimension=0, tiled=True
        ).astype(jnp.float32),
    )
    query_round = unrotate(query_grad, positions, head).astype(jnp.bfloat16)
    key_round = unrotate(key_own.reshape(block, kv_width), positions, head).astype(jnp.bfloat16)
    value_round = value_own.reshape(block, kv_width).astype(jnp.bfloat16)
    unit1, inverse1 = norm_stats(full)
    normed1 = (unit1 * gain_attn.astype(jnp.float32)).astype(jnp.bfloat16)
    grad_wq = matmul(normed1.T, query_round)
    grad_wk = matmul(normed1.T, key_round)
    grad_wv = matmul(normed1.T, value_round)
    normed1_grad = matmul(query_round, wq.T) + matmul(key_round, wk.T) + matmul(value_round, wv.T)
    first_terms, gain_attn_terms = norm_back(
        normed1_grad, unit1, inverse1, gain_attn.astype(jnp.float32)
    )
    first_part, gain_attn_part = (
        lax.psum_scatter(first_terms, TENSOR, scatter_dimension=0, tiled=True),
        lax.psum_scatter(
            gain_attn_terms.reshape(groups, parts, piece_width),
            TENSOR,
            scatter_dimension=1,
            tiled=True,
        ),
    )
    input_grad = second_grad + first_part
    return (
        input_grad,
        (
            grad_wq,
            grad_wk,
            grad_wv,
            grad_wo,
            grad_gate,
            grad_up,
            grad_down,
            gain_attn_part,
            gain_mlp_part,
        ),
    )


def reduce_grads(pieces):
    return (
        lax.psum_scatter(
            pieces[0].astype(jnp.bfloat16), DP, scatter_dimension=0, tiled=True
        ).astype(jnp.float32),
        lax.psum_scatter(
            pieces[1].astype(jnp.bfloat16), DP, scatter_dimension=0, tiled=True
        ).astype(jnp.float32),
        lax.psum_scatter(
            pieces[2].astype(jnp.bfloat16), DP, scatter_dimension=0, tiled=True
        ).astype(jnp.float32),
        lax.psum_scatter(
            pieces[3].astype(jnp.bfloat16), DP, scatter_dimension=1, tiled=True
        ).astype(jnp.float32),
        lax.psum_scatter(
            pieces[4].astype(jnp.bfloat16), DP, scatter_dimension=0, tiled=True
        ).astype(jnp.float32),
        lax.psum_scatter(
            pieces[5].astype(jnp.bfloat16), DP, scatter_dimension=0, tiled=True
        ).astype(jnp.float32),
        lax.psum_scatter(
            pieces[6].astype(jnp.bfloat16), DP, scatter_dimension=1, tiled=True
        ).astype(jnp.float32),
        lax.psum_scatter(
            pieces[7].astype(jnp.bfloat16), DP, scatter_dimension=0, tiled=True
        ).astype(jnp.float32),
        lax.psum_scatter(
            pieces[8].astype(jnp.bfloat16), DP, scatter_dimension=0, tiled=True
        ).astype(jnp.float32),
    )


def general_shards(inputs, table, cotangent, wq, wk, wv, wo, w_gate, w_up, w_down, gain_attn, gain_mlp):
    groups = lax.axis_size(DP)
    parts = lax.axis_size(TENSOR)
    micro_count = inputs.shape[0]
    section = lax.axis_index(SECTION)
    first_section = section == 0
    weights = (
        lax.all_gather(wq[0], DP, axis=0, tiled=True),
        lax.all_gather(wk[0], DP, axis=0, tiled=True),
        lax.all_gather(wv[0], DP, axis=0, tiled=True),
        lax.all_gather(wo[0], DP, axis=1, tiled=True),
        lax.all_gather(w_gate[0], DP, axis=0, tiled=True),
        lax.all_gather(w_up[0], DP, axis=0, tiled=True),
        lax.all_gather(w_down[0], DP, axis=1, tiled=True),
        lax.all_gather(gain_attn[0], DP, axis=0, tiled=True),
        lax.all_gather(gain_mlp[0], DP, axis=0, tiled=True),
    )
    head = HEAD_SIZE
    heads_kv = wk.shape[2] // head
    received = jnp.zeros_like(inputs[0])
    produced = []
    saved = []
    for step in range(micro_count + 1):
        own_rows = inputs[step] if step < micro_count else jnp.zeros_like(inputs[0])
        start_rows = jnp.where(first_section, own_rows, received)
        micro = jnp.clip(step - section, 0, micro_count - 1)
        result, context = layer_forward(start_rows, table, micro, weights, groups, heads_kv, head)
        produced.append(result)
        saved.append(context)
        if step < micro_count:
            received = passed_along(result, SECTION, 1)
    stacked = jnp.stack(produced)
    outputs = jnp.where(first_section, stacked[:micro_count], stacked[1:])[None]
    returned = jnp.zeros_like(inputs[0])
    returned_list = []
    totals = None
    for step in range(micro_count + 1):
        index = micro_count - 1 - step
        given = cotangent[index] if index >= 0 else jnp.zeros_like(cotangent[0])
        start_grad = jnp.where(first_section, returned, given)
        din, pieces = layer_backward(
            start_grad, saved[micro_count - step], weights, groups, parts, heads_kv, head
        )
        returned_list.append(din)
        if step < micro_count:
            returned = passed_along(din.astype(jnp.bfloat16), SECTION, -1).astype(din.dtype)
        totals = (
            pieces
            if totals is None
            else tuple((left + right for left, right in zip(totals, pieces)))
        )
    totals = reduce_grads(totals)
    reverse_stack = jnp.stack(returned_list[::-1])
    input_grad = jnp.where(first_section, reverse_stack[:micro_count], reverse_stack[1:])[None]
    (
        grad_wq,
        grad_wk,
        grad_wv,
        grad_wo,
        grad_gate,
        grad_up,
        grad_down,
        gain_attn_sum,
        gain_mlp_sum,
    ) = totals
    width_piece = gain_attn_sum.shape[-1]
    return (
        outputs,
        input_grad,
        grad_wq[None],
        grad_wk[None],
        grad_wv[None],
        grad_wo[None],
        grad_gate[None],
        grad_up[None],
        grad_down[None],
        gain_attn_sum.reshape(1, width_piece),
        gain_mlp_sum.reshape(1, width_piece),
    )


MESH = pl.DeviceIdType.MESH
SUBS = 4
HBM = pl.BlockSpec(memory_space=pl.ANY)
VMEM = pl.BlockSpec(memory_space=pltpu.VMEM)
SMEM = pl.BlockSpec(memory_space=pltpu.SMEM)
NARROW, WIDE = jnp.bfloat16, jnp.float32


def ring_place(index, count):
    return jnp.where(lax.rem(index, 2) == 0, index // 2, count - (index + 1) // 2)


def ring_index(place, count):
    place = lax.rem(place + 2 * count, count)
    return jnp.where(place < count // 2, 2 * place, 2 * count - 1 - 2 * place)


def greet(others):
    barrier = pltpu.get_barrier_semaphore()
    for other in others:
        pl.semaphore_signal(barrier, inc=1, device_id=other, device_id_type=MESH)
    pl.semaphore_wait(barrier, len(others))


def remote(source, target, send, recv, device):
    return pltpu.make_async_remote_copy(
        source, target, send, recv, device_id=device, device_id_type=MESH
    )


def partners(me, count):
    half = count // 2
    side, inside = me // half, lax.rem(me, half)
    peers = [(1 - side) * half + lax.rem(inside + k, half) for k in range(half)]
    peers += [side * half + lax.rem(inside + k, half) for k in range(1, half)]
    origins = [(1 - side) * half + lax.rem(inside + half - k, half) for k in range(half)]
    origins += [side * half + lax.rem(inside + half - k, half) for k in range(1, half)]
    return peers, origins


def aligned(start, size):
    return pl.ds(pl.multiple_of(start, size), size)


def tiles(size, tile):
    return [slice(at, at + tile) for at in range(0, size, tile)]


def loop(start, stop, body):
    if stop - start == 1:
        body(start)
    elif stop > start:

        def step(at, carry):
            body(at)
            return carry

        lax.fori_loop(start, stop, step, 0)


def dot(left, right, contract):
    return lax.dot_general(
        left, right, (contract, ((), ())), preferred_element_type=jnp.float32
    )


class Names:
    def __init__(self, **values):
        self.__dict__.update(values)


class Work:
    def __init__(self):
        self.items = []

    def add(self, body, count=1):
        self.items.append((body, 0, count))

    def first(self, body):
        self.items.insert(0, (body, 0, 1))

    def do(self, some=1 << 20):
        while some > 0 and self.items:
            body, start, stop = self.items.pop(0)
            until = min(stop, start + some)
            loop(start, until, body)
            some -= until - start
            if until < stop:
                self.items.insert(0, (body, until, stop))


class Copies:
    def __init__(self, sem):
        self.sem = sem
        self.used = 0

    def __call__(self, source, target):
        copy = pltpu.make_async_copy(source, target, self.sem.at[self.used])
        self.used += 1
        copy.start()
        return copy


class Ring:
    def __init__(self):
        self.count = lax.axis_size(DP)
        self.far = self.count // 2
        self.me = lax.axis_index(DP)
        self.core = lax.axis_index(TENSOR)
        self.place = ring_place(self.me, self.count)
        self.near = tuple({DP: ring_index(self.place + step, self.count)} for step in (1, -1))
        self.side = {TENSOR: 1 - self.core}

    def everyone(self):
        return [*self.near, self.side]

    def index(self, steps):
        return ring_index(self.place + steps, self.count)

    def orders(self):
        half = SUBS // 2
        for k in range(half):
            for sub in (k, k + half):
                yield sub, 0
                yield sub, 1


def gather_scratch(count):
    far = count // 2
    dma = pltpu.SemaphoreType.DMA
    return [
        dma((2, far, SUBS)), dma((2, far, SUBS)), dma((count, SUBS)), dma((count, SUBS)), dma((1,))
    ]


class Gather:
    def __init__(self, ring, x_ref, o_ref, sems):
        self.ring = ring
        self.x_ref, self.o_ref = x_ref, o_ref
        self.ring_send, self.ring_recv, self.side_send, self.side_recv, self.own_sem = sems
        self.rows = x_ref.shape[0]
        self.piece = self.rows // SUBS
        self.sends = []

    def spot(self, steps, sub, core):
        start = (self.ring.index(steps) * 2 + core) * self.rows + sub * self.piece
        return self.o_ref.at[aligned(start, self.piece), :]

    def mine(self, steps, sub):
        if steps == 0:
            return self.x_ref.at[sub * self.piece : (sub + 1) * self.piece, :]
        return self.spot(steps, sub, self.ring.core)

    def travels(self, way, hop, sub):
        return hop < self.ring.far or (sub < SUBS // 2) == (way == 0)

    def go(self, copy):
        copy.start()
        self.sends.append(copy)

    def pass_on(self, way, hop, sub):
        steps = 1 - hop if way == 0 else hop - 1
        self.go(
            remote(
                self.mine(steps, sub),
                self.spot(steps, sub, self.ring.core),
                self.ring_send.at[way, hop - 1, sub],
                self.ring_recv.at[way, hop - 1, sub],
                self.ring.near[way],
            )
        )

    def hand_over(self, steps, sub, slot):
        self.go(
            remote(
                self.mine(steps, sub),
                self.spot(steps, sub, self.ring.core),
                self.side_send.at[slot, sub],
                self.side_recv.at[slot, sub],
                self.ring.side,
            )
        )

    def start_piece(self, sub):
        for way in range(2):
            self.pass_on(way, 1, sub)
        self.hand_over(0, sub, 0)

    def start(self):
        for sub, way in self.ring.orders():
            if way == 0:
                self.start_piece(sub)
        self.started()

    def started(self):
        self.own = pltpu.make_async_copy(
            self.x_ref,
            self.o_ref.at[aligned((self.ring.me * 2 + self.ring.core) * self.rows, self.rows), :],
            self.own_sem.at[0],
        )
        self.own.start()

    def hop(self, hop, between=None):
        far, count = self.ring.far, self.ring.count
        for sub, way in self.ring.orders():
            if not self.travels(way, hop, sub):
                continue
            steps = -hop if way == 0 else hop
            here = self.spot(steps, sub, self.ring.core)
            remote(
                here, here, self.ring_send.at[way, hop - 1, sub],
                self.ring_recv.at[way, hop - 1, sub], self.ring.near[way],
            ).wait_recv()
            if hop < far and self.travels(way, hop + 1, sub):
                self.pass_on(way, hop + 1, sub)
            self.hand_over(steps, sub, hop if way == 0 or hop == far else count - hop)
            if way == 1 and between is not None:
                between()

    def side_arrived(self, steps):
        slot = -steps if steps <= 0 else self.ring.count - steps
        slot = self.ring.far if abs(steps) == self.ring.far else slot
        for sub in range(SUBS):
            there = self.spot(steps, sub, 1 - self.ring.core)
            remote(
                there, there, self.side_send.at[slot, sub], self.side_recv.at[slot, sub],
                self.ring.side,
            ).wait_recv()

    def around(self, hop):
        return (-hop, hop) if hop < self.ring.far else (-hop,)

    def sent(self):
        for copy in self.sends:
            copy.wait_send()

    def finish(self):
        self.own.wait()
        self.side_arrived(0)
        for hop in range(1, self.ring.far + 1):
            for steps in self.around(hop):
                self.side_arrived(steps)
        self.sent()

    def run(self, use, work):
        self.started()
        self.own.wait()
        waiting = [0]

        def between():
            if waiting:
                steps = waiting.pop(0)
                self.side_arrived(steps)
                use(self.ring.index(steps))
            else:
                work.do(1)

        for hop in range(1, self.ring.far + 1):
            self.hop(hop, between)
            waiting += self.around(hop)
        while waiting:
            between()
        self.sent()


def line_scratch(count):
    lines = count // 2
    dma = pltpu.SemaphoreType.DMA
    return [
        dma((2, lines)), dma((2, lines)), dma((2 * lines,)), dma((2 * lines,)),
        dma((2, 2 * lines)), dma((2, 2 * lines)), dma((1,)),
    ]


class LineGather:
    def __init__(self, ring, x_ref, o_ref, sems):
        self.ring = ring
        self.x_ref, self.o_ref = x_ref, o_ref
        self.lines = ring.count // 2
        self.line, self.column = ring.me // 2, lax.rem(ring.me, 2)
        self.next = {DP: ring.me + 1 - 2 * self.column}
        self.send, self.recv, self.next_send, self.next_recv = sems[:4]
        self.side_send, self.side_recv, self.own_sem = sems[4:]
        self.rows = x_ref.shape[0]
        self.sends = []

    def spot(self, steps, core, column):
        index = (self.line + steps) * 2 + column
        return self.o_ref.at[aligned((index * 2 + core) * self.rows, self.rows), :]

    def there(self, steps):
        if steps == 0:
            return None
        return self.line >= -steps if steps < 0 else self.line + steps < self.lines

    def if_there(self, condition, do):
        if condition is None:
            do()
        else:
            pl.when(condition)(do)

    def go(self, condition, copy):
        self.if_there(condition, copy.start)
        self.sends.append((condition, copy))

    def spread(self, steps):
        ring, slot = self.ring, steps + self.lines
        source = self.x_ref if steps == 0 else self.spot(steps, ring.core, self.column)
        target = self.spot(steps, ring.core, self.column)
        here = self.there(steps)
        both = lambda other: other if here is None else jnp.logical_and(here, other)
        for way, ahead in enumerate((self.line + 1 < self.lines, self.line > 0)):
            passed = -steps if way == 0 else steps
            if passed >= 0 and passed < self.lines - 1:
                self.go(
                    both(ahead),
                    remote(
                        source, target, self.send.at[way, passed], self.recv.at[way, passed],
                        {DP: ring.me + 2 - 4 * way},
                    ),
                )
        self.go(
            here, remote(source, target, self.next_send.at[slot], self.next_recv.at[slot], self.next)
        )
        self.go(
            here,
            remote(source, target, self.side_send.at[0, slot], self.side_recv.at[0, slot], ring.side),
        )

    def start(self):
        self.spread(0)
        self.own = pltpu.make_async_copy(
            self.x_ref, self.spot(0, self.ring.core, self.column), self.own_sem.at[0]
        )
        self.own.start()

    def hop(self, hop):
        for way, steps in enumerate((-hop, hop)):
            here = self.spot(steps, self.ring.core, self.column)
            copy = remote(
                here, here, self.send.at[way, hop - 1], self.recv.at[way, hop - 1], self.next
            )
            self.if_there(self.there(steps), copy.wait_recv)
            self.spread(steps)

    def finish(self):
        ring = self.ring
        every = range(1 - self.lines, self.lines)
        for steps in every:
            slot = steps + self.lines
            here = self.spot(steps, ring.core, 1 - self.column)
            copy = remote(here, here, self.next_send.at[slot], self.next_recv.at[slot], self.next)
            self.if_there(self.there(steps), copy.wait_recv)
            self.go(
                self.there(steps),
                remote(here, here, self.side_send.at[1, slot], self.side_recv.at[1, slot], ring.side),
            )
        for which, column in enumerate((self.column, 1 - self.column)):
            for steps in every:
                slot = steps + self.lines
                here = self.spot(steps, 1 - ring.core, column)
                copy = remote(
                    here, here, self.side_send.at[which, slot], self.side_recv.at[which, slot], ring.side
                )
                self.if_there(self.there(steps), copy.wait_recv)
        for condition, copy in self.sends:
            self.if_there(condition, copy.wait_send)
        self.own.wait()


def reduce_scratch(count, rows, width):
    far = count // 2
    dma = pltpu.SemaphoreType.DMA
    return [
        pltpu.VMEM((count * 2 * rows, width), NARROW),
        pltpu.VMEM((count, rows, width), NARROW),
        pltpu.VMEM((2, far, rows, width), NARROW),
        pltpu.VMEM((2, far, rows, width), NARROW),
        dma((2, far, SUBS)), dma((2, far, SUBS)), dma((count,)), dma((count,)),
    ]


class Reduce:
    def __init__(self, ring, scratch):
        self.ring = ring
        self.parts, self.beside, self.outgoing, self.incoming = scratch[:4]
        self.ring_send, self.ring_recv, self.side_send, self.side_recv = scratch[4:]
        self.rows = self.beside.shape[1]
        self.piece = self.rows // SUBS

    def span(self, sub):
        return slice(sub * self.piece, (sub + 1) * self.piece)

    def spot(self, steps, core, sub=None):
        start = (self.ring.index(steps) * 2 + core) * self.rows
        if sub is None:
            return aligned(start, self.rows)
        return aligned(start + sub * self.piece, self.piece)

    def make(self):
        steps = self.to_make.pop(0)
        self.produce(self.ring.index(steps), self.parts)
        slot = len(self.slots)
        copy = remote(
            self.parts.at[self.spot(steps, 1 - self.ring.core), :], self.beside.at[slot],
            self.side_send.at[slot], self.side_recv.at[slot], self.ring.side,
        )
        copy.start()
        self.slots[steps] = (slot, copy)

    def mine(self, steps, sub):
        while steps not in self.slots:
            self.make()
        slot, copy = self.slots[steps]
        if steps not in self.joined:
            copy.wait_recv()
            self.joined.add(steps)
        return self.parts[self.spot(steps, self.ring.core, sub), :].astype(
            jnp.float32
        ) + self.beside[slot, self.span(sub), :].astype(jnp.float32)

    def travels(self, way, step, sub):
        return step > 1 or (sub < SUBS // 2) == (way == 0)

    def ring_copy(self, way, step, sub):
        return remote(
            self.outgoing.at[way, step - 1, self.span(sub), :],
            self.incoming.at[way, step - 1, self.span(sub), :],
            self.ring_send.at[way, step - 1, sub],
            self.ring_recv.at[way, step - 1, sub],
            self.ring.near[way],
        )

    def step(self, step):
        far = self.ring.far
        for sub, way in self.ring.orders():
            if not self.travels(way, step, sub):
                continue
            steps = far + 1 - step
            steps = steps if way == 0 or steps == far else -steps
            value = self.mine(steps, sub)
            if step > 1 and self.travels(way, step - 1, sub):
                self.ring_copy(way, step - 1, sub).wait_recv()
                value = value + self.incoming[way, step - 2, self.span(sub), :].astype(jnp.float32)
            self.outgoing[way, step - 1, self.span(sub), :] = value.astype(NARROW)
            copy = self.ring_copy(way, step, sub)
            copy.start()
            self.sends.append(copy)
            if way == 1:
                if self.to_make:
                    self.make()
                else:
                    self.work.do(1)

    def begin(self, produce, work):
        self.produce, self.work = produce, work
        self.slots, self.joined, self.sends = {}, set(), []
        far = self.ring.far
        self.to_make = [far]
        for steps in range(far - 1, 0, -1):
            self.to_make += [steps, -steps]
        self.to_make.append(0)
        self.make()
        self.make()

    def end(self, finish):
        far = self.ring.far
        while self.to_make:
            self.make()
        for sub, way in self.ring.orders():
            if way == 1:
                continue
            value = self.mine(0, sub)
            for way in range(2):
                self.ring_copy(way, far, sub).wait_recv()
                value = value + self.incoming[way, far - 1, self.span(sub), :].astype(jnp.float32)
            finish(sub, self.span(sub), value)
        for copy in self.sends:
            copy.wait_send()
        for _, copy in self.slots.values():
            copy.wait_send()

    def run(self, produce, finish, work, beside=()):
        beside = list(beside)
        self.begin(produce, work)
        for step in range(1, self.ring.far + 1):
            self.step(step)
            if beside:
                beside.pop(0)()
        self.end(finish)
        return beside


def products(left, right, transposed, tile=2048):
    width = right.shape[0] if transposed else right.shape[1]
    tile = math.gcd(tile, width)
    number = width // tile

    def produce(index, parts):
        block = parts.shape[0] // lax.axis_size(DP)
        rows = aligned(index * block, block)

        def one(at):
            cols = aligned(at * tile, tile)
            if transposed:
                part = dot(left[rows, :], right[cols, :], ((1,), (1,)))
            else:
                part = dot(left[rows, :], right[:, cols], ((1,), (0,)))
            parts[rows, cols] = part.astype(NARROW)

        loop(0, number, one)

    return produce


def add_gradient(work, left, right, out, tile=512):
    tile = math.gcd(tile, max(out.shape))
    if out.shape[0] >= out.shape[1]:

        def piece(at):
            cols = aligned(at * tile, tile)
            out[cols, :] = dot(left[:, cols], right[...], ((0,), (0,))).astype(NARROW)

        work.add(piece, out.shape[0] // tile)
    else:

        def piece(at):
            cols = aligned(at * tile, tile)
            out[:, cols] = dot(left[...], right[:, cols], ((0,), (0,))).astype(NARROW)

        work.add(piece, out.shape[1] // tile)


def unit_rows(value):
    inverse = lax.rsqrt(jnp.mean(value * value, axis=-1, keepdims=True) + epsilon)
    return value * inverse, inverse


def through_norm(grad, value, gain):
    unit, inverse = unit_rows(value)
    scaled = grad * gain
    inner = jnp.mean(scaled * unit, axis=-1, keepdims=True)
    return inverse * (scaled - unit * inner), jnp.sum(grad * unit, axis=0, keepdims=True)


def shape_of(*dims, kind=NARROW):
    return jax.ShapeDtypeStruct(dims, kind)


def call_fused(name, body, cid, us, ins, outs, scratch):
    def kernel(*refs):
        refs = list(refs)
        named = {key: refs.pop(0) for key in [*ins, *outs]}
        for key, kind in scratch.items():
            named[key] = [refs.pop(0) for _ in kind] if isinstance(kind, list) else refs.pop(0)
        body(Names(**named))

    flat = []
    for kind in scratch.values():
        flat += kind if isinstance(kind, list) else [kind]
    result = pl.pallas_call(
        kernel,
        out_shape=tuple(shape for shape, _ in outs.values()),
        in_specs=[spec for _, spec in ins.values()],
        out_specs=tuple(spec for _, spec in outs.values()),
        scratch_shapes=flat,
        compiler_params=pltpu.CompilerParams(
            collective_id=cid, has_side_effects=True, vmem_limit_bytes=63 * 1024 * 1024
        ),
        cost_estimate=pl.CostEstimate(
            flops=0, bytes_accessed=int(us * 3.69e6), transcendentals=0
        ),
        name=name,
    )(*[value for value, _ in ins.values()])
    return Names(**dict(zip(outs, result)))


def swap_halves(rows, head):
    width = rows.shape[1]
    lane = lax.broadcasted_iota(jnp.int32, rows.shape, 1)
    half = head // 2
    return jnp.where(
        lax.rem(lane, head) < half, pltpu.roll(rows, width - half, 1), pltpu.roll(rows, half, 1)
    )


def low_lanes(shape, head):
    return lax.broadcasted_iota(jnp.int32, shape, 1) < head


def two_heads(rows, head):
    low = low_lanes(rows.shape, head)
    zero = jnp.zeros_like(rows)
    return jnp.concatenate([jnp.where(low, rows, zero), jnp.where(low, zero, rows)], axis=0)


def one_row(rows, head):
    half = rows.shape[0] // 2
    return jnp.where(low_lanes((half, rows.shape[1]), head), rows[:half], rows[half:])


def triangle(block, keys):
    row = lax.rem(lax.broadcasted_iota(jnp.int32, (2 * block, keys), 0), block)
    column = lax.broadcasted_iota(jnp.int32, (2 * block, keys), 1)
    return column <= row + (keys - block)


def in_order(ref, order, spot, block):
    value = ref[:block, :]
    for other in range(1, ref.shape[0] // block):
        there = order[spot] == other
        value = jnp.where(there, ref[other * block : (other + 1) * block, :], value)
    return value


def attend_here(slots, qkv, cosine, sine, kept, lse, mixed, key2, value2):
    groups = slots.shape[0]
    tokens = qkv.shape[0]
    block = tokens // groups
    span = groups // 2
    wide = qkv.shape[1] // 2
    head = wide // 2
    scale = 1.0 / math.sqrt(head)
    for spot in range(groups):
        here = slice(spot * block, (spot + 1) * block)
        turn_rows = slice(spot % span * block, (spot % span + 1) * block)
        turned_by, turned_sine = cosine[turn_rows, :], sine[turn_rows, :]
        rows = in_order(qkv, slots, spot, block)
        query, pair = rows[:, :wide], rows[:, wide:]
        low = low_lanes(pair.shape, head)
        query = query * turned_by + swap_halves(query, head) * turned_sine
        pair = jnp.where(low, pair * turned_by + swap_halves(pair, head) * turned_sine, pair)
        other = pltpu.roll(pair, head, 1)
        kept[here, :wide] = query.astype(kept.dtype)
        kept[here, wide:] = pair.astype(kept.dtype)
        key2[here, :] = jnp.where(low, pair, other).astype(key2.dtype)
        value2[here, :] = jnp.where(low, other, pair).astype(value2.dtype)
    for spot in range(groups):
        here = slice(spot * block, (spot + 1) * block)
        first = spot // span * span * block
        keys = (spot % span + 1) * block
        query = two_heads(kept[here, :wide], head)
        score = dot(query, key2[first : first + keys, :], ((1,), (1,))) * scale
        allowed = triangle(block, keys)
        power = jnp.where(allowed, jnp.exp(score), 0.0)
        total = jnp.sum(power, axis=1, keepdims=True)
        log_total = jnp.log(total)
        probs = (power * (1.0 / total)).astype(jnp.bfloat16)
        value = dot(probs, value2[first : first + keys, :], ((1,), (0,)))
        mixed[here, :] = one_row(value, head).astype(mixed.dtype)
        lse[spot] = log_total


def attend_back_here(
    slots, grad, kept, lse, cosine, sine, out, key2, value2, key_sum, value_sum, between=None
):
    groups = slots.shape[0]
    tokens = kept.shape[0]
    block = tokens // groups
    span = groups // 2
    wide = kept.shape[1] // 2
    head = wide // 2
    scale = 1.0 / math.sqrt(head)
    for spot in range(groups):
        here = slice(spot * block, (spot + 1) * block)
        pair = kept[here, wide:].astype(jnp.float32)
        low = low_lanes(pair.shape, head)
        other = pltpu.roll(pair, head, 1)
        key2[here, :] = jnp.where(low, pair, other).astype(key2.dtype)
        value2[here, :] = jnp.where(low, other, pair).astype(value2.dtype)
    for spot in range(groups - 1, -1, -1):
        here = slice(spot * block, (spot + 1) * block)
        place = spot % span
        turn_rows = slice(place * block, (place + 1) * block)
        first = spot // span * span * block
        keys = (place + 1) * block
        query = two_heads(kept[here, :wide], head)
        given = two_heads(in_order(grad, slots, spot, block), head)
        key = key2[first : first + keys, :]
        value = value2[first : first + keys, :]
        score = dot(query, key, ((1,), (1,))) * scale
        probs = jnp.where(triangle(block, keys), jnp.exp(score - lse[spot]), 0.0)
        prob_grad = dot(given, value, ((1,), (1,)))
        rowdot = jnp.sum(probs * prob_grad, axis=1, keepdims=True)
        score_grad = (probs * (prob_grad - rowdot) * scale).astype(jnp.bfloat16)
        value_part = dot(probs.astype(jnp.bfloat16), given, ((0,), (0,)))
        key_part = dot(score_grad, query, ((0,), (0,)))
        if place == span - 1:
            value_sum[first : first + keys, :] = value_part
            key_sum[first : first + keys, :] = key_part
        else:
            value_sum[first : first + keys, :] += value_part
            key_sum[first : first + keys, :] += key_part
        query_grad = one_row(dot(score_grad, key, ((1,), (0,))), head)
        query_grad = query_grad * cosine[turn_rows, :] - swap_halves(query_grad, head) * sine[turn_rows, :]
        out[here, :wide] = query_grad.astype(out.dtype)
        if between is not None:
            between(spot)
    for spot in range(groups):
        here = slice(spot * block, (spot + 1) * block)
        turn_rows = slice(spot % span * block, (spot % span + 1) * block)
        key = key_sum[here, :]
        key = key + pltpu.roll(key, head, 1)
        key = key * cosine[turn_rows, :] - swap_halves(key, head) * sine[turn_rows, :]
        value = value_sum[here, :]
        value = value + pltpu.roll(value, head, 1)
        out[here, wide:] = jnp.where(low_lanes(key.shape, head), key, value).astype(out.dtype)


def put_back(source, target, row):
    groups = row.shape[0]
    block = source.shape[0] // groups
    for spot in range(groups):
        target[spot * block : (spot + 1) * block, :] = in_order(source, row, spot, block)


def attend_scratch(tokens, head, back=False):
    vmem = pltpu.VMEM
    wide = 2 * head
    kinds = dict(
        key2=vmem((tokens, wide), jnp.bfloat16),
        value2=vmem((tokens, wide), jnp.bfloat16),
        by_number=vmem((tokens, 2 * wide if back else wide), jnp.bfloat16),
    )
    if back:
        kinds.update(
            key_sum=vmem((tokens, wide), jnp.float32), value_sum=vmem((tokens, wide), jnp.float32)
        )
    return kinds


def rope_tables(tokens, head):
    index = np.arange(head // 2, dtype=np.float32)
    base = (1.0 / np.float32(500000.0) ** (index * 2.0 / head)).astype(np.float32)
    wavelength = 2.0 * math.pi / base
    blend = (8192.0 / wavelength - 1.0) / 3.0
    middle = (1.0 - blend) * base / 32.0 + blend * base
    slow = np.where(wavelength > 8192.0, base / 32.0, middle)
    frequencies = np.where(wavelength < 2048.0, base, slow).astype(np.float32)
    angle = np.arange(tokens, dtype=np.float32)[:, None] * frequencies[None, :]
    cosine, sine = np.cos(angle), np.sin(angle)
    return (
        jnp.asarray(np.concatenate([cosine] * 4, axis=1)),
        jnp.asarray(np.concatenate([-sine, sine] * 2, axis=1)),
    )


def weight_pieces(source, target, count, heads, srcs, dsts, layer):
    qkv, wo, gate, up, down = srcs
    out_qkv, out_wo, out_gu, out_down = dsts
    depth = gate.shape[1]
    hidden = gate.shape[2] // count
    q_rows = wo.shape[1] // count
    kv_rows = (qkv.shape[0] - wo.shape[1]) // 2
    shared = count * heads // kv_rows
    cols = aligned(source * depth, depth)
    k_from = pl.multiple_of(wo.shape[1] + target // shared * heads, heads)
    v_from = pl.multiple_of(wo.shape[1] + kv_rows + target // shared * heads, heads)
    mine = aligned(target * hidden, hidden)
    return (
        (qkv.at[aligned(target * q_rows, q_rows), :], out_qkv.at[layer, pl.ds(0, q_rows), cols]),
        (qkv.at[pl.ds(k_from, heads), :], out_qkv.at[layer, pl.ds(q_rows, heads), cols]),
        (qkv.at[pl.ds(v_from, heads), :], out_qkv.at[layer, pl.ds(q_rows + heads, heads), cols]),
        (wo.at[0, aligned(target * q_rows, q_rows), :], out_wo.at[layer, :, cols]),
        (gate.at[0, :, mine], out_gu.at[layer, cols, pl.ds(0, hidden)]),
        (up.at[0, :, mine], out_gu.at[layer, cols, pl.ds(hidden, hidden)]),
        (down.at[0, mine, :], out_down.at[layer, :, cols]),
    )


KINDS, ATTENTION_KINDS = 7, 4


class Spread:
    def __init__(self, ring, heads, srcs, dsts, sems):
        self.ring = ring
        self.layer = lax.axis_index(SECTION)
        self.across = {SECTION: 1 - self.layer}
        self.peers, self.origins = partners(ring.me, ring.count)
        self.send, self.recv, self.cross_send, self.cross_recv, self.own_sem = sems
        self.pieces = lambda source, target, layer: weight_pieces(
            source, target, ring.count, heads, srcs, dsts, layer
        )
        self.started, self.local = [], {}
        half = ring.count // 2
        self.near, self.far = list(range(half, ring.count - 1)), list(range(half))

    def go(self, copy):
        copy.start()
        self.started.append(copy)

    def own(self, kinds):
        last = self.ring.count - 1
        for kind in kinds:
            source, target = self.pieces(self.ring.me, self.ring.me, self.layer)[kind]
            self.go(
                remote(
                    source, target, self.cross_send.at[kind, last], self.cross_recv.at[kind, last],
                    self.across,
                )
            )
            self.local[kind] = pltpu.make_async_copy(source, target, self.own_sem.at[kind])
            self.local[kind].start()

    def out(self, kind, places):
        for k in places:
            source, target = self.pieces(self.ring.me, self.peers[k], self.layer)[kind]
            self.go(
                remote(
                    source, target, self.send.at[kind, k], self.recv.at[kind, k],
                    {DP: self.peers[k]},
                )
            )

    def pass_on(self, kind, places):
        for k in places:
            here = self.pieces(self.origins[k], self.ring.me, self.layer)[kind][1]
            remote(
                here, here, self.send.at[kind, k], self.recv.at[kind, k], {DP: self.origins[k]}
            ).wait_recv()
            self.go(
                remote(
                    here, here, self.cross_send.at[kind, k], self.cross_recv.at[kind, k], self.across
                )
            )

    def here(self, kinds):
        for kind in kinds:
            self.local[kind].wait()
            for k in range(self.ring.count):
                origin = self.origins[k] if k < self.ring.count - 1 else self.ring.me
                there = self.pieces(origin, self.ring.me, 1 - self.layer)[kind][1]
                remote(
                    there, there, self.cross_send.at[kind, k], self.cross_recv.at[kind, k], self.across
                ).wait_recv()

    def sent(self):
        for copy in self.started:
            copy.wait_send()


def chip_rows(index, local):
    return aligned(index * 2 * local, 2 * local)


def feed_forward_use(s, local, after):
    width = s.hidden.shape[1]
    tile = 256
    number = width // tile

    def use(index):
        rows = chip_rows(index, local)

        def one(at):
            start = at * tile
            cols, right = aligned(start, tile), aligned(start + width, tile)
            value = s.normed2[rows, :]
            gate = dot(value, s.gu[:, cols], ((1,), (0,)))
            upper = dot(value, s.gu[:, right], ((1,), (0,)))
            s.hidden[rows, cols] = (gate * jax.nn.sigmoid(gate) * upper).astype(NARROW)
            after(rows, cols, right, gate, upper)

        loop(0, number, one)

    return use


def feed_forward_back(s, rows, cols, right, gate, upper):
    hidden_grad = dot(s.out_grad[rows, :], s.down[cols, :], ((1,), (1,)))
    sigma = jax.nn.sigmoid(gate)
    gate_grad = hidden_grad * upper * sigma * (1.0 + gate * (1.0 - sigma))
    s.gu_grad[rows, cols] = gate_grad.astype(NARROW)
    s.gu_grad[rows, right] = (hidden_grad * gate * sigma).astype(NARROW)


def opening_body(s):
    ring = Ring()
    layer = lax.axis_index(SECTION)
    peers, origins = partners(ring.me, ring.count)
    holders = [{DP: peer} for peer in peers] + [
        {SECTION: 1 - layer, DP: peer} for peer in [*peers, ring.me]
    ]
    greet([*holders, ring.side])
    copies = Copies(s.copy_sem)
    rows_in = copies(s.inputs.at[layer], s.rows)
    given_in = copies(s.cotangent.at[layer], s.given)
    spread = Spread(
        ring, s.kept0.shape[1] // 4, (s.qkv, s.wo, s.gate, s.up, s.down_in),
        (s.out_qkv, s.out_wo, s.out_gu, s.out_down), s.spread_sems,
    )
    attention, feed = range(ATTENTION_KINDS), range(ATTENTION_KINDS, KINDS)
    local, depth = s.rows.shape[0], s.gain_attn.shape[1]

    s.gain_piece[...] = jnp.zeros_like(s.gain_piece)
    s.gain_piece[0:1, :] = s.gain_attn[...].astype(WIDE)
    s.gain_piece[1:2, :] = s.gain_mlp[...].astype(WIDE)
    gain_send, gain_recv = s.gain_sems
    spot = lambda at, source: s.gains.at[at, :, aligned(source * depth, depth)]
    for k, holder in enumerate(holders):
        spread.go(remote(s.gain_piece, spot(layer, ring.me), gain_send.at[k], gain_recv.at[k], holder))
    own_gains = copies(s.gain_piece, spot(layer, ring.me))
    spread.own(attention)
    own_gains.wait()
    for k, holder in enumerate(holders):
        at, place = (layer, k) if k < ring.count - 1 else (1 - layer, k - ring.count + 1)
        here = spot(at, origins[place] if place < ring.count - 1 else ring.me)
        remote(here, here, gain_send.at[k], gain_recv.at[k], holder).wait_recv()

    rows_in.wait()
    unit, _ = unit_rows(s.rows[...])
    s.shard0[...] = (unit * s.gains[0, 0:1, :]).astype(NARROW)
    first = LineGather(ring, s.shard0, s.normed1, s.line_sems)
    first.start()
    for kind in attention:
        spread.out(kind, spread.far + spread.near)
    for hop in range(1, ring.far):
        first.hop(hop)
    given_in.wait()
    s.shard1[...] = s.given[...].astype(NARROW)
    grads = LineGather(ring, s.shard1, s.out_grad, s.grads_sems)
    grads.start()
    for kind in attention:
        spread.pass_on(kind, spread.near + spread.far)
    gate, up, down = feed
    spread.out(gate, spread.far + spread.near)
    spread.own(feed)
    first.finish()
    spread.here(attention)
    loads = [
        copies(s.out_qkv.at[0], s.qkv_w), copies(s.out_qkv.at[1], s.next_qkv_w),
        copies(s.out_wo.at[0], s.wo_w),
    ]
    stores = [copies(s.normed1, s.normed1_out)]
    for load in loads:
        load.wait()
    tile = 2 * local

    def project(at):
        rows = aligned(at * tile, tile)
        s.projected[rows, :] = dot(s.normed1[rows, :], s.qkv_w[...], ((1,), (1,)))

    loop(0, s.projected.shape[0] // tile, project)
    attend_here(s.slots, s.projected, s.cosine, s.sine, s.kept0, s.lse0, s.by_number, s.key2, s.value2)
    put_back(s.by_number, s.mixed0, s.row)
    stores[0].wait()
    grads.hop(1)

    reduce = Reduce(ring, s.reduce)
    none = Work()

    second_rows = Gather(ring, s.shard2, s.normed2, s.gather_sems)
    next_rows = Gather(ring, s.shard0, s.normed1, s.first_sems)

    def second(sub, span, value):
        value = s.rows[span, :] + value
        s.second[span, :] = value
        unit, _ = unit_rows(value)
        s.shard2[span, :] = (unit * s.gains[0, 1:2, :]).astype(NARROW)
        second_rows.start_piece(sub)

    middle = len(spread.far) // 2
    early, late = spread.near + spread.far[:middle], spread.far[middle:]

    def stage(number):
        kind, places = ((up, early), (up, late), (down, early), (down, late))[number]
        spread.out(kind, places)
        if number == 0:
            spread.pass_on(gate, spread.near + spread.far)
        else:
            kind, places = ((up, early), (up, late), (down, early))[number - 1]
            spread.pass_on(kind, places)
        if number + 2 < ring.far:
            grads.hop(number + 2)

    left = reduce.run(
        products(s.mixed0, s.wo_w, False), second, none,
        [functools.partial(stage, number) for number in range(4)],
    )
    for do in left:
        do()
    spread.pass_on(down, late)
    spread.here((gate, up))
    copies(s.out_gu.at[0], s.gu).wait()

    def keep(rows, cols, right, gate, upper):
        s.gate_up[rows, cols] = gate
        s.gate_up[rows, right] = upper

    second_rows.run(feed_forward_use(s, local, keep), none)
    spread.here((down,))
    load = copies(s.out_down.at[0], s.down)
    grads.finish()
    stores += [
        copies(s.out_grad, s.out_grad_out), copies(s.normed2, s.normed2_out),
        copies(s.gate_up, s.gate_up_out),
    ]
    load.wait()

    def result(sub, span, value):
        value = s.second[span, :] + value
        s.result[span, :] = value
        unit, _ = unit_rows(value)
        s.shard0[span, :] = (unit * s.gains[1, 0:1, :]).astype(NARROW)
        next_rows.start_piece(sub)

    reduce.run(products(s.hidden, s.down, False), result, none)

    def use(index):
        rows = chip_rows(index, local)
        s.projected[rows, :] = dot(s.normed1[rows, :], s.next_qkv_w[...], ((1,), (1,)))

    next_rows.run(use, none)
    stores.append(copies(s.normed1, s.next_normed1_out))
    attend_here(s.slots, s.projected, s.cosine, s.sine, s.kept1, s.lse1, s.by_number, s.key2, s.value2)
    put_back(s.by_number, s.mixed1, s.row)
    for store in stores[1:]:
        store.wait()
    spread.sent()


def opening(slots, row, cosine, sine, inputs, cotangent, qkv, wo, gate, up, down, gain_attn, gain_mlp, count, head):
    local, width = inputs.shape[1:]
    tokens = count * 2 * local
    depth = gate.shape[1]
    hidden = gate.shape[2] // count
    q_rows = wo.shape[1] // count
    vmem, dma = pltpu.VMEM, pltpu.SemaphoreType.DMA
    lse = shape_of(count, 2 * tokens // count, 1, kind=WIDE)
    return call_fused(
        "opening", opening_body, 0, 360,
        dict(
            slots=(slots, SMEM), row=(row, SMEM), cosine=(cosine, VMEM), sine=(sine, VMEM),
            inputs=(inputs, HBM), cotangent=(cotangent, HBM), qkv=(qkv, HBM), wo=(wo, HBM),
            gate=(gate, HBM), up=(up, HBM), down_in=(down, HBM),
            gain_attn=(gain_attn, VMEM), gain_mlp=(gain_mlp, VMEM),
        ),
        dict(
            out_qkv=(shape_of(2, q_rows + 2 * head, width), HBM),
            out_wo=(shape_of(2, q_rows, width), HBM),
            out_gu=(shape_of(2, width, 2 * hidden), HBM),
            out_down=(shape_of(2, hidden, width), HBM),
            gains=(shape_of(2, 8, width, kind=WIDE), VMEM),
            normed1_out=(shape_of(tokens, width), HBM),
            next_normed1_out=(shape_of(tokens, width), HBM),
            normed2_out=(shape_of(tokens, width), HBM),
            out_grad_out=(shape_of(tokens, width), HBM),
            gate_up_out=(shape_of(tokens, 2 * hidden, kind=WIDE), HBM),
            second=(shape_of(local, width, kind=WIDE), VMEM),
            result=(shape_of(local, width, kind=WIDE), VMEM),
            hidden=(shape_of(tokens, hidden), VMEM),
            mixed0=(shape_of(tokens, 2 * head), VMEM), mixed1=(shape_of(tokens, 2 * head), VMEM),
            kept0=(shape_of(tokens, 4 * head), VMEM), kept1=(shape_of(tokens, 4 * head), VMEM),
            lse0=(lse, VMEM), lse1=(lse, VMEM),
        ),
        dict(
            rows=vmem((local, width), WIDE), given=vmem((local, width), WIDE),
            gain_piece=vmem((8, depth), WIDE),
            shard0=vmem((local, width), NARROW), shard1=vmem((local, width), NARROW),
            shard2=vmem((local, width), NARROW),
            normed1=vmem((tokens, width), NARROW), normed2=vmem((tokens, width), NARROW),
            out_grad=vmem((tokens, width), NARROW), gate_up=vmem((tokens, 2 * hidden), WIDE),
            qkv_w=vmem((q_rows + 2 * head, width), NARROW),
            next_qkv_w=vmem((q_rows + 2 * head, width), NARROW),
            wo_w=vmem((q_rows, width), NARROW), gu=vmem((width, 2 * hidden), NARROW),
            down=vmem((hidden, width), NARROW), projected=vmem((tokens, 4 * head), WIDE),
            key2=vmem((tokens, 2 * head), NARROW), value2=vmem((tokens, 2 * head), NARROW),
            by_number=vmem((tokens, 2 * head), NARROW),
            reduce=reduce_scratch(count, local, width),
            first_sems=gather_scratch(count), gather_sems=gather_scratch(count),
            line_sems=line_scratch(count), grads_sems=line_scratch(count),
            gain_sems=[dma((2 * count - 1,)), dma((2 * count - 1,))],
            spread_sems=[
                dma((KINDS, count - 1)), dma((KINDS, count - 1)),
                dma((KINDS, count)), dma((KINDS, count)), dma((KINDS,)),
            ],
            copy_sem=dma((16,)),
        ),
    )


def back_through_feed_forward(at, s, ring, reduce, work, beside, tile, piece):
    local = s.given.shape[0]
    add_gradient(work, s.hidden, s.out_grad, s.grad_down, piece)
    add_gradient(work, s.normed2, s.gu_grad, s.grad_gu, piece)

    gather = Gather(ring, s.shard2, s.attn_grad, s.gather_sems)
    s.gain_mlp_grad[...] = jnp.zeros_like(s.gain_mlp_grad)

    def through(sub, span, value):
        part, gain_part = through_norm(value, s.second[span, :], s.gains[at, 1:2, :])
        value = s.given[span, :] + part
        s.second_grad[span, :] = value
        s.shard2[span, :] = value.astype(NARROW)
        gather.start_piece(sub)
        s.gain_mlp_grad[...] += gain_part

    left = reduce.run(products(s.gu_grad, s.gu, True, tile), through, work, beside)

    def use(index):
        rows = chip_rows(index, local)
        s.mixed_grad[rows, :] = dot(s.attn_grad[rows, :], s.wo[...], ((1,), (1,))).astype(NARROW)

    for do in left:
        do()
    gather.run(use, work)
    work.do()


def turn_body(at, s):
    ring = Ring()
    greet(ring.everyone())
    copies = Copies(s.copy_sem)
    wo_in = copies(s.wo_in.at[at], s.wo)
    ins = [
        copies(s.gu_in.at[at], s.gu), copies(s.down_in.at[at], s.down),
        copies(s.out_grad_in, s.out_grad), copies(s.cotangent.at[lax.axis_index(SECTION)], s.given),
    ]
    reduce, other = Reduce(ring, s.reduce), Reduce(ring, s.other)
    work = Work()
    tile = 512

    second_rows = Gather(ring, s.shard, s.normed2, s.first_sems)

    def second(sub, span, value):
        value = s.rows[span, :] + value
        s.second[span, :] = value
        unit, _ = unit_rows(value)
        s.shard[span, :] = (unit * s.gains[at, 1:2, :]).astype(NARROW)
        second_rows.start_piece(sub)

    wo_in.wait()
    reduce.run(products(s.mixed, s.wo, False, tile), second, work)
    for load in ins:
        load.wait()
    second_rows.run(
        feed_forward_use(s, s.rows.shape[0], functools.partial(feed_forward_back, s)), work
    )

    def result(sub, span, value):
        s.result[span, :] = s.second[span, :] + value

    beside = [lambda: other.begin(products(s.hidden, s.down, False, tile), Work())]
    beside += [functools.partial(other.step, step) for step in range(1, ring.far + 1)]
    beside += [lambda: other.end(result)]
    early = ring.far - 1
    back_through_feed_forward(at, s, ring, reduce, work, beside[:early], tile, 256)
    beside = beside[early:]

    def between(spot):
        if beside and spot % 2:
            beside.pop(0)()

    stores = [
        copies(s.grad_down, s.grad_down_out), copies(s.grad_gu, s.grad_gu_out),
        copies(s.attn_grad, s.attn_grad_out),
    ]
    attend_back_here(
        s.slots, s.mixed_grad, s.kept, s.lse, s.cosine, s.sine, s.by_number, s.key2, s.value2,
        s.key_sum, s.value_sum, between,
    )
    for do in beside:
        do()
    put_back(s.by_number, s.qkv_grad, s.row)
    for store in stores:
        store.wait()


def turn(at, known, rows, mixed, kept, lse, out_grad, cotangent, weights, count):
    _, wo, gu, down, gains = weights
    local, width = rows.shape
    tokens = mixed.shape[0]
    hidden = down.shape[1]
    head = mixed.shape[1] // 2
    vmem, dma = pltpu.VMEM, pltpu.SemaphoreType.DMA
    return call_fused(
        "turn", functools.partial(turn_body, at), 1, 140,
        dict(
            **known, rows=(rows, VMEM), mixed=(mixed, VMEM), kept=(kept, VMEM), lse=(lse, VMEM),
            gains=(gains, VMEM), out_grad_in=(out_grad, HBM), cotangent=(cotangent, HBM),
            wo_in=(wo, HBM), gu_in=(gu, HBM), down_in=(down, HBM),
        ),
        dict(
            result=(shape_of(local, width, kind=WIDE), VMEM),
            second_grad=(shape_of(local, width, kind=WIDE), VMEM),
            qkv_grad=(shape_of(tokens, 4 * head), VMEM),
            attn_grad_out=(shape_of(tokens, width), HBM),
            gain_mlp_grad=(shape_of(1, width, kind=WIDE), VMEM),
            grad_down_out=(shape_of(hidden, width), HBM),
            grad_gu_out=(shape_of(width, 2 * hidden), HBM),
        ),
        dict(
            reduce=reduce_scratch(count, local, width), other=reduce_scratch(count, local, width),
            first_sems=gather_scratch(count), gather_sems=gather_scratch(count),
            gu=vmem(gu.shape[1:], NARROW), down=vmem(down.shape[1:], NARROW), wo=vmem(wo.shape[1:], NARROW),
            out_grad=vmem((tokens, width), NARROW), normed2=vmem((tokens, width), NARROW),
            attn_grad=vmem((tokens, width), NARROW), mixed_grad=vmem((tokens, 2 * head), NARROW),
            hidden=vmem((tokens, hidden), NARROW), gu_grad=vmem((tokens, 2 * hidden), NARROW),
            grad_down=vmem((hidden, width), NARROW), grad_gu=vmem((width, 2 * hidden), NARROW),
            given=vmem((local, width), WIDE), second=vmem((local, width), WIDE),
            shard=vmem((local, width), NARROW), shard2=vmem((local, width), NARROW),
            **attend_scratch(tokens, head, True),
            copy_sem=dma((8,)),
        ),
    )


def attention_back(at, s, reduce, work, then, beside=()):
    s.gain_attn_grad[...] = jnp.zeros_like(s.gain_attn_grad)

    def through(sub, span, value):
        part, gain_part = through_norm(value, s.rows[span, :], s.gains[at, 0:1, :])
        value = s.second_grad_in[span, :] + part
        s.input_grad[span, :] = value
        then(sub, span, value)
        s.gain_attn_grad[...] += gain_part

    reduce.run(products(s.qkv_grad, s.qkv_w, False), through, work, beside)


def backward_body(upper, lower, s):
    ring = Ring()
    local = s.rows.shape[0]
    greet(ring.everyone())
    copies = Copies(s.copy_sem)
    qkv_in = copies(s.qkv_w_in.at[upper], s.qkv_w)
    upper_in = [copies(s.attn_grad_in, s.attn_grad), copies(s.normed1_in, s.normed2)]
    first_in = [copies(s.down_in.at[lower], s.down), copies(s.gate_up_in, s.gate_up)]
    then_in = [copies(s.gu_in.at[lower], s.gu), copies(s.wo_in.at[lower], s.wo)]
    reduce = Reduce(ring, s.reduce)
    work = Work()

    def wait(_):
        for load in upper_in:
            load.wait()

    work.add(wait)
    add_gradient(work, s.mixed, s.attn_grad, s.grad_wo)
    add_gradient(work, s.normed2, s.qkv_grad, s.grad_qkv)
    qkv_in.wait()
    gather = Gather(ring, s.shard, s.out_grad, s.first_sems)

    def go_on(sub, span, value):
        s.shard[span, :] = value.astype(NARROW)
        s.given[span, :] = value
        gather.start_piece(sub)

    attention_back(upper, s, reduce, work, go_on)
    work.do()
    then_in.append(copies(s.normed2_in, s.normed2))
    stores = [copies(s.grad_wo, s.grad_wo_out), copies(s.grad_qkv, s.grad_qkv_out)]
    for load in first_in:
        load.wait()
    width = s.hidden.shape[1]
    tile = 256
    number = width // tile

    def use(index):
        rows = chip_rows(index, local)

        def one(at):
            start = at * tile
            cols, right = aligned(start, tile), aligned(start + width, tile)
            feed_forward_back(s, rows, cols, right, s.gate_up[rows, cols], s.gate_up[rows, right])

        loop(0, number, one)

    gather.run(use, work)
    for load in then_in:
        load.wait()
    back_through_feed_forward(lower, s, ring, reduce, work, [], 2048, 512)
    stores += [
        copies(s.grad_down, s.grad_down_out), copies(s.grad_gu, s.grad_gu_out),
        copies(s.attn_grad, s.attn_grad_out),
    ]
    for store in stores:
        store.wait()


def backward_between(at, upper, lower, weights, count):
    qkv_w, wo, gu, down, gains = weights
    local, width = upper.rows.shape
    tokens = upper.mixed.shape[0]
    hidden = down.shape[1]
    q_rows = wo.shape[1]
    vmem, dma = pltpu.VMEM, pltpu.SemaphoreType.DMA
    return call_fused(
        "backward_between", functools.partial(backward_body, at, at - 1), 2, 115,
        dict(
            rows=(upper.rows, VMEM), second_grad_in=(upper.second_grad, VMEM),
            qkv_grad=(upper.qkv_grad, VMEM), mixed=(upper.mixed, VMEM), gains=(gains, VMEM),
            attn_grad_in=(upper.attn_grad, HBM), normed1_in=(upper.normed1, HBM),
            second=(lower.second, VMEM), hidden=(lower.hidden, VMEM),
            gate_up_in=(lower.gate_up, HBM), normed2_in=(lower.normed2, HBM),
            qkv_w_in=(qkv_w, HBM), wo_in=(wo, HBM), gu_in=(gu, HBM), down_in=(down, HBM),
        ),
        dict(
            input_grad=(shape_of(local, width, kind=WIDE), VMEM),
            second_grad=(shape_of(local, width, kind=WIDE), VMEM),
            mixed_grad=(shape_of(tokens, q_rows), VMEM),
            attn_grad_out=(shape_of(tokens, width), HBM),
            gain_attn_grad=(shape_of(1, width, kind=WIDE), VMEM),
            gain_mlp_grad=(shape_of(1, width, kind=WIDE), VMEM),
            grad_wo_out=(shape_of(q_rows, width), HBM),
            grad_qkv_out=(shape_of(width, qkv_w.shape[1]), HBM),
            grad_down_out=(shape_of(hidden, width), HBM),
            grad_gu_out=(shape_of(width, 2 * hidden), HBM),
        ),
        dict(
            reduce=reduce_scratch(count, local, width),
            first_sems=gather_scratch(count), gather_sems=gather_scratch(count),
            gu=vmem(gu.shape[1:], NARROW), down=vmem(down.shape[1:], NARROW), wo=vmem(wo.shape[1:], NARROW),
            qkv_w=vmem(qkv_w.shape[1:], NARROW), gate_up=vmem((tokens, 2 * hidden), WIDE),
            out_grad=vmem((tokens, width), NARROW), normed2=vmem((tokens, width), NARROW),
            attn_grad=vmem((tokens, width), NARROW), gu_grad=vmem((tokens, 2 * hidden), NARROW),
            grad_wo=vmem((q_rows, width), NARROW), grad_qkv=vmem((width, qkv_w.shape[1]), NARROW),
            grad_down=vmem((hidden, width), NARROW), grad_gu=vmem((width, 2 * hidden), NARROW),
            given=vmem((local, width), WIDE),
            shard=vmem((local, width), NARROW), shard2=vmem((local, width), NARROW),
            copy_sem=dma((16,)),
        ),
    )


def gradient_pieces(target, count, refs):
    down, gu, wo, qkv = refs
    depth = down.shape[1] // count
    hidden = down.shape[0]
    cols = aligned(target * depth, depth)
    return (
        down.at[:, cols],
        gu.at[cols, pl.ds(0, hidden)],
        gu.at[cols, pl.ds(hidden, hidden)],
        wo.at[:, cols],
        qkv.at[cols, :],
    )


def owned_pieces(source, refs, sizes):
    down, gate, up, wo, qkv = refs
    return (
        down.at[aligned(source * sizes[0][0], sizes[0][0]), :],
        gate.at[:, aligned(source * sizes[1][1], sizes[1][1])],
        up.at[:, aligned(source * sizes[2][1], sizes[2][1])],
        wo.at[aligned(source * sizes[3][0], sizes[3][0]), :],
        qkv.at[source],
    )


GRADS, FEED_GRADS = 5, 3


class Return:
    def __init__(self, ring, partial, outs, landed, mine, sems):
        self.ring = ring
        self.layer = lax.axis_index(SECTION)
        self.across = {SECTION: 1 - self.layer}
        peers, self.origins = partners(ring.me, ring.count)
        self.order = [*peers, ring.me]
        self.partial, self.outs, self.landed, self.mine = partial, outs, landed, mine
        self.cross_send, self.cross_recv, self.load_sem, self.send, self.recv, self.own_sem = sems
        self.sizes = [ref.shape[1:] for ref in mine]
        self.crossing, self.loads, self.sends, self.events = {}, {}, [], []

    def cross(self, kinds):
        count = self.ring.count
        for kind in kinds:
            for k, owner in enumerate(self.order):
                pieces = [gradient_pieces(owner, count, refs)[kind] for refs in self.partial]
                for at in range(2):
                    copy = remote(
                        pieces[1 - at], self.landed[kind].at[k],
                        self.cross_send.at[kind, k], self.cross_recv.at[kind, k], self.across,
                    )
                    load = pltpu.make_async_copy(
                        pieces[at], self.mine[kind].at[k], self.load_sem.at[kind, k]
                    )

                    @pl.when(self.layer == at)
                    def _():
                        copy.start()
                        load.start()

                self.crossing[kind, k], self.loads[kind, k] = copy, load
                self.events.append((kind, k))

    def some(self, number):
        for kind, k in self.events[:number]:
            self.loads[kind, k].wait()
            self.crossing[kind, k].wait_recv()
            mine, theirs = self.mine[kind], self.landed[kind]
            tile = 64

            def add(at):
                rows = aligned(at * tile, tile)
                total = mine[k, rows, :].astype(WIDE) + theirs[k, rows, :].astype(WIDE)
                mine[k, rows, :] = total.astype(NARROW)

            loop(0, mine.shape[1] // tile, add)
            target = owned_pieces(self.ring.me, self.outs, self.sizes)[kind]
            if k < self.ring.count - 1:
                copy = remote(
                    mine.at[k], target, self.send.at[kind, k], self.recv.at[kind, k],
                    {DP: self.order[k]},
                )
            else:
                copy = pltpu.make_async_copy(mine.at[k], target, self.own_sem.at[kind])
            copy.start()
            self.sends.append((k, copy))
        self.events = self.events[number:]

    def finish(self):
        for copy in self.crossing.values():
            copy.wait_send()
        for k, copy in self.sends:
            if k < self.ring.count - 1:
                copy.wait_send()
            else:
                copy.wait()
        for kind in range(GRADS):
            for k in range(self.ring.count - 1):
                here = owned_pieces(self.origins[k], self.outs, self.sizes)[kind]
                remote(
                    self.mine[kind].at[k], here, self.send.at[kind, k], self.recv.at[kind, k],
                    {DP: self.origins[k]},
                ).wait_recv()


def closing_body(at, s):
    ring = Ring()
    layer = lax.axis_index(SECTION)
    count = ring.count
    everyone = 4 * count
    this = (layer * count + ring.me) * 2 + ring.core

    def device(k):
        other = lax.rem(this + k, everyone)
        return {SECTION: other // (2 * count), DP: lax.rem(other // 2, count), TENSOR: lax.rem(other, 2)}

    greet([device(k) for k in range(1, everyone)])
    copies = Copies(s.copy_sem)
    qkv_in = copies(s.qkv_w_in.at[at], s.qkv_w)
    ins = [copies(s.attn_grad_in, s.attn_grad), copies(s.normed1_in, s.normed1)]
    rows_in = copies(s.inputs.at[layer], s.rows)
    back = Return(
        ring,
        ((s.down0, s.gu0, s.grad_wo, s.grad_qkv), (s.down1, s.gu1, s.wo1, s.qkv1)),
        (s.down_out, s.gate_out, s.up_out, s.wo_out, s.qkv_out), s.landed, s.mine, s.back_sems,
    )
    back.cross(range(FEED_GRADS))

    swap_send, swap_recv = s.swap_sems
    swaps = []

    def swap(which, out, values):
        for section in range(2):
            copy = remote(
                values[1 - section], out.at[section], swap_send.at[which], swap_recv.at[which],
                {SECTION: 1 - layer},
            )
            own = pltpu.make_async_copy(values[section], out.at[section], s.own_sems.at[which])

            @pl.when(layer == section)
            def _():
                copy.start()
                own.start()

        swaps.append((copy, own))

    swap(0, s.results, (s.result0, s.result1))
    attend_back_here(
        s.slots, s.mixed_grad, s.kept, s.lse, s.cosine, s.sine, s.by_number, s.key2, s.value2,
        s.key_sum, s.value_sum, lambda spot: back.some(1) if spot == 1 else None,
    )
    put_back(s.by_number, s.qkv_grad, s.row)
    work = Work()
    for load in ins:
        load.wait()
    add_gradient(work, s.mixed, s.attn_grad, s.grad_wo)
    add_gradient(work, s.normed1, s.qkv_grad, s.grad_qkv)
    qkv_in.wait()
    rows_in.wait()

    def rest():
        work.do()
        back.cross(range(FEED_GRADS, GRADS))
        back.some(1)

    beside = [functools.partial(back.some, 1)] * 2 + [rest] + [functools.partial(back.some, 1)] * (ring.far - 3)
    attention_back(at, s, Reduce(ring, s.reduce), work, lambda *_: None, beside)
    swap(1, s.input_grads, (s.input_grad, s.input_grad1))

    lanes = s.gain_out.shape[1]
    for section, (attn, mlp) in enumerate(((s.gain_attn_grad, s.gain_mlp0), (s.gain_attn1, s.gain_mlp1))):
        for owner in range(2 * count):
            s.gain_in[section * 2 * count + owner] = jnp.zeros_like(s.gain_out)
            cols = slice(owner * lanes, (owner + 1) * lanes)
            s.gain_in[section * 2 * count + owner, 0:1, :] = attn[:, cols]
            s.gain_in[section * 2 * count + owner, 1:2, :] = mlp[:, cols]
    gain_send, gain_recv = s.gain_sems
    gain_copies = []
    for k in range(1, everyone):
        copy = remote(
            s.gain_in.at[lax.rem(this + k, everyone)], s.gain_landed.at[k - 1],
            gain_send.at[k - 1], gain_recv.at[k - 1], device(k),
        )
        copy.start()
        gain_copies.append(copy)
    back.some(len(back.events))
    total = s.gain_in[this]
    for k, copy in enumerate(gain_copies):
        copy.wait_recv()
        total = total + s.gain_landed[k]
    s.gain_out[...] = total
    for copy in gain_copies:
        copy.wait_send()
    for copy, own in swaps:
        copy.wait()
        own.wait()
    back.finish()


def closing(at, known, inputs, first, last, feed0, grads1, gains_of, weights, count):
    qkv_w, _, _, _, gains = weights
    local, width = inputs.shape[1:]
    tokens = first.mixed.shape[0]
    head = first.mixed.shape[1] // 2
    down0, gu0 = feed0
    down1, gu1, wo1, qkv1 = grads1
    hidden, q_rows, qkv_rows = down0.shape[0], wo1.shape[0], qkv1.shape[1]
    depth = width // count
    sizes = [(hidden, depth), (depth, hidden), (depth, hidden), (q_rows, depth), (depth, qkv_rows)]
    everyone = 4 * count
    lanes = width // (2 * count)
    vmem, dma = pltpu.VMEM, pltpu.SemaphoreType.DMA
    pieces = lambda: [vmem((count, *size), NARROW) for size in sizes]
    return call_fused(
        "closing", functools.partial(closing_body, at), 3, 210,
        dict(
            **known, inputs=(inputs, HBM), gains=(gains, VMEM), qkv_w_in=(qkv_w, HBM),
            second_grad_in=(first.second_grad, VMEM), mixed_grad=(first.mixed_grad, VMEM),
            mixed=(first.mixed, VMEM), kept=(first.kept, VMEM), lse=(first.lse, VMEM),
            attn_grad_in=(first.attn_grad, HBM), normed1_in=(first.normed1, HBM),
            result0=(first.result, VMEM), result1=(last.result, VMEM),
            input_grad1=(last.input_grad, VMEM),
            down0=(down0, HBM), gu0=(gu0, HBM),
            down1=(down1, HBM), gu1=(gu1, HBM), wo1=(wo1, HBM), qkv1=(qkv1, HBM),
            gain_mlp0=(gains_of[0], VMEM), gain_attn1=(gains_of[1], VMEM), gain_mlp1=(gains_of[2], VMEM),
        ),
        dict(
            results=(shape_of(2, local, width, kind=WIDE), HBM),
            input_grads=(shape_of(2, local, width, kind=WIDE), HBM),
            down_out=(shape_of(count * hidden, depth), HBM),
            gate_out=(shape_of(depth, count * hidden), HBM),
            up_out=(shape_of(depth, count * hidden), HBM),
            wo_out=(shape_of(count * q_rows, depth), HBM),
            qkv_out=(shape_of(count, depth, qkv_rows), HBM),
            gain_out=(shape_of(8, lanes, kind=WIDE), VMEM),
        ),
        dict(
            reduce=reduce_scratch(count, local, width),
            qkv_w=vmem(qkv_w.shape[1:], NARROW), rows=vmem((local, width), WIDE),
            attn_grad=vmem((tokens, width), NARROW), normed1=vmem((tokens, width), NARROW),
            qkv_grad=vmem((tokens, 4 * head), NARROW),
            grad_wo=vmem((q_rows, width), NARROW), grad_qkv=vmem((width, qkv_rows), NARROW),
            input_grad=vmem((local, width), WIDE),
            gain_attn_grad=vmem((1, width), WIDE),
            landed=pieces(), mine=pieces(),
            gain_in=vmem((everyone, 8, lanes), WIDE), gain_landed=vmem((everyone - 1, 8, lanes), WIDE),
            **attend_scratch(tokens, head, True),
            back_sems=[
                dma((GRADS, count)), dma((GRADS, count)), dma((GRADS, count)),
                dma((GRADS, count - 1)), dma((GRADS, count - 1)), dma((GRADS,)),
            ],
            gain_sems=[dma((everyone - 1,)), dma((everyone - 1,))],
            swap_sems=[dma((2,)), dma((2,))], own_sems=dma((2,)),
            copy_sem=dma((8,)),
        ),
    )


def widen_kernel(heads, down, gate, up, wo, qkv, every, gain, *outs):
    down_out, gate_out, up_out, wo_out, wq_out, wk_out, wv_out, attn_out, mlp_out = outs
    for source, out in ((down, down_out), (gate, gate_out), (up, up_out), (wo, wo_out)):
        out[0] = source[...].astype(WIDE)
    queries = wq_out.shape[2]
    wq_out[0] = qkv[0, :, :queries].astype(WIDE)

    @pl.when(pl.program_id(0) == 0)
    def _():
        attn_out[...] = gain[0:1, :]
        mlp_out[...] = gain[1:2, :]
        width = 2 * heads
        shared = every.shape[0] * heads // wk_out.shape[2]

        def one(head):
            chips = range(head * shared, (head + 1) * shared)
            return sum(every[chip, :, queries:].astype(WIDE) for chip in chips)

        for pair in range(wk_out.shape[2] // width):
            left, right = one(2 * pair), one(2 * pair + 1)
            low = low_lanes(left.shape, heads)
            cols = slice(pair * width, (pair + 1) * width)
            wk_out[0, :, cols] = jnp.where(low, left, pltpu.roll(right, heads, 1))
            wv_out[0, :, cols] = jnp.where(low, pltpu.roll(left, heads, 1), right)


def widen(end, kv_cols, count, head):
    depth = end.gate_out.shape[0]
    hidden = end.gate_out.shape[1] // count
    q_rows = end.wo_out.shape[0] // count
    lanes = end.gain_out.shape[1]
    down = (hidden, depth)
    across = (depth, hidden)
    result = lambda *dims: shape_of(1, *dims, kind=WIDE)
    by_rows = lambda at: (at, 0)
    by_cols = lambda at: (0, at)
    none = lambda at: (0, 0)
    flat = lambda index: lambda at: (0, *index(at))
    return pl.pallas_call(
        functools.partial(widen_kernel, head),
        grid=(count,),
        out_shape=(
            result(count * hidden, depth), result(depth, count * hidden), result(depth, count * hidden),
            result(count * q_rows, depth), result(depth, count * q_rows),
            result(depth, kv_cols), result(depth, kv_cols), result(lanes), result(lanes),
        ),
        in_specs=[
            pl.BlockSpec(down, by_rows), pl.BlockSpec(across, by_cols), pl.BlockSpec(across, by_cols),
            pl.BlockSpec((q_rows, depth), by_rows),
            pl.BlockSpec((1, *end.qkv_out.shape[1:]), lambda at: (at, 0, 0)),
            pl.BlockSpec(end.qkv_out.shape, lambda at: (0, 0, 0)),
            pl.BlockSpec(end.gain_out.shape, none),
        ],
        out_specs=(
            pl.BlockSpec((1, *down), flat(by_rows)), pl.BlockSpec((1, *across), flat(by_cols)),
            pl.BlockSpec((1, *across), flat(by_cols)), pl.BlockSpec((1, q_rows, depth), flat(by_rows)),
            pl.BlockSpec((1, depth, q_rows), flat(by_cols)),
            pl.BlockSpec((1, depth, kv_cols), flat(none)), pl.BlockSpec((1, depth, kv_cols), flat(none)),
            pl.BlockSpec((1, lanes), none), pl.BlockSpec((1, lanes), none),
        ),
        name="widen",
    )(end.down_out, end.gate_out, end.up_out, end.wo_out, end.qkv_out, end.qkv_out, end.gain_out)


def fast_shards(inputs, table, cotangent, wq, wk, wv, wo, w_gate, w_up, w_down, gain_attn, gain_mlp):
    count = lax.axis_size(DP)
    parts = lax.axis_size(TENSOR)
    head = HEAD_SIZE
    section = lax.axis_index(SECTION)
    block = inputs.shape[1] * parts

    row = lax.dynamic_index_in_dim(table, section, 0, keepdims=False)
    ids = jnp.arange(count, dtype=jnp.int32)
    slots = jnp.sum(jnp.where(row[None, :] == ids[:, None], ids[None, :], 0), axis=1)
    cosine, sine = rope_tables(count // 2 * block, head)
    qkv_t = jnp.concatenate([wq[0], wk[0], wv[0]], axis=1).T
    s = opening(
        slots, row, cosine, sine, inputs, cotangent, qkv_t, wo, w_gate, w_up, w_down,
        gain_attn, gain_mlp, count, head,
    )
    weights = (s.out_qkv, s.out_wo, s.out_gu, s.out_down, s.gains)
    known = dict(
        slots=(slots, SMEM), row=(row, SMEM), cosine=(cosine, VMEM), sine=(sine, VMEM)
    )
    top = turn(
        1, known, s.result, s.mixed1, s.kept1, s.lse1, s.out_grad_out, cotangent, weights, count
    )
    upper = Names(
        rows=s.result, second_grad=top.second_grad, qkv_grad=top.qkv_grad, mixed=s.mixed1,
        attn_grad=top.attn_grad_out, normed1=s.next_normed1_out,
    )
    lower = Names(
        second=s.second, hidden=s.hidden, gate_up=s.gate_up_out, normed2=s.normed2_out
    )
    back = backward_between(1, upper, lower, weights, count)
    first = Names(
        second_grad=back.second_grad, mixed_grad=back.mixed_grad, mixed=s.mixed0, kept=s.kept0,
        lse=s.lse0, attn_grad=back.attn_grad_out, normed1=s.normed1_out, result=s.result,
    )
    last = Names(result=top.result, input_grad=back.input_grad)
    end = closing(
        0, known, inputs, first, last,
        (back.grad_down_out, back.grad_gu_out),
        (top.grad_down_out, top.grad_gu_out, back.grad_wo_out, back.grad_qkv_out),
        (back.gain_mlp_grad, back.gain_attn_grad, top.gain_mlp_grad),
        weights, count,
    )
    grad_down, grad_gate, grad_up, grad_wo, grad_wq, grad_wk, grad_wv, sum_attn, sum_mlp = widen(
        end, wk.shape[2], count, head
    )
    return (
        end.results[None],
        end.input_grads[None],
        grad_wq,
        grad_wk,
        grad_wv,
        grad_wo,
        grad_gate,
        grad_up,
        grad_down,
        sum_attn,
        sum_mlp,
    )


def fits(mesh, inputs, table, cotangent, wq, wk, wv, wo, w_gate, w_up, w_down, gain_attn, gain_mlp):
    sections, count, parts = (mesh.shape[axis] for axis in (SECTION, DP, TENSOR))
    head = HEAD_SIZE
    if sections != 2 or parts != 2 or inputs.shape[0] != sections or count % 4 or count < 8:
        return False
    devices = count * parts
    queries, keys = wq.shape[2] // head, wk.shape[2] // head
    if queries != 2 * devices or devices % keys or keys % parts or 4 * head != 256:
        return False
    return (
        wq.shape[1] % (128 * count) == 0
        and wq.shape[1] % 512 == 0
        and w_gate.shape[2] % (256 * devices) == 0
        and inputs.shape[1] % (64 * devices) == 0
    )


def shards(mesh, whole, *args):
    if fits(mesh, *whole):
        return fast_shards(*args)
    return general_shards(*args)


def solution(mesh):
    in_specs = (
        P(None, (DP, TENSOR), None),
        P(),
        P(None, (DP, TENSOR), None),
        P(SECTION, DP, TENSOR),
        P(SECTION, DP, TENSOR),
        P(SECTION, DP, TENSOR),
        P(SECTION, TENSOR, DP),
        P(SECTION, DP, TENSOR),
        P(SECTION, DP, TENSOR),
        P(SECTION, TENSOR, DP),
        P(SECTION, DP),
        P(SECTION, DP),
    )
    out_specs = (
        P(SECTION, None, (DP, TENSOR), None),
        P(SECTION, None, (DP, TENSOR), None),
        P(SECTION, DP, TENSOR),
        P(SECTION, DP, TENSOR),
        P(SECTION, DP, TENSOR),
        P(SECTION, TENSOR, DP),
        P(SECTION, DP, TENSOR),
        P(SECTION, DP, TENSOR),
        P(SECTION, TENSOR, DP),
        P(SECTION, (DP, TENSOR)),
        P(SECTION, (DP, TENSOR)),
    )

    def step(*args):
        return jax.shard_map(
            functools.partial(shards, mesh, args),
            mesh=mesh,
            in_specs=in_specs,
            out_specs=out_specs,
            check_vma=False,
        )(*args)

    return step
```
